128 devices in a mesh: rep: 4 (over x), fsdp: 32 (over z, y, core).
Axes of the slice: x: 4, y: 4, z: 4, core: 2. Of those that a mesh axis runs over, the one named last changes fastest.
Arguments:
- x_tokens: bfloat16 [256, 257, 1408], P(('rep', 'fsdp'))
- grad_z: bfloat16 [256, 257, 1408], P(('rep', 'fsdp'))
- w_qkv: float32 [1408, 4224], P('fsdp')
- b_qkv: float32 [4224], P('fsdp')
- w_out: float32 [1408, 1408], P('fsdp')
- w_up: float32 [1408, 6144], P('fsdp')
- b_up: float32 [6144], P('fsdp')
- w_down: float32 [6144, 1408], P('fsdp')
- vec_params: float32 [8, 1408], P(None, 'fsdp')
Outputs:
- output 1: bfloat16 [256, 257, 1408], P(('rep', 'fsdp'))
- output 2: bfloat16 [256, 257, 1408], P(('rep', 'fsdp'))
- output 3: float32 [1408, 4224], P('fsdp')
- output 4: float32 [4224], P('fsdp')
- output 5: float32 [1408, 1408], P('fsdp')
- output 6: float32 [1408, 6144], P('fsdp')
- output 7: float32 [6144], P('fsdp')
- output 8: float32 [6144, 1408], P('fsdp')
- output 9: float32 [8, 1408], P(None, 'fsdp')
All inputs are finite; a program needn't handle non-finite values.
Results may differ from the reference program's by a relative error of at most 0.02.
Values are sent between devices in bfloat16 or wider.
A program may use at most 1 GiB of HBM per device.

```python
import jax
import jax.numpy as jnp
from jax import lax

D = 1408
FF = 6144
SEQ = 257
HEADS = 16
SEQS_DEV = 2
DEVICES = 128
BATCH = SEQS_DEV * DEVICES
HEAD = D // HEADS
LN_EPS = 1e-5


def setup_inputs(seed: int = 0) -> dict:
    keys = jax.random.split(jax.random.key(seed), 12)
    seq_scale = jax.random.uniform(keys[0], (BATCH, 1, 1), minval=0.5, maxval=2.0)
    x_tokens = (jax.random.normal(keys[1], (BATCH, SEQ, D)) * seq_scale).astype(jnp.bfloat16)
    grad_scale = jax.random.uniform(keys[2], (BATCH, 1, 1), minval=0.25, maxval=2.0)
    grad_z = (jax.random.normal(keys[3], (BATCH, SEQ, D)) * grad_scale).astype(jnp.bfloat16)
    w_qkv = jax.random.normal(keys[4], (D, 3 * D)) * D ** -0.5
    b_qkv = 0.5 * jax.random.normal(keys[5], (3 * D,))
    w_out = jax.random.normal(keys[6], (D, D)) * D ** -0.5
    w_up = jax.random.normal(keys[7], (D, FF)) * D ** -0.5
    b_up = 0.5 * jax.random.normal(keys[8], (FF,))
    w_down = jax.random.normal(keys[9], (FF, D)) * FF ** -0.5
    is_scale = jnp.array([0.0, 0.0, 0.0, 1.0, 0.0, 0.0, 0.0, 1.0], jnp.float32)[:, None]
    row_offset = jnp.array([1.0, 0.0, 0.0, 0.0, 1.0, 0.0, 0.0, 0.0], jnp.float32)[:, None]
    normal_rows = row_offset + 0.25 * jax.random.normal(keys[10], (8, D))
    scale_rows = jax.random.uniform(keys[11], (8, D), minval=0.5, maxval=1.5)
    vec_params = is_scale * scale_rows + (1.0 - is_scale) * normal_rows
    return {"x_tokens": x_tokens, "grad_z": grad_z, "w_qkv": w_qkv, "b_qkv": b_qkv, "w_out": w_out,
            "w_up": w_up, "b_up": b_up, "w_down": w_down, "vec_params": vec_params}


def normalize(t):
    mean = jnp.mean(t, axis=-1, keepdims=True)
    centered = t - mean
    variance = jnp.mean(centered * centered, axis=-1, keepdims=True)
    return centered * lax.rsqrt(variance + LN_EPS)


def gelu_exact(t):
    return jax.nn.gelu(t, approximate=False)


def layer_pass(x_seq, dz_seq, matrices, bias_qkv, bias_up, vec_rows):
    w_qkv, w_out, w_up, w_down = matrices
    ln1_gain, ln1_bias, out_bias, scale_attn, ln2_gain, ln2_bias, down_bias, scale_mlp = vec_rows
    score_scale = HEAD ** -0.5
    x_float = x_seq.astype(jnp.float32)
    xhat_one, norm_one_back = jax.vjp(normalize, x_float)
    h_one = (xhat_one * ln1_gain + ln1_bias).astype(jnp.bfloat16)
    qkv_proj = (jnp.dot(h_one, w_qkv, preferred_element_type=jnp.float32) + bias_qkv).astype(jnp.bfloat16)
    qkv_heads = qkv_proj.reshape(SEQ, 3, HEADS, HEAD).astype(jnp.float32)
    q_heads = qkv_heads[:, 0]
    k_heads = qkv_heads[:, 1]
    v_heads = qkv_heads[:, 2]
    scores = jnp.einsum("qhe,khe->hqk", q_heads, k_heads) * score_scale
    attn_probs = jax.nn.softmax(scores, axis=-1)
    probs_bf = attn_probs.astype(jnp.bfloat16).astype(jnp.float32)
    head_out = jnp.einsum("hqk,khe->qhe", probs_bf, v_heads).astype(jnp.bfloat16).reshape(SEQ, D)
    att_out = jnp.dot(head_out, w_out, preferred_element_type=jnp.float32) + out_bias
    resid_mid = x_float + scale_attn * att_out
    xhat_two, norm_two_back = jax.vjp(normalize, resid_mid)
    h_two = (xhat_two * ln2_gain + ln2_bias).astype(jnp.bfloat16)
    pre_act = jnp.dot(h_two, w_up, preferred_element_type=jnp.float32) + bias_up
    act_float, gelu_back = jax.vjp(gelu_exact, pre_act)
    mlp_act = act_float.astype(jnp.bfloat16)
    mlp_out = jnp.dot(mlp_act, w_down, preferred_element_type=jnp.float32) + down_bias
    z_seq = (resid_mid + scale_mlp * mlp_out).astype(jnp.bfloat16)
    g_out = dz_seq.astype(jnp.float32)
    grad_scale_mlp = jnp.sum(g_out * mlp_out, axis=0)
    d_mlp = g_out * scale_mlp
    grad_down_bias = jnp.sum(d_mlp, axis=0)
    d_mlp_bf = d_mlp.astype(jnp.bfloat16)
    grad_w_down = jnp.dot(mlp_act.T, d_mlp_bf, preferred_element_type=jnp.float32)
    d_act = jnp.dot(d_mlp_bf, w_down.T, preferred_element_type=jnp.float32)
    d_pre = gelu_back(d_act)[0]
    grad_b_up = jnp.sum(d_pre, axis=0)
    d_pre_bf = d_pre.astype(jnp.bfloat16)
    grad_w_up = jnp.dot(h_two.T, d_pre_bf, preferred_element_type=jnp.float32)
    d_h_two = jnp.dot(d_pre_bf, w_up.T, preferred_element_type=jnp.float32)
    grad_ln2_gain = jnp.sum(d_h_two * xhat_two, axis=0)
    grad_ln2_bias = jnp.sum(d_h_two, axis=0)
    g_resid = g_out + norm_two_back(d_h_two * ln2_gain)[0]
    grad_scale_attn = jnp.sum(g_resid * att_out, axis=0)
    d_att = g_resid * scale_attn
    grad_out_bias = jnp.sum(d_att, axis=0)
    d_att_bf = d_att.astype(jnp.bfloat16)
    grad_w_out = jnp.dot(head_out.T, d_att_bf, preferred_element_type=jnp.float32)
    d_heads = jnp.dot(d_att_bf, w_out.T, preferred_element_type=jnp.float32).astype(jnp.bfloat16)
    d_heads = d_heads.reshape(SEQ, HEADS, HEAD).astype(jnp.float32)
    d_probs = jnp.einsum("qhe,khe->hqk", d_heads, v_heads)
    grad_v = jnp.einsum("hqk,qhe->khe", probs_bf, d_heads)
    d_scores = attn_probs * (d_probs - jnp.sum(d_probs * attn_probs, axis=-1, keepdims=True))
    d_scores_bf = (d_scores * score_scale).astype(jnp.bfloat16).astype(jnp.float32)
    grad_q = jnp.einsum("hqk,khe->qhe", d_scores_bf, k_heads)
    grad_k = jnp.einsum("hqk,qhe->khe", d_scores_bf, q_heads)
    d_qkv = jnp.stack([grad_q, grad_k, grad_v], axis=1).reshape(SEQ, 3 * D)
    grad_b_qkv = jnp.sum(d_qkv, axis=0)
    d_qkv_bf = d_qkv.astype(jnp.bfloat16)
    grad_w_qkv = jnp.dot(h_one.T, d_qkv_bf, preferred_element_type=jnp.float32)
    d_h_one = jnp.dot(d_qkv_bf, w_qkv.T, preferred_element_type=jnp.float32)
    grad_ln1_gain = jnp.sum(d_h_one * xhat_one, axis=0)
    grad_ln1_bias = jnp.sum(d_h_one, axis=0)
    dx_seq = (g_resid + norm_one_back(d_h_one * ln1_gain)[0]).astype(jnp.bfloat16)
    grad_vec = jnp.stack([grad_ln1_gain, grad_ln1_bias, grad_out_bias, grad_scale_attn,
                          grad_ln2_gain, grad_ln2_bias, grad_down_bias, grad_scale_mlp])
    return z_seq, dx_seq, (grad_w_qkv, grad_b_qkv, grad_w_out, grad_w_up, grad_b_up, grad_w_down, grad_vec)


def reference(x_tokens, grad_z, w_qkv, b_qkv, w_out, w_up, b_up, w_down, vec_params):
    matrices = (w_qkv.astype(jnp.bfloat16), w_out.astype(jnp.bfloat16),
                w_up.astype(jnp.bfloat16), w_down.astype(jnp.bfloat16))
    bias_qkv = b_qkv.astype(jnp.bfloat16).astype(jnp.float32)
    bias_up = b_up.astype(jnp.bfloat16).astype(jnp.float32)
    vec_rows = vec_params.astype(jnp.bfloat16).astype(jnp.float32)

    def step(running, pair):
        z_seq, dx_seq, seq_grads = layer_pass(pair[0], pair[1], matrices, bias_qkv, bias_up, vec_rows)
        return jax.tree.map(jnp.add, running, seq_grads), (z_seq, dx_seq)

    zero_grads = (jnp.zeros((D, 3 * D), jnp.float32), jnp.zeros((3 * D,), jnp.float32),
                  jnp.zeros((D, D), jnp.float32), jnp.zeros((D, FF), jnp.float32),
                  jnp.zeros((FF,), jnp.float32), jnp.zeros((FF, D), jnp.float32),
                  jnp.zeros((8, D), jnp.float32))
    totals, seq_outs = lax.scan(step, zero_grads, (x_tokens, grad_z))
    grad_w_qkv, grad_b_qkv, grad_w_out, grad_w_up, grad_b_up, grad_w_down, grad_vec = totals
    return (seq_outs[0], seq_outs[1], grad_w_qkv, grad_b_qkv, grad_w_out, grad_w_up, grad_b_up,
            grad_w_down, grad_vec)
```

```python
import functools
import math

import jax
import jax.numpy as jnp
from jax import lax
from jax.experimental import pallas as pl
from jax.experimental.pallas import tpu as pltpu
from jax.sharding import PartitionSpec as P

HEADS = 16
LN_EPS = 1e-5
D = 1408
FF = 6144
SEQ = 257
HEAD = D // HEADS
SCALE = HEAD ** -0.5
QCOLS = 1536
HALF = 768
LANES = 128
F32 = jnp.float32
BF16 = jnp.bfloat16
VMEM_LIMIT = 62 * 1000 * 1000
G1, C1, BO, S1, G2, C2, B2, S2 = range(8)
Q, K, V, O = range(4)
SEQS = (2, SEQ, D)


def sds(dtype, *shape):
    return jax.ShapeDtypeStruct(shape, dtype)


MESH_ID = pl.DeviceIdType.MESH
SIDE = 4
PAIR = 2
COLOURS = range(3)
COLOUR_DIMS = ("xyz", "yzx", "zxy")
FIRST, SECOND, THIRD, LAST = range(4)
WAYS = range(PAIR)
NEAR, FAR, ADDED = 0, 2, 4
WIDE, DOWN = "wide", "down"
ANY = pl.BlockSpec(memory_space=pl.ANY)
ALL = slice(None)


def duo(m):
    return pl.ds(PAIR * m, PAIR)


def toward(m):
    return 1 - PAIR * (m % PAIR)


class Torus:
    def __init__(self):
        f = lax.axis_index("fsdp")
        self.at = {"x": lax.axis_index("rep"), "z": lax.div(f, SIDE * PAIR), "y": lax.rem(lax.div(f, PAIR), SIDE),
                   "c": lax.rem(f, PAIR)}

    def shift(self, dim, by):
        return lax.rem(self.at[dim] + (SIDE + by), SIDE)

    def device(self, **moved):
        p = {**self.at, **moved}
        return (p["x"], (p["z"] * SIDE + p["y"]) * PAIR + p["c"])

    def neighbour(self, dim, by):
        return self.device(**{dim: self.shift(dim, by)})

    def partner(self):
        return self.device(c=1 - self.at["c"])


def enter():
    me = Torus()
    barrier = pltpu.get_barrier_semaphore()
    others = [me.neighbour(d, toward(m)) for d in COLOUR_DIMS[0] for m in WAYS] + [me.partner()]
    for other in others:
        pl.semaphore_signal(barrier, device_id=other, device_id_type=MESH_ID)
    pl.semaphore_wait(barrier, len(others))


def remote(src, dst, sems, slot, device):
    return pltpu.make_async_remote_copy(src_ref=src, dst_ref=dst, send_sem=sems[0].at[slot], recv_sem=sems[1].at[slot],
                                        device_id=device, device_id_type=MESH_ID)


class Gather:
    def __init__(self, kind, src, dst, hop_send, hop_recv, push_send, push_recv, local):
        self.kind, self.src, self.dst, self.local = kind, src, dst, local
        self.hops, self.pushes = (hop_send, hop_recv), (push_send, push_recv)
        self.cols, self.cut = (256, 128) if kind == WIDE else (D, HALF)

    @staticmethod
    def semaphores():
        dma = pltpu.SemaphoreType.DMA
        return [dma((3, 3, 4))] * PAIR + [dma((3, 5))] * PAIR + [dma((3,))]

    @staticmethod
    def shape(kind):
        return (4, 4, 4, 88, QCOLS) if kind == WIDE else (4, 4, 2, 4, 3, 16, D)

    def source(self, k):
        return self.src.at[:, pl.ds(self.cols * k, self.cols)] if self.kind == WIDE else self.src.at[k]

    def piece(self, me, k, s, v, half=None):
        dims = COLOUR_DIMS[k]
        at = {**me.at, **{d: ALL for d in dims[:s]}, dims[s]: v}
        off, width = 0, self.cols
        if half is not None and s == FIRST:
            off, width = self.cut * half, (self.cut, self.cols - self.cut)[half]
        elif half is not None:
            at[dims[0]] = duo(half)
        if self.kind == WIDE:
            cols = pl.ds(pl.multiple_of(at["c"] * HALF + self.cols * k + off, 128), width)
            return self.dst.at[at["x"], at["z"], at["y"], :, cols]
        return self.dst.at[at["z"], at["y"], at["c"], at["x"], k, :, pl.ds(off, width)]

    def hop(self, k, s, m):
        me = Torus()
        dim = COLOUR_DIMS[k][s]
        by = toward(m)
        if m < FAR:
            ref = self.piece(me, k, s, me.at[dim])
        else:
            ref = self.piece(me, k, s, me.shift(dim, -by), m - FAR)
        src = self.source(k) if s == FIRST and m < FAR else ref
        return remote(src, ref, self.hops, (k, s, m), me.neighbour(dim, by))

    def push(self, k, n):
        me = Torus()
        dim = COLOUR_DIMS[k][THIRD]
        if n < FAR:
            ref = self.piece(me, k, THIRD, me.shift(dim, -toward(n)))
        elif n < ADDED:
            ref = self.piece(me, k, THIRD, me.shift(dim, FAR), n - FAR)
        else:
            ref = self.piece(me, k, THIRD, me.at[dim])
        return remote(ref, ref, self.pushes, (k, n), me.partner())

    def own(self, k):
        me = Torus()
        return pltpu.make_async_copy(self.source(k), self.piece(me, k, FIRST, me.at[COLOUR_DIMS[k][FIRST]]), self.local.at[k])

    def launch(self, s):
        for k in COLOURS:
            for m in WAYS:
                self.hop(k, s, m).start()
            if s == THIRD:
                self.push(k, ADDED).start()

    def relay(self, k, s):
        for m in WAYS:
            self.hop(k, s, m).wait_recv()
            self.hop(k, s, FAR + m).start()
            if s == THIRD:
                self.push(k, m).start()

    def settle(self, s):
        for k in COLOURS:
            for m in WAYS:
                self.hop(k, s, FAR + m).wait_recv()
                if s == THIRD:
                    self.push(k, FAR + m).start()
            if s == FIRST:
                self.own(k).wait()
        if s < THIRD:
            self.launch(s + 1)

    def begin(self):
        for k in COLOURS:
            self.own(k).start()
        self.launch(FIRST)

    def finish(self):
        for k in COLOURS:
            for s in COLOURS:
                for m in range(ADDED):
                    self.hop(k, s, m).wait_send()
            for n in range(ADDED + 1):
                self.push(k, n).wait()

    def steps(self):
        out = [self.begin]
        for s in COLOURS:
            out += [functools.partial(self.relay, k, s) for k in COLOURS] + [functools.partial(self.settle, s)]
        return out + [self.finish]


def add_into(total, *others):
    lead = total.shape[:-2]

    def body(i, carry):
        idx = []
        for n in reversed(lead):
            idx.insert(0, lax.rem(i, n))
            i = lax.div(i, n)
        value = total[tuple(idx)]
        for other in others:
            value = value + other[tuple(idx)]
        total[tuple(idx)] = value
        return carry

    lax.fori_loop(0, math.prod(lead), body, 0)


class Scatter:
    def __init__(self, kind, part, out, own, passed, relay1, in1, relay2, in2, relay3, in3, result, send, recv, load, store):
        self.kind, self.part, self.out, self.own, self.passed, self.result = kind, part, out, own, passed, result
        self.relays, self.ins = (relay1, relay2, relay3), (in1, in2, in3)
        self.sems, self.load_sem, self.store_sem = (send, recv), load, store
        self.order = "xzy" if kind == WIDE else "zyx"
        self.half = result.shape[-1] // PAIR

    @staticmethod
    def scratch(kind):
        rows, cols = Scatter.unit(kind)
        vm = lambda *shape: pltpu.VMEM(shape + (rows, cols), F32)
        dma = pltpu.SemaphoreType.DMA
        return [vm(3, 4, 4), vm(3, 2, 2, 4), vm(3, 2, 2, 4), vm(3, 2, 4, 4), vm(3, 2, 2), vm(3, 2, 4),
                pltpu.VMEM((3, 2, rows, cols // PAIR), F32), vm(3, 2), vm(4, 3),
                dma((3, 4, 6)), dma((3, 4, 6)), dma((3, 3)), dma]

    @staticmethod
    def unit(kind):
        return (88, 256) if kind == WIDE else (32, HALF)

    def rest(self, k):
        return [d for d in self.order if d != COLOUR_DIMS[k][FIRST]]

    def terms(self, k, s, v, half=None):
        if s == FIRST:
            at = {d: ALL for d in self.order}
            at[COLOUR_DIMS[k][FIRST]] = v
            if half is not None:
                at[self.rest(k)[0]] = duo(half)
            lead = tuple(at[d] for d in self.order)
            return self.part.at[lead + ((ALL, pl.ds(256 * k, 256)) if self.kind == WIDE else (k,))]
        if s == SECOND:
            other = ALL if half is None else duo(half)
            return self.own.at[(k, v, other) if self.rest(k)[0] == COLOUR_DIMS[k][SECOND] else (k, other, v)]
        return self.ins[SECOND].at[(k, 0, v) + (() if half is None else (ALL, self.cols(half)))]

    def cols(self, m):
        return pl.ds(self.half * m, self.half)

    def landing(self, k, s, m, half):
        return self.ins[s].at[(k, m) + ((ALL, self.cols(half)) if s == THIRD else (duo(half),))]

    def hop(self, k, s, m):
        me = Torus()
        way, by = m % PAIR, toward(m)
        dim = "x" if s == LAST else COLOUR_DIMS[k][s]
        if s == LAST:
            src = self.result.at[me.at["x"], k] if m < FAR else self.result.at[me.shift("x", -by), k, :, self.cols(way)]
            dst = src
        elif m < FAR:
            src, dst = self.terms(k, s, me.shift(dim, FAR), way), self.relays[s].at[k, way]
        elif m < ADDED:
            src, dst = self.terms(k, s, me.shift(dim, by), 1 - way), self.landing(k, s, way, 1 - way)
        else:
            src, dst = (self.passed if s == FIRST else self.relays[s]).at[k, way], self.landing(k, s, way, way)
        return remote(src, dst, self.sems, (k, s, m), me.neighbour(dim, by))

    def load(self, k, m):
        me = Torus()
        dim = COLOUR_DIMS[k][FIRST]
        if m in WAYS:
            src, dst = self.terms(k, FIRST, me.shift(dim, toward(m)), m), self.passed.at[k, m]
        else:
            src, dst = self.terms(k, FIRST, me.at[dim]), self.own.at[k]
        return pltpu.make_async_copy(src, dst, self.load_sem.at[k, m])

    def begin(self):
        for base in (NEAR, FAR):
            for k in COLOURS:
                for m in WAYS:
                    self.hop(k, FIRST, base + m).start()
        for m in COLOURS:
            for k in COLOURS:
                self.load(k, m).start()

    def relay(self, k, s):
        me = Torus()
        for m in WAYS:
            self.hop(k, s, m).wait_recv()
            mine = self.relays[s].at[k, m]
            if s == FIRST:
                self.load(k, m).wait()
                add_into(self.passed.at[k, m], mine)
            else:
                terms = self.terms(k, s, me.shift(COLOUR_DIMS[k][s], toward(m)), m)
                if s == SECOND:
                    add_into(mine, terms)
                else:
                    mine[...] += terms[...]
            self.hop(k, s, ADDED + m).start()

    def settle(self, k, s):
        me = Torus()
        if s == FIRST:
            self.load(k, FAR).wait()
        for m in WAYS:
            self.hop(k, s, FAR + m).wait_recv()
            self.hop(k, s, ADDED + m).wait_recv()
        plus, minus = (self.ins[s].at[k, m] for m in WAYS)
        if s == FIRST:
            add_into(self.own.at[k], plus, minus)
        elif s == SECOND:
            add_into(plus, minus, self.terms(k, s, me.at[COLOUR_DIMS[k][s]]))
        else:
            mine = self.terms(k, s, me.at[COLOUR_DIMS[k][s]])
            self.result[me.at["x"], k] = mine[...] + plus[...] + minus[...]
        for base in (NEAR,) if s == THIRD else (NEAR, FAR):
            for m in WAYS:
                self.hop(k, s + 1, base + m).start()

    def spread(self, k):
        for m in WAYS:
            self.hop(k, LAST, m).wait_recv()
            self.hop(k, LAST, FAR + m).start()

    def finish(self):
        for k in COLOURS:
            for m in WAYS:
                self.hop(k, LAST, FAR + m).wait_recv()
        store = pltpu.make_async_copy(self.result, self.out, self.store_sem)
        store.start()
        for k in COLOURS:
            for s in range(SIDE):
                for m in range(ADDED if s == LAST else ADDED + PAIR):
                    self.hop(k, s, m).wait_send()
        store.wait()

    def steps(self):
        out = [self.begin]
        for s in COLOURS:
            for what in (self.relay, self.settle):
                out += [functools.partial(what, k, s) for k in COLOURS]
        return out + [functools.partial(self.spread, k) for k in COLOURS] + [self.finish]


def comm_params(collective_id):
    return pltpu.CompilerParams(collective_id=collective_id, has_side_effects=True, vmem_limit_bytes=VMEM_LIMIT)


def torus_gather(kind, piece, collective_id):
    def kernel(*refs):
        enter()
        for step in Gather(kind, *refs).steps():
            step()

    return pl.pallas_call(
        kernel, out_shape=sds(BF16, *Gather.shape(kind)), in_specs=[ANY], out_specs=ANY,
        scratch_shapes=Gather.semaphores(), compiler_params=comm_params(collective_id), name="gather_" + kind)(piece)


def torus_scatter(kind, part, collective_id):
    def kernel(*refs):
        enter()
        for step in Scatter(kind, *refs).steps():
            step()

    return pl.pallas_call(
        kernel, out_shape=sds(F32, 4, 3, *Scatter.unit(kind)), in_specs=[ANY], out_specs=ANY,
        scratch_shapes=Scatter.scratch(kind), compiler_params=comm_params(collective_id), name="scatter_" + kind)(part)


SEQ_PAIR = range(SEQS[0])
NT = (((1,), (1,)), ((), ()))
TN = (((0,), (0,)), ((), ()))


def dot(a, b):
    return jnp.dot(a, b, preferred_element_type=F32)


def dot_nt(a, b):
    return lax.dot_general(a, b, NT, preferred_element_type=F32)


def dot_tn(a, b):
    return lax.dot_general(a, b, TN, preferred_element_type=F32)


def zeros_but(n, axis, value):
    return tuple(value if i == axis else 0 for i in range(n))


def whole(*shape):
    return pl.BlockSpec(shape, lambda *_: (0,) * len(shape))


def along(axis, *block, index=lambda j: j):
    return pl.BlockSpec(block, lambda j: zeros_but(len(block), axis, index(j)))


def compute_params():
    return pltpu.CompilerParams(dimension_semantics=("arbitrary",), vmem_limit_bytes=VMEM_LIMIT)


def work(flops):
    return pl.CostEstimate(flops=flops, bytes_accessed=D * FF, transcendentals=0)


def row(vec, i):
    return vec[i:i + 1]


def row_mean(t):
    return jnp.mean(t, axis=-1, keepdims=True)


def norm_stats(t):
    centered = t - row_mean(t)
    rstd = lax.rsqrt(row_mean(centered * centered) + LN_EPS)
    return centered * rstd, rstd


def norm_back(xhat, rstd, g):
    return rstd * (g - row_mean(g) - xhat * row_mean(g * xhat))


def col_sum(t):
    return jnp.sum(t, axis=0, keepdims=True)


def at_step(j):
    return pl.when(pl.program_id(0) == j)


def accumulate(ref, value):
    @at_step(0)
    def _():
        ref[...] = value

    @pl.when(pl.program_id(0) > 0)
    def _():
        ref[...] += value


def qkv_kernel(x, w, b, vec, qkv, h1):
    @at_step(0)
    def _():
        for s in SEQ_PAIR:
            xhat, _ = norm_stats(x[s].astype(F32))
            h1[s] = (xhat * row(vec, G1) + row(vec, C1)).astype(BF16)

    for s in SEQ_PAIR:
        qkv[0, s] = (dot(h1[s], w[0]) + b[0]).astype(BF16)


def qkv_call(x, w_attn, b_qkv, vec):
    return pl.pallas_call(
        qkv_kernel, grid=(O,), out_shape=(sds(BF16, O, *SEQS), sds(BF16, *SEQS)),
        in_specs=[whole(*SEQS), along(0, 1, D, D), along(0, 1, 1, D), whole(8, D)],
        out_specs=(along(0, 1, *SEQS), whole(*SEQS)),
        compiler_params=compute_params(), cost_estimate=work(SEQ * D * D), name="ln1_qkv",
    )(x, w_attn, b_qkv, vec)


def window(h):
    start = h * HEAD // LANES * LANES
    stop = min(D, -(-(h + 1) * HEAD // LANES) * LANES)
    lane = lax.broadcasted_iota(jnp.int32, (1, stop - start), 1) + (start - h * HEAD)
    return slice(start, stop), (lane >= 0) & (lane < HEAD)


def only(mask, t):
    return jnp.where(mask, t, jnp.zeros_like(t))


def softmax(scores):
    e = jnp.exp(scores - jnp.max(scores, axis=-1, keepdims=True))
    return e * (1.0 / jnp.sum(e, axis=-1, keepdims=True))


def attn_kernel(qkv, x, w_out, vec, o, att, h2, acc):
    acc[...] = jnp.zeros_like(acc)
    for h in range(HEADS):
        lanes, mask = window(h)
        k = only(mask, qkv[K, 0, :, lanes])
        v = only(mask, qkv[V, 0, :, lanes])
        probs = softmax(dot_nt(qkv[Q, 0, :, lanes], k) * SCALE).astype(BF16)
        acc[:, lanes] += dot(probs, v)
    heads = acc[...].astype(BF16)
    o[0] = heads
    a = dot(heads, w_out[0]) + row(vec, BO)
    att[0] = a
    xhat, _ = norm_stats(x[0].astype(F32) + row(vec, S1) * a)
    h2[0] = (xhat * row(vec, G2) + row(vec, C2)).astype(BF16)


def one_seq():
    return along(0, 1, SEQ, D)


def w_out_block():
    return along(0, 1, D, D, index=lambda j: O)


def attn_call(qkv, x, w_attn, vec):
    return pl.pallas_call(
        attn_kernel, grid=SEQS[:1], out_shape=(sds(BF16, *SEQS), sds(F32, *SEQS), sds(BF16, *SEQS)),
        in_specs=[along(1, O, 1, SEQ, D), one_seq(), w_out_block(), whole(8, D)],
        out_specs=(one_seq(),) * O, scratch_shapes=[pltpu.VMEM((SEQ, D), F32)],
        compiler_params=compute_params(), cost_estimate=work(SEQ * D * D), name="attn_wo_ln2",
    )(qkv, x, w_attn, vec)


def mlp_kernel(h2, gz, w_up, b_up, w_down, vec, act, d_pre, db_up, mlp, d_h2, dm_halves, dm):
    @at_step(0)
    def _():
        mlp[...] = jnp.zeros_like(mlp)
        d_h2[...] = jnp.zeros_like(d_h2)
        for s in SEQ_PAIR:
            d = (gz[s].astype(F32) * row(vec, S2)).astype(BF16)
            dm[s] = d
            dm_halves[0, s] = d[:, :HALF]
            dm_halves[1, s] = d[:, D - HALF:]

    db = jnp.zeros((1, HALF), F32)
    for s in SEQ_PAIR:
        u = dot(h2[s], w_up[0]) + b_up[0]
        phi = 0.5 * (1.0 + lax.erf(u * math.sqrt(0.5)))
        a = (u * phi).astype(BF16)
        act[s] = a
        slope = phi + u * (jnp.exp(-0.5 * u * u) * (math.sqrt(0.5 / math.pi)))
        mlp[s] += dot(a, w_down[...])
        d = dot_nt(dm[s], w_down[...]) * slope
        db = db + col_sum(d)
        d = d.astype(BF16)
        d_pre[0, 0, s] = d
        d_h2[s] += dot_nt(d, w_up[0])
    db_up[0] = db


def mlp_call(h2, gz, w_up, b_up, w_down, vec):
    n = FF // HALF
    tiled = along(2, 2, SEQ, HALF)
    bias = along(0, 1, 1, HALF)
    halved = pl.BlockSpec((1, 1, 2, SEQ, HALF), lambda j: (j % PAIR, j // PAIR, 0, 0, 0))
    return pl.pallas_call(
        mlp_kernel, grid=(n,),
        out_shape=(sds(BF16, 2, SEQ, FF), sds(BF16, 2, 4, 2, SEQ, HALF), sds(F32, n, 1, HALF), sds(F32, *SEQS),
                   sds(F32, *SEQS), sds(BF16, 2, 2, SEQ, HALF)),
        in_specs=[whole(*SEQS), whole(*SEQS), pl.BlockSpec((1, D, HALF), lambda j: (j // PAIR, 0, j % PAIR)), bias,
                  along(0, HALF, D), whole(8, D)],
        out_specs=(tiled, halved, bias, whole(*SEQS), whole(*SEQS), whole(2, 2, SEQ, HALF)),
        scratch_shapes=[pltpu.VMEM(SEQS, BF16)],
        compiler_params=compute_params(), cost_estimate=work(SEQ * D * FF), name="mlp",
    )(h2, gz, w_up, b_up.reshape(n, 1, HALF), w_down, vec)


def halves_of(t):
    return t[:, :HALF], jnp.concatenate([t[:, HALF:], jnp.zeros((SEQ, QCOLS - D), t.dtype)], axis=1)


def mid_kernel(mlp, d_h2, att, x, gz, vec, w_out, z, g_res, d_att, d_o, sums):
    a = att[0]
    y = x[0].astype(F32) + row(vec, S1) * a
    m = mlp[0] + row(vec, B2)
    g = gz[0].astype(F32)
    z[0] = (y + row(vec, S2) * m).astype(BF16)
    xhat, rstd = norm_stats(y)
    dh = d_h2[0]
    gr = g + norm_back(xhat, rstd, dh * row(vec, G2))
    g_res[0] = gr
    da = gr * row(vec, S1)
    terms = (da, gr * a, dh * xhat, dh, g * row(vec, S2), g * m)
    accumulate(sums, jnp.concatenate([jnp.zeros((BO, D), F32)] + [col_sum(t) for t in terms], axis=0))
    da = da.astype(BF16)
    for i, t in enumerate(halves_of(da)):
        d_att[i, 0] = t
    d_o[0] = dot_nt(da, w_out[0]).astype(BF16)


def mid_call(mlp, d_h2, att, x, gz, vec, w_attn):
    return pl.pallas_call(
        mid_kernel, grid=SEQS[:1],
        out_shape=(sds(BF16, *SEQS), sds(F32, *SEQS), sds(BF16, 2, 2, SEQ, HALF), sds(BF16, *SEQS), sds(F32, 8, D)),
        in_specs=[one_seq()] * len("mdaxg") + [whole(8, D), w_out_block()],
        out_specs=(one_seq(), one_seq(), along(1, 2, 1, SEQ, HALF), one_seq(), whole(8, D)),
        compiler_params=compute_params(), cost_estimate=work(SEQ * D * D), name="ln2_back_wo",
    )(mlp, d_h2, att, x, gz, vec, w_attn)


def attn_back_kernel(qkv, d_o, d_qkv, db, acc):
    acc[...] = jnp.zeros_like(acc)
    for h in range(HEADS):
        lanes, mask = window(h)
        q, k, v = (only(mask, qkv[i, 0, :, lanes]) for i in (Q, K, V))
        do = only(mask, d_o[0, :, lanes])
        probs = softmax(dot_nt(q, k) * SCALE)
        acc[V, :, lanes] += dot_tn(probs.astype(BF16), do)
        dp = dot_nt(do, v)
        ds = probs * (dp - jnp.sum(dp * probs, axis=-1, keepdims=True))
        ds = (ds * SCALE).astype(BF16)
        acc[Q, :, lanes] += dot(ds, k)
        acc[K, :, lanes] += dot_tn(ds, q)
    accumulate(db, jnp.concatenate([col_sum(acc[i]) for i in (Q, K, V)], axis=0))
    for n in (Q, K, V):
        for i, t in enumerate(halves_of(acc[n].astype(BF16))):
            d_qkv[i, n, 0] = t


def attn_back_call(qkv, d_o):
    return pl.pallas_call(
        attn_back_kernel, grid=SEQS[:1], out_shape=(sds(BF16, 2, O, 2, SEQ, HALF), sds(F32, O, D)),
        in_specs=[along(1, O, 1, SEQ, D), one_seq()], out_specs=(along(2, 2, O, 1, SEQ, HALF), whole(O, D)),
        scratch_shapes=[pltpu.VMEM((O, SEQ, D), F32)],
        compiler_params=compute_params(), cost_estimate=work(SEQ * D * D), name="attn_back",
    )(qkv, d_o)


def in_back_kernel(d_qkv, w, x, g_res, vec, dx, sums, acc):
    rest = D - HALF
    for s in SEQ_PAIR:
        part = dot_nt(d_qkv[0, 0, s], w[0, :, :HALF]) + dot_nt(d_qkv[1, 0, s, :, :rest], w[0, :, HALF:])
        accumulate(acc.at[s], part)

    @at_step(V)
    def _():
        total = jnp.zeros((BO, D), F32)
        for s in SEQ_PAIR:
            xhat, rstd = norm_stats(x[s].astype(F32))
            dh = acc[s]
            total = total + jnp.concatenate([col_sum(dh * xhat), col_sum(dh)], axis=0)
            dx[s] = (g_res[s] + norm_back(xhat, rstd, dh * row(vec, G1))).astype(BF16)
        sums[...] = total


def in_back_call(d_qkv, w_attn, x, g_res, vec):
    return pl.pallas_call(
        in_back_kernel, grid=(O,), out_shape=(sds(BF16, *SEQS), sds(F32, BO, D)),
        in_specs=[along(1, 2, 1, 2, SEQ, HALF), along(0, 1, D, D), whole(*SEQS), whole(*SEQS), whole(8, D)],
        out_specs=(whole(*SEQS), whole(BO, D)), scratch_shapes=[pltpu.VMEM(SEQS, F32)],
        compiler_params=compute_params(), cost_estimate=work(SEQ * D * D), name="ln1_back",
    )(d_qkv, w_attn, x, g_res, vec)


BODY = SEQ - 1
ROWS = 4 * SEQ + 12


def stack_tokens(dst, seqs):
    for i, seq in enumerate(seqs):
        dst[pl.ds(BODY * i, BODY)] = seq[:BODY]
    last = [seq[BODY:].astype(F32) for seq in seqs]
    tail = jnp.concatenate(last + [jnp.zeros((ROWS - len(seqs) * SEQ, dst.shape[1]), F32)], axis=0)
    dst[pl.ds(len(seqs) * BODY, ROWS - len(seqs) * BODY)] = tail.astype(BF16)


def grad_kernel(new_a, new_b, a_own, a_pair, b_own, b_pair, *rest):
    extra, (out, a_rows, b_rows) = rest[:-3], rest[-3:]
    j = pl.program_id(0)

    def fill(dst, own, pair):
        lead = (0,) * (len(own.shape) - len(SEQS))
        stack_tokens(dst, [ref[lead + (s,)] for ref in (own, pair) for s in SEQ_PAIR])

    pl.when(new_a(j))(lambda: fill(a_rows, a_own, a_pair))
    pl.when(new_b(j))(lambda: fill(b_rows, b_own, b_pair))
    value = dot_tn(a_rows[...], b_rows[...])
    out[...] = value.reshape(out.shape)
    if extra:
        @at_step(0)
        def _():
            out[0, :, HALF - LANES:] += extra[0][...]


def grad_call(name, grid, a, a_spec, b, b_spec, new_a, new_b, out_shape, out_spec, extra=()):
    return pl.pallas_call(
        functools.partial(grad_kernel, new_a, new_b), grid=(grid,), out_shape=out_shape,
        in_specs=[a_spec] * PAIR + [b_spec] * PAIR + [whole(*e.shape) for e in extra], out_specs=out_spec,
        scratch_shapes=[pltpu.VMEM((ROWS, a_spec.block_shape[-1]), BF16), pltpu.VMEM((ROWS, HALF), BF16)],
        compiler_params=compute_params(), cost_estimate=work(SEQ * D * FF), name=name,
    )(*a, *b, *extra)


def wide_grads(name, a, b, new_a, a_index, extra=()):
    return grad_call(name, SIDE, a, along(0, 1, *SEQS, index=a_index), b, along(0, 1, 2, SEQ, HALF), new_a,
                     lambda j: j >= 0, sds(F32, SIDE, D, HALF), along(0, 1, D, HALF), extra)


def down_grads(a, b):
    return grad_call("dw_down", FF // HALF, a, along(2, 2, SEQ, HALF), b, whole(2, SEQ, HALF), lambda j: j >= 0,
                     lambda j: j == 0, sds(F32, FF, HALF), along(0, HALF, HALF))


OWN = 44
CHIP = OWN * PAIR
BQ, BU, VEC = 3 * D // 32, 3 * D // 32 + FF // 32, 3 * D // 32 + FF // 32 + 8 * OWN
DEVICES = 32


def pair_swap(a):
    return lax.ppermute(a, "fsdp", [(i, i ^ 1) for i in range(DEVICES)])


def by_core(first, a, b):
    return jnp.where(first, a, b), jnp.where(first, b, a)


def my_pieces(shards, first):
    w_qkv, b_qkv, w_out, w_up, b_up, w_down, vec_params = shards
    x = lax.axis_index("rep")
    small = jnp.concatenate([b_qkv, b_up, vec_params.reshape(-1)])
    small = jnp.pad(small, (0, OWN * LANES - VEC)).reshape(OWN, LANES)
    attn = lax.dynamic_slice_in_dim(jnp.concatenate([w_qkv, w_out], axis=1), x * D, D, 1)
    attn = jnp.concatenate([attn, small], axis=1)
    up = lax.dynamic_slice_in_dim(w_up, x * QCOLS, QCOLS, 1)
    wide = jnp.stack([attn, up]).astype(BF16)
    mine, theirs = by_core(first, wide[..., :HALF], wide[..., HALF:])
    theirs = pair_swap(theirs)
    piece = jnp.concatenate(by_core(first, mine, theirs), axis=1)
    down = lax.dynamic_slice_in_dim(w_down, x * 48, 48, 0).astype(BF16).reshape(3, 16, D)
    return piece[0], piece[1], down


def small_params(w_attn):
    small = w_attn[0, :, D:].astype(F32).reshape(DEVICES, OWN * LANES)
    vec = small[:, BU:VEC].reshape(DEVICES, 8, OWN).transpose(1, 0, 2).reshape(8, D)
    return small[:, :BQ].reshape(O, 1, D), small[:, BQ:BU].reshape(FF), vec


def small_grads(db_qkv, db_up, sums, core):
    vec = sums.reshape(8, DEVICES, OWN).transpose(1, 0, 2).reshape(DEVICES, VEC - BU)
    small = jnp.concatenate([db_qkv.reshape(DEVICES, BQ), db_up.reshape(DEVICES, BU - BQ), vec], axis=1)
    small = (small + pair_swap(small)) * core.astype(F32)
    return jnp.pad(small, ((0, 0), (0, OWN * LANES - VEC))).reshape(D, LANES)


def final_rows(total, first):
    keep, give = by_core(first, total[:, :, :OWN], total[:, :, OWN:])
    pair = jnp.stack(by_core(first, keep, pair_swap(give)), axis=1)
    return pair.transpose(3, 0, 1, 2, 4).reshape(OWN, SIDE, QCOLS)


def final_down(down, first):
    keep, give = by_core(first, down[:FF // DEVICES], down[FF // DEVICES:])
    left, right = by_core(first, keep, pair_swap(give))
    return jnp.concatenate([left, right[:, 2 * HALF - D:]], axis=1)


def device_step(x, gz, *shards):
    core = lax.rem(lax.axis_index("fsdp"), PAIR)
    first = core == 0
    attn, up, down = my_pieces(shards, first)
    w_attn = torus_gather(WIDE, attn, 0).reshape(SIDE, D, QCOLS)
    w_up = torus_gather(WIDE, up, 1).reshape(SIDE, D, QCOLS)
    w_down = torus_gather(DOWN, down, 2).reshape(FF, D)
    b_qkv, b_up, vec = small_params(w_attn)
    pick = lambda a, i: lax.dynamic_index_in_dim(a, i, 0, keepdims=False)
    both = lambda a: (a, pair_swap(a))
    halves = lambda a: (pick(a, core), pair_swap(pick(a, 1 - core)))

    qkv, h1 = qkv_call(x, w_attn, b_qkv, vec)
    o, att, h2 = attn_call(qkv, x, w_attn, vec)
    act, d_pre, db_up, mlp, d_h2, d_mlp = mlp_call(h2, gz, w_up, b_up, w_down, vec)
    part_down = down_grads(both(act), halves(d_mlp))
    z, g_res, d_att, d_o, sums = mid_call(mlp, d_h2, att, x, gz, vec, w_attn)
    part_up = wide_grads("dw_up", both(h2[None]), halves(d_pre), lambda j: j == 0, lambda j: 0)
    d_qkv, db_qkv = attn_back_call(qkv, d_o)
    dx, in_sums = in_back_call(d_qkv, w_attn, x, g_res, vec)
    small = small_grads(db_qkv, db_up, jnp.concatenate([in_sums, sums[BO:]], axis=0), core)
    d_cols = jnp.concatenate([d_qkv, d_att[:, None]], axis=1)
    part_attn = wide_grads("dw_attn", both(jnp.stack([h1, o])), halves(d_cols), lambda j: (j == Q) | (j == O),
                           lambda j: j // O, (small,))

    down = torus_scatter(DOWN, part_down.reshape(4, 4, 4, 3, 32, HALF), 3).reshape(FF // 16, HALF)
    up = torus_scatter(WIDE, part_up.reshape(4, 4, 4, CHIP, HALF), 4)
    attn = torus_scatter(WIDE, part_attn.reshape(4, 4, 4, CHIP, HALF), 5)
    g_up = final_rows(up, first).reshape(OWN, FF)
    attn = final_rows(attn, first)
    small = attn[:, 0, D:].reshape(OWN * LANES)
    return (z, dx, attn[:, :O, :D].reshape(OWN, O * D), small[:BQ], attn[:, O, :D], g_up, small[BQ:BU],
            final_down(down, first), small[BU:VEC].reshape(8, OWN))


def solution(mesh):
    batch = P(("rep", "fsdp"), None, None)
    rows, flat, cols = P("fsdp", None), P("fsdp"), P(None, "fsdp")
    shards = (rows, flat, rows, rows, flat, rows, cols)
    return jax.shard_map(device_step, mesh=mesh, in_specs=(batch, batch) + shards,
                         out_specs=(batch, batch) + shards, check_vma=False)
```

```python
import functools
import math

import jax
import jax.numpy as jnp
from jax import lax
from jax.experimental import pallas as pl
from jax.experimental.pallas import tpu as pltpu
from jax.sharding import PartitionSpec as P

HEADS = 16
LN_EPS = 1e-5
D = 1408
FF = 6144
SEQ = 257
HEAD = D // HEADS
SCALE = HEAD ** -0.5
QCOLS = 1536
HALF = 768
LANES = 128
F32 = jnp.float32
BF16 = jnp.bfloat16
VMEM_LIMIT = 66 * 1000 * 1000
G1, C1, BO, S1, G2, C2, B2, S2 = range(8)
Q, K, V, O = range(4)
SEQS = (2, SEQ, D)
SEQ_PAIR = range(SEQS[0])
TAIL = 8
BODY = SEQ - 1
TOK = BODY + TAIL
TOKS = (2, TOK, D)
ROWS = 4 * TOK


def sds(dtype, *shape):
    return jax.ShapeDtypeStruct(shape, dtype)


MESH_ID = pl.DeviceIdType.MESH
SIDE = 4
PAIR = 2
COLOURS = range(3)
COLOUR_DIMS = ("xyz", "yzx", "zxy")
FIRST, SECOND, THIRD, LAST = range(4)
WAYS = range(PAIR)
NEAR, FAR, ADDED = 0, 2, 4
WIDE, DOWN = "wide", "down"
ANY = pl.BlockSpec(memory_space=pl.ANY)
ALL = slice(None)


def duo(m):
    return pl.ds(PAIR * m, PAIR)


def toward(m):
    return 1 - PAIR * (m % PAIR)


class Torus:
    def __init__(self):
        f = lax.axis_index("fsdp")
        self.at = {"x": lax.axis_index("rep"), "z": lax.div(f, SIDE * PAIR), "y": lax.rem(lax.div(f, PAIR), SIDE),
                   "c": lax.rem(f, PAIR)}

    def shift(self, dim, by):
        return lax.rem(self.at[dim] + (SIDE + by), SIDE)

    def device(self, **moved):
        p = {**self.at, **moved}
        return (p["x"], (p["z"] * SIDE + p["y"]) * PAIR + p["c"])

    def neighbour(self, dim, by):
        return self.device(**{dim: self.shift(dim, by)})

    def partner(self):
        return self.device(c=1 - self.at["c"])


def enter():
    me = Torus()
    barrier = pltpu.get_barrier_semaphore()
    others = [me.neighbour(d, toward(m)) for d in COLOUR_DIMS[0] for m in WAYS] + [me.partner()]
    for other in others:
        pl.semaphore_signal(barrier, device_id=other, device_id_type=MESH_ID)
    pl.semaphore_wait(barrier, len(others))


def remote(src, dst, sems, slot, device):
    return pltpu.make_async_remote_copy(src_ref=src, dst_ref=dst, send_sem=sems[0].at[slot], recv_sem=sems[1].at[slot],
                                        device_id=device, device_id_type=MESH_ID)


class Gather:
    def __init__(self, kind, src, dst, hop_send, hop_recv, push_send, push_recv, local):
        self.kind, self.src, self.dst, self.local = kind, src, dst, local
        self.hops, self.pushes = (hop_send, hop_recv), (push_send, push_recv)
        self.cols, self.cut = (256, 128) if kind == WIDE else (D, HALF)

    @staticmethod
    def semaphores():
        dma = pltpu.SemaphoreType.DMA
        return [dma((3, 3, 4))] * PAIR + [dma((3, 5))] * PAIR + [dma((3,))]

    @staticmethod
    def shape(kind):
        return (4, 4, 4, 88, QCOLS) if kind == WIDE else (4, 4, 2, 4, 3, 16, D)

    def source(self, k):
        return self.src.at[:, pl.ds(self.cols * k, self.cols)] if self.kind == WIDE else self.src.at[k]

    def piece(self, me, k, s, v, half=None):
        dims = COLOUR_DIMS[k]
        at = {**me.at, **{d: ALL for d in dims[:s]}, dims[s]: v}
        off, width = 0, self.cols
        if half is not None and s == FIRST:
            off, width = self.cut * half, (self.cut, self.cols - self.cut)[half]
        elif half is not None:
            at[dims[0]] = duo(half)
        if self.kind == WIDE:
            cols = pl.ds(pl.multiple_of(at["c"] * HALF + self.cols * k + off, 128), width)
            return self.dst.at[at["x"], at["z"], at["y"], :, cols]
        return self.dst.at[at["z"], at["y"], at["c"], at["x"], k, :, pl.ds(off, width)]

    def hop(self, k, s, m):
        me = Torus()
        dim = COLOUR_DIMS[k][s]
        by = toward(m)
        if m < FAR:
            ref = self.piece(me, k, s, me.at[dim])
        else:
            ref = self.piece(me, k, s, me.shift(dim, -by), m - FAR)
        src = self.source(k) if s == FIRST and m < FAR else ref
        return remote(src, ref, self.hops, (k, s, m), me.neighbour(dim, by))

    def push(self, k, n):
        me = Torus()
        dim = COLOUR_DIMS[k][THIRD]
        if n < FAR:
            ref = self.piece(me, k, THIRD, me.shift(dim, -toward(n)))
        elif n < ADDED:
            ref = self.piece(me, k, THIRD, me.shift(dim, FAR), n - FAR)
        else:
            ref = self.piece(me, k, THIRD, me.at[dim])
        return remote(ref, ref, self.pushes, (k, n), me.partner())

    def own(self, k):
        me = Torus()
        return pltpu.make_async_copy(self.source(k), self.piece(me, k, FIRST, me.at[COLOUR_DIMS[k][FIRST]]), self.local.at[k])

    def launch(self, s):
        for k in COLOURS:
            for m in WAYS:
                self.hop(k, s, m).start()
            if s == THIRD:
                self.push(k, ADDED).start()

    def relay(self, k, s):
        for m in WAYS:
            self.hop(k, s, m).wait_recv()
            self.hop(k, s, FAR + m).start()
            if s == THIRD:
                self.push(k, m).start()

    def settle(self, s):
        for k in COLOURS:
            for m in WAYS:
                self.hop(k, s, FAR + m).wait_recv()
                if s == THIRD:
                    self.push(k, FAR + m).start()
            if s == FIRST:
                self.own(k).wait()
        if s < THIRD:
            self.launch(s + 1)

    def begin(self):
        for k in COLOURS:
            self.own(k).start()
        self.launch(FIRST)

    def finish(self):
        for k in COLOURS:
            for s in COLOURS:
                for m in range(ADDED):
                    self.hop(k, s, m).wait_send()
            for n in range(ADDED + 1):
                self.push(k, n).wait()

    def steps(self):
        out = [self.begin]
        for s in COLOURS:
            out += [functools.partial(self.relay, k, s) for k in COLOURS] + [functools.partial(self.settle, s)]
        return out + [self.finish]


def add_into(total, *others):
    lead = total.shape[:-2]

    def body(i, carry):
        idx = []
        for n in reversed(lead):
            idx.insert(0, lax.rem(i, n))
            i = lax.div(i, n)
        value = total[tuple(idx)]
        for other in others:
            value = value + other[tuple(idx)]
        total[tuple(idx)] = value
        return carry

    lax.fori_loop(0, math.prod(lead), body, 0)


class Scatter:
    def __init__(self, kind, part, out, own, passed, relay1, in1, relay2, in2, relay3, in3, result, send, recv, load, store):
        self.kind, self.part, self.out, self.own, self.passed, self.result = kind, part, out, own, passed, result
        self.relays, self.ins = (relay1, relay2, relay3), (in1, in2, in3)
        self.sems, self.load_sem, self.store_sem = (send, recv), load, store
        self.order = "xzy" if kind == WIDE else "zyx"
        self.half = result.shape[-1] // PAIR

    @staticmethod
    def scratch(kind):
        rows, cols = Scatter.unit(kind)
        vm = lambda *shape: pltpu.VMEM(shape + (rows, cols), F32)
        dma = pltpu.SemaphoreType.DMA
        return [vm(3, 4, 4), vm(3, 2, 2, 4), vm(3, 2, 2, 4), vm(3, 2, 4, 4), vm(3, 2, 2), vm(3, 2, 4),
                pltpu.VMEM((3, 2, rows, cols // PAIR), F32), vm(3, 2), vm(4, 3),
                dma((3, 4, 6)), dma((3, 4, 6)), dma((3, 3)), dma]

    @staticmethod
    def total(kind):
        return sds(F32, 4, 3, *Scatter.unit(kind))

    @staticmethod
    def unit(kind):
        return (88, 256) if kind == WIDE else (32, HALF)

    def rest(self, k):
        return [d for d in self.order if d != COLOUR_DIMS[k][FIRST]]

    def terms(self, k, s, v, half=None):
        if s == FIRST:
            at = {d: ALL for d in self.order}
            at[COLOUR_DIMS[k][FIRST]] = v
            if half is not None:
                at[self.rest(k)[0]] = duo(half)
            lead = tuple(at[d] for d in self.order)
            return self.part.at[lead + ((ALL, pl.ds(256 * k, 256)) if self.kind == WIDE else (k,))]
        if s == SECOND:
            other = ALL if half is None else duo(half)
            return self.own.at[(k, v, other) if self.rest(k)[0] == COLOUR_DIMS[k][SECOND] else (k, other, v)]
        return self.ins[SECOND].at[(k, 0, v) + (() if half is None else (ALL, self.cols(half)))]

    def cols(self, m):
        return pl.ds(self.half * m, self.half)

    def landing(self, k, s, m, half):
        return self.ins[s].at[(k, m) + ((ALL, self.cols(half)) if s == THIRD else (duo(half),))]

    def hop(self, k, s, m):
        me = Torus()
        way, by = m % PAIR, toward(m)
        dim = "x" if s == LAST else COLOUR_DIMS[k][s]
        if s == LAST:
            src = self.result.at[me.at["x"], k] if m < FAR else self.result.at[me.shift("x", -by), k, :, self.cols(way)]
            dst = src
        elif m < FAR:
            src, dst = self.terms(k, s, me.shift(dim, FAR), way), self.relays[s].at[k, way]
        elif m < ADDED:
            src, dst = self.terms(k, s, me.shift(dim, by), 1 - way), self.landing(k, s, way, 1 - way)
        else:
            src, dst = (self.passed if s == FIRST else self.relays[s]).at[k, way], self.landing(k, s, way, way)
        return remote(src, dst, self.sems, (k, s, m), me.neighbour(dim, by))

    def load(self, k, m):
        me = Torus()
        dim = COLOUR_DIMS[k][FIRST]
        if m in WAYS:
            src, dst = self.terms(k, FIRST, me.shift(dim, toward(m)), m), self.passed.at[k, m]
        else:
            src, dst = self.terms(k, FIRST, me.at[dim]), self.own.at[k]
        return pltpu.make_async_copy(src, dst, self.load_sem.at[k, m])

    def begin(self):
        for base in (NEAR, FAR):
            for k in COLOURS:
                for m in WAYS:
                    self.hop(k, FIRST, base + m).start()
        for m in COLOURS:
            for k in COLOURS:
                self.load(k, m).start()

    def relay(self, k, s):
        me = Torus()
        for m in WAYS:
            self.hop(k, s, m).wait_recv()
            mine = self.relays[s].at[k, m]
            if s == FIRST:
                self.load(k, m).wait()
                add_into(self.passed.at[k, m], mine)
            else:
                terms = self.terms(k, s, me.shift(COLOUR_DIMS[k][s], toward(m)), m)
                if s == SECOND:
                    add_into(mine, terms)
                else:
                    mine[...] += terms[...]
            self.hop(k, s, ADDED + m).start()

    def settle(self, k, s):
        me = Torus()
        if s == FIRST:
            self.load(k, FAR).wait()
        for m in WAYS:
            self.hop(k, s, FAR + m).wait_recv()
            self.hop(k, s, ADDED + m).wait_recv()
        plus, minus = (self.ins[s].at[k, m] for m in WAYS)
        if s == FIRST:
            add_into(self.own.at[k], plus, minus)
        elif s == SECOND:
            add_into(plus, minus, self.terms(k, s, me.at[COLOUR_DIMS[k][s]]))
        else:
            mine = self.terms(k, s, me.at[COLOUR_DIMS[k][s]])
            self.result[me.at["x"], k] = mine[...] + plus[...] + minus[...]
        for base in (NEAR,) if s == THIRD else (NEAR, FAR):
            for m in WAYS:
                self.hop(k, s + 1, base + m).start()

    def spread(self, k):
        for m in WAYS:
            self.hop(k, LAST, m).wait_recv()
            self.hop(k, LAST, FAR + m).start()

    def finish(self):
        for k in COLOURS:
            for m in WAYS:
                self.hop(k, LAST, FAR + m).wait_recv()
        store = pltpu.make_async_copy(self.result, self.out, self.store_sem)
        store.start()
        for k in COLOURS:
            for s in range(SIDE):
                for m in range(ADDED if s == LAST else ADDED + PAIR):
                    self.hop(k, s, m).wait_send()
        store.wait()

    def steps(self):
        out = [self.begin]
        for s in COLOURS:
            for what in (self.relay, self.settle):
                out += [functools.partial(what, k, s) for k in COLOURS]
        return out + [functools.partial(self.spread, k) for k in COLOURS] + [self.finish]


def comm_params(collective_id):
    return pltpu.CompilerParams(collective_id=collective_id, has_side_effects=True, vmem_limit_bytes=VMEM_LIMIT)


def torus_gather(kind, piece, collective_id):
    def kernel(*refs):
        enter()
        for step in Gather(kind, *refs).steps():
            step()

    return pl.pallas_call(
        kernel, out_shape=sds(BF16, *Gather.shape(kind)), in_specs=[ANY], out_specs=ANY,
        scratch_shapes=Gather.semaphores(), compiler_params=comm_params(collective_id), name="gather_" + kind)(piece)


def torus_scatter(kind, part, collective_id):
    def kernel(*refs):
        enter()
        for step in Scatter(kind, *refs).steps():
            step()

    return pl.pallas_call(
        kernel, out_shape=Scatter.total(kind), in_specs=[ANY], out_specs=ANY,
        scratch_shapes=Scatter.scratch(kind), compiler_params=comm_params(collective_id), name="scatter_" + kind)(part)


class Background:
    def __init__(self, steps, plan):
        self.steps, self.plan = steps, plan

    def visit(self, place):
        for j, first, end in self.plan.get(place, ()):
            @at_step(j)
            def _():
                for step in self.steps[first:end]:
                    step()


class Exchange:
    def __init__(self, mine, theirs, rows, sems, slot):
        self.moves = []
        for s in SEQ_PAIR:
            for i, (start, size) in enumerate(((0, BODY), (BODY, TAIL))):
                place = lambda n: rows.at[pl.ds(start * len(SEQ_PAIR) * PAIR + size * n, size)]
                n = len(SEQ_PAIR) + s
                at = slot + (PAIR * s + i,)
                local = pltpu.make_async_copy(mine.at[s, pl.ds(start, size)], place(s), sems[2].at[at])
                far = remote(theirs.at[s, pl.ds(start, size)], place(n), sems, at, Torus().partner())
                self.moves.append((local, far))

    @staticmethod
    def semaphores(*lead):
        return [pltpu.SemaphoreType.DMA(lead + (2 * PAIR,))] * 3

    def start(self):
        for local, far in self.moves:
            far.start()
            local.start()

    def wait(self):
        for local, far in self.moves:
            local.wait()
            far.wait_recv()

    def finish(self):
        for _, far in self.moves:
            far.wait_send()


NT = (((1,), (1,)), ((), ()))
TN = (((0,), (0,)), ((), ()))


def dot(a, b):
    return jnp.dot(a, b, preferred_element_type=F32)


def dot_nt(a, b):
    return lax.dot_general(a, b, NT, preferred_element_type=F32)


def dot_tn(a, b):
    return lax.dot_general(a, b, TN, preferred_element_type=F32)


def zeros_but(n, axis, value):
    return tuple(value if i == axis else 0 for i in range(n))


def whole(*shape):
    return pl.BlockSpec(shape, lambda *_: (0,) * len(shape))


def along(axis, *block, index=lambda j: j):
    return pl.BlockSpec(block, lambda j: zeros_but(len(block), axis, index(j)))


def compute_params():
    return pltpu.CompilerParams(dimension_semantics=("arbitrary",), vmem_limit_bytes=VMEM_LIMIT)


def work(flops):
    return pl.CostEstimate(flops=flops, bytes_accessed=D * FF, transcendentals=0)


def row(vec, i):
    return vec[i:i + 1]


def row_mean(t):
    return jnp.mean(t, axis=-1, keepdims=True)


def norm_stats(t):
    centered = t - row_mean(t)
    rstd = lax.rsqrt(row_mean(centered * centered) + LN_EPS)
    return centered * rstd, rstd


def norm_back(xhat, rstd, g):
    return rstd * (g - row_mean(g) - xhat * row_mean(g * xhat))


def col_sum(t):
    return jnp.sum(t, axis=0, keepdims=True)


def at_step(j):
    return pl.when(pl.program_id(0) == j)


def accumulate(ref, value):
    @at_step(0)
    def _():
        ref[...] = value

    @pl.when(pl.program_id(0) > 0)
    def _():
        ref[...] += value


def pad(t):
    return jnp.concatenate([t.astype(F32), jnp.zeros((TOK - SEQ, t.shape[1]), F32)], axis=0).astype(BF16)


def window(h):
    start = h * HEAD // LANES * LANES
    stop = min(D, -(-(h + 1) * HEAD // LANES) * LANES)
    lane = lax.broadcasted_iota(jnp.int32, (1, stop - start), 1) + (start - h * HEAD)
    return slice(start, stop), (lane >= 0) & (lane < HEAD)


def only(mask, t):
    return jnp.where(mask, t, jnp.zeros_like(t))


def softmax(scores):
    e = jnp.exp(scores - jnp.max(scores, axis=-1, keepdims=True))
    return e * (1.0 / jnp.sum(e, axis=-1, keepdims=True))


def attention(s, rows, x, w_out, vec, o, att, h2, acc, visit):
    acc[...] = jnp.zeros_like(acc)
    for h in range(HEADS):
        lanes, mask = window(h)
        k = only(mask, rows[K, s, :, lanes])
        v = only(mask, rows[V, s, :, lanes])
        probs = softmax(dot_nt(rows[Q, s, :, lanes], k) * SCALE).astype(BF16)
        acc[:, lanes] += dot(probs, v)
        visit(h)
    heads = acc[...]
    o[0] = pad(heads)
    a = dot(heads.astype(BF16), w_out[0]) + row(vec, BO)
    att[0] = a
    xhat, _ = norm_stats(x[s].astype(F32) + row(vec, S1) * a)
    h2[0] = pad(xhat * row(vec, G2) + row(vec, C2))


FRONT_PLAN = {"qkv": ((0, 0, 1), (1, 1, 5), (2, 5, 8)), HEADS - 2: ((O, 8, 9),), "end": ((O + 1, 9, None),)}


def front_kernel(x, w, b, vec, up_src, down_src, qkv, h1, o, att, h2, up, down, rows, acc, *sems):
    n = len(sems) // 2
    gathers = Gather(WIDE, up_src, up, *sems[:n]), Gather(DOWN, down_src, down, *sems[n:])
    steps = [lambda pair=pair: [step() for step in pair] for pair in zip(*(g.steps() for g in gathers))]
    hosted = Background(steps, FRONT_PLAN)
    j = pl.program_id(0)
    at_step(0)(enter)
    hosted.visit("qkv")

    @at_step(0)
    def _():
        for s in SEQ_PAIR:
            xhat, _ = norm_stats(x[s].astype(F32))
            h1[s] = pad(xhat * row(vec, G1) + row(vec, C1))

    @pl.when(j < O)
    def _():
        for s in SEQ_PAIR:
            t = (dot(h1[s, :SEQ], w[0]) + b[0]).astype(BF16)
            qkv[0, s] = t
            rows[j, s] = t

    @pl.when(j >= O)
    def _():
        attention(j - O, rows, x, w, vec, o, att, h2, acc, hosted.visit)

    hosted.visit("end")


def front_call(x, w_attn, b_qkv, vec, up, down, collective_id):
    upto = lambda n: lambda j: jnp.minimum(j, n)
    seq = lambda tokens: along(0, 1, tokens, D, index=lambda j: jnp.maximum(j - O, 0))
    return pl.pallas_call(
        front_kernel, grid=(O + PAIR,),
        out_shape=(sds(BF16, O, *SEQS), sds(BF16, *TOKS), sds(BF16, *TOKS), sds(F32, *SEQS), sds(BF16, *TOKS),
                   sds(BF16, *Gather.shape(WIDE)), sds(BF16, *Gather.shape(DOWN))),
        in_specs=[whole(*SEQS), along(0, 1, D, D, index=upto(O)), along(0, 1, 1, D, index=upto(V)), whole(8, D), ANY, ANY],
        out_specs=(along(0, 1, *SEQS, index=upto(V)), whole(*TOKS), seq(TOK), seq(SEQ), seq(TOK), ANY, ANY),
        scratch_shapes=[pltpu.VMEM((O, *SEQS), BF16), pltpu.VMEM((SEQ, D), F32)] + Gather.semaphores() * PAIR,
        compiler_params=comm_params(collective_id), name="front",
    )(x, w_attn, b_qkv, vec, up, down)


def one_seq():
    return along(0, 1, SEQ, D)


def w_out_block():
    return along(0, 1, D, D, index=lambda j: O)


def mlp_kernel(h2, gz, w_up, b_up, w_down, vec, act, d_pre, db_up, mlp, d_h2, dm_halves, dm):
    @at_step(0)
    def _():
        mlp[...] = jnp.zeros_like(mlp)
        d_h2[...] = jnp.zeros_like(d_h2)
        for s in SEQ_PAIR:
            d = (gz[s].astype(F32) * row(vec, S2)).astype(BF16)
            dm[s] = d
            d = pad(d)
            dm_halves[0, s] = d[:, :HALF]
            dm_halves[1, s] = d[:, D - HALF:]

    db = jnp.zeros((1, HALF), F32)
    for s in SEQ_PAIR:
        h = h2[s, :SEQ]
        u = dot(h, w_up[0]) + b_up[0]
        phi = 0.5 * (1.0 + lax.erf(u * math.sqrt(0.5)))
        a = (u * phi).astype(BF16)
        act[s] = pad(a)
        slope = phi + u * (jnp.exp(-0.5 * u * u) * (math.sqrt(0.5 / math.pi)))
        mlp[s] += dot(a, w_down[...])
        d = dot_nt(dm[s], w_down[...]) * slope
        db = db + col_sum(d)
        d = d.astype(BF16)
        d_pre[0, 0, s] = pad(d)
        d_h2[s] += dot_nt(d, w_up[0])
    db_up[0] = db


def mlp_call(h2, gz, w_up, b_up, w_down, vec):
    n = FF // HALF
    tiled = along(2, 2, TOK, HALF)
    bias = along(0, 1, 1, HALF)
    halved = pl.BlockSpec((1, 1, 2, TOK, HALF), lambda j: (j % PAIR, j // PAIR, 0, 0, 0))
    return pl.pallas_call(
        mlp_kernel, grid=(n,),
        out_shape=(sds(BF16, 2, TOK, FF), sds(BF16, 2, 4, 2, TOK, HALF), sds(F32, n, 1, HALF), sds(F32, *SEQS),
                   sds(F32, *SEQS), sds(BF16, 2, 2, TOK, HALF)),
        in_specs=[whole(*TOKS), whole(*SEQS), pl.BlockSpec((1, D, HALF), lambda j: (j // PAIR, 0, j % PAIR)), bias,
                  along(0, HALF, D), whole(8, D)],
        out_specs=(tiled, halved, bias, whole(*SEQS), whole(*SEQS), whole(2, 2, TOK, HALF)),
        scratch_shapes=[pltpu.VMEM(SEQS, BF16)],
        compiler_params=compute_params(), cost_estimate=work(SEQ * D * FF), name="mlp",
    )(h2, gz, w_up, b_up.reshape(n, 1, HALF), w_down, vec)


def halves_of(t):
    t = pad(t)
    return t[:, :HALF], jnp.concatenate([t[:, HALF:], jnp.zeros((TOK, QCOLS - D), BF16)], axis=1)


def mid_kernel(mlp, d_h2, att, x, gz, vec, w_out, z, g_res, d_att, d_o, sums):
    a = att[0]
    y = x[0].astype(F32) + row(vec, S1) * a
    m = mlp[0] + row(vec, B2)
    g = gz[0].astype(F32)
    z[0] = (y + row(vec, S2) * m).astype(BF16)
    xhat, rstd = norm_stats(y)
    dh = d_h2[0]
    gr = g + norm_back(xhat, rstd, dh * row(vec, G2))
    g_res[0] = gr
    da = gr * row(vec, S1)
    terms = (da, gr * a, dh * xhat, dh, g * row(vec, S2), g * m)
    accumulate(sums, jnp.concatenate([jnp.zeros((BO, D), F32)] + [col_sum(t) for t in terms], axis=0))
    for i, t in enumerate(halves_of(da)):
        d_att[i, 0] = t
    d_o[0] = dot_nt(da.astype(BF16), w_out[0]).astype(BF16)


def mid_call(mlp, d_h2, att, x, gz, vec, w_attn):
    return pl.pallas_call(
        mid_kernel, grid=SEQS[:1],
        out_shape=(sds(BF16, *SEQS), sds(F32, *SEQS), sds(BF16, 2, 2, TOK, HALF), sds(BF16, *SEQS), sds(F32, 8, D)),
        in_specs=[one_seq()] * len("mdaxg") + [whole(8, D), w_out_block()],
        out_specs=(one_seq(), one_seq(), along(1, 2, 1, TOK, HALF), one_seq(), whole(8, D)),
        compiler_params=compute_params(), cost_estimate=work(SEQ * D * D), name="ln2_back_wo",
    )(mlp, d_h2, att, x, gz, vec, w_attn)


def attention_back(qkv, d_o, d_qkv, db, acc, visit):
    acc[...] = jnp.zeros_like(acc)
    for h in range(HEADS):
        lanes, mask = window(h)
        q, k, v = (only(mask, qkv[i, 0, :, lanes]) for i in (Q, K, V))
        do = only(mask, d_o[0, :, lanes])
        probs = softmax(dot_nt(q, k) * SCALE)
        acc[V, :, lanes] += dot_tn(probs.astype(BF16), do)
        dp = dot_nt(do, v)
        ds = probs * (dp - jnp.sum(dp * probs, axis=-1, keepdims=True))
        ds = (ds * SCALE).astype(BF16)
        acc[Q, :, lanes] += dot(ds, k)
        acc[K, :, lanes] += dot_tn(ds, q)
        visit(h)
    accumulate(db, jnp.concatenate([col_sum(acc[i]) for i in (Q, K, V)], axis=0))
    for n in (Q, K, V):
        for i, t in enumerate(halves_of(acc[n])):
            d_qkv[i, n, 0] = t


THIN = HALF // PAIR


class WideGrads:
    def __init__(self, a, a_of, b, out, base, a_rows, b_rows, *sems):
        self.a, self.a_of, self.b, self.out, self.base, self.a_rows, self.b_rows = a, a_of, b, out, base, a_rows, b_rows
        self.a_sems, self.b_sems = sems[:3], sems[3:]

    @staticmethod
    def scratch(inputs):
        return ([pltpu.VMEM((inputs, ROWS, D), BF16), pltpu.VMEM((SIDE, ROWS, HALF), BF16)] +
                Exchange.semaphores(inputs) + Exchange.semaphores(SIDE))

    def input(self, i):
        return Exchange(self.a[i], self.a[i], self.a_rows.at[i], self.a_sems, (i,))

    def cotangent(self, n):
        c = Torus().at["c"]
        b = self.b[n]
        return Exchange(b(c), b(1 - c), self.b_rows.at[n], self.b_sems, (n,))

    def begin(self):
        for n in range(SIDE):
            if n == 0 or self.a_of[n] != self.a_of[n - 1]:
                self.input(self.a_of[n]).start()
            self.cotangent(n).start()

    def step(self):
        j = pl.program_id(0)
        for n in range(SIDE):
            @at_step(self.base + PAIR * n)
            def _():
                if n == 0 or self.a_of[n] != self.a_of[n - 1]:
                    self.input(self.a_of[n]).wait()
                self.cotangent(n).wait()

        @pl.when(j >= self.base)
        def _():
            n = lax.div(j - self.base, PAIR)
            cols = pl.ds(pl.multiple_of(lax.rem(j - self.base, PAIR) * THIN, LANES), THIN)
            a = self.a_rows[0 if len(self.a) == 1 else lax.div(n, O)]
            self.out[0] = dot_tn(a, self.b_rows[n, :, cols])

    def finish(self):
        for i in range(len(self.a)):
            self.input(i).finish()
        for n in range(SIDE):
            self.cotangent(n).finish()


def grads_block(base):
    def index(j):
        n = jnp.maximum(j - base, 0)
        return n // PAIR, 0, n % PAIR

    return pl.BlockSpec((1, D, THIN), index)


LAST_SEQ = SEQS[0] - 1
ATTN_PLAN = {"start": ((0, 0, 1),), SIDE: ((LAST_SEQ, 1, 4),), "end": ((LAST_SEQ + PAIR * SIDE, 4, None),)}


def attn_back_kernel(qkv, d_o, h2, d_pre, part, d_qkv, db, d_up, total, acc, *scratch):
    n = len(WideGrads.scratch(1))
    grads = WideGrads((h2,), (0,) * SIDE, [lambda c, i=i: d_pre.at[c, i] for i in range(SIDE)], d_up, SEQS[0], *scratch[:n])
    hosted = Background(Scatter(DOWN, part, total, *scratch[n:]).steps(), ATTN_PLAN)
    at_step(0)(enter)
    hosted.visit("start")
    at_step(0)(grads.begin)

    @pl.when(pl.program_id(0) < SEQS[0])
    def _():
        attention_back(qkv, d_o, d_qkv, db, acc, hosted.visit)

    grads.step()
    hosted.visit("end")
    at_step(LAST_SEQ + PAIR * SIDE)(grads.finish)


def attn_back_call(qkv, d_o, h2, d_pre, part, collective_id):
    upto = lambda j: jnp.minimum(j, LAST_SEQ)
    return pl.pallas_call(
        attn_back_kernel, grid=(SEQS[0] + PAIR * SIDE,),
        out_shape=(sds(BF16, 2, O, 2, TOK, HALF), sds(F32, O, D), sds(F32, SIDE, D, HALF), Scatter.total(DOWN)),
        in_specs=[along(1, O, 1, SEQ, D, index=upto), along(0, 1, SEQ, D, index=upto), ANY, ANY, ANY],
        out_specs=(along(2, 2, O, 1, TOK, HALF, index=upto), whole(O, D), grads_block(SEQS[0]), ANY),
        scratch_shapes=[pltpu.VMEM((O, SEQ, D), F32)] + WideGrads.scratch(1) + Scatter.scratch(DOWN),
        compiler_params=comm_params(collective_id), name="attn_back",
    )(qkv, d_o, h2, d_pre, part)


IN_STEPS = PAIR * O
IN_PLAN = {"start": ((0, 0, 1), (IN_STEPS, 1, 4)), "end": ((IN_STEPS + PAIR * SIDE - 1, 4, None),)}


def in_back_kernel(d_half, w, x, g_res, vec, h1, o, d_qkv, d_att, part, dx, sums, d_attn, total, acc, *scratch):
    n = len(WideGrads.scratch(2))
    b = [lambda c, i=i: d_qkv.at[c, i] for i in range(O)] + [lambda c: d_att.at[c]]
    grads = WideGrads((h1, o), (0,) * O + (1,), b, d_attn, IN_STEPS, *scratch[:n])
    hosted = Background(Scatter(WIDE, part, total, *scratch[n:]).steps(), IN_PLAN)
    at_step(0)(enter)
    hosted.visit("start")
    at_step(0)(grads.begin)

    @pl.when(pl.program_id(0) < IN_STEPS)
    def _():
        for s in SEQ_PAIR:
            accumulate(acc.at[s], dot_nt(d_half[0, 0, s, :SEQ], w[0]))

    @at_step(IN_STEPS - 1)
    def _():
        rows = jnp.zeros((BO, D), F32)
        for s in SEQ_PAIR:
            xhat, rstd = norm_stats(x[s].astype(F32))
            dh = acc[s]
            rows = rows + jnp.concatenate([col_sum(dh * xhat), col_sum(dh)], axis=0)
            dx[s] = (g_res[s] + norm_back(xhat, rstd, dh * row(vec, G1))).astype(BF16)
        sums[...] = rows

    grads.step()
    hosted.visit("end")
    at_step(IN_STEPS + PAIR * SIDE - 1)(grads.finish)


def in_back_call(d_qkv, w_attn, x, g_res, vec, h1, o, d_att, part, collective_id):
    def at(j):
        n = jnp.minimum(j, IN_STEPS - 1)
        return n // PAIR, n % PAIR

    once = lambda *shape: pl.BlockSpec(shape, lambda j: (0,) * len(shape), pipeline_mode=pl.Buffered(1))
    return pl.pallas_call(
        in_back_kernel, grid=(IN_STEPS + PAIR * SIDE,),
        out_shape=(sds(BF16, *SEQS), sds(F32, BO, D), sds(F32, SIDE, D, HALF), Scatter.total(WIDE)),
        in_specs=[pl.BlockSpec((1, 1, 2, TOK, HALF), lambda j: (at(j)[1], at(j)[0], 0, 0, 0)),
                  pl.BlockSpec((1, D, HALF), lambda j: (at(j)[0], 0, at(j)[1])), once(*SEQS), once(*SEQS), whole(8, D),
                  ANY, ANY, ANY, ANY, ANY],
        out_specs=(whole(*SEQS), whole(BO, D), grads_block(IN_STEPS), ANY),
        scratch_shapes=[pltpu.VMEM(SEQS, F32)] + WideGrads.scratch(2) + Scatter.scratch(WIDE),
        compiler_params=comm_params(collective_id), name="in_back",
    )(d_qkv, w_attn, x, g_res, vec, h1, o, d_qkv, d_att, part)


DOWN_TILES = FF // HALF


def down_kernel(act, d_mlp, out, a_rows, b_rows, *sems):
    c = Torus().at["c"]
    both = Exchange(d_mlp.at[c], d_mlp.at[1 - c], b_rows, sems[3:], ())

    def tile(j):
        mine = act.at[:, :, pl.ds(HALF * j, HALF)]
        return Exchange(mine, mine, a_rows.at[j], sems[:3], (j,))

    @at_step(0)
    def _():
        enter()
        both.start()
        for j in range(DOWN_TILES):
            tile(j).start()
        both.wait()

    for j in range(DOWN_TILES):
        at_step(j)(tile(j).wait)
    out[...] = dot_tn(a_rows[pl.program_id(0)], b_rows[...])

    @at_step(DOWN_TILES - 1)
    def _():
        both.finish()
        for j in range(DOWN_TILES):
            tile(j).finish()


def down_grads(act, d_mlp, collective_id):
    return pl.pallas_call(
        down_kernel, grid=(DOWN_TILES,), out_shape=sds(F32, FF, HALF), in_specs=[ANY, ANY],
        out_specs=along(0, HALF, HALF),
        scratch_shapes=[pltpu.VMEM((DOWN_TILES, ROWS, HALF), BF16), pltpu.VMEM((ROWS, HALF), BF16)] +
        Exchange.semaphores(DOWN_TILES) + Exchange.semaphores(),
        compiler_params=comm_params(collective_id), name="dw_down",
    )(act, d_mlp)


OWN = 44
CHIP = OWN * PAIR
BQ, BU, VEC = 3 * D // 32, 3 * D // 32 + FF // 32, 3 * D // 32 + FF // 32 + 8 * OWN
DEVICES = 32


def pair_swap(a):
    return lax.ppermute(a, "fsdp", [(i, i ^ 1) for i in range(DEVICES)])


def by_core(first, a, b):
    return jnp.where(first, a, b), jnp.where(first, b, a)


def my_pieces(shards, first):
    w_qkv, b_qkv, w_out, w_up, b_up, w_down, vec_params = shards
    x = lax.axis_index("rep")
    small = jnp.concatenate([b_qkv, b_up, vec_params.reshape(-1)])
    small = jnp.pad(small, (0, OWN * LANES - VEC)).reshape(OWN, LANES)
    attn = lax.dynamic_slice_in_dim(jnp.concatenate([w_qkv, w_out], axis=1), x * D, D, 1)
    attn = jnp.concatenate([attn, small], axis=1)
    up = lax.dynamic_slice_in_dim(w_up, x * QCOLS, QCOLS, 1)
    wide = jnp.stack([attn, up]).astype(BF16)
    mine, theirs = by_core(first, wide[..., :HALF], wide[..., HALF:])
    theirs = pair_swap(theirs)
    piece = jnp.concatenate(by_core(first, mine, theirs), axis=1)
    down = lax.dynamic_slice_in_dim(w_down, x * 48, 48, 0).astype(BF16).reshape(3, 16, D)
    return piece[0], piece[1], down


def small_params(w_attn):
    small = w_attn[0, :, D:].astype(F32).reshape(DEVICES, OWN * LANES)
    vec = small[:, BU:VEC].reshape(DEVICES, 8, OWN).transpose(1, 0, 2).reshape(8, D)
    return small[:, :BQ].reshape(O, 1, D), small[:, BQ:BU].reshape(FF), vec


def small_grads(db_qkv, db_up, sums, core):
    vec = sums.reshape(8, DEVICES, OWN).transpose(1, 0, 2).reshape(DEVICES, VEC - BU)
    small = jnp.concatenate([db_qkv.reshape(DEVICES, BQ), db_up.reshape(DEVICES, BU - BQ), vec], axis=1)
    small = (small + pair_swap(small)) * core.astype(F32)
    return jnp.pad(small, ((0, 0), (0, OWN * LANES - VEC))).reshape(D, LANES)


def final_rows(total, first):
    keep, give = by_core(first, total[:, :, :OWN], total[:, :, OWN:])
    pair = jnp.stack(by_core(first, keep, pair_swap(give)), axis=1)
    return pair.transpose(3, 0, 1, 2, 4).reshape(OWN, SIDE, QCOLS)


def final_down(down, first):
    keep, give = by_core(first, down[:FF // DEVICES], down[FF // DEVICES:])
    left, right = by_core(first, keep, pair_swap(give))
    return jnp.concatenate([left, right[:, 2 * HALF - D:]], axis=1)


def device_step(x, gz, *shards):
    core = lax.rem(lax.axis_index("fsdp"), PAIR)
    first = core == 0
    attn, up, down = my_pieces(shards, first)
    w_attn = torus_gather(WIDE, attn, 0).reshape(SIDE, D, QCOLS)
    b_qkv, b_up, vec = small_params(w_attn)
    qkv, h1, o, att, h2, w_up, w_down = front_call(x, w_attn, b_qkv, vec, up, down, 1)
    act, d_pre, db_up, mlp, d_h2, d_mlp = mlp_call(h2, gz, w_up.reshape(SIDE, D, QCOLS), b_up, w_down.reshape(FF, D), vec)
    z, g_res, d_att, d_o, sums = mid_call(mlp, d_h2, att, x, gz, vec, w_attn)
    part = down_grads(act, d_mlp, 2).reshape(4, 4, 4, 3, 32, HALF)
    d_qkv, db_qkv, part, down = attn_back_call(qkv, d_o, h2, d_pre, part, 3)
    part = part.reshape(4, 4, 4, CHIP, HALF)
    dx, in_sums, part, up = in_back_call(d_qkv, w_attn, x, g_res, vec, h1, o, d_att, part, 4)
    small = small_grads(db_qkv, db_up, jnp.concatenate([in_sums, sums[BO:]], axis=0), core)
    part = part.at[0, :, HALF - LANES:].add(small).reshape(4, 4, 4, CHIP, HALF)
    attn = torus_scatter(WIDE, part, 5)
    g_up = final_rows(up, first).reshape(OWN, FF)
    attn = final_rows(attn, first)
    small = attn[:, 0, D:].reshape(OWN * LANES)
    return (z, dx, attn[:, :O, :D].reshape(OWN, O * D), small[:BQ], attn[:, O, :D], g_up, small[BQ:BU],
            final_down(down.reshape(FF // 16, HALF), first), small[BU:VEC].reshape(8, OWN))


def solution(mesh):
    batch = P(("rep", "fsdp"), None, None)
    rows, flat, cols = P("fsdp", None), P("fsdp"), P(None, "fsdp")
    shards = (rows, flat, rows, rows, flat, rows, cols)
    return jax.shard_map(device_step, mesh=mesh, in_specs=(batch, batch) + shards,
                         out_specs=(batch, batch) + shards, check_vma=False)
```

```python
import functools
import math

import jax
import jax.numpy as jnp
from jax import lax
from jax.experimental import pallas as pl
from jax.experimental.pallas import tpu as pltpu
from jax.sharding import PartitionSpec as P

HEADS = 16
LN_EPS = 1e-5
D = 1408
FF = 6144
SEQ = 257
HEAD = D // HEADS
SCALE = HEAD ** -0.5
QCOLS = 1536
HALF = 768
OWN = 44
CHIP = 2 * OWN
LANES = 128
F32 = jnp.float32
BF16 = jnp.bfloat16
VMEM_LIMIT = 66 * 1000 * 1000
G1, C1, BO, S1, G2, C2, B2, S2 = range(8)
Q, K, V, O = range(4)
SEQS = (2, SEQ, D)
SEQ_PAIR = range(SEQS[0])
TAIL = 8
BODY = SEQ - 1
TOK = BODY + TAIL
TOKS = (2, TOK, D)
ROWS = 4 * TOK


def sds(dtype, *shape):
    return jax.ShapeDtypeStruct(shape, dtype)


MESH_ID = pl.DeviceIdType.MESH
SIDE = 4
PAIR = 2
C = 3
COLOURS = range(C)
COLOUR_DIMS = ("xyz", "yzx", "zxy")
FIRST, SECOND, THIRD, LAST = range(4)
WAYS = range(PAIR)
NEAR, FAR, ADDED = 0, 2, 4
WIDE, DOWN = "wide", "down"
ANY = pl.BlockSpec(memory_space=pl.ANY)
ALL = slice(None)


def duo(m):
    return pl.ds(PAIR * m, PAIR)


def toward(m):
    return 1 - PAIR * (m % PAIR)


class Torus:
    def __init__(self):
        f = lax.axis_index("fsdp")
        self.at = {"x": lax.axis_index("rep"), "z": lax.div(f, SIDE * PAIR), "y": lax.rem(lax.div(f, PAIR), SIDE),
                   "c": lax.rem(f, PAIR)}

    def shift(self, dim, by):
        return lax.rem(self.at[dim] + (SIDE + by), SIDE)

    def device(self, **moved):
        p = {**self.at, **moved}
        return (p["x"], (p["z"] * SIDE + p["y"]) * PAIR + p["c"])

    def neighbour(self, dim, by):
        return self.device(**{dim: self.shift(dim, by)})

    def partner(self):
        return self.device(c=1 - self.at["c"])


def enter():
    me = Torus()
    barrier = pltpu.get_barrier_semaphore()
    others = [me.neighbour(d, toward(m)) for d in COLOUR_DIMS[0] for m in WAYS] + [me.partner()]
    for other in others:
        pl.semaphore_signal(barrier, device_id=other, device_id_type=MESH_ID)
    pl.semaphore_wait(barrier, len(others))


def remote(src, dst, sems, slot, device):
    return pltpu.make_async_remote_copy(src_ref=src, dst_ref=dst, send_sem=sems[0].at[slot], recv_sem=sems[1].at[slot],
                                        device_id=device, device_id_type=MESH_ID)


class Gather:
    def __init__(self, kind, src, dst, hop_send, hop_recv, push_send, push_recv, local):
        self.kind, self.src, self.dst, self.local = kind, src, dst, local
        self.hops, self.pushes = (hop_send, hop_recv), (push_send, push_recv)
        self.cols, self.cut = (256, 128) if kind == WIDE else (D, HALF)

    @staticmethod
    def semaphores():
        dma = pltpu.SemaphoreType.DMA
        return [dma((C, C, ADDED))] * PAIR + [dma((C, ADDED + 1))] * PAIR + [dma((C,))]

    @staticmethod
    def shape(kind):
        return (SIDE,) * 3 + (CHIP, QCOLS) if kind == WIDE else (SIDE, SIDE, PAIR, SIDE, C, 16, D)

    def source(self, k):
        return self.src.at[:, pl.ds(self.cols * k, self.cols)] if self.kind == WIDE else self.src.at[k]

    def piece(self, me, k, s, v, half=None):
        dims = COLOUR_DIMS[k]
        at = {**me.at, **{d: ALL for d in dims[:s]}, dims[s]: v}
        off, width = 0, self.cols
        if half is not None and s == FIRST:
            off, width = self.cut * half, (self.cut, self.cols - self.cut)[half]
        elif half is not None:
            at[dims[0]] = duo(half)
        if self.kind == WIDE:
            cols = pl.ds(pl.multiple_of(at["c"] * HALF + self.cols * k + off, 128), width)
            return self.dst.at[at["x"], at["z"], at["y"], :, cols]
        return self.dst.at[at["z"], at["y"], at["c"], at["x"], k, :, pl.ds(off, width)]

    def hop(self, k, s, m):
        me = Torus()
        dim = COLOUR_DIMS[k][s]
        by = toward(m)
        if m < FAR:
            ref = self.piece(me, k, s, me.at[dim])
        else:
            ref = self.piece(me, k, s, me.shift(dim, -by), m - FAR)
        src = self.source(k) if s == FIRST and m < FAR else ref
        return remote(src, ref, self.hops, (k, s, m), me.neighbour(dim, by))

    def push(self, k, n):
        me = Torus()
        dim = COLOUR_DIMS[k][THIRD]
        if n < FAR:
            ref = self.piece(me, k, THIRD, me.shift(dim, -toward(n)))
        elif n < ADDED:
            ref = self.piece(me, k, THIRD, me.shift(dim, FAR), n - FAR)
        else:
            ref = self.piece(me, k, THIRD, me.at[dim])
        return remote(ref, ref, self.pushes, (k, n), me.partner())

    def own(self, k):
        me = Torus()
        return pltpu.make_async_copy(self.source(k), self.piece(me, k, FIRST, me.at[COLOUR_DIMS[k][FIRST]]), self.local.at[k])

    def launch(self, s):
        for k in COLOURS:
            for m in WAYS:
                self.hop(k, s, m).start()
            if s == THIRD:
                self.push(k, ADDED).start()

    def relay(self, k, s):
        for m in WAYS:
            self.hop(k, s, m).wait_recv()
            self.hop(k, s, FAR + m).start()
            if s == THIRD:
                self.push(k, m).start()

    def settle(self, s):
        for k in COLOURS:
            for m in WAYS:
                self.hop(k, s, FAR + m).wait_recv()
                if s == THIRD:
                    self.push(k, FAR + m).start()
            if s == FIRST:
                self.own(k).wait()
        if s < THIRD:
            self.launch(s + 1)

    def begin(self):
        for k in COLOURS:
            self.own(k).start()
        self.launch(FIRST)

    def finish(self):
        for k in COLOURS:
            for s in COLOURS:
                for m in range(ADDED):
                    self.hop(k, s, m).wait_send()
            for n in range(ADDED + 1):
                self.push(k, n).wait()

    def steps(self):
        out = [self.begin]
        for s in COLOURS:
            out += [functools.partial(self.relay, k, s) for k in COLOURS] + [functools.partial(self.settle, s)]
        return out + [self.finish]


def add_into(total, *others):
    lead = total.shape[:-2]

    def body(i, carry):
        idx = []
        for n in reversed(lead):
            idx.insert(0, lax.rem(i, n))
            i = lax.div(i, n)
        value = total[tuple(idx)]
        for other in others:
            value = value + other[tuple(idx)]
        total[tuple(idx)] = value
        return carry

    lax.fori_loop(0, math.prod(lead), body, 0)


class Ring:
    def __init__(self, s, terms, passed, relay, landing, send, recv, rows=None):
        self.s, self.terms, self.passed, self.relay, self.landing = s, terms, passed, relay, landing
        self.sems, self.rows = (send, recv), rows

    def zone(self, k, way, half):
        return self.landing.at[k, way, self.rows[half] if self.rows else duo(half)]

    def carried(self, ref, k, way):
        return ref.at[k, way, pl.ds(0, self.rows[way].size)] if self.rows else ref.at[k, way]

    def hop(self, k, m):
        me = Torus()
        dim = COLOUR_DIMS[k][self.s]
        way, by = m % PAIR, toward(m)
        if m < FAR:
            src, dst = self.terms(k, me.shift(dim, FAR), way), self.carried(self.relay, k, way)
        elif m < ADDED:
            src, dst = self.terms(k, me.shift(dim, by), 1 - way), self.zone(k, way, 1 - way)
        else:
            src, dst = self.carried(self.passed, k, way), self.zone(k, way, way)
        return remote(src, dst, self.sems, (k, m), me.neighbour(dim, by))

    def start(self, k, base):
        for m in WAYS:
            self.hop(k, base + m).start()

    def arrived(self, k, base):
        for m in WAYS:
            self.hop(k, base + m).wait_recv()

    def finish(self):
        for k in COLOURS:
            for m in range(ADDED + PAIR):
                self.hop(k, m).wait_send()

    @staticmethod
    def semaphores():
        return [pltpu.SemaphoreType.DMA((C, ADDED + PAIR))] * PAIR


UNITS = {WIDE: (CHIP, LANES), DOWN: (FF // 192, HALF // PAIR)}


def unit_array(kind, *lead):
    return lead + UNITS[kind]


class First:
    def __init__(self, kind, half, part, acc, own, passed, relay, landing, send, recv, load, store):
        self.kind, self.half, self.part, self.acc, self.own, self.passed = kind, half, part, acc, own, passed
        self.relay_in, self.landing, self.load_sem, self.store_sem = relay, landing, load, store
        self.ring = Ring(FIRST, self.terms, passed, relay, landing, send, recv)

    @staticmethod
    def scratch(kind):
        vm = lambda *lead: pltpu.VMEM(unit_array(kind, *lead), F32)
        dma = pltpu.SemaphoreType.DMA
        relays = [vm(C, PAIR, PAIR, SIDE)] * PAIR
        return [vm(C, SIDE, SIDE), *relays, vm(C, PAIR, SIDE, SIDE), *Ring.semaphores(), dma((C, C)), dma((C,))]

    @staticmethod
    def sums(kind):
        return sds(F32, *unit_array(kind, C, SIDE, SIDE))

    def terms(self, k, v, half=None):
        order = ORDERS[self.kind]
        at = {d: ALL for d in order}
        at[COLOUR_DIMS[k][FIRST]] = v
        if half is not None:
            at[rest_dims(self.kind, k)[0]] = duo(half)
        lead = tuple(at[d] for d in order)
        width = UNITS[self.kind][1]
        if self.kind == WIDE:
            return self.part.at[lead + (ALL, pl.ds(width * (PAIR * k + self.half), width))]
        return self.part.at[lead + (k, ALL, pl.ds(width * self.half, width))]

    def load(self, k, m):
        me = Torus()
        dim = COLOUR_DIMS[k][FIRST]
        if m in WAYS:
            src, dst = self.terms(k, me.shift(dim, toward(m)), m), self.passed.at[k, m]
        else:
            src, dst = self.terms(k, me.at[dim]), self.own.at[k]
        return pltpu.make_async_copy(src, dst, self.load_sem.at[k, m])

    def store(self, k):
        return pltpu.make_async_copy(self.own.at[k], self.acc.at[k], self.store_sem.at[k])

    def near(self):
        for k in COLOURS:
            self.ring.start(k, NEAR)

    def far(self):
        for k in COLOURS:
            self.ring.start(k, FAR)
        for m in COLOURS:
            for k in COLOURS:
                self.load(k, m).start()

    def relay(self):
        for k in COLOURS:
            self.ring.arrived(k, NEAR)
            for m in WAYS:
                self.load(k, m).wait()
                add_into(self.passed.at[k, m], self.relay_in.at[k, m])
            self.ring.start(k, ADDED)

    def settle(self, then=None):
        for k in COLOURS:
            self.load(k, FAR).wait()
            for base in (FAR, ADDED):
                self.ring.arrived(k, base)
            add_into(self.own.at[k], *(self.landing.at[k, m] for m in WAYS))
            if then is None:
                self.store(k).start()
            else:
                then(k)

    def finish(self):
        self.ring.finish()
        if self.acc is not None:
            for k in COLOURS:
                self.store(k).wait()


ORDERS = {WIDE: "xzy", DOWN: "zyx"}


def rest_dims(kind, k):
    return [d for d in ORDERS[kind] if d != COLOUR_DIMS[k][FIRST]]


class Rest:
    def __init__(self, kind, acc, result, own, relay2, in2, relay3, in3, *sems):
        self.kind, self.acc, self.own, self.result = kind, acc, own, result
        self.in2, self.in3, self.relay2, self.relay3, self.load_sem, self.store_sem = in2, in3, relay2, relay3, *sems[-2:]
        rows, cut = UNITS[kind][0], relay3.shape[2]
        cuts = pl.ds(0, cut), pl.ds(cut, rows - cut)
        self.second = Ring(SECOND, functools.partial(self.terms, acc), relay2, relay2, in2, *sems[:PAIR])
        third = lambda k, v, half=None: in2.at[(k, 0, v) + (() if half is None else (cuts[half],))]
        self.third = Ring(THIRD, third, relay3, relay3, in3, *sems[PAIR:2 * PAIR], rows=cuts)

    @staticmethod
    def scratch(kind):
        vm = lambda *lead: pltpu.VMEM(unit_array(kind, *lead), F32)
        rows, cols = UNITS[kind]
        dma = pltpu.SemaphoreType.DMA
        cut = (rows // TAIL + 1) // PAIR * TAIL
        return [vm(C, SIDE, SIDE), vm(C, PAIR, PAIR), vm(C, PAIR, SIDE), pltpu.VMEM((C, PAIR, cut, cols), F32), vm(C, PAIR),
                *Ring.semaphores(), *Ring.semaphores(), dma((C,)), dma((C,))]

    @staticmethod
    def sums(kind):
        return sds(F32, *unit_array(kind, C))

    def terms(self, ref, k, v, half=None):
        other = ALL if half is None else duo(half)
        return ref.at[(k, v, other) if rest_dims(self.kind, k)[0] == COLOUR_DIMS[k][SECOND] else (k, other, v)]

    def load(self, k):
        return pltpu.make_async_copy(self.acc.at[k], self.own.at[k], self.load_sem.at[k])

    def store(self, k):
        return pltpu.make_async_copy(self.in3.at[k, 0], self.result.at[k], self.store_sem.at[k])

    def send(self, k):
        for base in (NEAR, FAR):
            self.second.start(k, base)

    def begin(self):
        for k in COLOURS:
            self.send(k)
        for k in COLOURS:
            self.load(k).start()

    def loaded(self):
        for k in COLOURS:
            self.load(k).wait()

    def relay(self):
        me = Torus()
        for k in COLOURS:
            self.second.arrived(k, NEAR)
            for m in WAYS:
                add_into(self.relay2.at[k, m], self.terms(self.own, k, me.shift(COLOUR_DIMS[k][SECOND], toward(m)), m))
            self.second.start(k, ADDED)

    def settle(self):
        me = Torus()
        for k in COLOURS:
            for base in (FAR, ADDED):
                self.second.arrived(k, base)
            add_into(self.in2.at[k, 0], self.in2.at[k, 1], self.terms(self.own, k, me.at[COLOUR_DIMS[k][SECOND]]))
            for base in (NEAR, FAR):
                self.third.start(k, base)

    def relay_third(self):
        me = Torus()
        for k in COLOURS:
            self.third.arrived(k, NEAR)
            for m in WAYS:
                mine = self.third.carried(self.relay3, k, m)
                mine[...] += self.third.terms(k, me.shift(COLOUR_DIMS[k][THIRD], toward(m)), m)[...]
            self.third.start(k, ADDED)

    def settle_third(self):
        me = Torus()
        for k in COLOURS:
            for base in (FAR, ADDED):
                self.third.arrived(k, base)
            self.in3[k, 0] += self.in3[k, 1] + self.third.terms(k, me.at[COLOUR_DIMS[k][THIRD]])[...]
            if self.result is not None:
                self.store(k).start()

    def finish(self):
        self.second.finish()
        self.third.finish()
        if self.result is not None:
            for k in COLOURS:
                self.store(k).wait()


class Spread:
    def __init__(self, kind, result, total, send, recv, local):
        rows = UNITS[kind][0]
        cut = rows // TAIL // PAIR * TAIL
        self.result, self.total, self.sems, self.local = result, total, (send, recv), local
        self.cuts = pl.ds(0, cut), pl.ds(cut, rows - cut)

    @staticmethod
    def scratch():
        return [pltpu.SemaphoreType.DMA((C, ADDED))] * PAIR + [pltpu.SemaphoreType.DMA((C,))]

    @staticmethod
    def sums(kind):
        return sds(F32, *unit_array(kind, SIDE, C))

    def hop(self, k, m):
        me = Torus()
        by = toward(m)
        if m < FAR:
            src, dst = self.result.at[k], self.total.at[me.at["x"], k]
        else:
            dst = src = self.total.at[me.shift("x", -by), k, self.cuts[m - FAR]]
        return remote(src, dst, self.sems, (k, m), me.neighbour("x", by))

    def own(self, k):
        return pltpu.make_async_copy(self.result.at[k], self.total.at[Torus().at["x"], k], self.local.at[k])

    def begin(self):
        for k in COLOURS:
            self.own(k).start()
            for m in WAYS:
                self.hop(k, m).start()

    def forward(self):
        for k in COLOURS:
            for m in WAYS:
                self.hop(k, m).wait_recv()
                self.hop(k, FAR + m).start()

    def finish(self):
        for k in COLOURS:
            for m in WAYS:
                self.hop(k, FAR + m).wait_recv()
            self.own(k).wait()
            for m in range(ADDED):
                self.hop(k, m).wait_send()


def comm_params(collective_id):
    return pltpu.CompilerParams(collective_id=collective_id, has_side_effects=True, vmem_limit_bytes=VMEM_LIMIT)


def torus_gather(kind, piece, collective_id):
    def kernel(*refs):
        enter()
        for step in Gather(kind, *refs).steps():
            step()

    return pl.pallas_call(
        kernel, out_shape=sds(BF16, *Gather.shape(kind)), in_specs=[ANY], out_specs=ANY,
        scratch_shapes=Gather.semaphores(), compiler_params=comm_params(collective_id), name="gather_" + kind)(piece)


def last_scatter_kernel(part, acc_up, result_up, *refs):
    outs, refs = refs[:SIDE], list(refs[SIDE:])
    take = lambda like: [refs.pop(0) for _ in like]
    a, b = (First(WIDE, h, part, None, *take(First.scratch(WIDE))) for h in WAYS)
    rest_a, rest_b = (Rest(WIDE, f.own, None, f.own, *take(Rest.scratch(WIDE)[1:])) for f in (a, b))
    late = Rest(WIDE, acc_up, None, *take(Rest.scratch(WIDE)))
    results = [rest.in3.at[:, 0] for rest in (rest_a, rest_b, late)]
    spread_a, spread_b, spread_late, early = (
        Spread(WIDE, *pair, *take(Spread.scratch())) for pair in zip([*results, result_up], outs))
    enter()
    for step in (late.begin, early.begin, a.near, late.loaded, late.relay, a.far, early.forward, late.settle, a.relay, b.near,
                 late.relay_third, late.settle_third, b.far, late.finish, spread_late.begin,
                 functools.partial(a.settle, rest_a.send), b.relay, rest_a.relay, spread_late.forward, rest_a.settle,
                 rest_a.relay_third, functools.partial(b.settle, rest_b.send), rest_a.settle_third, rest_b.relay,
                 rest_a.finish, spread_a.begin, rest_b.settle, spread_a.forward, rest_b.relay_third, rest_b.settle_third,
                 rest_b.finish, spread_b.begin, spread_b.forward, early.finish, spread_late.finish, spread_a.finish,
                 spread_b.finish, a.finish, b.finish):
        step()


def last_scatter(part, acc_up, result_up, collective_id):
    return pl.pallas_call(
        last_scatter_kernel, out_shape=(Spread.sums(WIDE),) * SIDE, in_specs=[ANY] * O, out_specs=(ANY,) * SIDE,
        scratch_shapes=First.scratch(WIDE) * PAIR + Rest.scratch(WIDE)[1:] * PAIR + Rest.scratch(WIDE) +
        Spread.scratch() * SIDE,
        compiler_params=comm_params(collective_id), name="last_scatter")(part, acc_up, result_up)


class Background:
    def __init__(self, steps, plan):
        self.steps, self.plan = steps, plan

    def visit(self, place):
        for j, first, end in self.plan.get(place, ()):
            @at_step(j)
            def _():
                for step in self.steps[first:end]:
                    step()


class Pipeline:
    def __init__(self, places, first, rest=None, spread=None):
        rest_steps = (rest.loaded, rest.relay) if rest else ()
        groups = [[*((rest.begin,) if rest else ()), *((spread.begin,) if spread else ()), first.near],
                  [*rest_steps, first.far, *((spread.forward,) if spread else ())],
                  [*((rest.settle,) if rest else ()), first.relay],
                  [rest.relay_third] if rest else [],
                  [first.settle, *((rest.settle_third,) if rest else ()), first.finish, *((rest.finish,) if rest else ()),
                   *((spread.finish,) if spread else ())]]
        self.groups = list(zip([("start", 0), *places], groups))

    def visit(self, place):
        for (where, j), group in self.groups:
            if where == place:
                @at_step(j)
                def _():
                    for step in group:
                        step()


class Push:
    def __init__(self, src, tail, rows, sems, slot):
        body = BODY * len(SEQ_PAIR)
        tails = TAIL * len(SEQ_PAIR)
        self.copies = [
            remote(src.at[pl.ds(start, size)], rows.at[pl.ds(to, size)], sems, (slot, i), Torus().partner())
            for i, (start, to, size) in enumerate(((0, body, body), (tail, PAIR * body + tails, tails)))]

    @staticmethod
    def semaphores(n):
        return [pltpu.SemaphoreType.DMA((n, PAIR))] * PAIR

    def start(self):
        for copy in self.copies:
            copy.start()

    def wait(self):
        for copy in self.copies:
            copy.wait_recv()

    def finish(self):
        for copy in self.copies:
            copy.wait_send()


class Exchange:
    def __init__(self, mine, theirs, rows, sems, slot):
        self.moves = []
        for s in SEQ_PAIR:
            for i, (start, size) in enumerate(((0, BODY), (BODY, TAIL))):
                place = lambda n: rows.at[pl.ds(start * len(SEQ_PAIR) * PAIR + size * n, size)]
                n = len(SEQ_PAIR) + s
                at = slot + (PAIR * s + i,)
                local = pltpu.make_async_copy(mine.at[s, pl.ds(start, size)], place(s), sems[2].at[at])
                far = remote(theirs.at[s, pl.ds(start, size)], place(n), sems, at, Torus().partner())
                self.moves.append((local, far))

    @staticmethod
    def semaphores(*lead):
        return [pltpu.SemaphoreType.DMA(lead + (2 * PAIR,))] * 3

    def start(self):
        for local, far in self.moves:
            far.start()
            local.start()

    def wait(self):
        for local, far in self.moves:
            local.wait()
            far.wait_recv()

    def finish(self):
        for _, far in self.moves:
            far.wait_send()


NT = (((1,), (1,)), ((), ()))
TN = (((0,), (0,)), ((), ()))


def dot(a, b):
    return jnp.dot(a, b, preferred_element_type=F32)


def dot_nt(a, b):
    return lax.dot_general(a, b, NT, preferred_element_type=F32)


def dot_tn(a, b):
    return lax.dot_general(a, b, TN, preferred_element_type=F32)


def zeros_but(n, axis, value):
    return tuple(value if i == axis else 0 for i in range(n))


def whole(*shape):
    return pl.BlockSpec(shape, lambda *_: (0,) * len(shape))


def along(axis, *block, index=lambda j: j):
    return pl.BlockSpec(block, lambda j: zeros_but(len(block), axis, index(j)))


def row(vec, i):
    return vec[i:i + 1]


def row_mean(t):
    return jnp.mean(t, axis=-1, keepdims=True)


def norm_stats(t):
    centered = t - row_mean(t)
    rstd = lax.rsqrt(row_mean(centered * centered) + LN_EPS)
    return centered * rstd, rstd


def norm_back(xhat, rstd, g):
    return rstd * (g - row_mean(g) - xhat * row_mean(g * xhat))


def col_sum(t):
    return jnp.sum(t, axis=0, keepdims=True)


def at_step(j):
    return pl.when(pl.program_id(0) == j)


def accumulate(ref, value):
    @at_step(0)
    def _():
        ref[...] = value

    @pl.when(pl.program_id(0) > 0)
    def _():
        ref[...] += value


def pad(t):
    return jnp.concatenate([t.astype(F32), jnp.zeros((TOK - SEQ, t.shape[1]), F32)], axis=0).astype(BF16)


def window(h):
    start = h * HEAD // LANES * LANES
    stop = min(D, -(-(h + 1) * HEAD // LANES) * LANES)
    lane = lax.broadcasted_iota(jnp.int32, (1, stop - start), 1) + (start - h * HEAD)
    return slice(start, stop), (lane >= 0) & (lane < HEAD)


def only(mask, t):
    return jnp.where(mask, t, jnp.zeros_like(t))


def softmax(scores):
    e = jnp.exp(scores - jnp.max(scores, axis=-1, keepdims=True))
    return e * (1.0 / jnp.sum(e, axis=-1, keepdims=True))


def attention(s, rows, x, w_out, vec, o, att, h2, acc, visit):
    acc[...] = jnp.zeros_like(acc)
    for h in range(HEADS):
        lanes, mask = window(h)
        k = only(mask, rows[K, s, :, lanes])
        v = only(mask, rows[V, s, :, lanes])
        probs = softmax(dot_nt(rows[Q, s, :, lanes], k) * SCALE).astype(BF16)
        acc[:, lanes] += dot(probs, v)
        visit(h)
    heads = acc[...]
    o[0] = pad(heads)
    a = dot(heads.astype(BF16), w_out[0]) + row(vec, BO)
    att[0] = a
    xhat, _ = norm_stats(x[s].astype(F32) + row(vec, S1) * a)
    h2[0] = pad(xhat * row(vec, G2) + row(vec, C2))


FRONT_PLAN = {"qkv": ((0, 0, 1), (1, 1, 5), (2, 5, 8)), 2: ((O, 8, 9),), "end": ((O + 1, 9, None),)}


def front_kernel(x, w, b, vec, up_src, qkv, h1, o, att, h2, up, rows, acc, *sems):
    hosted = Background(Gather(WIDE, up_src, up, *sems).steps(), FRONT_PLAN)
    j = pl.program_id(0)
    at_step(0)(enter)
    hosted.visit("qkv")

    @at_step(0)
    def _():
        for s in SEQ_PAIR:
            xhat, _ = norm_stats(x[s].astype(F32))
            h1[s] = pad(xhat * row(vec, G1) + row(vec, C1))

    @pl.when(j < O)
    def _():
        for s in SEQ_PAIR:
            t = (dot(h1[s, :SEQ], w[0]) + b[0]).astype(BF16)
            qkv[0, s] = t
            rows[j, s] = t

    @pl.when(j >= O)
    def _():
        attention(j - O, rows, x, w, vec, o, att, h2, acc, hosted.visit)

    hosted.visit("end")


def front_call(x, w_attn, b_qkv, vec, up, collective_id):
    upto = lambda n: lambda j: jnp.minimum(j, n)
    seq = lambda tokens: along(0, 1, tokens, D, index=lambda j: jnp.maximum(j - O, 0))
    return pl.pallas_call(
        front_kernel, grid=(O + PAIR,),
        out_shape=(sds(BF16, O, *SEQS), sds(BF16, *TOKS), sds(BF16, *TOKS), sds(F32, *SEQS), sds(BF16, *TOKS),
                   sds(BF16, *Gather.shape(WIDE))),
        in_specs=[whole(*SEQS), along(0, 1, D, D, index=upto(O)), along(0, 1, 1, D, index=upto(V)), whole(8, D), ANY],
        out_specs=(along(0, 1, *SEQS, index=upto(V)), whole(*TOKS), seq(TOK), seq(SEQ), seq(TOK), ANY),
        scratch_shapes=[pltpu.VMEM((O, *SEQS), BF16), pltpu.VMEM((SEQ, D), F32)] + Gather.semaphores(),
        compiler_params=comm_params(collective_id), name="front",
    )(x, w_attn, b_qkv, vec, up)


def w_out_block():
    return along(0, 1, D, D, index=lambda j: O)


TILES = FF // HALF
OWN_BODY = BODY * len(SEQ_PAIR)
TAILS = ROWS - TAIL * PAIR * len(SEQ_PAIR)


def put_rows(ref, tail, s, t):
    ref[pl.ds(BODY * s, BODY)] = t[:BODY]
    ref[pl.ds(tail + TAIL * s, TAIL)] = t[BODY:]


DOWN_PLAN = {"start": ((0, 0, 1),), "end": ((1, 1, 5), (3, 5, 8), (5, 8, 9), (TILES + 4, 9, 12), (2 * TILES - 1, 12, None))}


def mlp_in_kernel(h2, gz, w_up, b_up, vec, src, act, slope, d_down, down, a_rows, b_rows, b_away, *sems):
    a_sems, b_sems, sems = sems[:PAIR], sems[PAIR:2 * PAIR], sems[2 * PAIR:]
    hosted = Background(Gather(DOWN, src, down, *sems).steps(), DOWN_PLAN)
    j = pl.program_id(0)
    away = Push(b_away, OWN_BODY, b_rows, b_sems, 0)
    tile = lambda n: Push(a_rows.at[n], TAILS, a_rows.at[n], a_sems, n)
    at_step(0)(enter)
    hosted.visit("start")

    @at_step(0)
    def _():
        first = Torus().at["c"] == 0
        for s in SEQ_PAIR:
            d = pad(gz[s].astype(F32) * row(vec, S2))
            left, right = d[:, :HALF], d[:, D - HALF:]
            put_rows(b_rows, TAILS, s, jnp.where(first, left, right))
            put_rows(b_away, OWN_BODY, s, jnp.where(first, right, left))

    at_step(1)(away.start)
    for n in range(TILES):
        at_step(n + 1)(tile(n).start)

    @pl.when(j < TILES)
    def _():
        for s in SEQ_PAIR:
            u = dot(h2[s, :SEQ], w_up[0]) + b_up[0]
            phi = 0.5 * (1.0 + lax.erf(u * math.sqrt(0.5)))
            slope[s] = phi + u * (jnp.exp(-0.5 * u * u) * math.sqrt(0.5 / math.pi))
            a = pad(u * phi)
            act[s] = a
            put_rows(a_rows.at[j], TAILS, s, a)

    at_step(TILES)(away.wait)
    for n in range(TILES):
        at_step(TILES + n)(tile(n).wait)

    @pl.when(j >= TILES)
    def _():
        d_down[...] = dot_tn(a_rows[j - TILES], b_rows[...])

    hosted.visit("end")

    @at_step(2 * TILES - 1)
    def _():
        away.finish()
        for n in range(TILES):
            tile(n).finish()


def mlp_in_call(h2, gz, w_up, b_up, vec, down, collective_id):
    low = lambda j: jnp.minimum(j, TILES - 1)
    high = lambda j: jnp.maximum(j - TILES, 0)
    return pl.pallas_call(
        mlp_in_kernel, grid=(2 * TILES,),
        out_shape=(sds(BF16, 2, TOK, FF), sds(F32, 2, SEQ, FF), sds(F32, FF, HALF), sds(BF16, *Gather.shape(DOWN))),
        in_specs=[whole(*TOKS), whole(*SEQS), up_tile(low), along(0, 1, 1, HALF, index=low), whole(8, D), ANY],
        out_specs=(along(2, 2, TOK, HALF, index=low), along(2, 2, SEQ, HALF, index=low),
                   along(0, HALF, HALF, index=high), ANY),
        scratch_shapes=[pltpu.VMEM((TILES, ROWS, HALF), BF16), pltpu.VMEM((ROWS, HALF), BF16),
                        pltpu.VMEM((PAIR * TOK, HALF), BF16)] + Push.semaphores(TILES) + Push.semaphores(1) +
        Gather.semaphores(),
        compiler_params=comm_params(collective_id), name="mlp_in",
    )(h2, gz, w_up, b_up.reshape(TILES, 1, HALF), vec, down)


def up_tile(index=lambda j: j):
    return pl.BlockSpec((1, D, HALF), lambda j: (index(j) // PAIR, 0, index(j) % PAIR))


MLP_PLACES = (("end", 0), ("end", 2), ("end", 3), ("end", TILES - 1))


def mlp_out_kernel(act, slope, gz, w_up, w_down, vec, part, d_pre, db_up, mlp, d_h2, sums, dm, *scratch):
    hosted = Pipeline(MLP_PLACES, First(DOWN, 0, part, sums, *scratch))
    at_step(0)(enter)
    hosted.visit("start")

    @at_step(0)
    def _():
        for s in SEQ_PAIR:
            dm[s] = (gz[s].astype(F32) * row(vec, S2)).astype(BF16)

    db = jnp.zeros((1, HALF), F32)
    for s in SEQ_PAIR:
        accumulate(mlp.at[s], dot(act[s, :SEQ], w_down[...]))
        d = dot_nt(dm[s], w_down[...]) * slope[s]
        db = db + col_sum(d)
        d_pre[0, 0, s] = pad(d)
        accumulate(d_h2.at[s], dot_nt(d.astype(BF16), w_up[0]))
    db_up[0] = db
    hosted.visit("end")


def mlp_out_call(act, slope, gz, w_up, w_down, vec, part, collective_id):
    return pl.pallas_call(
        mlp_out_kernel, grid=(TILES,),
        out_shape=(sds(BF16, 2, 4, 2, TOK, HALF), sds(F32, TILES, 1, HALF), sds(F32, *SEQS), sds(F32, *SEQS),
                   First.sums(DOWN)),
        in_specs=[along(2, 2, TOK, HALF), along(2, 2, SEQ, HALF), whole(*SEQS), up_tile(), along(0, HALF, D), whole(8, D),
                  ANY],
        out_specs=(pl.BlockSpec((1, 1, 2, TOK, HALF), lambda j: (j % PAIR, j // PAIR, 0, 0, 0)), along(0, 1, 1, HALF),
                   whole(*SEQS), whole(*SEQS), ANY),
        scratch_shapes=[pltpu.VMEM(SEQS, BF16)] + First.scratch(DOWN),
        compiler_params=comm_params(collective_id), name="mlp_out",
    )(act, slope, gz, w_up, w_down, vec, part)


def halves_of(t):
    t = pad(t)
    return t[:, :HALF], jnp.concatenate([t[:, HALF:], jnp.zeros((TOK, QCOLS - D), BF16)], axis=1)


def mid(mlp, d_h2, att, x, gz, vec, w_out, z, g_res, d_att, d_o, sums):
    a = att[0]
    y = x[0].astype(F32) + row(vec, S1) * a
    m = mlp[0] + row(vec, B2)
    g = gz[0].astype(F32)
    z[0] = (y + row(vec, S2) * m).astype(BF16)
    xhat, rstd = norm_stats(y)
    dh = d_h2[0]
    gr = g + norm_back(xhat, rstd, dh * row(vec, G2))
    g_res[0] = gr
    da = gr * row(vec, S1)
    terms = (da, gr * a, dh * xhat, dh, g * row(vec, S2), g * m)
    accumulate(sums, jnp.concatenate([jnp.zeros((BO, D), F32)] + [col_sum(t) for t in terms], axis=0))
    for i, t in enumerate(halves_of(da)):
        d_att[i, 0] = t
    d_o[0] = dot_nt(da.astype(BF16), w_out[0]).astype(BF16)


def attention_back(qkv, d_o, d_qkv, db, acc, visit):
    acc[...] = jnp.zeros_like(acc)
    for h in range(HEADS):
        lanes, mask = window(h)
        q, k, v = (only(mask, qkv[i, 0, :, lanes]) for i in (Q, K, V))
        do = only(mask, d_o[0, :, lanes])
        probs = softmax(dot_nt(q, k) * SCALE)
        acc[V, :, lanes] += dot_tn(probs.astype(BF16), do)
        dp = dot_nt(do, v)
        ds = probs * (dp - jnp.sum(dp * probs, axis=-1, keepdims=True))
        ds = (ds * SCALE).astype(BF16)
        acc[Q, :, lanes] += dot(ds, k)
        acc[K, :, lanes] += dot_tn(ds, q)
        visit(h)
    accumulate(db, jnp.concatenate([col_sum(acc[i]) for i in (Q, K, V)], axis=0))
    for n in (Q, K, V):
        for i, t in enumerate(halves_of(acc[n])):
            d_qkv[i, n, 0] = t


THIN = HALF // PAIR


class WideGrads:
    def __init__(self, a, a_of, b, out, base, a_rows, b_rows, *sems):
        self.a, self.a_of, self.b, self.out, self.base, self.a_rows, self.b_rows = a, a_of, b, out, base, a_rows, b_rows
        self.a_sems, self.b_sems = sems[:3], sems[3:]

    @staticmethod
    def scratch(inputs):
        return ([pltpu.VMEM((inputs, ROWS, D), BF16), pltpu.VMEM((SIDE, ROWS, HALF), BF16)] +
                Exchange.semaphores(inputs) + Exchange.semaphores(SIDE))

    def input(self, i):
        return Exchange(self.a[i], self.a[i], self.a_rows.at[i], self.a_sems, (i,))

    def cotangent(self, n):
        c = Torus().at["c"]
        b = self.b[n]
        return Exchange(b(c), b(1 - c), self.b_rows.at[n], self.b_sems, (n,))

    def begin(self):
        for n in range(SIDE):
            if n == 0 or self.a_of[n] != self.a_of[n - 1]:
                self.input(self.a_of[n]).start()
            self.cotangent(n).start()

    def step(self):
        j = pl.program_id(0)
        for n in range(SIDE):
            @at_step(self.base + PAIR * n)
            def _():
                if n == 0 or self.a_of[n] != self.a_of[n - 1]:
                    self.input(self.a_of[n]).wait()
                self.cotangent(n).wait()

        @pl.when(j >= self.base)
        def _():
            n = lax.div(j - self.base, PAIR)
            cols = pl.ds(pl.multiple_of(lax.rem(j - self.base, PAIR) * THIN, LANES), THIN)
            a = self.a_rows[0 if len(self.a) == 1 else lax.div(n, O)]
            self.out[0] = dot_tn(a, self.b_rows[n, :, cols])

    def finish(self):
        for i in range(len(self.a)):
            self.input(i).finish()
        for n in range(SIDE):
            self.cotangent(n).finish()


def grads_block(base):
    def index(j):
        n = jnp.maximum(j - base, 0)
        return n // PAIR, 0, n % PAIR

    return pl.BlockSpec((1, D, THIN), index)


LAST_SEQ = SEQS[0] - 1
GRAD_STEPS = PAIR * SIDE


def upto(n):
    return lambda j: jnp.minimum(j, n)


def seq_block(tokens=SEQ):
    return along(0, 1, tokens, D, index=upto(LAST_SEQ))


MID_PLACES = (("end", 0), ("end", 3), ("end", 7), ("end", LAST_SEQ + GRAD_STEPS))


def mid_kernel(*refs):
    refs = list(refs)
    take = lambda n: [refs.pop(0) for _ in range(n)]
    ins, (h2, d_pre, part, acc), outs, (d_up, sums, result) = take(7), take(4), take(5), take(3)
    grads = WideGrads((h2,), (0,) * SIDE, [lambda c, i=i: d_pre.at[c, i] for i in range(SIDE)], d_up, SEQS[0],
                      *take(len(WideGrads.scratch(1))))
    first = First(DOWN, 1, part, sums, *take(len(First.scratch(DOWN))))
    hosted = Pipeline(MID_PLACES, first, Rest(DOWN, acc, result, *refs))
    at_step(0)(enter)
    hosted.visit("start")
    at_step(0)(grads.begin)
    pl.when(pl.program_id(0) < SEQS[0])(lambda: mid(*ins, *outs))
    grads.step()
    hosted.visit("end")
    at_step(LAST_SEQ + GRAD_STEPS)(grads.finish)


def mid_call(mlp, d_h2, att, x, gz, vec, w_attn, h2, d_pre, part, acc, collective_id):
    return pl.pallas_call(
        mid_kernel, grid=(SEQS[0] + GRAD_STEPS,),
        out_shape=(sds(BF16, *SEQS), sds(F32, *SEQS), sds(BF16, 2, 2, TOK, HALF), sds(BF16, *SEQS), sds(F32, 8, D),
                   sds(F32, SIDE, D, HALF), First.sums(DOWN), Rest.sums(DOWN)),
        in_specs=[seq_block()] * len("mdaxg") + [whole(8, D), w_out_block()] + [ANY] * SIDE,
        out_specs=(seq_block(), seq_block(), along(1, 2, 1, TOK, HALF, index=upto(LAST_SEQ)), seq_block(), whole(8, D),
                   grads_block(SEQS[0]), ANY, ANY),
        scratch_shapes=WideGrads.scratch(1) + First.scratch(DOWN) + Rest.scratch(DOWN),
        compiler_params=comm_params(collective_id), name="mid",
    )(mlp, d_h2, att, x, gz, vec, w_attn, h2, d_pre, part, acc)


ATTN_PLACES = ((6, 0), (1, LAST_SEQ), (11, LAST_SEQ), ("end", LAST_SEQ))


def attn_back_kernel(qkv, d_o, part, acc_down, result_down, d_qkv, db, sums, result, total, acc, *scratch):
    n, m = len(First.scratch(WIDE)), len(Rest.scratch(DOWN))
    hosted = Pipeline(ATTN_PLACES, First(WIDE, 0, part, sums, *scratch[:n]),
                      Rest(DOWN, acc_down, result, *scratch[n:n + m]), Spread(DOWN, result_down, total, *scratch[n + m:]))
    at_step(0)(enter)
    hosted.visit("start")
    attention_back(qkv, d_o, d_qkv, db, acc, hosted.visit)
    hosted.visit("end")


def attn_back_call(qkv, d_o, part, acc_down, result_down, collective_id):
    return pl.pallas_call(
        attn_back_kernel, grid=SEQS[:1],
        out_shape=(sds(BF16, 2, O, 2, TOK, HALF), sds(F32, O, D), First.sums(WIDE), Rest.sums(DOWN), Spread.sums(DOWN)),
        in_specs=[along(1, O, 1, SEQ, D), seq_block()] + [ANY] * O,
        out_specs=(along(2, 2, O, 1, TOK, HALF), whole(O, D)) + (ANY,) * O,
        scratch_shapes=[pltpu.VMEM((O, SEQ, D), F32)] + First.scratch(WIDE) + Rest.scratch(DOWN) + Spread.scratch(),
        compiler_params=comm_params(collective_id), name="attn_back",
    )(qkv, d_o, part, acc_down, result_down)


IN_STEPS = PAIR * O
IN_PLACES = (("end", 1), ("end", IN_STEPS - 1), ("end", IN_STEPS + O), ("end", IN_STEPS + GRAD_STEPS - 1))


def in_back_kernel(*refs):
    refs = list(refs)
    take = lambda n: [refs.pop(0) for _ in range(n)]
    (d_half, w, x, g_res, vec), (h1, o, d_qkv, d_att, part, acc_up, result_down) = take(5), take(7)
    (dx, sums, d_attn), outs, acc = take(3), take(3), refs.pop(0)
    b = [lambda c, i=i: d_qkv.at[c, i] for i in range(O)] + [lambda c: d_att.at[c]]
    grads = WideGrads((h1, o), (0,) * O + (1,), b, d_attn, IN_STEPS, *take(len(WideGrads.scratch(2))))
    first = First(WIDE, 1, part, outs[0], *take(len(First.scratch(WIDE))))
    rest = Rest(WIDE, acc_up, outs[1], *take(len(Rest.scratch(WIDE))))
    hosted = Pipeline(IN_PLACES, first, rest, Spread(DOWN, result_down, outs[2], *refs))
    at_step(0)(enter)
    hosted.visit("start")
    at_step(0)(grads.begin)

    @pl.when(pl.program_id(0) < IN_STEPS)
    def _():
        for s in SEQ_PAIR:
            accumulate(acc.at[s], dot_nt(d_half[0, 0, s, :SEQ], w[0]))

    @at_step(IN_STEPS - 1)
    def _():
        rows = jnp.zeros((BO, D), F32)
        for s in SEQ_PAIR:
            xhat, rstd = norm_stats(x[s].astype(F32))
            dh = acc[s]
            rows = rows + jnp.concatenate([col_sum(dh * xhat), col_sum(dh)], axis=0)
            dx[s] = (g_res[s] + norm_back(xhat, rstd, dh * row(vec, G1))).astype(BF16)
        sums[...] = rows

    grads.step()
    hosted.visit("end")
    at_step(IN_STEPS + GRAD_STEPS - 1)(grads.finish)


def in_back_call(d_qkv, w_attn, x, g_res, vec, h1, o, d_att, part, acc_up, result_down, collective_id):
    low = upto(IN_STEPS - 1)
    return pl.pallas_call(
        in_back_kernel, grid=(IN_STEPS + GRAD_STEPS,),
        out_shape=(sds(BF16, *SEQS), sds(F32, BO, D), sds(F32, SIDE, D, HALF), First.sums(WIDE), Rest.sums(WIDE),
                   Spread.sums(DOWN)),
        in_specs=[pl.BlockSpec((1, 1, 2, TOK, HALF), lambda j: (low(j) % PAIR, low(j) // PAIR, 0, 0, 0)), up_tile(low),
                  whole(*SEQS), whole(*SEQS), whole(8, D)] + [ANY] * 7,
        out_specs=(whole(*SEQS), whole(BO, D), grads_block(IN_STEPS), ANY, ANY, ANY),
        scratch_shapes=[pltpu.VMEM(SEQS, F32)] + WideGrads.scratch(2) + First.scratch(WIDE) + Rest.scratch(WIDE) +
        Spread.scratch(),
        compiler_params=comm_params(collective_id), name="in_back",
    )(d_qkv, w_attn, x, g_res, vec, h1, o, d_qkv, d_att, part, acc_up, result_down)


BQ, BU, VEC = 3 * D // 32, 3 * D // 32 + FF // 32, 3 * D // 32 + FF // 32 + 8 * OWN
DEVICES = 32


def pair_swap(a):
    return lax.ppermute(a, "fsdp", [(i, i ^ 1) for i in range(DEVICES)])


def by_core(first, a, b):
    return jnp.where(first, a, b), jnp.where(first, b, a)


def my_pieces(shards, first):
    w_qkv, b_qkv, w_out, w_up, b_up, w_down, vec_params = shards
    x = lax.axis_index("rep")
    small = jnp.concatenate([b_qkv, b_up, vec_params.reshape(-1)])
    small = jnp.pad(small, (0, OWN * LANES - VEC)).reshape(OWN, LANES)
    attn = lax.dynamic_slice_in_dim(jnp.concatenate([w_qkv, w_out], axis=1), x * D, D, 1)
    attn = jnp.concatenate([attn, small], axis=1)
    up = lax.dynamic_slice_in_dim(w_up, x * QCOLS, QCOLS, 1)
    wide = jnp.stack([attn, up]).astype(BF16)
    mine, theirs = by_core(first, wide[..., :HALF], wide[..., HALF:])
    theirs = pair_swap(theirs)
    piece = jnp.concatenate(by_core(first, mine, theirs), axis=1)
    down = lax.dynamic_slice_in_dim(w_down, x * 48, 48, 0).astype(BF16).reshape(3, 16, D)
    return piece[0], piece[1], down


def small_params(w_attn):
    small = w_attn[0, :, D:].astype(F32).reshape(DEVICES, OWN * LANES)
    vec = small[:, BU:VEC].reshape(DEVICES, 8, OWN).transpose(1, 0, 2).reshape(8, D)
    return small[:, :BQ].reshape(O, 1, D), small[:, BQ:BU].reshape(FF), vec


def small_grads(db_qkv, db_up, sums, core):
    vec = sums.reshape(8, DEVICES, OWN).transpose(1, 0, 2).reshape(DEVICES, VEC - BU)
    small = jnp.concatenate([db_qkv.reshape(DEVICES, BQ), db_up.reshape(DEVICES, BU - BQ), vec], axis=1)
    small = (small + pair_swap(small)) * core.astype(F32)
    return jnp.pad(small, ((0, 0), (0, OWN * LANES - VEC))).reshape(D, LANES)


def final_rows(halves, first):
    total = jnp.stack(halves, axis=2)
    keep, give = by_core(first, total[..., :OWN, :], total[..., OWN:, :])
    pair = jnp.stack(by_core(first, keep, pair_swap(give)), axis=1)
    return pair.transpose(4, 0, 1, 2, 3, 5).reshape(OWN, SIDE, QCOLS)


def final_down(halves, first):
    down = jnp.concatenate(halves, axis=-1).reshape(FF // 16, HALF)
    keep, give = by_core(first, down[:FF // DEVICES], down[FF // DEVICES:])
    left, right = by_core(first, keep, pair_swap(give))
    return jnp.concatenate([left, right[:, 2 * HALF - D:]], axis=1)


def device_step(x, gz, *shards):
    core = lax.rem(lax.axis_index("fsdp"), PAIR)
    first = core == 0
    attn, up, down = my_pieces(shards, first)
    w_attn = torus_gather(WIDE, attn, 0).reshape(SIDE, D, QCOLS)
    b_qkv, b_up, vec = small_params(w_attn)
    qkv, h1, o, att, h2, w_up = front_call(x, w_attn, b_qkv, vec, up, 1)
    w_up = w_up.reshape(SIDE, D, QCOLS)
    act, slope, part, w_down = mlp_in_call(h2, gz, w_up, b_up, vec, down, 2)
    part = part.reshape((SIDE,) * 3 + (C, 32, HALF))
    d_pre, db_up, mlp, d_h2, acc0 = mlp_out_call(act, slope, gz, w_up, w_down.reshape(FF, D), vec, part, 3)
    z, g_res, d_att, d_o, sums, part, acc1, result0 = mid_call(mlp, d_h2, att, x, gz, vec, w_attn, h2, d_pre, part, acc0, 4)
    part = part.reshape((SIDE,) * 3 + (CHIP, HALF))
    d_qkv, db_qkv, acc0, result1, down0 = attn_back_call(qkv, d_o, part, acc1, result0, 5)
    dx, in_sums, part, acc1, result0, down1 = in_back_call(d_qkv, w_attn, x, g_res, vec, h1, o, d_att, part, acc0, result1, 6)
    small = small_grads(db_qkv, db_up, jnp.concatenate([in_sums, sums[BO:]], axis=0), core)
    part = part.at[0, :, HALF - LANES:].add(small).reshape((SIDE,) * 3 + (CHIP, HALF))
    attn0, attn1, up1, up0 = last_scatter(part, acc1, result0, 7)
    g_up = final_rows((up0, up1), first).reshape(OWN, FF)
    attn = final_rows((attn0, attn1), first)
    small = attn[:, 0, D:].reshape(OWN * LANES)
    return (z, dx, attn[:, :O, :D].reshape(OWN, O * D), small[:BQ], attn[:, O, :D], g_up, small[BQ:BU],
            final_down((down0, down1), first), small[BU:VEC].reshape(8, OWN))


def solution(mesh):
    batch = P(("rep", "fsdp"), None, None)
    rows, flat, cols = P("fsdp", None), P("fsdp"), P(None, "fsdp")
    shards = (rows, flat, rows, rows, flat, rows, cols)
    return jax.shard_map(device_step, mesh=mesh, in_specs=(batch, batch) + shards,
                         out_specs=(batch, batch) + shards, check_vma=False)
```

```python
import functools
import math

import jax
import jax.numpy as jnp
from jax import lax
from jax.experimental import pallas as pl
from jax.experimental.pallas import tpu as pltpu
from jax.sharding import PartitionSpec as P

HEADS = 16
LN_EPS = 1e-5
D = 1408
FF = 6144
SEQ = 257
HEAD = D // HEADS
SCALE = HEAD ** -0.5
QCOLS = 1536
HALF = 768
OWN = 44
CHIP = 2 * OWN
LANES = 128
F32 = jnp.float32
BF16 = jnp.bfloat16
VMEM_LIMIT = 66 * 1000 * 1000
G1, C1, BO, S1, G2, C2, B2, S2 = range(8)
Q, K, V, O = range(4)
SEQS = (2, SEQ, D)
LAST_SEQ = SEQS[0] - 1
SEQ_PAIR = range(SEQS[0])
TAIL = 16
BODY = SEQ - 1
TOK = BODY + TAIL
TT = 2 * TOK
ROWS = 4 * TOK
STEP = 256


def sds(dtype, *shape):
    return jax.ShapeDtypeStruct(shape, dtype)


MESH_ID = pl.DeviceIdType.MESH
SIDE = 4
SUB = 8
PAIR = 2
C = 3
COLOURS = range(C)
COLOUR_DIMS = ("xyz", "yzx", "zxy")
FIRST, SECOND, THIRD, LAST = range(4)
WAYS = range(PAIR)
NEAR, FAR, ADDED = 0, 2, 4
WIDE, DOWN = "wide", "down"
ANY = pl.BlockSpec(memory_space=pl.ANY)
ALL = slice(None)


def duo(m):
    return pl.ds(PAIR * m, PAIR)


def toward(m):
    return 1 - PAIR * (m % PAIR)


class Torus:
    def __init__(self):
        f = lax.axis_index("fsdp")
        self.at = {"x": lax.axis_index("rep"), "z": lax.div(f, SIDE * PAIR), "y": lax.rem(lax.div(f, PAIR), SIDE),
                   "c": lax.rem(f, PAIR)}

    def shift(self, dim, by):
        return lax.rem(self.at[dim] + (SIDE + by), SIDE)

    def device(self, **moved):
        p = {**self.at, **moved}
        return (p["x"], (p["z"] * SIDE + p["y"]) * PAIR + p["c"])

    def neighbour(self, dim, by):
        return self.device(**{dim: self.shift(dim, by)})

    def partner(self):
        return self.device(c=1 - self.at["c"])


def enter():
    me = Torus()
    barrier = pltpu.get_barrier_semaphore()
    others = [me.neighbour(d, toward(m)) for d in COLOUR_DIMS[0] for m in WAYS] + [me.partner()]
    for other in others:
        pl.semaphore_signal(barrier, device_id=other, device_id_type=MESH_ID)
    pl.semaphore_wait(barrier, len(others))


def remote(src, dst, sems, slot, device):
    return pltpu.make_async_remote_copy(src_ref=src, dst_ref=dst, send_sem=sems[0].at[slot], recv_sem=sems[1].at[slot],
                                        device_id=device, device_id_type=MESH_ID)


class Gather:
    def __init__(self, kind, src, dst, hop_send, hop_recv, push_send, push_recv, local):
        self.kind, self.src, self.dst, self.local = kind, src, dst, local
        self.hops, self.pushes = (hop_send, hop_recv), (push_send, push_recv)
        self.cols, self.cut = (256, 128) if kind == WIDE else (D, HALF)

    @staticmethod
    def semaphores():
        dma = pltpu.SemaphoreType.DMA
        return [dma((C, C, ADDED))] * PAIR + [dma((C, ADDED + 1))] * PAIR + [dma((C,))]

    @staticmethod
    def shape(kind):
        return (SIDE,) * 3 + (CHIP, QCOLS) if kind == WIDE else (SIDE, SIDE, PAIR, SIDE, C, 16, D)

    def source(self, k):
        return self.src.at[:, pl.ds(self.cols * k, self.cols)] if self.kind == WIDE else self.src.at[k]

    def piece(self, me, k, s, v, half=None):
        dims = COLOUR_DIMS[k]
        at = {**me.at, **{d: ALL for d in dims[:s]}, dims[s]: v}
        off, width = 0, self.cols
        if half is not None and s == FIRST:
            off, width = self.cut * half, (self.cut, self.cols - self.cut)[half]
        elif half is not None:
            at[dims[0]] = duo(half)
        if self.kind == WIDE:
            cols = pl.ds(pl.multiple_of(at["c"] * HALF + self.cols * k + off, 128), width)
            return self.dst.at[at["x"], at["z"], at["y"], :, cols]
        return self.dst.at[at["z"], at["y"], at["c"], at["x"], k, :, pl.ds(off, width)]

    def hop(self, k, s, m):
        me = Torus()
        dim = COLOUR_DIMS[k][s]
        by = toward(m)
        if m < FAR:
            ref = self.piece(me, k, s, me.at[dim])
        else:
            ref = self.piece(me, k, s, me.shift(dim, -by), m - FAR)
        src = self.source(k) if s == FIRST and m < FAR else ref
        return remote(src, ref, self.hops, (k, s, m), me.neighbour(dim, by))

    def push(self, k, n):
        me = Torus()
        dim = COLOUR_DIMS[k][THIRD]
        if n < FAR:
            ref = self.piece(me, k, THIRD, me.shift(dim, -toward(n)))
        elif n < ADDED:
            ref = self.piece(me, k, THIRD, me.shift(dim, FAR), n - FAR)
        else:
            ref = self.piece(me, k, THIRD, me.at[dim])
        return remote(ref, ref, self.pushes, (k, n), me.partner())

    def own(self, k):
        me = Torus()
        return pltpu.make_async_copy(self.source(k), self.piece(me, k, FIRST, me.at[COLOUR_DIMS[k][FIRST]]), self.local.at[k])

    def launch(self, s):
        for k in COLOURS:
            for m in WAYS:
                self.hop(k, s, m).start()
            if s == THIRD:
                self.push(k, ADDED).start()

    def relay(self, k, s):
        for m in WAYS:
            self.hop(k, s, m).wait_recv()
            self.hop(k, s, FAR + m).start()
            if s == THIRD:
                self.push(k, m).start()

    def settle(self, s):
        for k in COLOURS:
            for m in WAYS:
                self.hop(k, s, FAR + m).wait_recv()
                if s == THIRD:
                    self.push(k, FAR + m).start()
            if s == FIRST:
                self.own(k).wait()
        if s < THIRD:
            self.launch(s + 1)

    def begin(self):
        for k in COLOURS:
            self.own(k).start()
        self.launch(FIRST)

    def finish(self):
        for k in COLOURS:
            for s in COLOURS:
                for m in range(ADDED):
                    self.hop(k, s, m).wait_send()
            for n in range(ADDED + 1):
                self.push(k, n).wait()

    def steps(self):
        out = [self.begin]
        for s in COLOURS:
            out += [functools.partial(self.relay, k, s) for k in COLOURS] + [functools.partial(self.settle, s)]
        return out + [self.finish]


def add_into(total, *others):
    lead = total.shape[:-2]

    def body(i, carry):
        idx = []
        for n in reversed(lead):
            idx.insert(0, lax.rem(i, n))
            i = lax.div(i, n)
        value = total[tuple(idx)]
        for other in others:
            value = value + other[tuple(idx)]
        total[tuple(idx)] = value
        return carry

    lax.fori_loop(0, math.prod(lead), body, 0)


class Ring:
    def __init__(self, s, terms, passed, relay, landing, send, recv, rows=None):
        self.s, self.terms, self.passed, self.relay, self.landing = s, terms, passed, relay, landing
        self.sems, self.rows = (send, recv), rows

    def zone(self, k, way, half):
        return self.landing.at[k, way, self.rows[half] if self.rows else duo(half)]

    def carried(self, ref, k, way):
        return ref.at[k, way, pl.ds(0, self.rows[way].size)] if self.rows else ref.at[k, way]

    def hop(self, k, m):
        me = Torus()
        dim = COLOUR_DIMS[k][self.s]
        way, by = m % PAIR, toward(m)
        if m < FAR:
            src, dst = self.terms(k, me.shift(dim, FAR), way), self.carried(self.relay, k, way)
        elif m < ADDED:
            src, dst = self.terms(k, me.shift(dim, by), 1 - way), self.zone(k, way, 1 - way)
        else:
            src, dst = self.carried(self.passed, k, way), self.zone(k, way, way)
        return remote(src, dst, self.sems, (k, m), me.neighbour(dim, by))

    def start(self, k, base):
        for m in WAYS:
            self.hop(k, base + m).start()

    def arrived(self, k, base):
        for m in WAYS:
            self.hop(k, base + m).wait_recv()

    def finish(self):
        for k in COLOURS:
            for m in range(ADDED + PAIR):
                self.hop(k, m).wait_send()

    @staticmethod
    def semaphores():
        return [pltpu.SemaphoreType.DMA((C, ADDED + PAIR))] * PAIR


UNITS = {WIDE: (CHIP, LANES), DOWN: (FF // 192, HALF // PAIR)}


def unit_array(kind, *lead):
    return lead + UNITS[kind]


class First:
    def __init__(self, kind, half, part, acc, own, passed, relay, landing, send, recv, load, store):
        self.kind, self.half, self.part, self.acc, self.own, self.passed = kind, half, part, acc, own, passed
        self.relay_in, self.landing, self.load_sem, self.store_sem = relay, landing, load, store
        self.ring = Ring(FIRST, self.terms, passed, relay, landing, send, recv)

    @staticmethod
    def scratch(kind):
        vm = lambda *lead: pltpu.VMEM(unit_array(kind, *lead), F32)
        dma = pltpu.SemaphoreType.DMA
        relays = [vm(C, PAIR, PAIR, SIDE)] * PAIR
        return [vm(C, SIDE, SIDE), *relays, vm(C, PAIR, SIDE, SIDE), *Ring.semaphores(), dma((C, C)), dma((C,))]

    @staticmethod
    def sums(kind):
        return sds(F32, *unit_array(kind, C, SIDE, SIDE))

    def terms(self, k, v, half=None):
        order = ORDERS[self.kind]
        at = {d: ALL for d in order}
        at[COLOUR_DIMS[k][FIRST]] = v
        if half is not None:
            at[rest_dims(self.kind, k)[0]] = duo(half)
        lead = tuple(at[d] for d in order)
        width = UNITS[self.kind][1]
        if self.kind == WIDE:
            return self.part.at[lead + (ALL, pl.ds(width * (PAIR * k + self.half), width))]
        return self.part.at[lead + (k, ALL, pl.ds(width * self.half, width))]

    def load(self, k, m):
        me = Torus()
        dim = COLOUR_DIMS[k][FIRST]
        if m in WAYS:
            src, dst = self.terms(k, me.shift(dim, toward(m)), m), self.passed.at[k, m]
        else:
            src, dst = self.terms(k, me.at[dim]), self.own.at[k]
        return pltpu.make_async_copy(src, dst, self.load_sem.at[k, m])

    def store(self, k):
        return pltpu.make_async_copy(self.own.at[k], self.acc.at[k], self.store_sem.at[k])

    def near(self):
        for k in COLOURS:
            self.ring.start(k, NEAR)

    def far(self):
        for k in COLOURS:
            self.ring.start(k, FAR)
        for m in COLOURS:
            for k in COLOURS:
                self.load(k, m).start()

    def relay(self):
        for k in COLOURS:
            self.ring.arrived(k, NEAR)
            for m in WAYS:
                self.load(k, m).wait()
                add_into(self.passed.at[k, m], self.relay_in.at[k, m])
            self.ring.start(k, ADDED)

    def settle(self, then=None):
        for k in COLOURS:
            self.load(k, FAR).wait()
            for base in (FAR, ADDED):
                self.ring.arrived(k, base)
            add_into(self.own.at[k], *(self.landing.at[k, m] for m in WAYS))
            if then is None:
                self.store(k).start()
            else:
                then(k)

    def finish(self):
        self.ring.finish()
        if self.acc is not None:
            for k in COLOURS:
                self.store(k).wait()


ORDERS = {WIDE: "xzy", DOWN: "zyx"}


def rest_dims(kind, k):
    return [d for d in ORDERS[kind] if d != COLOUR_DIMS[k][FIRST]]


class Rest:
    def __init__(self, kind, acc, result, own, relay2, in2, relay3, in3, *sems):
        self.kind, self.acc, self.own, self.result = kind, acc, own, result
        self.in2, self.in3, self.relay2, self.relay3, self.load_sem, self.store_sem = in2, in3, relay2, relay3, *sems[-2:]
        rows, cut = UNITS[kind][0], relay3.shape[2]
        cuts = pl.ds(0, cut), pl.ds(cut, rows - cut)
        self.second = Ring(SECOND, functools.partial(self.terms, acc), relay2, relay2, in2, *sems[:PAIR])
        third = lambda k, v, half=None: in2.at[(k, 0, v) + (() if half is None else (cuts[half],))]
        self.third = Ring(THIRD, third, relay3, relay3, in3, *sems[PAIR:2 * PAIR], rows=cuts)

    @staticmethod
    def scratch(kind):
        vm = lambda *lead: pltpu.VMEM(unit_array(kind, *lead), F32)
        rows, cols = UNITS[kind]
        dma = pltpu.SemaphoreType.DMA
        cut = (rows // SUB + 1) // PAIR * SUB
        return [vm(C, SIDE, SIDE), vm(C, PAIR, PAIR), vm(C, PAIR, SIDE), pltpu.VMEM((C, PAIR, cut, cols), F32), vm(C, PAIR),
                *Ring.semaphores(), *Ring.semaphores(), dma((C,)), dma((C,))]

    @staticmethod
    def sums(kind):
        return sds(F32, *unit_array(kind, C))

    def terms(self, ref, k, v, half=None):
        other = ALL if half is None else duo(half)
        return ref.at[(k, v, other) if rest_dims(self.kind, k)[0] == COLOUR_DIMS[k][SECOND] else (k, other, v)]

    def load(self, k):
        return pltpu.make_async_copy(self.acc.at[k], self.own.at[k], self.load_sem.at[k])

    def store(self, k):
        return pltpu.make_async_copy(self.in3.at[k, 0], self.result.at[k], self.store_sem.at[k])

    def send(self, k):
        for base in (NEAR, FAR):
            self.second.start(k, base)

    def begin(self):
        for k in COLOURS:
            self.send(k)
        for k in COLOURS:
            self.load(k).start()

    def loaded(self):
        for k in COLOURS:
            self.load(k).wait()

    def relay(self):
        me = Torus()
        for k in COLOURS:
            self.second.arrived(k, NEAR)
            for m in WAYS:
                add_into(self.relay2.at[k, m], self.terms(self.own, k, me.shift(COLOUR_DIMS[k][SECOND], toward(m)), m))
            self.second.start(k, ADDED)

    def settle(self):
        me = Torus()
        for k in COLOURS:
            for base in (FAR, ADDED):
                self.second.arrived(k, base)
            add_into(self.in2.at[k, 0], self.in2.at[k, 1], self.terms(self.own, k, me.at[COLOUR_DIMS[k][SECOND]]))
            for base in (NEAR, FAR):
                self.third.start(k, base)

    def relay_third(self):
        me = Torus()
        for k in COLOURS:
            self.third.arrived(k, NEAR)
            for m in WAYS:
                mine = self.third.carried(self.relay3, k, m)
                mine[...] += self.third.terms(k, me.shift(COLOUR_DIMS[k][THIRD], toward(m)), m)[...]
            self.third.start(k, ADDED)

    def settle_third(self):
        me = Torus()
        for k in COLOURS:
            for base in (FAR, ADDED):
                self.third.arrived(k, base)
            self.in3[k, 0] += self.in3[k, 1] + self.third.terms(k, me.at[COLOUR_DIMS[k][THIRD]])[...]
            if self.result is not None:
                self.store(k).start()

    def finish(self):
        self.second.finish()
        self.third.finish()
        if self.result is not None:
            for k in COLOURS:
                self.store(k).wait()


class Spread:
    def __init__(self, kind, result, total, send, recv, local):
        rows = UNITS[kind][0]
        cut = rows // SUB // PAIR * SUB
        self.result, self.total, self.sems, self.local = result, total, (send, recv), local
        self.cuts = pl.ds(0, cut), pl.ds(cut, rows - cut)

    @staticmethod
    def scratch():
        return [pltpu.SemaphoreType.DMA((C, ADDED))] * PAIR + [pltpu.SemaphoreType.DMA((C,))]

    @staticmethod
    def sums(kind):
        return sds(F32, *unit_array(kind, SIDE, C))

    def hop(self, k, m):
        me = Torus()
        by = toward(m)
        if m < FAR:
            src, dst = self.result.at[k], self.total.at[me.at["x"], k]
        else:
            dst = src = self.total.at[me.shift("x", -by), k, self.cuts[m - FAR]]
        return remote(src, dst, self.sems, (k, m), me.neighbour("x", by))

    def own(self, k):
        return pltpu.make_async_copy(self.result.at[k], self.total.at[Torus().at["x"], k], self.local.at[k])

    def begin(self):
        for k in COLOURS:
            self.own(k).start()
            for m in WAYS:
                self.hop(k, m).start()

    def forward(self):
        for k in COLOURS:
            for m in WAYS:
                self.hop(k, m).wait_recv()
                self.hop(k, FAR + m).start()

    def finish(self):
        for k in COLOURS:
            for m in WAYS:
                self.hop(k, FAR + m).wait_recv()
            self.own(k).wait()
            for m in range(ADDED):
                self.hop(k, m).wait_send()


def comm_params(collective_id):
    return pltpu.CompilerParams(collective_id=collective_id, has_side_effects=True, vmem_limit_bytes=VMEM_LIMIT)


def torus_gather(kind, piece, collective_id):
    def kernel(*refs):
        enter()
        for step in Gather(kind, *refs).steps():
            step()

    return pl.pallas_call(
        kernel, out_shape=sds(BF16, *Gather.shape(kind)), in_specs=[ANY], out_specs=ANY,
        scratch_shapes=Gather.semaphores(), compiler_params=comm_params(collective_id), name="gather_" + kind)(piece)


def last_scatter_kernel(part, acc_up, result_up, *refs):
    outs, refs = refs[:SIDE], list(refs[SIDE:])
    take = lambda like: [refs.pop(0) for _ in like]
    a, b = (First(WIDE, h, part, None, *take(First.scratch(WIDE))) for h in WAYS)
    rest_a, rest_b = (Rest(WIDE, f.own, None, f.own, *take(Rest.scratch(WIDE)[1:])) for f in (a, b))
    late = Rest(WIDE, acc_up, None, *take(Rest.scratch(WIDE)))
    results = [rest.in3.at[:, 0] for rest in (rest_a, rest_b, late)]
    spread_a, spread_b, spread_late, early = (
        Spread(WIDE, *pair, *take(Spread.scratch())) for pair in zip([*results, result_up], outs))
    enter()
    for step in (late.begin, early.begin, a.near, late.loaded, late.relay, a.far, early.forward, late.settle, a.relay, b.near,
                 late.relay_third, late.settle_third, b.far, late.finish, spread_late.begin,
                 functools.partial(a.settle, rest_a.send), b.relay, rest_a.relay, spread_late.forward, rest_a.settle,
                 rest_a.relay_third, functools.partial(b.settle, rest_b.send), rest_a.settle_third, rest_b.relay,
                 rest_a.finish, spread_a.begin, rest_b.settle, spread_a.forward, rest_b.relay_third, rest_b.settle_third,
                 rest_b.finish, spread_b.begin, spread_b.forward, early.finish, spread_late.finish, spread_a.finish,
                 spread_b.finish, a.finish, b.finish):
        step()


def last_scatter(part, acc_up, result_up, collective_id):
    return pl.pallas_call(
        last_scatter_kernel, out_shape=(Spread.sums(WIDE),) * SIDE, in_specs=[ANY] * O, out_specs=(ANY,) * SIDE,
        scratch_shapes=First.scratch(WIDE) * PAIR + Rest.scratch(WIDE)[1:] * PAIR + Rest.scratch(WIDE) +
        Spread.scratch() * SIDE,
        compiler_params=comm_params(collective_id), name="last_scatter")(part, acc_up, result_up)


class Background:
    def __init__(self, steps, plan):
        self.steps, self.plan = steps, plan

    def visit(self, place):
        for j, first, end in self.plan.get(place, ()):
            @at_step(j)
            def _():
                for step in self.steps[first:end]:
                    step()


class Pipeline:
    def __init__(self, places, first, rest=None, spread=None):
        rest_steps = (rest.loaded, rest.relay) if rest else ()
        groups = [[*((rest.begin,) if rest else ()), *((spread.begin,) if spread else ()), first.near],
                  [*rest_steps, first.far, *((spread.forward,) if spread else ())],
                  [*((rest.settle,) if rest else ()), first.relay],
                  [rest.relay_third] if rest else [],
                  [first.settle, *((rest.settle_third,) if rest else ()), first.finish, *((rest.finish,) if rest else ()),
                   *((spread.finish,) if spread else ())]]
        self.groups = list(zip([("start", 0), *places], groups))

    def visit(self, place):
        for (where, j), group in self.groups:
            if where == place:
                @at_step(j)
                def _():
                    for step in group:
                        step()


class Push:
    def __init__(self, src, tail, rows, sems, slot):
        body = BODY * len(SEQ_PAIR)
        tails = TAIL * len(SEQ_PAIR)
        self.copies = [
            remote(src.at[pl.ds(start, size)], rows.at[pl.ds(to, size)], sems, (slot, i), Torus().partner())
            for i, (start, to, size) in enumerate(((0, body, body), (tail, PAIR * body + tails, tails)))]

    @staticmethod
    def semaphores(n):
        return [pltpu.SemaphoreType.DMA((n, PAIR))] * PAIR

    def start(self):
        for copy in self.copies:
            copy.start()

    def wait(self):
        for copy in self.copies:
            copy.wait_recv()

    def finish(self):
        for copy in self.copies:
            copy.wait_send()


class Exchange:
    def __init__(self, mine, theirs, rows, sems, slot):
        self.moves = []
        for s in SEQ_PAIR:
            for i, (start, size) in enumerate(((0, BODY), (BODY, TAIL))):
                place = lambda n: rows.at[pl.ds(start * len(SEQ_PAIR) * PAIR + size * n, size)]
                part = pl.ds(TOK * s + start, size)
                at = slot + (PAIR * s + i,)
                local = pltpu.make_async_copy(mine.at[part], place(s), sems[2].at[at])
                far = remote(theirs.at[part], place(len(SEQ_PAIR) + s), sems, at, Torus().partner())
                self.moves.append((local, far))

    @staticmethod
    def semaphores(*lead):
        return [pltpu.SemaphoreType.DMA(lead + (2 * PAIR,))] * 3

    def start(self):
        for local, far in self.moves:
            far.start()
            local.start()

    def wait(self):
        for local, far in self.moves:
            local.wait()
            far.wait_recv()

    def finish(self):
        for _, far in self.moves:
            far.wait_send()


NT = (((1,), (1,)), ((), ()))
TN = (((0,), (0,)), ((), ()))


def dot(a, b):
    return jnp.dot(a, b, preferred_element_type=F32)


def dot_nt(a, b):
    return lax.dot_general(a, b, NT, preferred_element_type=F32)


def dot_tn(a, b):
    return lax.dot_general(a, b, TN, preferred_element_type=F32)


def zeros_but(n, axis, value):
    return tuple(value if i == axis else 0 for i in range(n))


def whole(*shape):
    return pl.BlockSpec(shape, lambda *_: (0,) * len(shape))


def along(axis, *block, index=lambda j: j):
    return pl.BlockSpec(block, lambda j: zeros_but(len(block), axis, index(j)))


def row(vec, i):
    return vec[i:i + 1]


def row_mean(t):
    return jnp.mean(t, axis=-1, keepdims=True)


def norm_stats(t):
    centered = t - row_mean(t)
    rstd = lax.rsqrt(row_mean(centered * centered) + LN_EPS)
    return centered * rstd, rstd


def norm_back(xhat, rstd, g):
    return rstd * (g - row_mean(g) - xhat * row_mean(g * xhat))


def col_sum(t):
    return jnp.sum(t, axis=0, keepdims=True)


def at_step(j):
    return pl.when(pl.program_id(0) == j)


def accumulate(ref, value):
    @at_step(0)
    def _():
        ref[...] = value

    @pl.when(pl.program_id(0) > 0)
    def _():
        ref[...] += value


def pad(t):
    return jnp.concatenate([t.astype(F32), jnp.zeros((TOK - SEQ, t.shape[1]), F32)], axis=0).astype(BF16)


def window(h):
    start = h * HEAD // LANES * LANES
    stop = min(D, -(-(h + 1) * HEAD // LANES) * LANES)
    lane = lax.broadcasted_iota(jnp.int32, (1, stop - start), 1) + (start - h * HEAD)
    return slice(start, stop), (lane >= 0) & (lane < HEAD)


def only(mask, t):
    return jnp.where(mask, t, jnp.zeros_like(t))


def softmax(scores):
    e = jnp.exp(scores - jnp.max(scores, axis=-1, keepdims=True))
    return e * (1.0 / jnp.sum(e, axis=-1, keepdims=True))


def attention(s, rows, o, acc, visit):
    acc[...] = jnp.zeros_like(acc)
    start = pl.multiple_of(s * TOK, TAIL)
    tokens = pl.ds(start, SEQ)
    for h in range(HEADS):
        lanes, mask = window(h)
        k = only(mask, rows[K, tokens, lanes])
        v = only(mask, rows[V, tokens, lanes])
        probs = softmax(dot_nt(rows[Q, tokens, lanes], k) * SCALE).astype(BF16)
        acc[:, lanes] += dot(probs, v)
        visit(h)
    o[pl.ds(start, TOK)] = pad(acc[...])


def seq_rows(t, s):
    return t[TOK * s:TOK * s + SEQ]


def seq_tile(s):
    return pl.ds(TOK * s, TOK)


FRONT_PLAN = {"qkv": ((0, 0, 1), (1, 1, 5), (2, 5, 8)), 2: ((O, 8, 9),), "end": ((O + 1, 9, None),)}


def front_kernel(x, w, b, vec, up_src, qkv, h1, o, att, h2, up, rows, acc, *sems):
    hosted = Background(Gather(WIDE, up_src, up, *sems).steps(), FRONT_PLAN)
    j = pl.program_id(0)
    at_step(0)(enter)
    hosted.visit("qkv")

    @at_step(0)
    def _():
        for s in SEQ_PAIR:
            xhat, _ = norm_stats(x[s].astype(F32))
            h1[seq_tile(s)] = pad(xhat * row(vec, G1) + row(vec, C1))

    @pl.when(j < O)
    def _():
        t = (dot(h1[...], w[0]) + b[0]).astype(BF16)
        qkv[0] = t
        rows[j] = t

    pl.when(j >= O)(lambda: attention(j - O, rows, o, acc, hosted.visit))

    @at_step(O + LAST_SEQ)
    def _():
        a = dot(o[...], w[0]) + row(vec, BO)
        att[...] = a
        for s in SEQ_PAIR:
            xhat, _ = norm_stats(x[s].astype(F32) + row(vec, S1) * seq_rows(a, s))
            h2[seq_tile(s)] = pad(xhat * row(vec, G2) + row(vec, C2))

    hosted.visit("end")


def upto(n):
    return lambda j: jnp.minimum(j, n)


def front_call(x, w_attn, b_qkv, vec, up, collective_id):
    return pl.pallas_call(
        front_kernel, grid=(O + PAIR,),
        out_shape=(sds(BF16, O, TT, D), sds(BF16, TT, D), sds(BF16, TT, D), sds(F32, TT, D), sds(BF16, TT, D),
                   sds(BF16, *Gather.shape(WIDE))),
        in_specs=[whole(*SEQS), along(0, 1, D, D, index=upto(O)), along(0, 1, 1, D, index=upto(V)), whole(8, D), ANY],
        out_specs=(along(0, 1, TT, D, index=upto(V)),) + (whole(TT, D),) * SIDE + (ANY,),
        scratch_shapes=[pltpu.VMEM((O, TT, D), BF16), pltpu.VMEM((SEQ, D), F32)] + Gather.semaphores(),
        compiler_params=comm_params(collective_id), name="front",
    )(x, w_attn, b_qkv, vec, up)


def w_out_block():
    return pl.BlockSpec((1, D, D), lambda j: (O, 0, 0), pipeline_mode=pl.Buffered(1))


TILES = FF // HALF
OWN_BODY = BODY * len(SEQ_PAIR)
TAILS = ROWS - TAIL * PAIR * len(SEQ_PAIR)


def put_rows(ref, tail, s, t):
    ref[pl.ds(BODY * s, BODY)] = t[:BODY]
    ref[pl.ds(tail + TAIL * s, TAIL)] = t[BODY:]


DOWN_PLAN = {"start": ((0, 0, 1),), "end": ((1, 1, 5), (3, 5, 8), (5, 8, 9), (TILES + 4, 9, 12), (2 * TILES - 1, 12, None))}


def mlp_in_kernel(h2, gz, w_up, b_up, vec, src, act, slope, d_down, down, a_rows, b_rows, b_away, *sems):
    a_sems, b_sems, sems = sems[:PAIR], sems[PAIR:2 * PAIR], sems[2 * PAIR:]
    hosted = Background(Gather(DOWN, src, down, *sems).steps(), DOWN_PLAN)
    j = pl.program_id(0)
    away = Push(b_away, OWN_BODY, b_rows, b_sems, 0)
    tile = lambda n: Push(a_rows.at[n], TAILS, a_rows.at[n], a_sems, n)
    at_step(0)(enter)
    hosted.visit("start")

    @at_step(0)
    def _():
        first = Torus().at["c"] == 0
        for s in SEQ_PAIR:
            d = pad(gz[s].astype(F32) * row(vec, S2))
            left, right = d[:, :HALF], d[:, D - HALF:]
            put_rows(b_rows, TAILS, s, jnp.where(first, left, right))
            put_rows(b_away, OWN_BODY, s, jnp.where(first, right, left))

    at_step(1)(away.start)
    for n in range(TILES):
        at_step(n + 1)(tile(n).start)

    @pl.when(j < TILES)
    def _():
        u = dot(h2[...], w_up[0]) + b_up[0]
        phi = 0.5 * (1.0 + lax.erf(u * math.sqrt(0.5)))
        slope[...] = phi + u * (jnp.exp(-0.5 * u * u) * math.sqrt(0.5 / math.pi))
        place = lax.rem(lax.broadcasted_iota(jnp.int32, (TT, 1), 0), TOK)
        a = only(place < SEQ, u * phi).astype(BF16)
        act[...] = a
        for s in SEQ_PAIR:
            put_rows(a_rows.at[j], TAILS, s, a[TOK * s:TOK * s + TOK])

    at_step(TILES)(away.wait)
    for n in range(TILES):
        at_step(TILES + n)(tile(n).wait)

    @pl.when(j >= TILES)
    def _():
        d_down[...] = dot_tn(a_rows[j - TILES], b_rows[...])

    hosted.visit("end")

    @at_step(2 * TILES - 1)
    def _():
        away.finish()
        for n in range(TILES):
            tile(n).finish()


def mlp_in_call(h2, gz, w_up, b_up, vec, down, collective_id):
    low = lambda j: jnp.minimum(j, TILES - 1)
    high = lambda j: jnp.maximum(j - TILES, 0)
    return pl.pallas_call(
        mlp_in_kernel, grid=(2 * TILES,),
        out_shape=(sds(BF16, TT, FF), sds(F32, TT, FF), sds(F32, FF, HALF), sds(BF16, *Gather.shape(DOWN))),
        in_specs=[whole(TT, D), whole(*SEQS), up_tile(low), along(0, 1, 1, HALF, index=low), whole(8, D), ANY],
        out_specs=(along(1, TT, HALF, index=low), along(1, TT, HALF, index=low),
                   along(0, HALF, HALF, index=high), ANY),
        scratch_shapes=[pltpu.VMEM((TILES, ROWS, HALF), BF16), pltpu.VMEM((ROWS, HALF), BF16),
                        pltpu.VMEM((PAIR * TOK, HALF), BF16)] + Push.semaphores(TILES) + Push.semaphores(1) +
        Gather.semaphores(),
        compiler_params=comm_params(collective_id), name="mlp_in",
    )(h2, gz, w_up, b_up.reshape(TILES, 1, HALF), vec, down)


def up_tile(index=lambda j: j):
    return pl.BlockSpec((1, D, HALF), lambda j: (index(j) // PAIR, 0, index(j) % PAIR))


MLP_PLACES = (("end", 0), ("end", 2), ("end", 3), ("end", TILES - 1))


def mlp_out_kernel(act, slope, gz, w_up, w_down, vec, part, d_pre, db_up, mlp, d_h2, sums, dm, *scratch):
    hosted = Pipeline(MLP_PLACES, First(DOWN, 0, part, sums, *scratch))
    at_step(0)(enter)
    hosted.visit("start")

    @at_step(0)
    def _():
        for s in SEQ_PAIR:
            dm[seq_tile(s)] = pad(gz[s].astype(F32) * row(vec, S2))

    accumulate(mlp, dot(act[...], w_down[...]))
    d = dot_nt(dm[...], w_down[...]) * slope[...]
    db_up[0] = col_sum(d)
    d = d.astype(BF16)
    d_pre[0, 0] = d
    accumulate(d_h2, dot_nt(d, w_up[0]))
    hosted.visit("end")


def mlp_out_call(act, slope, gz, w_up, w_down, vec, part, collective_id):
    return pl.pallas_call(
        mlp_out_kernel, grid=(TILES,),
        out_shape=(sds(BF16, PAIR, SIDE, TT, HALF), sds(F32, TILES, 1, HALF), sds(F32, TT, D), sds(F32, TT, D),
                   First.sums(DOWN)),
        in_specs=[along(1, TT, HALF), along(1, TT, HALF), whole(*SEQS), up_tile(), along(0, HALF, D), whole(8, D), ANY],
        out_specs=(pl.BlockSpec((1, 1, TT, HALF), lambda j: (j % PAIR, j // PAIR, 0, 0)), along(0, 1, 1, HALF),
                   whole(TT, D), whole(TT, D), ANY),
        scratch_shapes=[pltpu.VMEM((TT, D), BF16)] + First.scratch(DOWN),
        compiler_params=comm_params(collective_id), name="mlp_out",
    )(act, slope, gz, w_up, w_down, vec, part)


def halves_of(t):
    t = pad(t)
    return t[:, :HALF], jnp.concatenate([t[:, HALF:], jnp.zeros((TOK, QCOLS - D), BF16)], axis=1)


def mid(mlp, d_h2, att, x, gz, vec, w_out, z, g_res, d_att, d_o, sums, da_rows):
    a = att[:SEQ]
    y = x[0].astype(F32) + row(vec, S1) * a
    m = mlp[:SEQ] + row(vec, B2)
    g = gz[0].astype(F32)
    z[0] = (y + row(vec, S2) * m).astype(BF16)
    xhat, rstd = norm_stats(y)
    dh = d_h2[:SEQ]
    gr = g + norm_back(xhat, rstd, dh * row(vec, G2))
    g_res[:SEQ] = gr
    da = gr * row(vec, S1)
    terms = (da, gr * a, dh * xhat, dh, g * row(vec, S2), g * m)
    accumulate(sums, jnp.concatenate([jnp.zeros((BO, D), F32)] + [col_sum(t) for t in terms], axis=0))
    for i, t in enumerate(halves_of(da)):
        d_att[i] = t
    da_rows[pl.ds(pl.multiple_of(pl.program_id(0) * TOK, TAIL), TOK)] = pad(da)

    @at_step(LAST_SEQ)
    def _():
        d_o[...] = dot_nt(da_rows[...], w_out[0]).astype(BF16)


def attention_back(qkv, d_o, d_qkv, db, acc, visit):
    acc[...] = jnp.zeros_like(acc)
    for h in range(HEADS):
        lanes, mask = window(h)
        q, k, v = (only(mask, qkv[i, :SEQ, lanes]) for i in (Q, K, V))
        do = only(mask, d_o[:SEQ, lanes])
        scores = dot_nt(k, q) * SCALE
        e = jnp.exp(scores - jnp.max(scores, axis=0, keepdims=True))
        probs = e * (1.0 / col_sum(e))
        acc[V, :, lanes] += dot(probs.astype(BF16), do)
        dp = dot_nt(v, do)
        ds = probs * (dp - col_sum(dp * probs))
        ds = (ds * SCALE).astype(BF16)
        acc[K, :, lanes] += dot(ds, q)
        acc[Q, :, lanes] += dot_tn(ds, k)
        visit(h)
    accumulate(db, jnp.concatenate([col_sum(acc[i]) for i in (Q, K, V)], axis=0))
    for n in (Q, K, V):
        for i, t in enumerate(halves_of(acc[n])):
            d_qkv[i, n] = t


PER = HALF // STEP


class WideGrads:
    def __init__(self, a, a_of, b, out, base, a_rows, a_cols, b_rows, *sems):
        self.a, self.a_of, self.b, self.out, self.base = a, a_of, b, out, base
        self.a_rows, self.a_cols, self.b_rows = a_rows, a_cols, b_rows
        self.a_sems, self.b_sems = sems[:C], sems[C:]

    @staticmethod
    def scratch(inputs):
        return ([pltpu.VMEM((inputs, ROWS, D), BF16), pltpu.VMEM((inputs, D, ROWS), BF16),
                 pltpu.VMEM((SIDE, ROWS, HALF), BF16)] + Exchange.semaphores(inputs) + Exchange.semaphores(SIDE))

    def input(self, i):
        return Exchange(self.a[i], self.a[i], self.a_rows.at[i], self.a_sems, (i,))

    def cotangent(self, n):
        c = Torus().at["c"]
        b = self.b[n]
        return Exchange(b(c), b(1 - c), self.b_rows.at[n], self.b_sems, (n,))

    def new_input(self, n):
        return n == 0 or self.a_of[n] != self.a_of[n - 1]

    def begin(self):
        for n in range(SIDE):
            if self.new_input(n):
                self.input(self.a_of[n]).start()
            self.cotangent(n).start()

    def step(self):
        j = pl.program_id(0)
        for n in range(SIDE):
            @at_step(self.base + PER * n)
            def _():
                if self.new_input(n):
                    i = self.a_of[n]
                    self.input(i).wait()
                    self.a_cols[i] = self.a_rows[i].T
                self.cotangent(n).wait()

        @pl.when(j >= self.base)
        def _():
            n = lax.div(j - self.base, PER)
            cols = pl.ds(pl.multiple_of(lax.rem(j - self.base, PER) * STEP, STEP), STEP)
            i = 0 if len(self.a) == 1 else lax.div(n, O)
            self.out[0] = dot(self.a_cols[i], self.b_rows[n, :, cols])

    def finish(self):
        for i in range(len(self.a)):
            self.input(i).finish()
        for n in range(SIDE):
            self.cotangent(n).finish()


def grads_block(base):
    def index(j):
        n = jnp.maximum(j - base, 0)
        return n // PER, 0, n % PER

    return pl.BlockSpec((1, D, STEP), index)


GRAD_STEPS = PER * SIDE


def tok_block():
    return along(0, TOK, D, index=upto(LAST_SEQ))


def seq_block():
    return along(0, 1, SEQ, D, index=upto(LAST_SEQ))


MID_PLACES = (("end", 0), ("end", 4), ("end", 10), ("end", LAST_SEQ + GRAD_STEPS))


def mid_kernel(*refs):
    refs = list(refs)
    take = lambda n: [refs.pop(0) for _ in range(n)]
    ins, (h2, d_pre, part, acc), outs, (d_up, sums, result) = take(7), take(4), take(5), take(3)
    outs.append(refs.pop(0))
    grads = WideGrads((h2,), (0,) * SIDE, [lambda c, i=i: d_pre.at[c, i] for i in range(SIDE)], d_up, SEQS[0],
                      *take(len(WideGrads.scratch(1))))
    first = First(DOWN, 1, part, sums, *take(len(First.scratch(DOWN))))
    hosted = Pipeline(MID_PLACES, first, Rest(DOWN, acc, result, *refs))
    at_step(0)(enter)
    hosted.visit("start")
    at_step(0)(grads.begin)
    pl.when(pl.program_id(0) < SEQS[0])(lambda: mid(*ins, *outs))
    grads.step()
    hosted.visit("end")
    at_step(LAST_SEQ + GRAD_STEPS)(grads.finish)


def mid_call(mlp, d_h2, att, x, gz, vec, w_attn, h2, d_pre, part, acc, collective_id):
    return pl.pallas_call(
        mid_kernel, grid=(SEQS[0] + GRAD_STEPS,),
        out_shape=(sds(BF16, *SEQS), sds(F32, TT, D), sds(BF16, PAIR, TT, HALF), sds(BF16, TT, D), sds(F32, 8, D),
                   sds(F32, SIDE, D, HALF), First.sums(DOWN), Rest.sums(DOWN)),
        in_specs=[tok_block()] * O + [seq_block()] * PAIR + [whole(8, D), w_out_block()] + [ANY] * SIDE,
        out_specs=(seq_block(), tok_block(), along(1, PAIR, TOK, HALF, index=upto(LAST_SEQ)), whole(TT, D), whole(8, D),
                   grads_block(SEQS[0]), ANY, ANY),
        scratch_shapes=[pltpu.VMEM((TT, D), BF16)] + WideGrads.scratch(1) + First.scratch(DOWN) + Rest.scratch(DOWN),
        compiler_params=comm_params(collective_id), name="mid",
    )(mlp, d_h2, att, x, gz, vec, w_attn, h2, d_pre, part, acc)


ATTN_PLACES = ((6, 0), (1, LAST_SEQ), (11, LAST_SEQ), ("end", LAST_SEQ))


def attn_back_kernel(qkv, d_o, part, acc_down, result_down, d_qkv, db, sums, result, total, acc, *scratch):
    n, m = len(First.scratch(WIDE)), len(Rest.scratch(DOWN))
    hosted = Pipeline(ATTN_PLACES, First(WIDE, 0, part, sums, *scratch[:n]),
                      Rest(DOWN, acc_down, result, *scratch[n:n + m]), Spread(DOWN, result_down, total, *scratch[n + m:]))
    at_step(0)(enter)
    hosted.visit("start")
    attention_back(qkv, d_o, d_qkv, db, acc, hosted.visit)
    hosted.visit("end")


def attn_back_call(qkv, d_o, part, acc_down, result_down, collective_id):
    return pl.pallas_call(
        attn_back_kernel, grid=SEQS[:1],
        out_shape=(sds(BF16, PAIR, O, TT, HALF), sds(F32, O, D), First.sums(WIDE), Rest.sums(DOWN), Spread.sums(DOWN)),
        in_specs=[along(1, O, TOK, D), tok_block()] + [ANY] * O,
        out_specs=(along(2, PAIR, O, TOK, HALF), whole(O, D)) + (ANY,) * O,
        scratch_shapes=[pltpu.VMEM((O, SEQ, D), F32)] + First.scratch(WIDE) + Rest.scratch(DOWN) + Spread.scratch(),
        compiler_params=comm_params(collective_id), name="attn_back",
    )(qkv, d_o, part, acc_down, result_down)


IN_STEPS = PAIR * O
IN_PLACES = (("end", 1), ("end", IN_STEPS - 1), ("end", IN_STEPS + SIDE), ("end", IN_STEPS + GRAD_STEPS - 1))


def in_back_kernel(*refs):
    refs = list(refs)
    take = lambda n: [refs.pop(0) for _ in range(n)]
    (d_half, w, x, g_res, vec), (h1, o, d_qkv, d_att, part, acc_up, result_down) = take(5), take(7)
    (dx, sums, d_attn), outs, acc = take(3), take(3), refs.pop(0)
    b = [lambda c, i=i: d_qkv.at[c, i] for i in range(O)] + [lambda c: d_att.at[c]]
    grads = WideGrads((h1, o), (0,) * O + (1,), b, d_attn, IN_STEPS, *take(len(WideGrads.scratch(2))))
    first = First(WIDE, 1, part, outs[0], *take(len(First.scratch(WIDE))))
    rest = Rest(WIDE, acc_up, outs[1], *take(len(Rest.scratch(WIDE))))
    hosted = Pipeline(IN_PLACES, first, rest, Spread(DOWN, result_down, outs[2], *refs))
    at_step(0)(enter)
    hosted.visit("start")
    at_step(0)(grads.begin)

    @pl.when(pl.program_id(0) < IN_STEPS)
    def _():
        accumulate(acc, dot_nt(d_half[0, 0], w[0]))

    @at_step(IN_STEPS - 1)
    def _():
        rows = jnp.zeros((BO, D), F32)
        for s in SEQ_PAIR:
            xhat, rstd = norm_stats(x[s].astype(F32))
            tokens = pl.ds(TOK * s, SEQ)
            dh = acc[tokens]
            rows = rows + jnp.concatenate([col_sum(dh * xhat), col_sum(dh)], axis=0)
            dx[s] = (g_res[tokens] + norm_back(xhat, rstd, dh * row(vec, G1))).astype(BF16)
        sums[...] = rows

    grads.step()
    hosted.visit("end")
    at_step(IN_STEPS + GRAD_STEPS - 1)(grads.finish)


def in_back_call(d_qkv, w_attn, x, g_res, vec, h1, o, d_att, part, acc_up, result_down, collective_id):
    low = upto(IN_STEPS - 1)
    return pl.pallas_call(
        in_back_kernel, grid=(IN_STEPS + GRAD_STEPS,),
        out_shape=(sds(BF16, *SEQS), sds(F32, BO, D), sds(F32, SIDE, D, HALF), First.sums(WIDE), Rest.sums(WIDE),
                   Spread.sums(DOWN)),
        in_specs=[pl.BlockSpec((1, 1, TT, HALF), lambda j: (low(j) % PAIR, low(j) // PAIR, 0, 0)), up_tile(low),
                  whole(*SEQS), whole(TT, D), whole(8, D)] + [ANY] * 7,
        out_specs=(whole(*SEQS), whole(BO, D), grads_block(IN_STEPS), ANY, ANY, ANY),
        scratch_shapes=[pltpu.VMEM((TT, D), F32)] + WideGrads.scratch(2) + First.scratch(WIDE) + Rest.scratch(WIDE) +
        Spread.scratch(),
        compiler_params=comm_params(collective_id), name="in_back",
    )(d_qkv, w_attn, x, g_res, vec, h1, o, d_qkv, d_att, part, acc_up, result_down)


BQ, BU, VEC = 3 * D // 32, 3 * D // 32 + FF // 32, 3 * D // 32 + FF // 32 + 8 * OWN
DEVICES = 32


def pair_swap(a):
    return lax.ppermute(a, "fsdp", [(i, i ^ 1) for i in range(DEVICES)])


def by_core(first, a, b):
    return jnp.where(first, a, b), jnp.where(first, b, a)


def my_pieces(shards, first):
    w_qkv, b_qkv, w_out, w_up, b_up, w_down, vec_params = shards
    x = lax.axis_index("rep")
    small = jnp.concatenate([b_qkv, b_up, vec_params.reshape(-1)])
    small = jnp.pad(small, (0, OWN * LANES - VEC)).reshape(OWN, LANES)
    attn = lax.dynamic_slice_in_dim(jnp.concatenate([w_qkv, w_out], axis=1), x * D, D, 1)
    attn = jnp.concatenate([attn, small], axis=1)
    up = lax.dynamic_slice_in_dim(w_up, x * QCOLS, QCOLS, 1)
    wide = jnp.stack([attn, up]).astype(BF16)
    mine, theirs = by_core(first, wide[..., :HALF], wide[..., HALF:])
    theirs = pair_swap(theirs)
    piece = jnp.concatenate(by_core(first, mine, theirs), axis=1)
    down = lax.dynamic_slice_in_dim(w_down, x * 48, 48, 0).astype(BF16).reshape(3, 16, D)
    return piece[0], piece[1], down


def small_params(w_attn):
    small = w_attn[0, :, D:].astype(F32).reshape(DEVICES, OWN * LANES)
    vec = small[:, BU:VEC].reshape(DEVICES, 8, OWN).transpose(1, 0, 2).reshape(8, D)
    return small[:, :BQ].reshape(O, 1, D), small[:, BQ:BU].reshape(FF), vec


def small_grads(db_qkv, db_up, sums, core):
    vec = sums.reshape(8, DEVICES, OWN).transpose(1, 0, 2).reshape(DEVICES, VEC - BU)
    small = jnp.concatenate([db_qkv.reshape(DEVICES, BQ), db_up.reshape(DEVICES, BU - BQ), vec], axis=1)
    small = (small + pair_swap(small)) * core.astype(F32)
    return jnp.pad(small, ((0, 0), (0, OWN * LANES - VEC))).reshape(D, LANES)


def final_rows(halves, first):
    total = jnp.stack(halves, axis=2)
    keep, give = by_core(first, total[..., :OWN, :], total[..., OWN:, :])
    pair = jnp.stack(by_core(first, keep, pair_swap(give)), axis=1)
    return pair.transpose(4, 0, 1, 2, 3, 5).reshape(OWN, SIDE, QCOLS)


def final_down(halves, first):
    down = jnp.concatenate(halves, axis=-1).reshape(FF // 16, HALF)
    keep, give = by_core(first, down[:FF // DEVICES], down[FF // DEVICES:])
    left, right = by_core(first, keep, pair_swap(give))
    return jnp.concatenate([left, right[:, 2 * HALF - D:]], axis=1)


def device_step(x, gz, *shards):
    core = lax.rem(lax.axis_index("fsdp"), PAIR)
    first = core == 0
    attn, up, down = my_pieces(shards, first)
    w_attn = torus_gather(WIDE, attn, 0).reshape(SIDE, D, QCOLS)
    b_qkv, b_up, vec = small_params(w_attn)
    qkv, h1, o, att, h2, w_up = front_call(x, w_attn, b_qkv, vec, up, 1)
    w_up = w_up.reshape(SIDE, D, QCOLS)
    act, slope, part, w_down = mlp_in_call(h2, gz, w_up, b_up, vec, down, 2)
    part = part.reshape((SIDE,) * 3 + (C, 32, HALF))
    d_pre, db_up, mlp, d_h2, acc0 = mlp_out_call(act, slope, gz, w_up, w_down.reshape(FF, D), vec, part, 3)
    z, g_res, d_att, d_o, sums, part, acc1, result0 = mid_call(mlp, d_h2, att, x, gz, vec, w_attn, h2, d_pre, part, acc0, 4)
    part = part.reshape((SIDE,) * 3 + (CHIP, HALF))
    d_qkv, db_qkv, acc0, result1, down0 = attn_back_call(qkv, d_o, part, acc1, result0, 5)
    dx, in_sums, part, acc1, result0, down1 = in_back_call(d_qkv, w_attn, x, g_res, vec, h1, o, d_att, part, acc0, result1, 6)
    small = small_grads(db_qkv, db_up, jnp.concatenate([in_sums, sums[BO:]], axis=0), core)
    part = part.at[0, :, HALF - LANES:].add(small).reshape((SIDE,) * 3 + (CHIP, HALF))
    attn0, attn1, up1, up0 = last_scatter(part, acc1, result0, 7)
    g_up = final_rows((up0, up1), first).reshape(OWN, FF)
    attn = final_rows((attn0, attn1), first)
    small = attn[:, 0, D:].reshape(OWN * LANES)
    return (z, dx, attn[:, :O, :D].reshape(OWN, O * D), small[:BQ], attn[:, O, :D], g_up, small[BQ:BU],
            final_down((down0, down1), first), small[BU:VEC].reshape(8, OWN))


def solution(mesh):
    batch = P(("rep", "fsdp"), None, None)
    rows, flat, cols = P("fsdp", None), P("fsdp"), P(None, "fsdp")
    shards = (rows, flat, rows, rows, flat, rows, cols)
    return jax.shard_map(device_step, mesh=mesh, in_specs=(batch, batch) + shards,
                         out_specs=(batch, batch) + shards, check_vma=False)
```

```python
import functools
import math

import jax
import jax.numpy as jnp
from jax import lax
from jax.experimental import pallas as pl
from jax.experimental.pallas import tpu as pltpu
from jax.sharding import PartitionSpec as P

HEADS = 16
LN_EPS = 1e-5
D = 1408
FF = 6144
SEQ = 257
HEAD = D // HEADS
SCALE = HEAD ** -0.5
QCOLS = 1536
HALF = 768
OWN = 44
CHIP = 2 * OWN
LANES = 128
DEVICES = 32
F32 = jnp.float32
BF16 = jnp.bfloat16
VMEM_LIMIT = 66 * 1000 * 1000
G1, C1, BO, S1, G2, C2, B2, S2 = range(8)
Q, K, V, O = range(4)
SEQS = (2, SEQ, D)
LAST_SEQ = SEQS[0] - 1
SEQ_PAIR = range(SEQS[0])
TAIL = 16
BODY = SEQ - 1
TOK = BODY + TAIL
TT = 2 * TOK
ROWS = 4 * TOK
STEP = 256


def sds(dtype, *shape):
    return jax.ShapeDtypeStruct(shape, dtype)


MESH_ID = pl.DeviceIdType.MESH
SIDE = 4
SUB = 8
PAIR = 2
C = 3
COLOURS = range(C)
COLOUR_DIMS = ("xyz", "yzx", "zxy")
FIRST, SECOND, THIRD, LAST = range(4)
WAYS = range(PAIR)
NEAR, FAR, ADDED = 0, 2, 4
WIDE, DOWN = "wide", "down"
ANY = pl.BlockSpec(memory_space=pl.ANY)
ALL = slice(None)


def duo(m):
    return pl.ds(PAIR * m, PAIR)


def toward(m):
    return 1 - PAIR * (m % PAIR)


class Torus:
    def __init__(self):
        f = lax.axis_index("fsdp")
        self.at = {"x": lax.axis_index("rep"), "z": lax.div(f, SIDE * PAIR), "y": lax.rem(lax.div(f, PAIR), SIDE),
                   "c": lax.rem(f, PAIR)}

    def shift(self, dim, by):
        return lax.rem(self.at[dim] + (SIDE + by), SIDE)

    def device(self, **moved):
        p = {**self.at, **moved}
        return (p["x"], (p["z"] * SIDE + p["y"]) * PAIR + p["c"])

    def neighbour(self, dim, by):
        return self.device(**{dim: self.shift(dim, by)})

    def partner(self):
        return self.device(c=1 - self.at["c"])


def enter():
    me = Torus()
    barrier = pltpu.get_barrier_semaphore()
    others = [me.neighbour(d, toward(m)) for d in COLOUR_DIMS[0] for m in WAYS] + [me.partner()]
    for other in others:
        pl.semaphore_signal(barrier, device_id=other, device_id_type=MESH_ID)
    pl.semaphore_wait(barrier, len(others))


def remote(src, dst, sems, slot, device):
    return pltpu.make_async_remote_copy(src_ref=src, dst_ref=dst, send_sem=sems[0].at[slot], recv_sem=sems[1].at[slot],
                                        device_id=device, device_id_type=MESH_ID)


class Gather:
    def __init__(self, kind, src, dst, hop_send, hop_recv, push_send, push_recv, local):
        self.kind, self.src, self.dst, self.local = kind, src, dst, local
        self.hops, self.pushes = (hop_send, hop_recv), (push_send, push_recv)
        self.cols, self.cut = (256, 128) if kind == WIDE else (D, HALF)

    @staticmethod
    def semaphores():
        dma = pltpu.SemaphoreType.DMA
        return [dma((C, C, ADDED))] * PAIR + [dma((C, ADDED + 1))] * PAIR + [dma((C,))]

    @staticmethod
    def shape(kind):
        return (SIDE,) * 3 + (CHIP, QCOLS) if kind == WIDE else (SIDE, SIDE, PAIR, SIDE, C, 16, D)

    def source(self, k):
        return self.src.at[:, pl.ds(self.cols * k, self.cols)] if self.kind == WIDE else self.src.at[k]

    def piece(self, me, k, s, v, half=None):
        dims = COLOUR_DIMS[k]
        at = {**me.at, **{d: ALL for d in dims[:s]}, dims[s]: v}
        off, width = 0, self.cols
        if half is not None and s == FIRST:
            off, width = self.cut * half, (self.cut, self.cols - self.cut)[half]
        elif half is not None:
            at[dims[0]] = duo(half)
        if self.kind == WIDE:
            cols = pl.ds(pl.multiple_of(at["c"] * HALF + self.cols * k + off, 128), width)
            return self.dst.at[at["x"], at["z"], at["y"], :, cols]
        return self.dst.at[at["z"], at["y"], at["c"], at["x"], k, :, pl.ds(off, width)]

    def hop(self, k, s, m):
        me = Torus()
        dim = COLOUR_DIMS[k][s]
        by = toward(m)
        if m < FAR:
            ref = self.piece(me, k, s, me.at[dim])
        else:
            ref = self.piece(me, k, s, me.shift(dim, -by), m - FAR)
        src = self.source(k) if s == FIRST and m < FAR else ref
        return remote(src, ref, self.hops, (k, s, m), me.neighbour(dim, by))

    def push(self, k, n):
        me = Torus()
        dim = COLOUR_DIMS[k][THIRD]
        if n < FAR:
            ref = self.piece(me, k, THIRD, me.shift(dim, -toward(n)))
        elif n < ADDED:
            ref = self.piece(me, k, THIRD, me.shift(dim, FAR), n - FAR)
        else:
            ref = self.piece(me, k, THIRD, me.at[dim])
        return remote(ref, ref, self.pushes, (k, n), me.partner())

    def own(self, k):
        me = Torus()
        return pltpu.make_async_copy(self.source(k), self.piece(me, k, FIRST, me.at[COLOUR_DIMS[k][FIRST]]), self.local.at[k])

    def launch(self, s):
        for k in COLOURS:
            for m in WAYS:
                self.hop(k, s, m).start()
            if s == THIRD:
                self.push(k, ADDED).start()

    def relay(self, k, s):
        for m in WAYS:
            self.hop(k, s, m).wait_recv()
            self.hop(k, s, FAR + m).start()
            if s == THIRD:
                self.push(k, m).start()

    def settle(self, s):
        for k in COLOURS:
            for m in WAYS:
                self.hop(k, s, FAR + m).wait_recv()
                if s == THIRD:
                    self.push(k, FAR + m).start()
            if s == FIRST:
                self.own(k).wait()
        if s < THIRD:
            self.launch(s + 1)

    def begin(self):
        for k in COLOURS:
            self.own(k).start()
        self.launch(FIRST)

    def finish(self):
        for k in COLOURS:
            for s in COLOURS:
                for m in range(ADDED):
                    self.hop(k, s, m).wait_send()
            for n in range(ADDED + 1):
                self.push(k, n).wait()

    def steps(self):
        out = [self.begin]
        for s in COLOURS:
            out += [functools.partial(self.relay, k, s) for k in COLOURS] + [functools.partial(self.settle, s)]
        return out + [self.finish]


def add_into(total, *others):
    lead = total.shape[:-2]

    def body(i, carry):
        idx = []
        for n in reversed(lead):
            idx.insert(0, lax.rem(i, n))
            i = lax.div(i, n)
        value = total[tuple(idx)]
        for other in others:
            value = value + other[tuple(idx)]
        total[tuple(idx)] = value
        return carry

    lax.fori_loop(0, math.prod(lead), body, 0)


class Ring:
    def __init__(self, s, bands, terms, passed, relay, landing, send, recv):
        self.s, self.bands, self.terms, self.passed, self.relay, self.landing = s, bands, terms, passed, relay, landing
        self.sems = (send, recv)

    def zone(self, k, way, half):
        if self.s == THIRD:
            return self.landing.at[k, way, self.bands.cuts(k)[half]]
        return self.bands.rows(self.landing.at[k, way, duo(half)], k)

    def carried(self, ref, k, way):
        if self.s == THIRD:
            return ref.at[k, way, pl.ds(0, self.bands.cuts(k)[way].size)]
        return self.bands.rows(ref.at[k, way], k)

    def hop(self, k, m):
        me = Torus()
        dim = COLOUR_DIMS[k][self.s]
        way, by = m % PAIR, toward(m)
        if m < FAR:
            src, dst = self.terms(k, me.shift(dim, FAR), way), self.carried(self.relay, k, way)
        elif m < ADDED:
            src, dst = self.terms(k, me.shift(dim, by), 1 - way), self.zone(k, way, 1 - way)
        else:
            src, dst = self.carried(self.passed, k, way), self.zone(k, way, way)
        return remote(src, dst, self.sems, (k, m), me.neighbour(dim, by))

    def start(self, k, base):
        for m in WAYS:
            self.hop(k, base + m).start()

    def arrived(self, k, base):
        for m in WAYS:
            self.hop(k, base + m).wait_recv()

    def finish(self):
        for k in COLOURS:
            for m in range(ADDED + PAIR):
                self.hop(k, m).wait_send()

    @staticmethod
    def semaphores():
        return [pltpu.SemaphoreType.DMA((C, ADDED + PAIR))] * PAIR


UNIT = 32
BANDS = {WIDE: ((0, 24), (24, UNIT), (56, UNIT)), DOWN: ((0, UNIT), (UNIT, UNIT), (2 * UNIT, UNIT))}
ORDERS = {WIDE: "xzy", DOWN: "zyx"}


class Bands:
    def __init__(self, kind, half=None):
        self.order, self.bands = ORDERS[kind], BANDS[kind]
        self.width = HALF if half is None else HALF // PAIR
        self.cols = pl.ds(self.width * (half or 0), self.width)

    def band(self, k):
        return pl.ds(*self.bands[k])

    def rows(self, ref, k):
        return ref.at[(ALL,) * (len(ref.shape) - PAIR) + (pl.ds(0, self.bands[k][1]),)]

    def cuts(self, k):
        rows = self.bands[k][1]
        cut = (rows // SUB + 1) // PAIR * SUB
        return pl.ds(0, cut), pl.ds(cut, rows - cut)

    def rest(self, k):
        return [d for d in self.order if d != COLOUR_DIMS[k][FIRST]]

    def units(self, *lead):
        return lead + (UNIT, self.width)

    def vmem(self, *lead):
        return pltpu.VMEM(self.units(*lead), F32)

    def sums(self):
        return sds(F32, *self.units(C, SIDE, SIDE))

    def result(self):
        return sds(F32, *self.units(C))

    def total(self):
        return sds(F32, *self.units(SIDE, C))

    def first(self):
        relays = [self.vmem(C, PAIR, PAIR, SIDE)] * PAIR
        dma = pltpu.SemaphoreType.DMA
        return [self.vmem(C, SIDE, SIDE), *relays, self.vmem(C, PAIR, SIDE, SIDE), *Ring.semaphores(), dma((C, C)), dma((C,))]

    def later(self):
        dma = pltpu.SemaphoreType.DMA
        return [self.vmem(C, SIDE, SIDE), self.vmem(C, PAIR, PAIR), self.vmem(C, PAIR, SIDE),
                pltpu.VMEM((C, PAIR, UNIT // PAIR, self.width), F32), self.vmem(C, PAIR),
                *Ring.semaphores(), *Ring.semaphores(), dma((C,)), dma((C,))]


class First:
    def __init__(self, bands, part, acc, own, passed, relay, landing, send, recv, load, store):
        self.bands, self.part, self.acc, self.own_all, self.passed = bands, part, acc, own, passed
        self.relay_in, self.landing, self.load_sem, self.store_sem = relay, landing, load, store
        self.ring = Ring(FIRST, bands, self.terms, passed, relay, landing, send, recv)

    def own(self, k):
        return self.bands.rows(self.own_all.at[k], k)

    def terms(self, k, v, half=None):
        b = self.bands
        at = {d: ALL for d in b.order}
        at[COLOUR_DIMS[k][FIRST]] = v
        if half is not None:
            at[b.rest(k)[0]] = duo(half)
        return self.part.at[tuple(at[d] for d in b.order) + (b.band(k), b.cols)]

    def load(self, k, m):
        me = Torus()
        dim = COLOUR_DIMS[k][FIRST]
        if m in WAYS:
            src, dst = self.terms(k, me.shift(dim, toward(m)), m), self.ring.carried(self.passed, k, m)
        else:
            src, dst = self.terms(k, me.at[dim]), self.own(k)
        return pltpu.make_async_copy(src, dst, self.load_sem.at[k, m])

    def store(self, k):
        return pltpu.make_async_copy(self.own(k), self.bands.rows(self.acc.at[k], k), self.store_sem.at[k])

    def near(self):
        for k in COLOURS:
            self.ring.start(k, NEAR)

    def far(self):
        for k in COLOURS:
            self.ring.start(k, FAR)
        for m in COLOURS:
            for k in COLOURS:
                self.load(k, m).start()

    def relay(self):
        for k in COLOURS:
            self.ring.arrived(k, NEAR)
            for m in WAYS:
                self.load(k, m).wait()
                add_into(self.ring.carried(self.passed, k, m), self.ring.carried(self.relay_in, k, m))
            self.ring.start(k, ADDED)

    def settle(self, then=None):
        for k in COLOURS:
            self.load(k, FAR).wait()
            for base in (FAR, ADDED):
                self.ring.arrived(k, base)
            add_into(self.own(k), *(self.bands.rows(self.landing.at[k, m], k) for m in WAYS))
            if then is None:
                self.store(k).start()
            else:
                then(k)

    def finish(self):
        self.ring.finish()
        if self.acc is not None:
            for k in COLOURS:
                self.store(k).wait()


class Rest:
    def __init__(self, bands, acc, result, own, relay2, in2, relay3, in3, *sems):
        self.bands, self.acc, self.own, self.result = bands, acc, own, result
        self.in2, self.in3, self.relay2, self.relay3, self.load_sem, self.store_sem = in2, in3, relay2, relay3, *sems[-2:]
        self.second = Ring(SECOND, bands, functools.partial(self.terms, acc), relay2, relay2, in2, *sems[:PAIR])
        self.third = Ring(THIRD, bands, self.final, relay3, relay3, in3, *sems[PAIR:2 * PAIR])

    def terms(self, ref, k, v, half=None):
        other = ALL if half is None else duo(half)
        first = self.bands.rest(k)[0] == COLOUR_DIMS[k][SECOND]
        return self.bands.rows(ref.at[(k, v, other) if first else (k, other, v)], k)

    def final(self, k, v, half=None):
        if half is None:
            return self.bands.rows(self.in2.at[k, 0, v], k)
        return self.in2.at[k, 0, v, self.bands.cuts(k)[half]]

    def load(self, k):
        return pltpu.make_async_copy(self.bands.rows(self.acc.at[k], k), self.bands.rows(self.own.at[k], k), self.load_sem.at[k])

    def store(self, k):
        rows = self.bands.rows
        return pltpu.make_async_copy(rows(self.in3.at[k, 0], k), rows(self.result.at[k], k), self.store_sem.at[k])

    def send(self, k):
        for base in (NEAR, FAR):
            self.second.start(k, base)

    def begin(self):
        for k in COLOURS:
            self.send(k)
        for k in COLOURS:
            self.load(k).start()

    def loaded(self):
        for k in COLOURS:
            self.load(k).wait()

    def relay(self):
        me = Torus()
        for k in COLOURS:
            self.second.arrived(k, NEAR)
            for m in WAYS:
                terms = self.terms(self.own, k, me.shift(COLOUR_DIMS[k][SECOND], toward(m)), m)
                add_into(self.second.carried(self.relay2, k, m), terms)
            self.second.start(k, ADDED)

    def settle(self):
        me = Torus()
        for k in COLOURS:
            for base in (FAR, ADDED):
                self.second.arrived(k, base)
            plus, minus = (self.bands.rows(self.in2.at[k, m], k) for m in WAYS)
            add_into(plus, minus, self.terms(self.own, k, me.at[COLOUR_DIMS[k][SECOND]]))
            for base in (NEAR, FAR):
                self.third.start(k, base)

    def relay_third(self):
        me = Torus()
        for k in COLOURS:
            self.third.arrived(k, NEAR)
            for m in WAYS:
                mine = self.third.carried(self.relay3, k, m)
                mine[...] += self.final(k, me.shift(COLOUR_DIMS[k][THIRD], toward(m)), m)[...]
            self.third.start(k, ADDED)

    def settle_third(self):
        me = Torus()
        for k in COLOURS:
            for base in (FAR, ADDED):
                self.third.arrived(k, base)
            plus, minus = (self.bands.rows(self.in3.at[k, m], k) for m in WAYS)
            plus[...] += minus[...] + self.final(k, me.at[COLOUR_DIMS[k][THIRD]])[...]
            if self.result is not None:
                self.store(k).start()

    def finish(self):
        self.second.finish()
        self.third.finish()
        if self.result is not None:
            for k in COLOURS:
                self.store(k).wait()

    def sums(self):
        return self.in3.at[:, 0]


class Spread:
    def __init__(self, bands, result, total, send, recv, local):
        self.bands, self.result, self.total, self.sems, self.local = bands, result, total, (send, recv), local

    @staticmethod
    def scratch():
        return [pltpu.SemaphoreType.DMA((C, ADDED))] * PAIR + [pltpu.SemaphoreType.DMA((C,))]

    def mine(self, k):
        return self.bands.rows(self.result.at[k], k)

    def place(self, k):
        return self.bands.rows(self.total.at[Torus().at["x"], k], k)

    def hop(self, k, m):
        me = Torus()
        by = toward(m)
        if m < FAR:
            src, dst = self.mine(k), self.place(k)
        else:
            dst = src = self.total.at[me.shift("x", -by), k, self.bands.cuts(k)[m - FAR]]
        return remote(src, dst, self.sems, (k, m), me.neighbour("x", by))

    def own(self, k):
        return pltpu.make_async_copy(self.mine(k), self.place(k), self.local.at[k])

    def begin(self):
        for k in COLOURS:
            self.own(k).start()
            for m in WAYS:
                self.hop(k, m).start()

    def forward(self):
        for k in COLOURS:
            for m in WAYS:
                self.hop(k, m).wait_recv()
                self.hop(k, FAR + m).start()

    def finish(self):
        for k in COLOURS:
            for m in WAYS:
                self.hop(k, FAR + m).wait_recv()
            self.own(k).wait()
            for m in range(ADDED):
                self.hop(k, m).wait_send()


def comm_params(collective_id):
    return pltpu.CompilerParams(collective_id=collective_id, has_side_effects=True, vmem_limit_bytes=VMEM_LIMIT)


def torus_gather(kind, piece, collective_id):
    def kernel(*refs):
        enter()
        for step in Gather(kind, *refs).steps():
            step()

    return pl.pallas_call(
        kernel, out_shape=sds(BF16, *Gather.shape(kind)), in_specs=[ANY], out_specs=ANY,
        scratch_shapes=Gather.semaphores(), compiler_params=comm_params(collective_id), name="gather_" + kind)(piece)


class Background:
    def __init__(self, steps, plan):
        self.steps, self.plan = steps, plan

    def visit(self, place):
        for j, first, end in self.plan.get(place, ()):
            @at_step(j)
            def _():
                for step in self.steps[first:end]:
                    step()


class Push:
    def __init__(self, src, tail, rows, sems, slot=0):
        body = BODY * len(SEQ_PAIR)
        tails = TAIL * len(SEQ_PAIR)
        self.copies = [
            remote(src.at[pl.ds(start, size)], rows.at[pl.ds(to, size)], sems, (slot, i), Torus().partner())
            for i, (start, to, size) in enumerate(((0, body, body), (tail, PAIR * body + tails, tails)))]

    @staticmethod
    def semaphores(n):
        return [pltpu.SemaphoreType.DMA((n, PAIR))] * PAIR

    def start(self):
        for copy in self.copies:
            copy.start()

    def wait(self):
        for copy in self.copies:
            copy.wait_recv()

    def finish(self):
        for copy in self.copies:
            copy.wait_send()


class Exchange:
    def __init__(self, mine, theirs, rows, sems, slot):
        self.moves = []
        for s in SEQ_PAIR:
            for i, (start, size) in enumerate(((0, BODY), (BODY, TAIL))):
                place = lambda n: rows.at[pl.ds(start * len(SEQ_PAIR) * PAIR + size * n, size)]
                part = pl.ds(TOK * s + start, size)
                at = slot + (PAIR * s + i,)
                local = pltpu.make_async_copy(mine.at[part], place(s), sems[2].at[at])
                far = remote(theirs.at[part], place(len(SEQ_PAIR) + s), sems, at, Torus().partner())
                self.moves.append((local, far))

    @staticmethod
    def semaphores(*lead):
        return [pltpu.SemaphoreType.DMA(lead + (2 * PAIR,))] * 3

    def start(self):
        for local, far in self.moves:
            far.start()
            local.start()

    def wait(self):
        for local, far in self.moves:
            local.wait()
            far.wait_recv()

    def finish(self):
        for _, far in self.moves:
            far.wait_send()


NT = (((1,), (1,)), ((), ()))
TN = (((0,), (0,)), ((), ()))


def dot(a, b):
    return jnp.dot(a, b, preferred_element_type=F32)


def dot_nt(a, b):
    return lax.dot_general(a, b, NT, preferred_element_type=F32)


def dot_tn(a, b):
    return lax.dot_general(a, b, TN, preferred_element_type=F32)


def zeros_but(n, axis, value):
    return tuple(value if i == axis else 0 for i in range(n))


def whole(*shape):
    return pl.BlockSpec(shape, lambda *_: (0,) * len(shape))


def along(axis, *block, index=lambda j: j):
    return pl.BlockSpec(block, lambda j: zeros_but(len(block), axis, index(j)))


def row(vec, i):
    return vec[i:i + 1]


def row_mean(t):
    return jnp.mean(t, axis=-1, keepdims=True)


def norm_stats(t):
    centered = t - row_mean(t)
    rstd = lax.rsqrt(row_mean(centered * centered) + LN_EPS)
    return centered * rstd, rstd


def norm_back(xhat, rstd, g):
    return rstd * (g - row_mean(g) - xhat * row_mean(g * xhat))


def col_sum(t):
    return jnp.sum(t, axis=0, keepdims=True)


def at_step(j):
    return pl.when(pl.program_id(0) == j)


def accumulate(ref, value):
    @at_step(0)
    def _():
        ref[...] = value

    @pl.when(pl.program_id(0) > 0)
    def _():
        ref[...] += value


def pad(t):
    return jnp.concatenate([t.astype(F32), jnp.zeros((TOK - SEQ, t.shape[1]), F32)], axis=0).astype(BF16)


def window(h):
    start = h * HEAD // LANES * LANES
    stop = min(D, -(-(h + 1) * HEAD // LANES) * LANES)
    lane = lax.broadcasted_iota(jnp.int32, (1, stop - start), 1) + (start - h * HEAD)
    return slice(start, stop), (lane >= 0) & (lane < HEAD)


def only(mask, t):
    return jnp.where(mask, t, jnp.zeros_like(t))


def softmax(scores):
    e = jnp.exp(scores - jnp.max(scores, axis=-1, keepdims=True))
    return e * (1.0 / jnp.sum(e, axis=-1, keepdims=True))


def attention(s, rows, o, acc, visit):
    acc[...] = jnp.zeros_like(acc)
    start = pl.multiple_of(s * TOK, TAIL)
    tokens = pl.ds(start, SEQ)
    for h in range(HEADS):
        lanes, mask = window(h)
        k = only(mask, rows[K, tokens, lanes])
        v = only(mask, rows[V, tokens, lanes])
        probs = softmax(dot_nt(rows[Q, tokens, lanes], k) * SCALE).astype(BF16)
        acc[:, lanes] += dot(probs, v)
        visit(h)
    o[pl.ds(start, TOK)] = pad(acc[...])


def seq_rows(t, s):
    return t[TOK * s:TOK * s + SEQ]


def seq_tile(s):
    return pl.ds(TOK * s, TOK)


FRONT_PLAN = {"qkv": ((0, 0, 1), (1, 1, 5), (2, 5, 8)), 2: ((O, 8, 9),), "end": ((O + 1, 9, None),)}


def front_kernel(x, w, b, vec, up_src, qkv, h1, o, att, h2, up, rows, acc, *sems):
    hosted = Background(Gather(WIDE, up_src, up, *sems).steps(), FRONT_PLAN)
    j = pl.program_id(0)
    at_step(0)(enter)
    hosted.visit("qkv")

    @at_step(0)
    def _():
        for s in SEQ_PAIR:
            xhat, _ = norm_stats(x[s].astype(F32))
            h1[seq_tile(s)] = pad(xhat * row(vec, G1) + row(vec, C1))

    @pl.when(j < O)
    def _():
        t = (dot(h1[...], w[0]) + b[0]).astype(BF16)
        qkv[0] = t
        rows[j] = t

    pl.when(j >= O)(lambda: attention(j - O, rows, o, acc, hosted.visit))

    @at_step(O + LAST_SEQ)
    def _():
        a = dot(o[...], w[0]) + row(vec, BO)
        att[...] = a
        for s in SEQ_PAIR:
            xhat, _ = norm_stats(x[s].astype(F32) + row(vec, S1) * seq_rows(a, s))
            h2[seq_tile(s)] = pad(xhat * row(vec, G2) + row(vec, C2))

    hosted.visit("end")


def upto(n):
    return lambda j: jnp.minimum(j, n)


def front_call(x, w_attn, b_qkv, vec, up, collective_id):
    return pl.pallas_call(
        front_kernel, grid=(O + PAIR,),
        out_shape=(sds(BF16, O, TT, D), sds(BF16, TT, D), sds(BF16, TT, D), sds(F32, TT, D), sds(BF16, TT, D),
                   sds(BF16, *Gather.shape(WIDE))),
        in_specs=[whole(*SEQS), along(0, 1, D, D, index=upto(O)), along(0, 1, 1, D, index=upto(V)), whole(8, D), ANY],
        out_specs=(along(0, 1, TT, D, index=upto(V)),) + (whole(TT, D),) * SIDE + (ANY,),
        scratch_shapes=[pltpu.VMEM((O, TT, D), BF16), pltpu.VMEM((SEQ, D), F32)] + Gather.semaphores(),
        compiler_params=comm_params(collective_id), name="front",
    )(x, w_attn, b_qkv, vec, up)


def w_out_block():
    return pl.BlockSpec((1, D, D), lambda j: (O, 0, 0), pipeline_mode=pl.Buffered(1))


TILES = FF // HALF
OWN_BODY = BODY * len(SEQ_PAIR)
TAILS = ROWS - TAIL * PAIR * len(SEQ_PAIR)


def put_rows(ref, tail, s, t):
    ref[pl.ds(pl.multiple_of(BODY * s, BODY), BODY)] = t[:BODY]
    ref[pl.ds(pl.multiple_of(tail + TAIL * s, TAIL), TAIL)] = t[BODY:]


DOWN_PLAN = {"start": ((0, 0, 1),), "end": ((1, 1, 5), (3, 5, 8), (5, 8, 9), (TILES + 4, 9, 12), (2 * TILES - 1, 12, None))}


def mlp_in_kernel(h2, gz, w_up, b_up, vec, src, act, slope, d_down, down, a_rows, b_rows, b_away, *sems):
    a_sems, b_sems, sems = sems[:PAIR], sems[PAIR:2 * PAIR], sems[2 * PAIR:]
    hosted = Background(Gather(DOWN, src, down, *sems).steps(), DOWN_PLAN)
    j = pl.program_id(0)
    away = Push(b_away, OWN_BODY, b_rows, b_sems, 0)
    tile = lambda n: Push(a_rows.at[n], TAILS, a_rows.at[n], a_sems, n)
    at_step(0)(enter)
    hosted.visit("start")

    @at_step(0)
    def _():
        first = Torus().at["c"] == 0
        for s in SEQ_PAIR:
            d = pad(gz[s].astype(F32) * row(vec, S2))
            left, right = d[:, :HALF], d[:, D - HALF:]
            put_rows(b_rows, TAILS, s, jnp.where(first, left, right))
            put_rows(b_away, OWN_BODY, s, jnp.where(first, right, left))

    at_step(1)(away.start)
    for n in range(TILES):
        at_step(n + 1)(tile(n).start)

    @pl.when(j < TILES)
    def _():
        u = dot(h2[...], w_up[0]) + b_up[0]
        phi = 0.5 * (1.0 + lax.erf(u * math.sqrt(0.5)))
        slope[...] = phi + u * (jnp.exp(-0.5 * u * u) * math.sqrt(0.5 / math.pi))
        place = lax.rem(lax.broadcasted_iota(jnp.int32, (TT, 1), 0), TOK)
        a = only(place < SEQ, u * phi).astype(BF16)
        act[...] = a
        for s in SEQ_PAIR:
            put_rows(a_rows.at[j], TAILS, s, a[TOK * s:TOK * s + TOK])

    at_step(TILES)(away.wait)
    for n in range(TILES):
        at_step(TILES + n)(tile(n).wait)

    @pl.when(j >= TILES)
    def _():
        d_down[...] = dot_tn(a_rows[j - TILES], b_rows[...])

    hosted.visit("end")

    @at_step(2 * TILES - 1)
    def _():
        away.finish()
        for n in range(TILES):
            tile(n).finish()


def mlp_in_call(h2, gz, w_up, b_up, vec, down, collective_id):
    low = lambda j: jnp.minimum(j, TILES - 1)
    high = lambda j: jnp.maximum(j - TILES, 0)
    return pl.pallas_call(
        mlp_in_kernel, grid=(2 * TILES,),
        out_shape=(sds(BF16, TT, FF), sds(F32, TT, FF), sds(F32, FF, HALF), sds(BF16, *Gather.shape(DOWN))),
        in_specs=[whole(TT, D), whole(*SEQS), up_tile(low), along(0, 1, 1, HALF, index=low), whole(8, D), ANY],
        out_specs=(along(1, TT, HALF, index=low), along(1, TT, HALF, index=low),
                   along(0, HALF, HALF, index=high), ANY),
        scratch_shapes=[pltpu.VMEM((TILES, ROWS, HALF), BF16), pltpu.VMEM((ROWS, HALF), BF16),
                        pltpu.VMEM((PAIR * TOK, HALF), BF16)] + Push.semaphores(TILES) + Push.semaphores(1) +
        Gather.semaphores(),
        compiler_params=comm_params(collective_id), name="mlp_in",
    )(h2, gz, w_up, b_up.reshape(TILES, 1, HALF), vec, down)


def up_tile(index=lambda j: j):
    return pl.BlockSpec((1, D, HALF), lambda j: (index(j) // PAIR, 0, index(j) % PAIR))


MLP_PLAN = {"start": ((0, 0, 2),), "end": ((3, 2, 3), (TILES - 1, 3, None))}


def mlp_out_kernel(act, slope, gz, w_up, w_down, vec, part, d_pre, db_up, mlp, d_h2, sums, dm, *scratch):
    first = First(Bands(DOWN), part, sums, *scratch)
    hosted = Background([first.near, first.far, first.relay, first.settle, first.finish], MLP_PLAN)
    at_step(0)(enter)
    hosted.visit("start")

    @at_step(0)
    def _():
        for s in SEQ_PAIR:
            dm[seq_tile(s)] = pad(gz[s].astype(F32) * row(vec, S2))

    accumulate(mlp, dot(act[...], w_down[...]))
    d = dot_nt(dm[...], w_down[...]) * slope[...]
    db_up[0] = col_sum(d)
    d = d.astype(BF16)
    d_pre[0, 0] = d
    accumulate(d_h2, dot_nt(d, w_up[0]))
    hosted.visit("end")


def mlp_out_call(act, slope, gz, w_up, w_down, vec, part, collective_id):
    return pl.pallas_call(
        mlp_out_kernel, grid=(TILES,),
        out_shape=(sds(BF16, PAIR, SIDE, TT, HALF), sds(F32, TILES, 1, HALF), sds(F32, TT, D), sds(F32, TT, D),
                   Bands(DOWN).sums()),
        in_specs=[along(1, TT, HALF), along(1, TT, HALF), whole(*SEQS), up_tile(), along(0, HALF, D), whole(8, D), ANY],
        out_specs=(pl.BlockSpec((1, 1, TT, HALF), lambda j: (j % PAIR, j // PAIR, 0, 0)), along(0, 1, 1, HALF),
                   whole(TT, D), whole(TT, D), ANY),
        scratch_shapes=[pltpu.VMEM((TT, D), BF16)] + Bands(DOWN).first(),
        compiler_params=comm_params(collective_id), name="mlp_out",
    )(act, slope, gz, w_up, w_down, vec, part)


def halves_of(t):
    t = pad(t)
    return t[:, :HALF], jnp.concatenate([t[:, HALF:], jnp.zeros((TOK, QCOLS - D), BF16)], axis=1)


def mid(mlp, d_h2, att, x, gz, vec, w_out, z, g_res, d_att, d_o, sums, da_rows):
    a = att[:SEQ]
    y = x[0].astype(F32) + row(vec, S1) * a
    m = mlp[:SEQ] + row(vec, B2)
    g = gz[0].astype(F32)
    z[0] = (y + row(vec, S2) * m).astype(BF16)
    xhat, rstd = norm_stats(y)
    dh = d_h2[:SEQ]
    gr = g + norm_back(xhat, rstd, dh * row(vec, G2))
    g_res[:SEQ] = gr
    da = gr * row(vec, S1)
    terms = (da, gr * a, dh * xhat, dh, g * row(vec, S2), g * m)
    accumulate(sums, jnp.concatenate([jnp.zeros((BO, D), F32)] + [col_sum(t) for t in terms], axis=0))
    for i, t in enumerate(halves_of(da)):
        d_att[i] = t
    da_rows[pl.ds(pl.multiple_of(pl.program_id(0) * TOK, TAIL), TOK)] = pad(da)

    @at_step(LAST_SEQ)
    def _():
        d_o[...] = dot_nt(da_rows[...], w_out[0]).astype(BF16)


def attention_back(s, qkv, d_o, d_qkv, db, acc, b_rows, away, first, visit):
    acc[...] = jnp.zeros_like(acc)
    for h in range(HEADS):
        lanes, mask = window(h)
        q, k, v = (only(mask, qkv[i, :SEQ, lanes]) for i in (Q, K, V))
        do = only(mask, d_o[:SEQ, lanes])
        scores = dot_nt(k, q) * SCALE
        e = jnp.exp(scores - jnp.max(scores, axis=0, keepdims=True))
        probs = e * (1.0 / col_sum(e))
        acc[V, :, lanes] += dot(probs.astype(BF16), do)
        dp = dot_nt(v, do)
        ds = probs * (dp - col_sum(dp * probs))
        ds = (ds * SCALE).astype(BF16)
        acc[K, :, lanes] += dot(ds, q)
        acc[Q, :, lanes] += dot_tn(ds, k)
        visit(h)
    accumulate(db, jnp.concatenate([col_sum(acc[i]) for i in (Q, K, V)], axis=0))
    for n in (Q, K, V):
        left, right = halves_of(acc[n])
        d_qkv[0, n] = left
        d_qkv[1, n] = right
        put_rows(b_rows.at[n], TAILS, s, jnp.where(first, left, right))
        put_rows(away.at[n], OWN_BODY, s, jnp.where(first, right, left))


PER = HALF // STEP


class WideGrads:
    def __init__(self, inputs, a_of, cotangents, out, base, lead, a_rows, a_cols, b_rows):
        self.inputs, self.a_of, self.cotangents, self.out, self.base, self.lead = inputs, a_of, cotangents, out, base, lead
        self.a_rows, self.a_cols, self.b_rows = a_rows, a_cols, b_rows

    @staticmethod
    def scratch(inputs):
        return [pltpu.VMEM((inputs, ROWS, D), BF16), pltpu.VMEM((inputs, D, ROWS), BF16), pltpu.VMEM((SIDE, ROWS, HALF), BF16)]

    def step(self):
        j = pl.program_id(0)
        done = []
        for t in range(SIDE):
            n = (t + self.lead) % SIDE

            @at_step(self.base + PER * t)
            def _():
                i = self.a_of[n]
                if i not in done:
                    self.inputs[i].wait()
                    self.a_cols[i] = self.a_rows[i].T
                    done.append(i)
                self.cotangents[n].wait()

        @pl.when(j >= self.base)
        def _():
            n = lax.rem(lax.div(j - self.base, PER) + self.lead, SIDE)
            cols = pl.ds(pl.multiple_of(lax.rem(j - self.base, PER) * STEP, STEP), STEP)
            i = 0 if len(self.inputs) == 1 else lax.div(n, O)
            self.out[0] = dot(self.a_cols[i], self.b_rows[n, :, cols])

    def finish(self):
        for move in (*self.inputs, *self.cotangents):
            move.finish()


def grads_block(base, lead):
    def index(j):
        n = jnp.maximum(j - base, 0)
        return (n // PER + lead) % SIDE, 0, n % PER

    return pl.BlockSpec((1, D, STEP), index)


GRAD_STEPS = PER * SIDE


def tok_block():
    return along(0, TOK, D, index=upto(LAST_SEQ))


def seq_block():
    return along(0, 1, SEQ, D, index=upto(LAST_SEQ))


MID_PLAN = {"start": ((0, 0, 1),), "end": ((1, 1, 3), (8, 3, 4), (11, 4, 5), (LAST_SEQ + GRAD_STEPS, 5, None))}


def mid_kernel(*refs):
    refs = list(refs)
    take = lambda n: [refs.pop(0) for _ in range(n)]
    ins, (h2, d_pre, acc), outs, (d_up, result), da_rows = take(7), take(3), take(5), take(2), refs.pop(0)
    rows, a_sems, b_sems = take(3), take(C), take(C)
    rest = Rest(Bands(DOWN), acc, result, *refs)
    hosted = Background([rest.begin, rest.loaded, rest.relay, rest.settle, rest.relay_third, rest.settle_third, rest.finish],
                        MID_PLAN)
    c = Torus().at["c"]
    grads = WideGrads(
        [Exchange(h2, h2, rows[0].at[0], a_sems, ())], (0,) * SIDE,
        [Exchange(d_pre.at[c, n], d_pre.at[1 - c, n], rows[2].at[n], b_sems, (n,)) for n in range(SIDE)], d_up, SEQS[0], 0, *rows)
    at_step(0)(enter)
    hosted.visit("start")

    @at_step(0)
    def _():
        for move in (*grads.inputs, *grads.cotangents):
            move.start()

    pl.when(pl.program_id(0) < SEQS[0])(lambda: mid(*ins, *outs, da_rows))
    grads.step()
    hosted.visit("end")
    at_step(LAST_SEQ + GRAD_STEPS)(grads.finish)


def mid_call(mlp, d_h2, att, x, gz, vec, w_attn, h2, d_pre, acc, collective_id):
    return pl.pallas_call(
        mid_kernel, grid=(SEQS[0] + GRAD_STEPS,),
        out_shape=(sds(BF16, *SEQS), sds(F32, TT, D), sds(BF16, PAIR, TT, HALF), sds(BF16, TT, D), sds(F32, 8, D),
                   sds(F32, SIDE, D, HALF), Bands(DOWN).result()),
        in_specs=[tok_block()] * O + [seq_block()] * PAIR + [whole(8, D), w_out_block()] + [ANY] * O,
        out_specs=(seq_block(), tok_block(), along(1, PAIR, TOK, HALF, index=upto(LAST_SEQ)), whole(TT, D), whole(8, D),
                   grads_block(SEQS[0], 0), ANY),
        scratch_shapes=[pltpu.VMEM((TT, D), BF16)] + WideGrads.scratch(1) + Exchange.semaphores() + Exchange.semaphores(SIDE) +
        Bands(DOWN).later(),
        compiler_params=comm_params(collective_id), name="mid",
    )(mlp, d_h2, att, x, gz, vec, w_attn, h2, d_pre, acc)


ATTN_PLAN = {"start": ((0, 0, 3),), 6: ((0, 3, 4),), "end": ((LAST_SEQ, 4, 5), (LAST_SEQ + GRAD_STEPS, 5, None))}


def attn_back_kernel(*refs):
    refs = list(refs)
    take = lambda n: [refs.pop(0) for _ in range(n)]
    (qkv, d_o), (h1, o, d_att, part, result), (d_qkv, db, d_attn, sums, total) = take(2), take(5), take(5)
    acc, away, rows = refs.pop(0), refs.pop(0), take(3)
    a_sems, b_sems, away_sems = take(C), take(C), take(PAIR)
    first = First(Bands(WIDE), part, sums, *take(len(Bands(WIDE).first())))
    spread = Spread(Bands(DOWN), result, total, *refs)
    hosted = Background([spread.begin, first.near, first.far, spread.forward, first.relay, first.settle, first.finish,
                         spread.finish], ATTN_PLAN)
    c = Torus().at["c"]
    pushes = [Push(away.at[n], OWN_BODY, rows[2].at[n], away_sems, n) for n in range(O)]
    grads = WideGrads(
        [Exchange(a, a, rows[0].at[i], a_sems, (i,)) for i, a in enumerate((h1, o))], (0,) * O + (1,),
        pushes + [Exchange(d_att.at[c], d_att.at[1 - c], rows[2].at[O], b_sems, ())], d_attn, SEQS[0], O, *rows)
    at_step(0)(enter)
    hosted.visit("start")

    @at_step(0)
    def _():
        for move in (*grads.inputs, grads.cotangents[O]):
            move.start()

    @at_step(SEQS[0])
    def _():
        for push in pushes:
            push.start()

    j = pl.program_id(0)
    pl.when(j < SEQS[0])(lambda: attention_back(j, qkv, d_o, d_qkv, db, acc, rows[2], away, c == 0, hosted.visit))

    grads.step()
    hosted.visit("end")
    at_step(LAST_SEQ + GRAD_STEPS)(grads.finish)


def attn_back_call(qkv, d_o, h1, o, d_att, part, result, collective_id):
    return pl.pallas_call(
        attn_back_kernel, grid=(SEQS[0] + GRAD_STEPS,),
        out_shape=(sds(BF16, PAIR, O, TT, HALF), sds(F32, O, D), sds(F32, SIDE, D, HALF), Bands(WIDE).sums(),
                   Bands(DOWN).total()),
        in_specs=[along(1, O, TOK, D, index=upto(LAST_SEQ)), tok_block()] + [ANY] * 5,
        out_specs=(along(2, PAIR, O, TOK, HALF, index=upto(LAST_SEQ)), whole(O, D), grads_block(SEQS[0], O), ANY, ANY),
        scratch_shapes=[pltpu.VMEM((O, SEQ, D), F32), pltpu.VMEM((O, PAIR * TOK, HALF), BF16)] + WideGrads.scratch(2) +
        Exchange.semaphores(PAIR) + Exchange.semaphores() + Push.semaphores(O) + Bands(WIDE).first() + Spread.scratch(),
        compiler_params=comm_params(collective_id), name="attn_back",
    )(qkv, d_o, h1, o, d_att, part, result)


IN_STEPS = PAIR * O
SLOT = 40
LAST_PLAN = {"start": ((0, 0, 2),), "end": ((O, 2, 5),)}


def last_kernel(*refs):
    refs = list(refs)
    take = lambda n: [refs.pop(0) for _ in range(n)]
    (d_half, w, x, g_res, vec), (small, acc_up, _), (dx, part, *totals) = take(5), take(3), take(5)
    acc, sums, pair_sums, block, block_sem, swap_sems = refs.pop(0), refs.pop(0), refs.pop(0), refs.pop(0), refs.pop(0), take(PAIR)
    halves = [Bands(WIDE, h) for h in WAYS]
    a, b = (First(bands, part, None, *take(len(bands.first()))) for bands in halves)
    rest_a, rest_b = (Rest(f.bands, f.own_all, None, f.own_all, *take(len(f.bands.later()) - 1)) for f in (a, b))
    rest_up = Rest(Bands(WIDE), acc_up, None, *take(len(Bands(WIDE).later())))
    spread_up, spread_a, spread_b = (
        Spread(r.bands, r.sums(), total, *take(len(Spread.scratch()))) for r, total in zip((rest_up, rest_a, rest_b), totals))
    hosted = Background([rest_up.begin, a.near, rest_up.loaded, rest_up.relay, a.far], LAST_PLAN)
    me = Torus()
    swap = remote(sums, pair_sums, swap_sems, (), me.partner())
    fetch = pltpu.make_async_copy(small, block, block_sem)
    at_step(0)(enter)
    hosted.visit("start")
    at_step(0)(fetch.start)

    @pl.when(pl.program_id(0) < IN_STEPS)
    def _():
        accumulate(acc, dot_nt(d_half[0, 0], w[0]))

    @at_step(IN_STEPS - 1)
    def _():
        rows = jnp.zeros((SUB, D), F32)
        for s in SEQ_PAIR:
            xhat, rstd = norm_stats(x[s].astype(F32))
            tokens = pl.ds(TOK * s, SEQ)
            dh = acc[tokens]
            rows = rows + jnp.concatenate([col_sum(dh * xhat), col_sum(dh), jnp.zeros((SUB - BO, D), F32)], axis=0)
            dx[s] = (g_res[tokens] + norm_back(xhat, rstd, dh * row(vec, G1))).astype(BF16)
        sums[...] = rows

    hosted.visit("end")

    @at_step(IN_STEPS)
    def _():
        swap.start()
        fetch.wait()
        rest_up.settle()
        a.relay()
        swap.wait()
        both = sums[...] + pair_sums[...]
        for d in range(DEVICES):
            at = CHIP * (d // PAIR) + SLOT + OWN * (d % PAIR)
            block[at:at + BO, :OWN] = both[:BO, OWN * d:OWN * d + OWN]

        @pl.when(me.at["c"] == 1)
        def _():
            for z in range(SIDE):
                for y in range(SIDE):
                    rows = block.at[pl.ds(CHIP * (SIDE * z + y), CHIP)]
                    put = pltpu.make_async_copy(rows, part.at[0, z, y, :, pl.ds(HALF - LANES, LANES)], block_sem)
                    put.start()
            pltpu.make_async_copy(block, small, block_sem).wait()

        for step in (b.near, rest_up.relay_third, b.far, functools.partial(a.settle, rest_a.send), rest_up.settle_third,
                     spread_up.begin, b.relay, rest_a.relay, rest_a.settle, spread_up.forward, rest_a.relay_third,
                     functools.partial(b.settle, rest_b.send), rest_a.settle_third, spread_a.begin, rest_b.relay, rest_b.settle,
                     spread_a.forward, rest_b.relay_third, rest_b.settle_third, spread_b.begin, spread_b.forward,
                     spread_up.finish, spread_a.finish, spread_b.finish, rest_up.finish, rest_a.finish, rest_b.finish,
                     a.finish, b.finish):
            step()


def last_call(d_qkv, w_attn, x, g_res, vec, small, acc_up, part, collective_id):
    low = upto(IN_STEPS - 1)
    halves = [Bands(WIDE, h) for h in WAYS]
    dma = pltpu.SemaphoreType.DMA
    return pl.pallas_call(
        last_kernel, grid=(IN_STEPS + 1,),
        out_shape=(sds(BF16, *SEQS), sds(F32, *part.shape), Bands(WIDE).total(), *(h.total() for h in halves)),
        in_specs=[pl.BlockSpec((1, 1, TT, HALF), lambda j: (low(j) % PAIR, low(j) // PAIR, 0, 0)), up_tile(low),
                  whole(*SEQS), whole(TT, D), whole(8, D)] + [ANY] * O,
        out_specs=(whole(*SEQS),) + (ANY,) * SIDE,
        scratch_shapes=[pltpu.VMEM((TT, D), F32), pltpu.VMEM((SUB, D), F32), pltpu.VMEM((SUB, D), F32),
                        pltpu.VMEM((D, LANES), F32), dma, dma, dma] + halves[0].first() * PAIR + halves[0].later()[1:] * PAIR +
        Bands(WIDE).later() + Spread.scratch() * O,
        input_output_aliases={7: 1},
        compiler_params=comm_params(collective_id), name="last",
    )(d_qkv, w_attn, x, g_res, vec, small, acc_up, part)


BQ, BU, VEC = 3 * D // 32, 3 * D // 32 + FF // 32, 3 * D // 32 + FF // 32 + 8 * OWN


def pair_swap(a):
    return lax.ppermute(a, "fsdp", [(i, i ^ 1) for i in range(DEVICES)])


def by_core(first, a, b):
    return jnp.where(first, a, b), jnp.where(first, b, a)


def my_pieces(shards, first):
    w_qkv, b_qkv, w_out, w_up, b_up, w_down, vec_params = shards
    x = lax.axis_index("rep")
    small = jnp.concatenate([b_qkv, b_up, vec_params.reshape(-1)])
    small = jnp.pad(small, (0, OWN * LANES - VEC)).reshape(OWN, LANES)
    attn = lax.dynamic_slice_in_dim(jnp.concatenate([w_qkv, w_out], axis=1), x * D, D, 1)
    attn = jnp.concatenate([attn, small], axis=1)
    up = lax.dynamic_slice_in_dim(w_up, x * QCOLS, QCOLS, 1)
    wide = jnp.stack([attn, up]).astype(BF16)
    mine, theirs = by_core(first, wide[..., :HALF], wide[..., HALF:])
    theirs = pair_swap(theirs)
    piece = jnp.concatenate(by_core(first, mine, theirs), axis=1)
    down = lax.dynamic_slice_in_dim(w_down, x * 48, 48, 0).astype(BF16).reshape(3, 16, D)
    return piece[0], piece[1], down


def small_params(w_attn):
    small = w_attn[0, :, D:].astype(F32).reshape(DEVICES, OWN * LANES)
    vec = small[:, BU:VEC].reshape(DEVICES, 8, OWN).transpose(1, 0, 2).reshape(8, D)
    return small[:, :BQ].reshape(O, 1, D), small[:, BQ:BU].reshape(FF), vec


ROOM = 5 * LANES


def small_grads(db_qkv, db_up, sums):
    vec = sums[BO:].reshape(8 - BO, DEVICES, OWN).transpose(1, 0, 2).reshape(DEVICES, VEC - BU - BO * OWN)
    small = jnp.concatenate([db_qkv.reshape(DEVICES, BQ), db_up.reshape(DEVICES, BU - BQ), vec], axis=1)
    small = small + pair_swap(small)
    small = jnp.pad(small, ((0, 0), (0, ROOM - small.shape[1]))).reshape(DEVICES, ROOM // LANES, LANES)
    return jnp.pad(small, ((0, 0), (0, OWN - ROOM // LANES), (0, 0))).reshape(D, LANES)


def rows_of(total):
    return jnp.concatenate([total[:, k, :n] for k, (_, n) in enumerate(BANDS[WIDE])], axis=1)


def final_rows(total, first):
    keep, give = by_core(first, total[:, :OWN], total[:, OWN:])
    pair = jnp.stack(by_core(first, keep, pair_swap(give)), axis=1)
    return pair.transpose(2, 0, 1, 3).reshape(OWN, SIDE, QCOLS)


def final_down(total, first):
    down = total.reshape(FF // 16, HALF)
    keep, give = by_core(first, down[:FF // DEVICES], down[FF // DEVICES:])
    left, right = by_core(first, keep, pair_swap(give))
    return jnp.concatenate([left, right[:, 2 * HALF - D:]], axis=1)


def device_step(x, gz, *shards):
    first = lax.rem(lax.axis_index("fsdp"), PAIR) == 0
    attn, up, down = my_pieces(shards, first)
    w_attn = torus_gather(WIDE, attn, 0).reshape(SIDE, D, QCOLS)
    b_qkv, b_up, vec = small_params(w_attn)
    qkv, h1, o, att, h2, w_up = front_call(x, w_attn, b_qkv, vec, up, 1)
    w_up = w_up.reshape(SIDE, D, QCOLS)
    act, slope, part, w_down = mlp_in_call(h2, gz, w_up, b_up, vec, down, 2)
    part = part.reshape((SIDE,) * 3 + (C * UNIT, HALF))
    d_pre, db_up, mlp, d_h2, acc = mlp_out_call(act, slope, gz, w_up, w_down.reshape(FF, D), vec, part, 3)
    z, g_res, d_att, d_o, sums, part, result = mid_call(mlp, d_h2, att, x, gz, vec, w_attn, h2, d_pre, acc, 4)
    part = part.reshape((SIDE,) * 3 + (CHIP, HALF))
    d_qkv, db_qkv, part, acc, down = attn_back_call(qkv, d_o, h1, o, d_att, part, result, 5)
    small = small_grads(db_qkv, db_up, sums)
    part = part.reshape((SIDE,) * 3 + (CHIP, HALF))
    dx, _, up, attn0, attn1 = last_call(d_qkv, w_attn, x, g_res, vec, small, acc, part, 6)
    g_up = final_rows(rows_of(up), first).reshape(OWN, FF)
    attn = final_rows(jnp.concatenate([rows_of(attn0), rows_of(attn1)], axis=-1), first)
    small = attn[:ROOM // LANES, 0, D:].reshape(ROOM)
    vec = jnp.concatenate([attn[SLOT:SLOT + BO, 0, D:D + OWN], small[BU:VEC - BO * OWN].reshape(8 - BO, OWN)], axis=0)
    return (z, dx, attn[:, :O, :D].reshape(OWN, O * D), small[:BQ], attn[:, O, :D], g_up, small[BQ:BU],
            final_down(down, first), vec)


def solution(mesh):
    batch = P(("rep", "fsdp"), None, None)
    rows, flat, cols = P("fsdp", None), P("fsdp"), P(None, "fsdp")
    shards = (rows, flat, rows, rows, flat, rows, cols)
    return jax.shard_map(device_step, mesh=mesh, in_specs=(batch, batch) + shards,
                         out_specs=(batch, batch) + shards, check_vma=False)
```

```python
import functools
import math

import jax
import jax.numpy as jnp
from jax import lax
from jax.experimental import pallas as pl
from jax.experimental.pallas import tpu as pltpu
from jax.sharding import PartitionSpec as P

HEADS = 16
LN_EPS = 1e-5
D = 1408
FF = 6144
SEQ = 257
HEAD = D // HEADS
SCALE = HEAD ** -0.5
QCOLS = 1536
HALF = 768
OWN = 44
CHIP = 2 * OWN
LANES = 128
DEVICES = 32
F32 = jnp.float32
BF16 = jnp.bfloat16
VMEM_LIMIT = 66 * 1000 * 1000
G1, C1, BO, S1, G2, C2, B2, S2 = range(8)
Q, K, V, O = range(4)
SEQS = (2, SEQ, D)
LAST_SEQ = SEQS[0] - 1
SEQ_PAIR = range(SEQS[0])
TAIL = 16
BODY = SEQ - 1
TOK = BODY + TAIL
TT = 2 * TOK
ROWS = 4 * TOK
STEP = 256


def sds(dtype, *shape):
    return jax.ShapeDtypeStruct(shape, dtype)


MESH_ID = pl.DeviceIdType.MESH
SIDE = 4
SUB = 8
PAIR = 2
C = 3
COLOURS = range(C)
COLOUR_DIMS = ("xyz", "yzx", "zxy")
FIRST, SECOND, THIRD, LAST = range(4)
WAYS = range(PAIR)
NEAR, FAR, ADDED = 0, 2, 4
WIDE, DOWN = "wide", "down"
ANY = pl.BlockSpec(memory_space=pl.ANY)
ALL = slice(None)


def duo(m):
    return pl.ds(PAIR * m, PAIR)


def toward(m):
    return 1 - PAIR * (m % PAIR)


class Torus:
    def __init__(self):
        f = lax.axis_index("fsdp")
        self.at = {"x": lax.axis_index("rep"), "z": lax.div(f, SIDE * PAIR), "y": lax.rem(lax.div(f, PAIR), SIDE),
                   "c": lax.rem(f, PAIR)}

    def shift(self, dim, by):
        return lax.rem(self.at[dim] + (SIDE + by), SIDE)

    def device(self, **moved):
        p = {**self.at, **moved}
        return (p["x"], (p["z"] * SIDE + p["y"]) * PAIR + p["c"])

    def neighbour(self, dim, by):
        return self.device(**{dim: self.shift(dim, by)})

    def partner(self):
        return self.device(c=1 - self.at["c"])


def enter():
    me = Torus()
    barrier = pltpu.get_barrier_semaphore()
    others = [me.neighbour(d, toward(m)) for d in COLOUR_DIMS[0] for m in WAYS] + [me.partner()]
    for other in others:
        pl.semaphore_signal(barrier, device_id=other, device_id_type=MESH_ID)
    pl.semaphore_wait(barrier, len(others))


def remote(src, dst, sems, slot, device):
    return pltpu.make_async_remote_copy(src_ref=src, dst_ref=dst, send_sem=sems[0].at[slot], recv_sem=sems[1].at[slot],
                                        device_id=device, device_id_type=MESH_ID)


class Gather:
    def __init__(self, kind, src, dst, hop_send, hop_recv, push_send, push_recv, local):
        self.kind, self.src, self.dst, self.local = kind, src, dst, local
        self.hops, self.pushes = (hop_send, hop_recv), (push_send, push_recv)
        self.cols, self.cut = (256, 128) if kind == WIDE else (D, HALF)

    @staticmethod
    def semaphores():
        dma = pltpu.SemaphoreType.DMA
        return [dma((C, C, ADDED))] * PAIR + [dma((C, ADDED + 1))] * PAIR + [dma((C,))]

    @staticmethod
    def shape(kind):
        return (SIDE,) * 3 + (CHIP, QCOLS) if kind == WIDE else (SIDE, SIDE, PAIR, SIDE, C, 16, D)

    def source(self, k):
        return self.src.at[:, pl.ds(self.cols * k, self.cols)] if self.kind == WIDE else self.src.at[k]

    def piece(self, me, k, s, v, half=None):
        dims = COLOUR_DIMS[k]
        at = {**me.at, **{d: ALL for d in dims[:s]}, dims[s]: v}
        off, width = 0, self.cols
        if half is not None and s == FIRST:
            off, width = self.cut * half, (self.cut, self.cols - self.cut)[half]
        elif half is not None:
            at[dims[0]] = duo(half)
        if self.kind == WIDE:
            cols = pl.ds(pl.multiple_of(at["c"] * HALF + self.cols * k + off, 128), width)
            return self.dst.at[at["x"], at["z"], at["y"], :, cols]
        return self.dst.at[at["z"], at["y"], at["c"], at["x"], k, :, pl.ds(off, width)]

    def hop(self, k, s, m):
        me = Torus()
        dim = COLOUR_DIMS[k][s]
        by = toward(m)
        if m < FAR:
            ref = self.piece(me, k, s, me.at[dim])
        else:
            ref = self.piece(me, k, s, me.shift(dim, -by), m - FAR)
        src = self.source(k) if s == FIRST and m < FAR else ref
        return remote(src, ref, self.hops, (k, s, m), me.neighbour(dim, by))

    def push(self, k, n):
        me = Torus()
        dim = COLOUR_DIMS[k][THIRD]
        if n < FAR:
            ref = self.piece(me, k, THIRD, me.shift(dim, -toward(n)))
        elif n < ADDED:
            ref = self.piece(me, k, THIRD, me.shift(dim, FAR), n - FAR)
        else:
            ref = self.piece(me, k, THIRD, me.at[dim])
        return remote(ref, ref, self.pushes, (k, n), me.partner())

    def own(self, k):
        me = Torus()
        return pltpu.make_async_copy(self.source(k), self.piece(me, k, FIRST, me.at[COLOUR_DIMS[k][FIRST]]), self.local.at[k])

    def launch(self, s):
        for k in COLOURS:
            for m in WAYS:
                self.hop(k, s, m).start()
            if s == THIRD:
                self.push(k, ADDED).start()

    def relay(self, s):
        for k in COLOURS:
            for m in WAYS:
                self.hop(k, s, m).wait_recv()
                self.hop(k, s, FAR + m).start()
                if s == THIRD:
                    self.push(k, m).start()

    def settle(self, s):
        for k in COLOURS:
            for m in WAYS:
                self.hop(k, s, FAR + m).wait_recv()
                if s == THIRD:
                    self.push(k, FAR + m).start()
            if s == FIRST:
                self.own(k).wait()

    def begin(self):
        for k in COLOURS:
            self.own(k).start()
        self.launch(FIRST)

    def sent(self, *rings):
        for k in COLOURS:
            for s in rings:
                for m in range(ADDED):
                    self.hop(k, s, m).wait_send()
            if THIRD in rings:
                for n in range(ADDED + 1):
                    self.push(k, n).wait()

    def last_ring(self):
        return [functools.partial(f, THIRD) for f in (self.launch, self.relay, self.settle, self.sent)]


def add_into(total, *others):
    lead = total.shape[:-2]

    def body(i, carry):
        idx = []
        for n in reversed(lead):
            idx.insert(0, lax.rem(i, n))
            i = lax.div(i, n)
        value = total[tuple(idx)]
        for other in others:
            value = value + other[tuple(idx)]
        total[tuple(idx)] = value
        return carry

    lax.fori_loop(0, math.prod(lead), body, 0)


class Ring:
    def __init__(self, s, bands, terms, passed, relay, landing, send, recv):
        self.s, self.bands, self.terms, self.passed, self.relay, self.landing = s, bands, terms, passed, relay, landing
        self.sems = (send, recv)

    def zone(self, k, way, half):
        if self.s == THIRD:
            return self.landing.at[k, way, self.bands.cuts(k)[half]]
        return self.bands.rows(self.landing.at[k, way, duo(half)], k)

    def carried(self, ref, k, way):
        if self.s == THIRD:
            return ref.at[k, way, pl.ds(0, self.bands.cuts(k)[way].size)]
        return self.bands.rows(ref.at[k, way], k)

    def hop(self, k, m):
        me = Torus()
        dim = COLOUR_DIMS[k][self.s]
        way, by = m % PAIR, toward(m)
        if m < FAR:
            src, dst = self.terms(k, me.shift(dim, FAR), way), self.carried(self.relay, k, way)
        elif m < ADDED:
            src, dst = self.terms(k, me.shift(dim, by), 1 - way), self.zone(k, way, 1 - way)
        else:
            src, dst = self.carried(self.passed, k, way), self.zone(k, way, way)
        return remote(src, dst, self.sems, (k, m), me.neighbour(dim, by))

    def start(self, k, base):
        for m in WAYS:
            self.hop(k, base + m).start()

    def arrived(self, k, base):
        for m in WAYS:
            self.hop(k, base + m).wait_recv()

    def finish(self):
        for k in COLOURS:
            for m in range(ADDED + PAIR):
                self.hop(k, m).wait_send()

    @staticmethod
    def semaphores():
        return [pltpu.SemaphoreType.DMA((C, ADDED + PAIR))] * PAIR


UNIT = 32
BANDS = {WIDE: ((0, 24), (24, UNIT), (56, UNIT)), DOWN: ((0, UNIT), (UNIT, UNIT), (2 * UNIT, UNIT))}
ORDERS = {WIDE: "xzy", DOWN: "zyx"}


class Bands:
    def __init__(self, kind, half=None):
        self.order, self.bands = ORDERS[kind], BANDS[kind]
        self.width = HALF if half is None else HALF // PAIR
        self.cols = pl.ds(self.width * (half or 0), self.width)

    def band(self, k):
        return pl.ds(*self.bands[k])

    def rows(self, ref, k):
        return ref.at[(ALL,) * (len(ref.shape) - PAIR) + (pl.ds(0, self.bands[k][1]),)]

    def cuts(self, k):
        rows = self.bands[k][1]
        cut = (rows // SUB + 1) // PAIR * SUB
        return pl.ds(0, cut), pl.ds(cut, rows - cut)

    def rest(self, k):
        return [d for d in self.order if d != COLOUR_DIMS[k][FIRST]]

    def units(self, *lead):
        return lead + (UNIT, self.width)

    def vmem(self, *lead):
        return pltpu.VMEM(self.units(*lead), F32)

    def sums(self):
        return sds(F32, *self.units(C, SIDE, SIDE))

    def result(self):
        return sds(F32, *self.units(C))

    def total(self):
        return sds(F32, *self.units(SIDE, C))

    def first(self):
        relays = [self.vmem(C, PAIR, PAIR, SIDE)] * PAIR
        dma = pltpu.SemaphoreType.DMA
        return [self.vmem(C, SIDE, SIDE), *relays, self.vmem(C, PAIR, SIDE, SIDE), *Ring.semaphores(), dma((C, C)), dma((C,))]

    def later(self):
        dma = pltpu.SemaphoreType.DMA
        return [self.vmem(C, SIDE, SIDE), self.vmem(C, PAIR, PAIR), self.vmem(C, PAIR, SIDE),
                pltpu.VMEM((C, PAIR, UNIT // PAIR, self.width), F32), self.vmem(C, PAIR),
                *Ring.semaphores(), *Ring.semaphores(), dma((C,)), dma((C,))]


class First:
    def __init__(self, bands, part, acc, own, passed, relay, landing, send, recv, load, store):
        self.bands, self.part, self.acc, self.own_all, self.passed = bands, part, acc, own, passed
        self.relay_in, self.landing, self.load_sem, self.store_sem = relay, landing, load, store
        self.ring = Ring(FIRST, bands, self.terms, passed, relay, landing, send, recv)

    def own(self, k):
        return self.bands.rows(self.own_all.at[k], k)

    def terms(self, k, v, half=None):
        b = self.bands
        at = {d: ALL for d in b.order}
        at[COLOUR_DIMS[k][FIRST]] = v
        if half is not None:
            at[b.rest(k)[0]] = duo(half)
        return self.part.at[tuple(at[d] for d in b.order) + (b.band(k), b.cols)]

    def load(self, k, m):
        me = Torus()
        dim = COLOUR_DIMS[k][FIRST]
        if m in WAYS:
            src, dst = self.terms(k, me.shift(dim, toward(m)), m), self.ring.carried(self.passed, k, m)
        else:
            src, dst = self.terms(k, me.at[dim]), self.own(k)
        return pltpu.make_async_copy(src, dst, self.load_sem.at[k, m])

    def store(self, k):
        return pltpu.make_async_copy(self.own(k), self.bands.rows(self.acc.at[k], k), self.store_sem.at[k])

    def near(self):
        for k in COLOURS:
            self.ring.start(k, NEAR)

    def far(self):
        for k in COLOURS:
            self.ring.start(k, FAR)
        for m in COLOURS:
            for k in COLOURS:
                self.load(k, m).start()

    def relay(self):
        for k in COLOURS:
            self.ring.arrived(k, NEAR)
            for m in WAYS:
                self.load(k, m).wait()
                add_into(self.ring.carried(self.passed, k, m), self.ring.carried(self.relay_in, k, m))
            self.ring.start(k, ADDED)

    def settle(self, then=None):
        for k in COLOURS:
            self.load(k, FAR).wait()
            for base in (FAR, ADDED):
                self.ring.arrived(k, base)
            add_into(self.own(k), *(self.bands.rows(self.landing.at[k, m], k) for m in WAYS))
            if then is None:
                self.store(k).start()
            else:
                then(k)

    def finish(self):
        self.ring.finish()
        if self.acc is not None:
            for k in COLOURS:
                self.store(k).wait()


class Rest:
    def __init__(self, bands, acc, result, own, relay2, in2, relay3, in3, *sems):
        self.bands, self.acc, self.own, self.result = bands, acc, own, result
        self.in2, self.in3, self.relay2, self.relay3, self.load_sem, self.store_sem = in2, in3, relay2, relay3, *sems[-2:]
        self.second = Ring(SECOND, bands, functools.partial(self.terms, acc), relay2, relay2, in2, *sems[:PAIR])
        self.third = Ring(THIRD, bands, self.final, relay3, relay3, in3, *sems[PAIR:2 * PAIR])

    def terms(self, ref, k, v, half=None):
        other = ALL if half is None else duo(half)
        first = self.bands.rest(k)[0] == COLOUR_DIMS[k][SECOND]
        return self.bands.rows(ref.at[(k, v, other) if first else (k, other, v)], k)

    def final(self, k, v, half=None):
        if half is None:
            return self.bands.rows(self.in2.at[k, 0, v], k)
        return self.in2.at[k, 0, v, self.bands.cuts(k)[half]]

    def load(self, k):
        return pltpu.make_async_copy(self.bands.rows(self.acc.at[k], k), self.bands.rows(self.own.at[k], k), self.load_sem.at[k])

    def store(self, k):
        rows = self.bands.rows
        return pltpu.make_async_copy(rows(self.in3.at[k, 0], k), rows(self.result.at[k], k), self.store_sem.at[k])

    def send(self, k):
        for base in (NEAR, FAR):
            self.second.start(k, base)

    def begin(self):
        for k in COLOURS:
            self.send(k)
        for k in COLOURS:
            self.load(k).start()

    def loaded(self):
        for k in COLOURS:
            self.load(k).wait()

    def relay(self):
        me = Torus()
        for k in COLOURS:
            self.second.arrived(k, NEAR)
            for m in WAYS:
                terms = self.terms(self.own, k, me.shift(COLOUR_DIMS[k][SECOND], toward(m)), m)
                add_into(self.second.carried(self.relay2, k, m), terms)
            self.second.start(k, ADDED)

    def settle(self):
        me = Torus()
        for k in COLOURS:
            for base in (FAR, ADDED):
                self.second.arrived(k, base)
            plus, minus = (self.bands.rows(self.in2.at[k, m], k) for m in WAYS)
            add_into(plus, minus, self.terms(self.own, k, me.at[COLOUR_DIMS[k][SECOND]]))
            for base in (NEAR, FAR):
                self.third.start(k, base)

    def relay_third(self):
        me = Torus()
        for k in COLOURS:
            self.third.arrived(k, NEAR)
            for m in WAYS:
                mine = self.third.carried(self.relay3, k, m)
                mine[...] += self.final(k, me.shift(COLOUR_DIMS[k][THIRD], toward(m)), m)[...]
            self.third.start(k, ADDED)

    def settle_third(self):
        me = Torus()
        for k in COLOURS:
            for base in (FAR, ADDED):
                self.third.arrived(k, base)
            plus, minus = (self.bands.rows(self.in3.at[k, m], k) for m in WAYS)
            plus[...] += minus[...] + self.final(k, me.at[COLOUR_DIMS[k][THIRD]])[...]
            if self.result is not None:
                self.store(k).start()

    def finish(self):
        self.second.finish()
        self.third.finish()
        if self.result is not None:
            for k in COLOURS:
                self.store(k).wait()

    def sums(self):
        return self.in3.at[:, 0]


class Spread:
    def __init__(self, bands, result, total, send, recv, local):
        self.bands, self.result, self.total, self.sems, self.local = bands, result, total, (send, recv), local

    @staticmethod
    def scratch():
        return [pltpu.SemaphoreType.DMA((C, ADDED))] * PAIR + [pltpu.SemaphoreType.DMA((C,))]

    def mine(self, k):
        return self.bands.rows(self.result.at[k], k)

    def place(self, k):
        return self.bands.rows(self.total.at[Torus().at["x"], k], k)

    def hop(self, k, m):
        me = Torus()
        by = toward(m)
        if m < FAR:
            src, dst = self.mine(k), self.place(k)
        else:
            dst = src = self.total.at[me.shift("x", -by), k, self.bands.cuts(k)[m - FAR]]
        return remote(src, dst, self.sems, (k, m), me.neighbour("x", by))

    def own(self, k):
        return pltpu.make_async_copy(self.mine(k), self.place(k), self.local.at[k])

    def begin(self):
        for k in COLOURS:
            self.own(k).start()
            for m in WAYS:
                self.hop(k, m).start()

    def forward(self):
        for k in COLOURS:
            for m in WAYS:
                self.hop(k, m).wait_recv()
                self.hop(k, FAR + m).start()

    def finish(self):
        for k in COLOURS:
            for m in WAYS:
                self.hop(k, FAR + m).wait_recv()
            self.own(k).wait()
            for m in range(ADDED):
                self.hop(k, m).wait_send()


def comm_params(collective_id):
    return pltpu.CompilerParams(collective_id=collective_id, has_side_effects=True, vmem_limit_bytes=VMEM_LIMIT)


def gather_kernel(*refs):
    n = len(Gather.semaphores())
    a, u, d = (Gather(kind, *refs[i::C][:PAIR], *refs[PAIR * C + n * i:][:n]) for i, kind in enumerate((WIDE, WIDE, DOWN)))
    enter()
    for gather in (a, u, d):
        gather.begin()
    for step, *ring in ((a.relay, FIRST), (u.relay, FIRST), (d.relay, FIRST), (a.settle, FIRST), (a.launch, SECOND),
                        (u.settle, FIRST), (u.launch, SECOND), (a.relay, SECOND), (d.settle, FIRST), (d.launch, SECOND),
                        (u.relay, SECOND), (a.settle, SECOND), (a.launch, THIRD), (d.relay, SECOND), (u.settle, SECOND),
                        (a.relay, THIRD), (d.settle, SECOND), (a.settle, THIRD), (u.sent, FIRST, SECOND),
                        (d.sent, FIRST, SECOND), (a.sent, FIRST, SECOND, THIRD)):
        step(*ring)


def gather_call(attn, up, down, collective_id):
    return pl.pallas_call(
        gather_kernel, out_shape=[sds(BF16, *Gather.shape(kind)) for kind in (WIDE, WIDE, DOWN)], in_specs=[ANY] * C,
        out_specs=[ANY] * C, scratch_shapes=Gather.semaphores() * C, compiler_params=comm_params(collective_id),
        name="gather")(attn, up, down)


class Background:
    def __init__(self, steps, plan):
        self.steps, self.plan = steps, plan

    def visit(self, place):
        for j, first, end in self.plan.get(place, ()):
            @at_step(j)
            def _():
                for step in self.steps[first:end]:
                    step()


class Push:
    def __init__(self, src, tail, rows, sems, slot=0):
        body = BODY * len(SEQ_PAIR)
        tails = TAIL * len(SEQ_PAIR)
        self.copies = [
            remote(src.at[pl.ds(start, size)], rows.at[pl.ds(to, size)], sems, (slot, i), Torus().partner())
            for i, (start, to, size) in enumerate(((0, body, body), (tail, PAIR * body + tails, tails)))]

    @staticmethod
    def semaphores(n):
        return [pltpu.SemaphoreType.DMA((n, PAIR))] * PAIR

    def start(self):
        for copy in self.copies:
            copy.start()

    def wait(self):
        for copy in self.copies:
            copy.wait_recv()

    def finish(self):
        for copy in self.copies:
            copy.wait_send()


class Exchange:
    def __init__(self, mine, theirs, rows, sems, slot):
        self.moves = []
        for s in SEQ_PAIR:
            for i, (start, size) in enumerate(((0, BODY), (BODY, TAIL))):
                place = lambda n: rows.at[pl.ds(start * len(SEQ_PAIR) * PAIR + size * n, size)]
                part = pl.ds(TOK * s + start, size)
                at = slot + (PAIR * s + i,)
                local = pltpu.make_async_copy(mine.at[part], place(s), sems[2].at[at])
                far = remote(theirs.at[part], place(len(SEQ_PAIR) + s), sems, at, Torus().partner())
                self.moves.append((local, far))

    @staticmethod
    def semaphores(*lead):
        return [pltpu.SemaphoreType.DMA(lead + (2 * PAIR,))] * 3

    def start(self):
        for local, far in self.moves:
            far.start()
            local.start()

    def wait(self):
        for local, far in self.moves:
            local.wait()
            far.wait_recv()

    def finish(self):
        for _, far in self.moves:
            far.wait_send()


NT = (((1,), (1,)), ((), ()))
TN = (((0,), (0,)), ((), ()))


def dot(a, b):
    return jnp.dot(a, b, preferred_element_type=F32)


def dot_nt(a, b):
    return lax.dot_general(a, b, NT, preferred_element_type=F32)


def dot_tn(a, b):
    return lax.dot_general(a, b, TN, preferred_element_type=F32)


def zeros_but(n, axis, value):
    return tuple(value if i == axis else 0 for i in range(n))


def whole(*shape):
    return pl.BlockSpec(shape, lambda *_: (0,) * len(shape))


def along(axis, *block, index=lambda j: j):
    return pl.BlockSpec(block, lambda j: zeros_but(len(block), axis, index(j)))


def row(vec, i):
    return vec[i:i + 1]


def row_mean(t):
    return jnp.mean(t, axis=-1, keepdims=True)


def norm_stats(t):
    centered = t - row_mean(t)
    rstd = lax.rsqrt(row_mean(centered * centered) + LN_EPS)
    return centered * rstd, rstd


def norm_back(xhat, rstd, g):
    return rstd * (g - row_mean(g) - xhat * row_mean(g * xhat))


def col_sum(t):
    return jnp.sum(t, axis=0, keepdims=True)


def at_step(j):
    return pl.when(pl.program_id(0) == j)


def accumulate(ref, value):
    @at_step(0)
    def _():
        ref[...] = value

    @pl.when(pl.program_id(0) > 0)
    def _():
        ref[...] += value


def pad(t):
    return jnp.concatenate([t.astype(F32), jnp.zeros((TOK - SEQ, t.shape[1]), F32)], axis=0).astype(BF16)


def window(h):
    start = h * HEAD // LANES * LANES
    stop = min(D, -(-(h + 1) * HEAD // LANES) * LANES)
    lane = lax.broadcasted_iota(jnp.int32, (1, stop - start), 1) + (start - h * HEAD)
    return slice(start, stop), (lane >= 0) & (lane < HEAD)


def only(mask, t):
    return jnp.where(mask, t, jnp.zeros_like(t))


def softmax(scores):
    e = jnp.exp(scores - jnp.max(scores, axis=-1, keepdims=True))
    return e * (1.0 / jnp.sum(e, axis=-1, keepdims=True))


def attention(s, rows, o, acc, visit):
    acc[...] = jnp.zeros_like(acc)
    start = pl.multiple_of(s * TOK, TAIL)
    tokens = pl.ds(start, SEQ)
    for h in range(HEADS):
        lanes, mask = window(h)
        k = only(mask, rows[K, tokens, lanes])
        v = only(mask, rows[V, tokens, lanes])
        probs = softmax(dot_nt(rows[Q, tokens, lanes], k) * SCALE).astype(BF16)
        acc[:, lanes] += dot(probs, v)
        visit(h)
    o[pl.ds(start, TOK)] = pad(acc[...])


def seq_rows(t, s):
    return t[TOK * s:TOK * s + SEQ]


def seq_tile(s):
    return pl.ds(TOK * s, TOK)


FRONT_PLAN = {"start": ((0, 0, 1),), "wo": ((O + 1, 1, 2),), "end": ((O + 1, 2, None),)}


def front_kernel(x, w, b, vec, _, qkv, h1, o, att, h2, up, rows, acc, *sems):
    hosted = Background(Gather(WIDE, None, up, *sems).last_ring(), FRONT_PLAN)
    j = pl.program_id(0)
    at_step(0)(enter)
    hosted.visit("start")

    @at_step(0)
    def _():
        for s in SEQ_PAIR:
            xhat, _ = norm_stats(x[s].astype(F32))
            h1[seq_tile(s)] = pad(xhat * row(vec, G1) + row(vec, C1))

    @pl.when(j < O)
    def _():
        t = (dot(h1[...], w[0]) + b[0]).astype(BF16)
        qkv[0] = t
        rows[j] = t

    pl.when(j >= O)(lambda: attention(j - O, rows, o, acc, hosted.visit))

    hosted.visit("wo")

    @at_step(O + LAST_SEQ)
    def _():
        a = dot(o[...], w[0]) + row(vec, BO)
        att[...] = a
        for s in SEQ_PAIR:
            xhat, _ = norm_stats(x[s].astype(F32) + row(vec, S1) * seq_rows(a, s))
            h2[seq_tile(s)] = pad(xhat * row(vec, G2) + row(vec, C2))

    hosted.visit("end")


def upto(n):
    return lambda j: jnp.minimum(j, n)


def front_call(x, w_attn, b_qkv, vec, up, collective_id):
    return pl.pallas_call(
        front_kernel, grid=(O + PAIR,),
        out_shape=(sds(BF16, O, TT, D), sds(BF16, TT, D), sds(BF16, TT, D), sds(F32, TT, D), sds(BF16, TT, D),
                   sds(BF16, *Gather.shape(WIDE))),
        in_specs=[whole(*SEQS), along(0, 1, D, D, index=upto(O)), along(0, 1, 1, D, index=upto(V)), whole(8, D), ANY],
        out_specs=(along(0, 1, TT, D, index=upto(V)),) + (whole(TT, D),) * SIDE + (ANY,),
        scratch_shapes=[pltpu.VMEM((O, TT, D), BF16), pltpu.VMEM((SEQ, D), F32)] + Gather.semaphores(),
        input_output_aliases={SIDE: SIDE + 1},
        compiler_params=comm_params(collective_id), name="front",
    )(x, w_attn, b_qkv, vec, up)


def w_out_block():
    return pl.BlockSpec((1, D, D), lambda j: (O, 0, 0), pipeline_mode=pl.Buffered(1))


TILES = FF // HALF
OWN_BODY = BODY * len(SEQ_PAIR)
TAILS = ROWS - TAIL * PAIR * len(SEQ_PAIR)


def put_rows(ref, tail, s, t):
    ref[pl.ds(pl.multiple_of(BODY * s, BODY), BODY)] = t[:BODY]
    ref[pl.ds(pl.multiple_of(tail + TAIL * s, TAIL), TAIL)] = t[BODY:]


DOWN_PLAN = {"start": ((0, 0, 1),), "end": ((TILES + 2, 1, 2), (2 * TILES - 1, 2, None))}


def mlp_in_kernel(h2, gz, w_up, b_up, vec, _, act, slope, d_down, down, a_rows, b_rows, b_away, *sems):
    a_sems, b_sems, sems = sems[:PAIR], sems[PAIR:2 * PAIR], sems[2 * PAIR:]
    hosted = Background(Gather(DOWN, None, down, *sems).last_ring(), DOWN_PLAN)
    j = pl.program_id(0)
    away = Push(b_away, OWN_BODY, b_rows, b_sems, 0)
    tile = lambda n: Push(a_rows.at[n], TAILS, a_rows.at[n], a_sems, n)
    at_step(0)(enter)
    hosted.visit("start")

    @at_step(0)
    def _():
        first = Torus().at["c"] == 0
        for s in SEQ_PAIR:
            d = pad(gz[s].astype(F32) * row(vec, S2))
            left, right = d[:, :HALF], d[:, D - HALF:]
            put_rows(b_rows, TAILS, s, jnp.where(first, left, right))
            put_rows(b_away, OWN_BODY, s, jnp.where(first, right, left))

    at_step(1)(away.start)
    for n in range(TILES):
        at_step(n + 1)(tile(n).start)

    @pl.when(j < TILES)
    def _():
        u = dot(h2[...], w_up[0]) + b_up[0]
        phi = 0.5 * (1.0 + lax.erf(u * math.sqrt(0.5)))
        slope[...] = phi + u * (jnp.exp(-0.5 * u * u) * math.sqrt(0.5 / math.pi))
        place = lax.rem(lax.broadcasted_iota(jnp.int32, (TT, 1), 0), TOK)
        a = only(place < SEQ, u * phi).astype(BF16)
        act[...] = a
        for s in SEQ_PAIR:
            put_rows(a_rows.at[j], TAILS, s, a[TOK * s:TOK * s + TOK])

    at_step(TILES)(away.wait)
    for n in range(TILES):
        at_step(TILES + n)(tile(n).wait)

    @pl.when(j >= TILES)
    def _():
        d_down[...] = dot_tn(a_rows[j - TILES], b_rows[...])

    hosted.visit("end")

    @at_step(2 * TILES - 1)
    def _():
        away.finish()
        for n in range(TILES):
            tile(n).finish()


def mlp_in_call(h2, gz, w_up, b_up, vec, down, collective_id):
    low = lambda j: jnp.minimum(j, TILES - 1)
    high = lambda j: jnp.maximum(j - TILES, 0)
    return pl.pallas_call(
        mlp_in_kernel, grid=(2 * TILES,),
        out_shape=(sds(BF16, TT, FF), sds(F32, TT, FF), sds(F32, FF, HALF), sds(BF16, *Gather.shape(DOWN))),
        in_specs=[whole(TT, D), whole(*SEQS), up_tile(low), along(0, 1, 1, HALF, index=low), whole(8, D), ANY],
        out_specs=(along(1, TT, HALF, index=low), along(1, TT, HALF, index=low),
                   along(0, HALF, HALF, index=high), ANY),
        scratch_shapes=[pltpu.VMEM((TILES, ROWS, HALF), BF16), pltpu.VMEM((ROWS, HALF), BF16),
                        pltpu.VMEM((PAIR * TOK, HALF), BF16)] + Push.semaphores(TILES) + Push.semaphores(1) +
        Gather.semaphores(),
        input_output_aliases={SIDE + 1: O},
        compiler_params=comm_params(collective_id), name="mlp_in",
    )(h2, gz, w_up, b_up.reshape(TILES, 1, HALF), vec, down)


def up_tile(index=lambda j: j):
    return pl.BlockSpec((1, D, HALF), lambda j: (index(j) // PAIR, 0, index(j) % PAIR))


MLP_PLAN = {"start": ((0, 0, 2),), "end": ((3, 2, 3), (TILES - 1, 3, None))}


def mlp_out_kernel(act, slope, gz, w_up, w_down, vec, part, d_pre, db_up, mlp, d_h2, sums, dm, *scratch):
    first = First(Bands(DOWN), part, sums, *scratch)
    hosted = Background([first.near, first.far, first.relay, first.settle, first.finish], MLP_PLAN)
    at_step(0)(enter)
    hosted.visit("start")

    @at_step(0)
    def _():
        for s in SEQ_PAIR:
            dm[seq_tile(s)] = pad(gz[s].astype(F32) * row(vec, S2))

    accumulate(mlp, dot(act[...], w_down[...]))
    d = dot_nt(dm[...], w_down[...]) * slope[...]
    db_up[0] = col_sum(d)
    d = d.astype(BF16)
    d_pre[0, 0] = d
    accumulate(d_h2, dot_nt(d, w_up[0]))
    hosted.visit("end")


def mlp_out_call(act, slope, gz, w_up, w_down, vec, part, collective_id):
    return pl.pallas_call(
        mlp_out_kernel, grid=(TILES,),
        out_shape=(sds(BF16, PAIR, SIDE, TT, HALF), sds(F32, TILES, 1, HALF), sds(F32, TT, D), sds(F32, TT, D),
                   Bands(DOWN).sums()),
        in_specs=[along(1, TT, HALF), along(1, TT, HALF), whole(*SEQS), up_tile(), along(0, HALF, D), whole(8, D), ANY],
        out_specs=(pl.BlockSpec((1, 1, TT, HALF), lambda j: (j % PAIR, j // PAIR, 0, 0)), along(0, 1, 1, HALF),
                   whole(TT, D), whole(TT, D), ANY),
        scratch_shapes=[pltpu.VMEM((TT, D), BF16)] + Bands(DOWN).first(),
        compiler_params=comm_params(collective_id), name="mlp_out",
    )(act, slope, gz, w_up, w_down, vec, part)


def halves_of(t):
    t = pad(t)
    return t[:, :HALF], jnp.concatenate([t[:, HALF:], jnp.zeros((TOK, QCOLS - D), BF16)], axis=1)


def mid(mlp, d_h2, att, x, gz, vec, w_out, z, g_res, d_att, d_o, sums, da_rows):
    a = att[:SEQ]
    y = x[0].astype(F32) + row(vec, S1) * a
    m = mlp[:SEQ] + row(vec, B2)
    g = gz[0].astype(F32)
    z[0] = (y + row(vec, S2) * m).astype(BF16)
    xhat, rstd = norm_stats(y)
    dh = d_h2[:SEQ]
    gr = g + norm_back(xhat, rstd, dh * row(vec, G2))
    g_res[:SEQ] = gr
    da = gr * row(vec, S1)
    terms = (da, gr * a, dh * xhat, dh, g * row(vec, S2), g * m)
    accumulate(sums, jnp.concatenate([jnp.zeros((BO, D), F32)] + [col_sum(t) for t in terms], axis=0))
    for i, t in enumerate(halves_of(da)):
        d_att[i] = t
    da_rows[pl.ds(pl.multiple_of(pl.program_id(0) * TOK, TAIL), TOK)] = pad(da)

    @at_step(LAST_SEQ)
    def _():
        d_o[...] = dot_nt(da_rows[...], w_out[0]).astype(BF16)


def attention_back(s, qkv, d_o, d_qkv, db, acc, b_rows, away, first, visit):
    acc[...] = jnp.zeros_like(acc)
    for h in range(HEADS):
        lanes, mask = window(h)
        q, k, v = (only(mask, qkv[i, :SEQ, lanes]) for i in (Q, K, V))
        do = only(mask, d_o[:SEQ, lanes])
        scores = dot_nt(k, q) * SCALE
        e = jnp.exp(scores - jnp.max(scores, axis=0, keepdims=True))
        probs = e * (1.0 / col_sum(e))
        acc[V, :, lanes] += dot(probs.astype(BF16), do)
        dp = dot_nt(v, do)
        ds = probs * (dp - col_sum(dp * probs))
        ds = (ds * SCALE).astype(BF16)
        acc[K, :, lanes] += dot(ds, q)
        acc[Q, :, lanes] += dot_tn(ds, k)
        visit(h)
    accumulate(db, jnp.concatenate([col_sum(acc[i]) for i in (Q, K, V)], axis=0))
    for n in (Q, K, V):
        left, right = halves_of(acc[n])
        d_qkv[0, n] = left
        d_qkv[1, n] = right
        put_rows(b_rows.at[n], TAILS, s, jnp.where(first, left, right))
        put_rows(away.at[n], OWN_BODY, s, jnp.where(first, right, left))


PER = HALF // STEP


class WideGrads:
    def __init__(self, inputs, a_of, cotangents, out, base, lead, a_rows, a_cols, b_rows):
        self.inputs, self.a_of, self.cotangents, self.out, self.base, self.lead = inputs, a_of, cotangents, out, base, lead
        self.a_rows, self.a_cols, self.b_rows = a_rows, a_cols, b_rows

    @staticmethod
    def scratch(inputs):
        return [pltpu.VMEM((inputs, ROWS, D), BF16), pltpu.VMEM((inputs, D, ROWS), BF16), pltpu.VMEM((SIDE, ROWS, HALF), BF16)]

    def step(self):
        j = pl.program_id(0)
        done = []
        for t in range(SIDE):
            n = (t + self.lead) % SIDE

            @at_step(self.base + PER * t)
            def _():
                i = self.a_of[n]
                if i not in done:
                    self.inputs[i].wait()
                    self.a_cols[i] = self.a_rows[i].T
                    done.append(i)
                self.cotangents[n].wait()

        @pl.when(j >= self.base)
        def _():
            n = lax.rem(lax.div(j - self.base, PER) + self.lead, SIDE)
            cols = pl.ds(pl.multiple_of(lax.rem(j - self.base, PER) * STEP, STEP), STEP)
            i = 0 if len(self.inputs) == 1 else lax.div(n, O)
            self.out[0] = dot(self.a_cols[i], self.b_rows[n, :, cols])

    def finish(self):
        for move in (*self.inputs, *self.cotangents):
            move.finish()


def grads_block(base, lead):
    def index(j):
        n = jnp.maximum(j - base, 0)
        return (n // PER + lead) % SIDE, 0, n % PER

    return pl.BlockSpec((1, D, STEP), index)


GRAD_STEPS = PER * SIDE


def tok_block():
    return along(0, TOK, D, index=upto(LAST_SEQ))


def seq_block():
    return along(0, 1, SEQ, D, index=upto(LAST_SEQ))


MID_PLAN = {"start": ((0, 0, 1),), "end": ((1, 1, 3), (8, 3, 4), (11, 4, 5), (LAST_SEQ + GRAD_STEPS, 5, None))}


def mid_kernel(*refs):
    refs = list(refs)
    take = lambda n: [refs.pop(0) for _ in range(n)]
    ins, (h2, d_pre, acc), outs, (d_up, result), da_rows = take(7), take(3), take(5), take(2), refs.pop(0)
    rows, a_sems, b_sems = take(3), take(C), take(C)
    rest = Rest(Bands(DOWN), acc, result, *refs)
    hosted = Background([rest.begin, rest.loaded, rest.relay, rest.settle, rest.relay_third, rest.settle_third, rest.finish],
                        MID_PLAN)
    c = Torus().at["c"]
    grads = WideGrads(
        [Exchange(h2, h2, rows[0].at[0], a_sems, ())], (0,) * SIDE,
        [Exchange(d_pre.at[c, n], d_pre.at[1 - c, n], rows[2].at[n], b_sems, (n,)) for n in range(SIDE)], d_up, SEQS[0], 0, *rows)
    at_step(0)(enter)
    hosted.visit("start")

    @at_step(0)
    def _():
        for move in (*grads.inputs, *grads.cotangents):
            move.start()

    pl.when(pl.program_id(0) < SEQS[0])(lambda: mid(*ins, *outs, da_rows))
    grads.step()
    hosted.visit("end")
    at_step(LAST_SEQ + GRAD_STEPS)(grads.finish)


def mid_call(mlp, d_h2, att, x, gz, vec, w_attn, h2, d_pre, acc, collective_id):
    return pl.pallas_call(
        mid_kernel, grid=(SEQS[0] + GRAD_STEPS,),
        out_shape=(sds(BF16, *SEQS), sds(F32, TT, D), sds(BF16, PAIR, TT, HALF), sds(BF16, TT, D), sds(F32, 8, D),
                   sds(F32, SIDE, D, HALF), Bands(DOWN).result()),
        in_specs=[tok_block()] * O + [seq_block()] * PAIR + [whole(8, D), w_out_block()] + [ANY] * O,
        out_specs=(seq_block(), tok_block(), along(1, PAIR, TOK, HALF, index=upto(LAST_SEQ)), whole(TT, D), whole(8, D),
                   grads_block(SEQS[0], 0), ANY),
        scratch_shapes=[pltpu.VMEM((TT, D), BF16)] + WideGrads.scratch(1) + Exchange.semaphores() + Exchange.semaphores(SIDE) +
        Bands(DOWN).later(),
        compiler_params=comm_params(collective_id), name="mid",
    )(mlp, d_h2, att, x, gz, vec, w_attn, h2, d_pre, acc)


ATTN_PLAN = {"start": ((0, 0, 3),), 6: ((0, 3, 4),), "end": ((LAST_SEQ, 4, 5), (LAST_SEQ + GRAD_STEPS, 5, None))}


def attn_back_kernel(*refs):
    refs = list(refs)
    take = lambda n: [refs.pop(0) for _ in range(n)]
    (qkv, d_o), (h1, o, d_att, part, result), (d_qkv, db, d_attn, sums, total) = take(2), take(5), take(5)
    acc, away, rows = refs.pop(0), refs.pop(0), take(3)
    a_sems, b_sems, away_sems = take(C), take(C), take(PAIR)
    first = First(Bands(WIDE), part, sums, *take(len(Bands(WIDE).first())))
    spread = Spread(Bands(DOWN), result, total, *refs)
    hosted = Background([spread.begin, first.near, first.far, spread.forward, first.relay, first.settle, first.finish,
                         spread.finish], ATTN_PLAN)
    c = Torus().at["c"]
    pushes = [Push(away.at[n], OWN_BODY, rows[2].at[n], away_sems, n) for n in range(O)]
    grads = WideGrads(
        [Exchange(a, a, rows[0].at[i], a_sems, (i,)) for i, a in enumerate((h1, o))], (0,) * O + (1,),
        pushes + [Exchange(d_att.at[c], d_att.at[1 - c], rows[2].at[O], b_sems, ())], d_attn, SEQS[0], O, *rows)
    at_step(0)(enter)
    hosted.visit("start")

    @at_step(0)
    def _():
        for move in (*grads.inputs, grads.cotangents[O]):
            move.start()

    @at_step(SEQS[0])
    def _():
        for push in pushes:
            push.start()

    j = pl.program_id(0)
    pl.when(j < SEQS[0])(lambda: attention_back(j, qkv, d_o, d_qkv, db, acc, rows[2], away, c == 0, hosted.visit))

    grads.step()
    hosted.visit("end")
    at_step(LAST_SEQ + GRAD_STEPS)(grads.finish)


def attn_back_call(qkv, d_o, h1, o, d_att, part, result, collective_id):
    return pl.pallas_call(
        attn_back_kernel, grid=(SEQS[0] + GRAD_STEPS,),
        out_shape=(sds(BF16, PAIR, O, TT, HALF), sds(F32, O, D), sds(F32, SIDE, D, HALF), Bands(WIDE).sums(),
                   Bands(DOWN).total()),
        in_specs=[along(1, O, TOK, D, index=upto(LAST_SEQ)), tok_block()] + [ANY] * 5,
        out_specs=(along(2, PAIR, O, TOK, HALF, index=upto(LAST_SEQ)), whole(O, D), grads_block(SEQS[0], O), ANY, ANY),
        scratch_shapes=[pltpu.VMEM((O, SEQ, D), F32), pltpu.VMEM((O, PAIR * TOK, HALF), BF16)] + WideGrads.scratch(2) +
        Exchange.semaphores(PAIR) + Exchange.semaphores() + Push.semaphores(O) + Bands(WIDE).first() + Spread.scratch(),
        compiler_params=comm_params(collective_id), name="attn_back",
    )(qkv, d_o, h1, o, d_att, part, result)


IN_STEPS = PAIR * O
SLOT = 40
LAST_PLAN = {"start": ((0, 0, 2),), "end": ((O, 2, None),)}


def last_kernel(*refs):
    refs = list(refs)
    take = lambda n: [refs.pop(0) for _ in range(n)]
    (d_half, w, x, g_res, vec), (small, acc_up, _), (dx, part, *totals) = take(5), take(3), take(5)
    acc, sums, pair_sums, block, block_sem, swap_sems = refs.pop(0), refs.pop(0), refs.pop(0), refs.pop(0), refs.pop(0), take(PAIR)
    halves = [Bands(WIDE, h) for h in WAYS]
    a, b = (First(bands, part, None, *take(len(bands.first()))) for bands in halves)
    rest_a, rest_b = (Rest(f.bands, f.own_all, None, f.own_all, *take(len(f.bands.later()) - 1)) for f in (a, b))
    rest_up = Rest(Bands(WIDE), acc_up, None, *take(len(Bands(WIDE).later())))
    spread_up, spread_a, spread_b = (
        Spread(r.bands, r.sums(), total, *take(len(Spread.scratch()))) for r, total in zip((rest_up, rest_a, rest_b), totals))
    hosted = Background([rest_up.begin, a.near, rest_up.loaded, rest_up.relay], LAST_PLAN)
    me = Torus()
    swap = remote(sums, pair_sums, swap_sems, (), me.partner())
    fetch = pltpu.make_async_copy(small, block, block_sem)
    at_step(0)(enter)
    hosted.visit("start")
    at_step(0)(fetch.start)

    @pl.when(pl.program_id(0) < IN_STEPS)
    def _():
        accumulate(acc, dot_nt(d_half[0, 0], w[0]))

    @at_step(IN_STEPS - 1)
    def _():
        rows = jnp.zeros((SUB, D), F32)
        for s in SEQ_PAIR:
            xhat, rstd = norm_stats(x[s].astype(F32))
            tokens = pl.ds(TOK * s, SEQ)
            dh = acc[tokens]
            rows = rows + jnp.concatenate([col_sum(dh * xhat), col_sum(dh), jnp.zeros((SUB - BO, D), F32)], axis=0)
            dx[s] = (g_res[tokens] + norm_back(xhat, rstd, dh * row(vec, G1))).astype(BF16)
        sums[...] = rows

    hosted.visit("end")

    @at_step(IN_STEPS)
    def _():
        swap.start()
        fetch.wait()
        swap.wait()
        both = sums[...] + pair_sums[...]
        for d in range(DEVICES):
            at = CHIP * (d // PAIR) + SLOT + OWN * (d % PAIR)
            block[at:at + BO, :OWN] = both[:BO, OWN * d:OWN * d + OWN]

        @pl.when(me.at["c"] == 1)
        def _():
            for z in range(SIDE):
                for y in range(SIDE):
                    rows = block.at[pl.ds(CHIP * (SIDE * z + y), CHIP)]
                    put = pltpu.make_async_copy(rows, part.at[0, z, y, :, pl.ds(HALF - LANES, LANES)], block_sem)
                    put.start()
            pltpu.make_async_copy(block, small, block_sem).wait()

        for step in (b.near, rest_up.settle, a.far, rest_up.relay_third, b.far, a.relay, rest_up.settle_third, spread_up.begin,
                     b.relay, spread_up.forward, functools.partial(a.settle, rest_a.send),
                     functools.partial(b.settle, rest_b.send), rest_a.relay, rest_b.relay, rest_a.settle, rest_b.settle,
                     rest_a.relay_third, rest_b.relay_third, rest_a.settle_third, spread_a.begin, rest_b.settle_third,
                     spread_b.begin, spread_a.forward, spread_b.forward, spread_up.finish, spread_a.finish, spread_b.finish,
                     rest_up.finish, rest_a.finish, rest_b.finish, a.finish, b.finish):
            step()


def last_call(d_qkv, w_attn, x, g_res, vec, small, acc_up, part, collective_id):
    low = upto(IN_STEPS - 1)
    halves = [Bands(WIDE, h) for h in WAYS]
    dma = pltpu.SemaphoreType.DMA
    return pl.pallas_call(
        last_kernel, grid=(IN_STEPS + 1,),
        out_shape=(sds(BF16, *SEQS), sds(F32, *part.shape), Bands(WIDE).total(), *(h.total() for h in halves)),
        in_specs=[pl.BlockSpec((1, 1, TT, HALF), lambda j: (low(j) % PAIR, low(j) // PAIR, 0, 0)), up_tile(low),
                  whole(*SEQS), whole(TT, D), whole(8, D)] + [ANY] * O,
        out_specs=(whole(*SEQS),) + (ANY,) * SIDE,
        scratch_shapes=[pltpu.VMEM((TT, D), F32), pltpu.VMEM((SUB, D), F32), pltpu.VMEM((SUB, D), F32),
                        pltpu.VMEM((D, LANES), F32), dma, dma, dma] + halves[0].first() * PAIR + halves[0].later()[1:] * PAIR +
        Bands(WIDE).later() + Spread.scratch() * O,
        input_output_aliases={7: 1},
        compiler_params=comm_params(collective_id), name="last",
    )(d_qkv, w_attn, x, g_res, vec, small, acc_up, part)


BQ, BU, VEC = 3 * D // 32, 3 * D // 32 + FF // 32, 3 * D // 32 + FF // 32 + 8 * OWN


def pair_swap(a):
    return lax.ppermute(a, "fsdp", [(i, i ^ 1) for i in range(DEVICES)])


def by_core(first, a, b):
    return jnp.where(first, a, b), jnp.where(first, b, a)


def my_pieces(shards, first):
    w_qkv, b_qkv, w_out, w_up, b_up, w_down, vec_params = shards
    x = lax.axis_index("rep")
    small = jnp.concatenate([b_qkv, b_up, vec_params.reshape(-1)])
    small = jnp.pad(small, (0, OWN * LANES - VEC)).reshape(OWN, LANES)
    attn = lax.dynamic_slice_in_dim(jnp.concatenate([w_qkv, w_out], axis=1), x * D, D, 1)
    attn = jnp.concatenate([attn, small], axis=1)
    up = lax.dynamic_slice_in_dim(w_up, x * QCOLS, QCOLS, 1)
    wide = jnp.stack([attn, up]).astype(BF16)
    mine, theirs = by_core(first, wide[..., :HALF], wide[..., HALF:])
    theirs = pair_swap(theirs)
    piece = jnp.concatenate(by_core(first, mine, theirs), axis=1)
    down = lax.dynamic_slice_in_dim(w_down, x * 48, 48, 0).astype(BF16).reshape(3, 16, D)
    return piece[0], piece[1], down


def small_params(w_attn):
    small = w_attn[0, :, D:].astype(F32).reshape(DEVICES, OWN * LANES)
    vec = small[:, BU:VEC].reshape(DEVICES, 8, OWN).transpose(1, 0, 2).reshape(8, D)
    return small[:, :BQ].reshape(O, 1, D), small[:, BQ:BU].reshape(FF), vec


ROOM = 5 * LANES


def small_grads(db_qkv, db_up, sums):
    vec = sums[BO:].reshape(8 - BO, DEVICES, OWN).transpose(1, 0, 2).reshape(DEVICES, VEC - BU - BO * OWN)
    small = jnp.concatenate([db_qkv.reshape(DEVICES, BQ), db_up.reshape(DEVICES, BU - BQ), vec], axis=1)
    small = small + pair_swap(small)
    small = jnp.pad(small, ((0, 0), (0, ROOM - small.shape[1]))).reshape(DEVICES, ROOM // LANES, LANES)
    return jnp.pad(small, ((0, 0), (0, OWN - ROOM // LANES), (0, 0))).reshape(D, LANES)


def rows_of(total):
    return jnp.concatenate([total[:, k, :n] for k, (_, n) in enumerate(BANDS[WIDE])], axis=1)


def final_rows(total, first):
    keep, give = by_core(first, total[:, :OWN], total[:, OWN:])
    pair = jnp.stack(by_core(first, keep, pair_swap(give)), axis=1)
    return pair.transpose(2, 0, 1, 3).reshape(OWN, SIDE, QCOLS)


def final_down(total, first):
    down = total.reshape(FF // 16, HALF)
    keep, give = by_core(first, down[:FF // DEVICES], down[FF // DEVICES:])
    left, right = by_core(first, keep, pair_swap(give))
    return jnp.concatenate([left, right[:, 2 * HALF - D:]], axis=1)


def device_step(x, gz, *shards):
    first = lax.rem(lax.axis_index("fsdp"), PAIR) == 0
    attn, up, down = my_pieces(shards, first)
    w_attn, up, down = gather_call(attn, up, down, 0)
    w_attn = w_attn.reshape(SIDE, D, QCOLS)
    b_qkv, b_up, vec = small_params(w_attn)
    qkv, h1, o, att, h2, w_up = front_call(x, w_attn, b_qkv, vec, up, 1)
    w_up = w_up.reshape(SIDE, D, QCOLS)
    act, slope, part, w_down = mlp_in_call(h2, gz, w_up, b_up, vec, down, 2)
    part = part.reshape((SIDE,) * 3 + (C * UNIT, HALF))
    d_pre, db_up, mlp, d_h2, acc = mlp_out_call(act, slope, gz, w_up, w_down.reshape(FF, D), vec, part, 3)
    z, g_res, d_att, d_o, sums, part, result = mid_call(mlp, d_h2, att, x, gz, vec, w_attn, h2, d_pre, acc, 4)
    part = part.reshape((SIDE,) * 3 + (CHIP, HALF))
    d_qkv, db_qkv, part, acc, down = attn_back_call(qkv, d_o, h1, o, d_att, part, result, 5)
    small = small_grads(db_qkv, db_up, sums)
    part = part.reshape((SIDE,) * 3 + (CHIP, HALF))
    dx, _, up, attn0, attn1 = last_call(d_qkv, w_attn, x, g_res, vec, small, acc, part, 6)
    g_up = final_rows(rows_of(up), first).reshape(OWN, FF)
    attn = final_rows(jnp.concatenate([rows_of(attn0), rows_of(attn1)], axis=-1), first)
    small = attn[:ROOM // LANES, 0, D:].reshape(ROOM)
    vec = jnp.concatenate([attn[SLOT:SLOT + BO, 0, D:D + OWN], small[BU:VEC - BO * OWN].reshape(8 - BO, OWN)], axis=0)
    return (z, dx, attn[:, :O, :D].reshape(OWN, O * D), small[:BQ], attn[:, O, :D], g_up, small[BQ:BU],
            final_down(down, first), vec)


def solution(mesh):
    batch = P(("rep", "fsdp"), None, None)
    rows, flat, cols = P("fsdp", None), P("fsdp"), P(None, "fsdp")
    shards = (rows, flat, rows, rows, flat, rows, cols)
    return jax.shard_map(device_step, mesh=mesh, in_specs=(batch, batch) + shards,
                         out_specs=(batch, batch) + shards, check_vma=False)
```

```python
import functools
import math

import jax
import jax.numpy as jnp
from jax import lax
from jax.experimental import pallas as pl
from jax.experimental.pallas import tpu as pltpu
from jax.sharding import PartitionSpec as P

HEADS = 16
LN_EPS = 1e-5
D = 1408
FF = 6144
SEQ = 257
HEAD = D // HEADS
SCALE = HEAD ** -0.5
QCOLS = 1536
HALF = 768
OWN = 44
CHIP = 2 * OWN
LANES = 128
DEVICES = 32
F32 = jnp.float32
BF16 = jnp.bfloat16
VMEM_LIMIT = 66 * 1000 * 1000
G1, C1, BO, S1, G2, C2, B2, S2 = range(8)
Q, K, V, O = range(4)
SEQS = (2, SEQ, D)
LAST_SEQ = SEQS[0] - 1
SEQ_PAIR = range(SEQS[0])
TAIL = 16
BODY = SEQ - 1
TOK = BODY + TAIL
TT = 2 * TOK
ROWS = 4 * TOK
STEP = 256


def sds(dtype, *shape):
    return jax.ShapeDtypeStruct(shape, dtype)


MESH_ID = pl.DeviceIdType.MESH
SIDE = 4
SUB = 8
PAIR = 2
C = 3
COLOURS = range(C)
COLOUR_DIMS = ("xyz", "yzx", "zxy")
FIRST, SECOND, THIRD, LAST = range(4)
WAYS = range(PAIR)
NEAR, FAR, ADDED = 0, 2, 4
WIDE, DOWN = "wide", "down"
ANY = pl.BlockSpec(memory_space=pl.ANY)
ALL = slice(None)


def duo(m):
    return pl.ds(PAIR * m, PAIR)


def toward(m):
    return 1 - PAIR * (m % PAIR)


class Torus:
    def __init__(self):
        f = lax.axis_index("fsdp")
        self.at = {"x": lax.axis_index("rep"), "z": lax.div(f, SIDE * PAIR), "y": lax.rem(lax.div(f, PAIR), SIDE),
                   "c": lax.rem(f, PAIR)}

    def shift(self, dim, by):
        return lax.rem(self.at[dim] + (SIDE + by), SIDE)

    def device(self, **moved):
        p = {**self.at, **moved}
        return (p["x"], (p["z"] * SIDE + p["y"]) * PAIR + p["c"])

    def neighbour(self, dim, by):
        return self.device(**{dim: self.shift(dim, by)})

    def partner(self):
        return self.device(c=1 - self.at["c"])


def enter():
    me = Torus()
    barrier = pltpu.get_barrier_semaphore()
    others = [me.neighbour(d, toward(m)) for d in COLOUR_DIMS[0] for m in WAYS] + [me.partner()]
    for other in others:
        pl.semaphore_signal(barrier, device_id=other, device_id_type=MESH_ID)
    pl.semaphore_wait(barrier, len(others))


def remote(src, dst, sems, slot, device):
    return pltpu.make_async_remote_copy(src_ref=src, dst_ref=dst, send_sem=sems[0].at[slot], recv_sem=sems[1].at[slot],
                                        device_id=device, device_id_type=MESH_ID)


class Gather:
    def __init__(self, kind, src, dst, hop_send, hop_recv, push_send, push_recv, local):
        self.kind, self.src, self.dst, self.local = kind, src, dst, local
        self.hops, self.pushes = (hop_send, hop_recv), (push_send, push_recv)
        self.cols, self.cut = (256, 128) if kind == WIDE else (D, HALF)

    @staticmethod
    def semaphores():
        dma = pltpu.SemaphoreType.DMA
        return [dma((C, C, ADDED))] * PAIR + [dma((C, ADDED + 1))] * PAIR + [dma((C,))]

    @staticmethod
    def shape(kind):
        return (SIDE,) * 3 + (CHIP, QCOLS) if kind == WIDE else (SIDE, SIDE, PAIR, SIDE, C, 16, D)

    def source(self, k):
        return self.src.at[:, pl.ds(self.cols * k, self.cols)] if self.kind == WIDE else self.src.at[k]

    def piece(self, me, k, s, v, half=None):
        dims = COLOUR_DIMS[k]
        at = {**me.at, **{d: ALL for d in dims[:s]}, dims[s]: v}
        off, width = 0, self.cols
        if half is not None and s == FIRST:
            off, width = self.cut * half, (self.cut, self.cols - self.cut)[half]
        elif half is not None:
            at[dims[0]] = duo(half)
        if self.kind == WIDE:
            cols = pl.ds(pl.multiple_of(at["c"] * HALF + self.cols * k + off, 128), width)
            return self.dst.at[at["x"], at["z"], at["y"], :, cols]
        return self.dst.at[at["z"], at["y"], at["c"], at["x"], k, :, pl.ds(off, width)]

    def hop(self, k, s, m):
        me = Torus()
        dim = COLOUR_DIMS[k][s]
        by = toward(m)
        if m < FAR:
            ref = self.piece(me, k, s, me.at[dim])
        else:
            ref = self.piece(me, k, s, me.shift(dim, -by), m - FAR)
        src = self.source(k) if s == FIRST and m < FAR else ref
        return remote(src, ref, self.hops, (k, s, m), me.neighbour(dim, by))

    def push(self, k, n):
        me = Torus()
        dim = COLOUR_DIMS[k][THIRD]
        if n < FAR:
            ref = self.piece(me, k, THIRD, me.shift(dim, -toward(n)))
        elif n < ADDED:
            ref = self.piece(me, k, THIRD, me.shift(dim, FAR), n - FAR)
        else:
            ref = self.piece(me, k, THIRD, me.at[dim])
        return remote(ref, ref, self.pushes, (k, n), me.partner())

    def own(self, k):
        me = Torus()
        return pltpu.make_async_copy(self.source(k), self.piece(me, k, FIRST, me.at[COLOUR_DIMS[k][FIRST]]), self.local.at[k])

    def launch(self, s):
        for k in COLOURS:
            for m in WAYS:
                self.hop(k, s, m).start()
            if s == THIRD:
                self.push(k, ADDED).start()

    def relay(self, s):
        for k in COLOURS:
            for m in WAYS:
                self.hop(k, s, m).wait_recv()
                self.hop(k, s, FAR + m).start()
                if s == THIRD:
                    self.push(k, m).start()

    def settle(self, s):
        for k in COLOURS:
            for m in WAYS:
                self.hop(k, s, FAR + m).wait_recv()
                if s == THIRD:
                    self.push(k, FAR + m).start()
            if s == FIRST:
                self.own(k).wait()

    def begin(self):
        for k in COLOURS:
            self.own(k).start()
        self.launch(FIRST)

    def sent(self, *rings):
        for k in COLOURS:
            for s in rings:
                for m in range(ADDED):
                    self.hop(k, s, m).wait_send()
            if THIRD in rings:
                for n in range(ADDED + 1):
                    self.push(k, n).wait()

    def last_ring(self):
        return [functools.partial(f, THIRD) for f in (self.launch, self.relay, self.settle, self.sent)]


def add_into(total, *others):
    lead = total.shape[:-2]

    def body(i, carry):
        idx = []
        for n in reversed(lead):
            idx.insert(0, lax.rem(i, n))
            i = lax.div(i, n)
        value = total[tuple(idx)]
        for other in others:
            value = value + other[tuple(idx)]
        total[tuple(idx)] = value
        return carry

    lax.fori_loop(0, math.prod(lead), body, 0)


class Ring:
    def __init__(self, s, bands, terms, passed, relay, landing, send, recv):
        self.s, self.bands, self.terms, self.passed, self.relay, self.landing = s, bands, terms, passed, relay, landing
        self.sems = (send, recv)

    def zone(self, k, way, half):
        if self.s == THIRD:
            return self.landing.at[k, way, self.bands.cuts(k)[half]]
        return self.bands.rows(self.landing.at[k, way, duo(half)], k)

    def carried(self, ref, k, way):
        if self.s == THIRD:
            return ref.at[k, way, pl.ds(0, self.bands.cuts(k)[way].size)]
        return self.bands.rows(ref.at[k, way], k)

    def hop(self, k, m):
        me = Torus()
        dim = COLOUR_DIMS[k][self.s]
        way, by = m % PAIR, toward(m)
        if m < FAR:
            src, dst = self.terms(k, me.shift(dim, FAR), way), self.carried(self.relay, k, way)
        elif m < ADDED:
            src, dst = self.terms(k, me.shift(dim, by), 1 - way), self.zone(k, way, 1 - way)
        else:
            src, dst = self.carried(self.passed, k, way), self.zone(k, way, way)
        return remote(src, dst, self.sems, (k, m), me.neighbour(dim, by))

    def start(self, k, base):
        for m in WAYS:
            self.hop(k, base + m).start()

    def arrived(self, k, base):
        for m in WAYS:
            self.hop(k, base + m).wait_recv()

    def finish(self):
        for k in COLOURS:
            for m in range(ADDED + PAIR):
                self.hop(k, m).wait_send()

    @staticmethod
    def semaphores():
        return [pltpu.SemaphoreType.DMA((C, ADDED + PAIR))] * PAIR


UNIT = 32
BANDS = {WIDE: ((0, 24), (24, UNIT), (56, UNIT)), DOWN: ((0, UNIT), (UNIT, UNIT), (2 * UNIT, UNIT))}
ORDERS = {WIDE: "xzy", DOWN: "zyx"}


class Bands:
    def __init__(self, kind, half=None):
        self.order, self.bands = ORDERS[kind], BANDS[kind]
        self.width = HALF if half is None else HALF // PAIR
        self.cols = pl.ds(self.width * (half or 0), self.width)

    def band(self, k):
        return pl.ds(*self.bands[k])

    def rows(self, ref, k):
        return ref.at[(ALL,) * (len(ref.shape) - PAIR) + (pl.ds(0, self.bands[k][1]),)]

    def cuts(self, k):
        rows = self.bands[k][1]
        cut = (rows // SUB + 1) // PAIR * SUB
        return pl.ds(0, cut), pl.ds(cut, rows - cut)

    def rest(self, k):
        return [d for d in self.order if d != COLOUR_DIMS[k][FIRST]]

    def units(self, *lead):
        return lead + (UNIT, self.width)

    def vmem(self, *lead):
        return pltpu.VMEM(self.units(*lead), F32)

    def sums(self):
        return sds(F32, *self.units(C, SIDE, SIDE))

    def result(self):
        return sds(F32, *self.units(C))

    def total(self):
        return sds(F32, *self.units(SIDE, C))

    def first(self):
        relays = [self.vmem(C, PAIR, PAIR, SIDE)] * PAIR
        dma = pltpu.SemaphoreType.DMA
        return [self.vmem(C, SIDE, SIDE), *relays, self.vmem(C, PAIR, SIDE, SIDE), *Ring.semaphores(), dma((C, C)), dma((C,))]

    def later(self):
        dma = pltpu.SemaphoreType.DMA
        return [self.vmem(C, SIDE, SIDE), self.vmem(C, PAIR, PAIR), self.vmem(C, PAIR, SIDE),
                pltpu.VMEM((C, PAIR, UNIT // PAIR, self.width), F32), self.vmem(C, PAIR),
                *Ring.semaphores(), *Ring.semaphores(), dma((C,)), dma((C,))]


class First:
    def __init__(self, bands, part, acc, own, passed, relay, landing, send, recv, load, store):
        self.bands, self.part, self.acc, self.own_all, self.passed = bands, part, acc, own, passed
        self.relay_in, self.landing, self.load_sem, self.store_sem = relay, landing, load, store
        self.ring = Ring(FIRST, bands, self.terms, passed, relay, landing, send, recv)

    def own(self, k):
        return self.bands.rows(self.own_all.at[k], k)

    def terms(self, k, v, half=None):
        b = self.bands
        at = {d: ALL for d in b.order}
        at[COLOUR_DIMS[k][FIRST]] = v
        if half is not None:
            at[b.rest(k)[0]] = duo(half)
        return self.part.at[tuple(at[d] for d in b.order) + (b.band(k), b.cols)]

    def load(self, k, m):
        me = Torus()
        dim = COLOUR_DIMS[k][FIRST]
        if m in WAYS:
            src, dst = self.terms(k, me.shift(dim, toward(m)), m), self.ring.carried(self.passed, k, m)
        else:
            src, dst = self.terms(k, me.at[dim]), self.own(k)
        return pltpu.make_async_copy(src, dst, self.load_sem.at[k, m])

    def store(self, k):
        return pltpu.make_async_copy(self.own(k), self.bands.rows(self.acc.at[k], k), self.store_sem.at[k])

    def near(self):
        for k in COLOURS:
            self.ring.start(k, NEAR)

    def far(self):
        for k in COLOURS:
            self.ring.start(k, FAR)
        for m in COLOURS:
            for k in COLOURS:
                self.load(k, m).start()

    def relay(self):
        for k in COLOURS:
            self.ring.arrived(k, NEAR)
            for m in WAYS:
                self.load(k, m).wait()
                add_into(self.ring.carried(self.passed, k, m), self.ring.carried(self.relay_in, k, m))
            self.ring.start(k, ADDED)

    def settle(self, then=None):
        for k in COLOURS:
            self.load(k, FAR).wait()
            for base in (FAR, ADDED):
                self.ring.arrived(k, base)
            add_into(self.own(k), *(self.bands.rows(self.landing.at[k, m], k) for m in WAYS))
            if then is None:
                self.store(k).start()
            else:
                then(k)

    def finish(self):
        self.ring.finish()
        if self.acc is not None:
            for k in COLOURS:
                self.store(k).wait()


class Rest:
    def __init__(self, bands, acc, result, own, relay2, in2, relay3, in3, *sems):
        self.bands, self.acc, self.own, self.result = bands, acc, own, result
        self.in2, self.in3, self.relay2, self.relay3, self.load_sem, self.store_sem = in2, in3, relay2, relay3, *sems[-2:]
        self.second = Ring(SECOND, bands, functools.partial(self.terms, acc), relay2, relay2, in2, *sems[:PAIR])
        self.third = Ring(THIRD, bands, self.final, relay3, relay3, in3, *sems[PAIR:2 * PAIR])

    def terms(self, ref, k, v, half=None):
        other = ALL if half is None else duo(half)
        first = self.bands.rest(k)[0] == COLOUR_DIMS[k][SECOND]
        return self.bands.rows(ref.at[(k, v, other) if first else (k, other, v)], k)

    def final(self, k, v, half=None):
        if half is None:
            return self.bands.rows(self.in2.at[k, 0, v], k)
        return self.in2.at[k, 0, v, self.bands.cuts(k)[half]]

    def load(self, k):
        return pltpu.make_async_copy(self.bands.rows(self.acc.at[k], k), self.bands.rows(self.own.at[k], k), self.load_sem.at[k])

    def store(self, k):
        rows = self.bands.rows
        return pltpu.make_async_copy(rows(self.in3.at[k, 0], k), rows(self.result.at[k], k), self.store_sem.at[k])

    def send(self, k):
        for base in (NEAR, FAR):
            self.second.start(k, base)

    def begin(self):
        for k in COLOURS:
            self.send(k)
        for k in COLOURS:
            self.load(k).start()

    def loaded(self):
        for k in COLOURS:
            self.load(k).wait()

    def relay(self):
        me = Torus()
        for k in COLOURS:
            self.second.arrived(k, NEAR)
            for m in WAYS:
                terms = self.terms(self.own, k, me.shift(COLOUR_DIMS[k][SECOND], toward(m)), m)
                add_into(self.second.carried(self.relay2, k, m), terms)
            self.second.start(k, ADDED)

    def settle(self):
        me = Torus()
        for k in COLOURS:
            for base in (FAR, ADDED):
                self.second.arrived(k, base)
            plus, minus = (self.bands.rows(self.in2.at[k, m], k) for m in WAYS)
            add_into(plus, minus, self.terms(self.own, k, me.at[COLOUR_DIMS[k][SECOND]]))
            for base in (NEAR, FAR):
                self.third.start(k, base)

    def relay_third(self):
        me = Torus()
        for k in COLOURS:
            self.third.arrived(k, NEAR)
            for m in WAYS:
                mine = self.third.carried(self.relay3, k, m)
                mine[...] += self.final(k, me.shift(COLOUR_DIMS[k][THIRD], toward(m)), m)[...]
            self.third.start(k, ADDED)

    def settle_third(self):
        me = Torus()
        for k in COLOURS:
            for base in (FAR, ADDED):
                self.third.arrived(k, base)
            plus, minus = (self.bands.rows(self.in3.at[k, m], k) for m in WAYS)
            plus[...] += minus[...] + self.final(k, me.at[COLOUR_DIMS[k][THIRD]])[...]
            if self.result is not None:
                self.store(k).start()

    def finish(self):
        self.second.finish()
        self.third.finish()
        if self.result is not None:
            for k in COLOURS:
                self.store(k).wait()

    def sums(self):
        return self.in3.at[:, 0]


class Spread:
    def __init__(self, bands, result, total, send, recv, local):
        self.bands, self.result, self.total, self.sems, self.local = bands, result, total, (send, recv), local

    @staticmethod
    def scratch():
        return [pltpu.SemaphoreType.DMA((C, ADDED))] * PAIR + [pltpu.SemaphoreType.DMA((C,))]

    def mine(self, k):
        return self.bands.rows(self.result.at[k], k)

    def place(self, k):
        return self.bands.rows(self.total.at[Torus().at["x"], k], k)

    def hop(self, k, m):
        me = Torus()
        by = toward(m)
        if m < FAR:
            src, dst = self.mine(k), self.place(k)
        else:
            dst = src = self.total.at[me.shift("x", -by), k, self.bands.cuts(k)[m - FAR]]
        return remote(src, dst, self.sems, (k, m), me.neighbour("x", by))

    def own(self, k):
        return pltpu.make_async_copy(self.mine(k), self.place(k), self.local.at[k])

    def begin(self):
        for k in COLOURS:
            if self.local is None:
                self.place(k)[...] = self.mine(k)[...]
            else:
                self.own(k).start()
            for m in WAYS:
                self.hop(k, m).start()

    def forward(self):
        for k in COLOURS:
            for m in WAYS:
                self.hop(k, m).wait_recv()
                self.hop(k, FAR + m).start()

    def finish(self):
        for k in COLOURS:
            for m in WAYS:
                self.hop(k, FAR + m).wait_recv()
            if self.local is not None:
                self.own(k).wait()
            for m in range(ADDED):
                self.hop(k, m).wait_send()


def comm_params(collective_id):
    return pltpu.CompilerParams(collective_id=collective_id, has_side_effects=True, vmem_limit_bytes=VMEM_LIMIT)


def gather_kernel(*refs):
    n = len(Gather.semaphores())
    a, u, d = (Gather(kind, *refs[i::C][:PAIR], *refs[PAIR * C + n * i:][:n]) for i, kind in enumerate((WIDE, WIDE, DOWN)))
    enter()
    for gather in (a, u, d):
        gather.begin()
    for step, *ring in ((a.relay, FIRST), (u.relay, FIRST), (d.relay, FIRST), (a.settle, FIRST), (a.launch, SECOND),
                        (u.settle, FIRST), (u.launch, SECOND), (a.relay, SECOND), (d.settle, FIRST), (d.launch, SECOND),
                        (u.relay, SECOND), (a.settle, SECOND), (a.launch, THIRD), (d.relay, SECOND), (u.settle, SECOND),
                        (a.relay, THIRD), (d.settle, SECOND), (a.settle, THIRD), (u.sent, FIRST, SECOND),
                        (d.sent, FIRST, SECOND), (a.sent, FIRST, SECOND, THIRD)):
        step(*ring)


def gather_call(attn, up, down, collective_id):
    return pl.pallas_call(
        gather_kernel, out_shape=[sds(BF16, *Gather.shape(kind)) for kind in (WIDE, WIDE, DOWN)], in_specs=[ANY] * C,
        out_specs=[ANY] * C, scratch_shapes=Gather.semaphores() * C, compiler_params=comm_params(collective_id),
        name="gather")(attn, up, down)


class Background:
    def __init__(self, steps, plan):
        self.steps, self.plan = steps, plan

    def visit(self, place):
        for j, first, end in self.plan.get(place, ()):
            @at_step(j)
            def _():
                for step in self.steps[first:end]:
                    step()


class Share:
    def __init__(self, mine, theirs, place, sems, slot):
        self.local = pltpu.make_async_copy(mine, place, sems[PAIR].at[slot])
        self.far = remote(theirs, place, sems, slot, Torus().partner())

    def start(self):
        self.far.start()
        self.local.start()

    def sent(self):
        self.local.wait()
        self.far.wait_send()

    def wait(self):
        self.sent()
        self.far.wait_recv()


class Push:
    def __init__(self, src, tail, rows, sems, slot=0):
        body = BODY * len(SEQ_PAIR)
        tails = TAIL * len(SEQ_PAIR)
        self.copies = [
            remote(src.at[pl.ds(start, size)], rows.at[pl.ds(to, size)], sems, (slot, i), Torus().partner())
            for i, (start, to, size) in enumerate(((0, body, body), (tail, PAIR * body + tails, tails)))]

    @staticmethod
    def semaphores(n):
        return [pltpu.SemaphoreType.DMA((n, PAIR))] * PAIR

    def start(self):
        for copy in self.copies:
            copy.start()

    def wait(self):
        for copy in self.copies:
            copy.wait_recv()

    def finish(self):
        for copy in self.copies:
            copy.wait_send()


class Exchange:
    def __init__(self, mine, theirs, rows, sems, slot):
        self.moves = []
        for s in SEQ_PAIR:
            for i, (start, size) in enumerate(((0, BODY), (BODY, TAIL))):
                place = lambda n: rows.at[pl.ds(start * len(SEQ_PAIR) * PAIR + size * n, size)]
                part = pl.ds(TOK * s + start, size)
                at = slot + (PAIR * s + i,)
                local = pltpu.make_async_copy(mine.at[part], place(s), sems[2].at[at])
                far = remote(theirs.at[part], place(len(SEQ_PAIR) + s), sems, at, Torus().partner())
                self.moves.append((local, far))

    @staticmethod
    def semaphores(*lead):
        return [pltpu.SemaphoreType.DMA(lead + (2 * PAIR,))] * 3

    def start(self):
        for local, far in self.moves:
            far.start()
            local.start()

    def wait(self):
        for local, far in self.moves:
            local.wait()
            far.wait_recv()

    def finish(self):
        for _, far in self.moves:
            far.wait_send()


NT = (((1,), (1,)), ((), ()))
TN = (((0,), (0,)), ((), ()))


def dot(a, b):
    return jnp.dot(a, b, preferred_element_type=F32)


def dot_nt(a, b):
    return lax.dot_general(a, b, NT, preferred_element_type=F32)


def dot_tn(a, b):
    return lax.dot_general(a, b, TN, preferred_element_type=F32)


def zeros_but(n, axis, value):
    return tuple(value if i == axis else 0 for i in range(n))


def whole(*shape):
    return pl.BlockSpec(shape, lambda *_: (0,) * len(shape))


def along(axis, *block, index=lambda j: j):
    return pl.BlockSpec(block, lambda j: zeros_but(len(block), axis, index(j)))


def row(vec, i):
    return vec[i:i + 1]


def row_mean(t):
    return jnp.mean(t, axis=-1, keepdims=True)


def norm_stats(t):
    centered = t - row_mean(t)
    rstd = lax.rsqrt(row_mean(centered * centered) + LN_EPS)
    return centered * rstd, rstd


def norm_back(xhat, rstd, g):
    return rstd * (g - row_mean(g) - xhat * row_mean(g * xhat))


def col_sum(t):
    return jnp.sum(t, axis=0, keepdims=True)


def at_step(j):
    return pl.when(pl.program_id(0) == j)


def accumulate(ref, value):
    @at_step(0)
    def _():
        ref[...] = value

    @pl.when(pl.program_id(0) > 0)
    def _():
        ref[...] += value


def pad(t):
    return jnp.concatenate([t.astype(F32), jnp.zeros((TOK - SEQ, t.shape[1]), F32)], axis=0).astype(BF16)


def window(h):
    start = h * HEAD // LANES * LANES
    stop = min(D, -(-(h + 1) * HEAD // LANES) * LANES)
    lane = lax.broadcasted_iota(jnp.int32, (1, stop - start), 1) + (start - h * HEAD)
    return slice(start, stop), (lane >= 0) & (lane < HEAD)


def only(mask, t):
    return jnp.where(mask, t, jnp.zeros_like(t))


def softmax(scores):
    e = jnp.exp(scores - jnp.max(scores, axis=-1, keepdims=True))
    return e * (1.0 / jnp.sum(e, axis=-1, keepdims=True))


def attention(s, rows, o, acc, visit):
    acc[...] = jnp.zeros_like(acc)
    start = pl.multiple_of(s * TOK, TAIL)
    tokens = pl.ds(start, SEQ)
    for h in range(HEADS):
        lanes, mask = window(h)
        k = only(mask, rows[K, tokens, lanes])
        v = only(mask, rows[V, tokens, lanes])
        probs = softmax(dot_nt(rows[Q, tokens, lanes], k) * SCALE).astype(BF16)
        acc[:, lanes] += dot(probs, v)
        visit(h)
    o[pl.ds(start, TOK)] = pad(acc[...])


def seq_rows(t, s):
    return t[TOK * s:TOK * s + SEQ]


def seq_tile(s):
    return pl.ds(TOK * s, TOK)


FRONT_PLAN = {"start": ((0, 0, 1),), "wo": ((O + 1, 1, 2),), "end": ((O + 1, 2, None),)}


def front_kernel(x, w, b, vec, _, qkv, h1, o, att, h2, up, rows, acc, *sems):
    hosted = Background(Gather(WIDE, None, up, *sems).last_ring(), FRONT_PLAN)
    j = pl.program_id(0)
    at_step(0)(enter)
    hosted.visit("start")

    @at_step(0)
    def _():
        for s in SEQ_PAIR:
            xhat, _ = norm_stats(x[s].astype(F32))
            h1[seq_tile(s)] = pad(xhat * row(vec, G1) + row(vec, C1))

    @pl.when(j < O)
    def _():
        t = (dot(h1[...], w[0]) + b[0]).astype(BF16)
        qkv[0] = t
        rows[j] = t

    pl.when(j >= O)(lambda: attention(j - O, rows, o, acc, hosted.visit))

    hosted.visit("wo")

    @at_step(O + LAST_SEQ)
    def _():
        a = dot(o[...], w[0]) + row(vec, BO)
        att[...] = a
        for s in SEQ_PAIR:
            xhat, _ = norm_stats(x[s].astype(F32) + row(vec, S1) * seq_rows(a, s))
            h2[seq_tile(s)] = pad(xhat * row(vec, G2) + row(vec, C2))

    hosted.visit("end")


def upto(n):
    return lambda j: jnp.minimum(j, n)


def front_call(x, w_attn, b_qkv, vec, up, collective_id):
    return pl.pallas_call(
        front_kernel, grid=(O + PAIR,),
        out_shape=(sds(BF16, O, TT, D), sds(BF16, TT, D), sds(BF16, TT, D), sds(F32, TT, D), sds(BF16, TT, D),
                   sds(BF16, *Gather.shape(WIDE))),
        in_specs=[whole(*SEQS), along(0, 1, D, D, index=upto(O)), along(0, 1, 1, D, index=upto(V)), whole(8, D), ANY],
        out_specs=(along(0, 1, TT, D, index=upto(V)),) + (whole(TT, D),) * SIDE + (ANY,),
        scratch_shapes=[pltpu.VMEM((O, TT, D), BF16), pltpu.VMEM((SEQ, D), F32)] + Gather.semaphores(),
        input_output_aliases={SIDE: SIDE + 1},
        compiler_params=comm_params(collective_id), name="front",
    )(x, w_attn, b_qkv, vec, up)


def w_out_block():
    return pl.BlockSpec((1, D, D), lambda j: (O, 0, 0), pipeline_mode=pl.Buffered(1))


TILES = FF // HALF
OWN_BODY = BODY * len(SEQ_PAIR)
TAILS = ROWS - TAIL * PAIR * len(SEQ_PAIR)


def put_rows(ref, tail, s, t):
    ref[pl.ds(pl.multiple_of(BODY * s, BODY), BODY)] = t[:BODY]
    ref[pl.ds(pl.multiple_of(tail + TAIL * s, TAIL), TAIL)] = t[BODY:]


DOWN_PLAN = {"start": ((0, 0, 1),), "end": ((TILES + 2, 1, 2), (2 * TILES - 1, 2, None))}


def mlp_in_kernel(h2, gz, w_up, b_up, vec, _, act, slope, d_down, down, a_rows, b_rows, b_away, *sems):
    a_sems, b_sems, sems = sems[:PAIR], sems[PAIR:2 * PAIR], sems[2 * PAIR:]
    hosted = Background(Gather(DOWN, None, down, *sems).last_ring(), DOWN_PLAN)
    j = pl.program_id(0)
    away = Push(b_away, OWN_BODY, b_rows, b_sems, 0)
    tile = lambda n: Push(a_rows.at[n], TAILS, a_rows.at[n], a_sems, n)
    at_step(0)(enter)
    hosted.visit("start")

    @at_step(0)
    def _():
        first = Torus().at["c"] == 0
        for s in SEQ_PAIR:
            d = pad(gz[s].astype(F32) * row(vec, S2))
            left, right = d[:, :HALF], d[:, D - HALF:]
            put_rows(b_rows, TAILS, s, jnp.where(first, left, right))
            put_rows(b_away, OWN_BODY, s, jnp.where(first, right, left))

    at_step(1)(away.start)
    for n in range(TILES):
        at_step(n + 1)(tile(n).start)

    @pl.when(j < TILES)
    def _():
        u = dot(h2[...], w_up[0]) + b_up[0]
        phi = 0.5 * (1.0 + lax.erf(u * math.sqrt(0.5)))
        slope[...] = phi + u * (jnp.exp(-0.5 * u * u) * math.sqrt(0.5 / math.pi))
        place = lax.rem(lax.broadcasted_iota(jnp.int32, (TT, 1), 0), TOK)
        a = only(place < SEQ, u * phi).astype(BF16)
        act[...] = a
        for s in SEQ_PAIR:
            put_rows(a_rows.at[j], TAILS, s, a[TOK * s:TOK * s + TOK])

    at_step(TILES)(away.wait)
    for n in range(TILES):
        at_step(TILES + n)(tile(n).wait)

    @pl.when(j >= TILES)
    def _():
        d_down[...] = dot_tn(a_rows[j - TILES], b_rows[...])

    hosted.visit("end")

    @at_step(2 * TILES - 1)
    def _():
        away.finish()
        for n in range(TILES):
            tile(n).finish()


def mlp_in_call(h2, gz, w_up, b_up, vec, down, collective_id):
    low = lambda j: jnp.minimum(j, TILES - 1)
    high = lambda j: jnp.maximum(j - TILES, 0)
    return pl.pallas_call(
        mlp_in_kernel, grid=(2 * TILES,),
        out_shape=(sds(BF16, TT, FF), sds(F32, TT, FF), sds(F32, FF, HALF), sds(BF16, *Gather.shape(DOWN))),
        in_specs=[whole(TT, D), whole(*SEQS), up_tile(low), along(0, 1, 1, HALF, index=low), whole(8, D), ANY],
        out_specs=(along(1, TT, HALF, index=low), along(1, TT, HALF, index=low),
                   along(0, HALF, HALF, index=high), ANY),
        scratch_shapes=[pltpu.VMEM((TILES, ROWS, HALF), BF16), pltpu.VMEM((ROWS, HALF), BF16),
                        pltpu.VMEM((PAIR * TOK, HALF), BF16)] + Push.semaphores(TILES) + Push.semaphores(1) +
        Gather.semaphores(),
        input_output_aliases={SIDE + 1: O},
        compiler_params=comm_params(collective_id), name="mlp_in",
    )(h2, gz, w_up, b_up.reshape(TILES, 1, HALF), vec, down)


def up_tile(index=lambda j: j):
    return pl.BlockSpec((1, D, HALF), lambda j: (index(j) // PAIR, 0, index(j) % PAIR))


MLP_PLAN = {"start": ((0, 0, 2),), "end": ((3, 2, 3), (TILES - 1, 3, None))}


def mlp_out_kernel(act, slope, gz, w_up, w_down, vec, part, d_pre, db_up, mlp, d_h2, sums, dm, *scratch):
    first = First(Bands(DOWN), part, sums, *scratch)
    hosted = Background([first.near, first.far, first.relay, first.settle, first.finish], MLP_PLAN)
    at_step(0)(enter)
    hosted.visit("start")

    @at_step(0)
    def _():
        for s in SEQ_PAIR:
            dm[seq_tile(s)] = pad(gz[s].astype(F32) * row(vec, S2))

    accumulate(mlp, dot(act[...], w_down[...]))
    d = dot_nt(dm[...], w_down[...]) * slope[...]
    db_up[0] = col_sum(d)
    d = d.astype(BF16)
    d_pre[0, 0] = d
    accumulate(d_h2, dot_nt(d, w_up[0]))
    hosted.visit("end")


def mlp_out_call(act, slope, gz, w_up, w_down, vec, part, collective_id):
    return pl.pallas_call(
        mlp_out_kernel, grid=(TILES,),
        out_shape=(sds(BF16, PAIR, SIDE, TT, HALF), sds(F32, TILES, 1, HALF), sds(F32, TT, D), sds(F32, TT, D),
                   Bands(DOWN).sums()),
        in_specs=[along(1, TT, HALF), along(1, TT, HALF), whole(*SEQS), up_tile(), along(0, HALF, D), whole(8, D), ANY],
        out_specs=(pl.BlockSpec((1, 1, TT, HALF), lambda j: (j % PAIR, j // PAIR, 0, 0)), along(0, 1, 1, HALF),
                   whole(TT, D), whole(TT, D), ANY),
        scratch_shapes=[pltpu.VMEM((TT, D), BF16)] + Bands(DOWN).first(),
        compiler_params=comm_params(collective_id), name="mlp_out",
    )(act, slope, gz, w_up, w_down, vec, part)


def halves_of(t):
    t = pad(t)
    return t[:, :HALF], jnp.concatenate([t[:, HALF:], jnp.zeros((TOK, QCOLS - D), BF16)], axis=1)


def mid(mlp, d_h2, att, x, gz, vec, w_out, z, g_res, d_att, d_o, sums, da_rows):
    a = att[:SEQ]
    y = x[0].astype(F32) + row(vec, S1) * a
    m = mlp[:SEQ] + row(vec, B2)
    g = gz[0].astype(F32)
    z[0] = (y + row(vec, S2) * m).astype(BF16)
    xhat, rstd = norm_stats(y)
    dh = d_h2[:SEQ]
    gr = g + norm_back(xhat, rstd, dh * row(vec, G2))
    g_res[:SEQ] = gr
    da = gr * row(vec, S1)
    terms = (da, gr * a, dh * xhat, dh, g * row(vec, S2), g * m)
    accumulate(sums, jnp.concatenate([jnp.zeros((BO, D), F32)] + [col_sum(t) for t in terms], axis=0))
    for i, t in enumerate(halves_of(da)):
        d_att[i] = t
    da_rows[pl.ds(pl.multiple_of(pl.program_id(0) * TOK, TAIL), TOK)] = pad(da)

    @at_step(LAST_SEQ)
    def _():
        d_o[...] = dot_nt(da_rows[...], w_out[0]).astype(BF16)


def attention_back(s, qkv, d_o, d_qkv, db, acc, b_rows, away, first, visit):
    acc[...] = jnp.zeros_like(acc)
    for h in range(HEADS):
        lanes, mask = window(h)
        q, k, v = (only(mask, qkv[i, :SEQ, lanes]) for i in (Q, K, V))
        do = only(mask, d_o[:SEQ, lanes])
        scores = dot_nt(k, q) * SCALE
        e = jnp.exp(scores - jnp.max(scores, axis=0, keepdims=True))
        probs = e * (1.0 / col_sum(e))
        acc[V, :, lanes] += dot(probs.astype(BF16), do)
        dp = dot_nt(v, do)
        ds = probs * (dp - col_sum(dp * probs))
        ds = (ds * SCALE).astype(BF16)
        acc[K, :, lanes] += dot(ds, q)
        acc[Q, :, lanes] += dot_tn(ds, k)
        visit(h)
    accumulate(db, jnp.concatenate([col_sum(acc[i]) for i in (Q, K, V)], axis=0))
    for n in (Q, K, V):
        left, right = halves_of(acc[n])
        d_qkv[0, n] = left
        d_qkv[1, n] = right
        put_rows(b_rows.at[n], TAILS, s, jnp.where(first, left, right))
        put_rows(away.at[n], OWN_BODY, s, jnp.where(first, right, left))


PER = HALF // STEP


class WideGrads:
    def __init__(self, inputs, a_of, cotangents, out, base, lead, a_rows, a_cols, b_rows):
        self.inputs, self.a_of, self.cotangents, self.out, self.base, self.lead = inputs, a_of, cotangents, out, base, lead
        self.a_rows, self.a_cols, self.b_rows = a_rows, a_cols, b_rows

    @staticmethod
    def scratch(inputs):
        return [pltpu.VMEM((inputs, ROWS, D), BF16), pltpu.VMEM((inputs, D, ROWS), BF16), pltpu.VMEM((SIDE, ROWS, HALF), BF16)]

    def step(self):
        j = pl.program_id(0)
        done = []
        for t in range(SIDE):
            n = (t + self.lead) % SIDE

            @at_step(self.base + PER * t)
            def _():
                i = self.a_of[n]
                if i not in done:
                    self.inputs[i].wait()
                    self.a_cols[i] = self.a_rows[i].T
                    done.append(i)
                self.cotangents[n].wait()

        @pl.when(j >= self.base)
        def _():
            n = lax.rem(lax.div(j - self.base, PER) + self.lead, SIDE)
            cols = pl.ds(pl.multiple_of(lax.rem(j - self.base, PER) * STEP, STEP), STEP)
            i = 0 if len(self.inputs) == 1 else lax.div(n, O)
            self.out[0] = dot(self.a_cols[i], self.b_rows[n, :, cols])

    def finish(self):
        for move in (*self.inputs, *self.cotangents):
            move.finish()


def grads_block(base, lead):
    def index(j):
        n = jnp.maximum(j - base, 0)
        return (n // PER + lead) % SIDE, 0, n % PER

    return pl.BlockSpec((1, D, STEP), index)


GRAD_STEPS = PER * SIDE


def tok_block():
    return along(0, TOK, D, index=upto(LAST_SEQ))


def seq_block():
    return along(0, 1, SEQ, D, index=upto(LAST_SEQ))


MID_PLAN = {"start": ((0, 0, 1),), "end": ((1, 1, 3), (8, 3, 4), (11, 4, 5), (LAST_SEQ + GRAD_STEPS, 5, None))}


def mid_kernel(*refs):
    refs = list(refs)
    take = lambda n: [refs.pop(0) for _ in range(n)]
    ins, (h2, d_pre, acc), outs, (d_up, result), da_rows = take(7), take(3), take(5), take(2), refs.pop(0)
    rows, a_sems, b_sems = take(3), take(C), take(C)
    rest = Rest(Bands(DOWN), acc, result, *refs)
    hosted = Background([rest.begin, rest.loaded, rest.relay, rest.settle, rest.relay_third, rest.settle_third, rest.finish],
                        MID_PLAN)
    c = Torus().at["c"]
    grads = WideGrads(
        [Exchange(h2, h2, rows[0].at[0], a_sems, ())], (0,) * SIDE,
        [Exchange(d_pre.at[c, n], d_pre.at[1 - c, n], rows[2].at[n], b_sems, (n,)) for n in range(SIDE)], d_up, SEQS[0], 0, *rows)
    at_step(0)(enter)
    hosted.visit("start")

    @at_step(0)
    def _():
        for move in (*grads.inputs, *grads.cotangents):
            move.start()

    pl.when(pl.program_id(0) < SEQS[0])(lambda: mid(*ins, *outs, da_rows))
    grads.step()
    hosted.visit("end")
    at_step(LAST_SEQ + GRAD_STEPS)(grads.finish)


def mid_call(mlp, d_h2, att, x, gz, vec, w_attn, h2, d_pre, acc, collective_id):
    return pl.pallas_call(
        mid_kernel, grid=(SEQS[0] + GRAD_STEPS,),
        out_shape=(sds(BF16, *SEQS), sds(F32, TT, D), sds(BF16, PAIR, TT, HALF), sds(BF16, TT, D), sds(F32, 8, D),
                   sds(F32, SIDE, D, HALF), Bands(DOWN).result()),
        in_specs=[tok_block()] * O + [seq_block()] * PAIR + [whole(8, D), w_out_block()] + [ANY] * O,
        out_specs=(seq_block(), tok_block(), along(1, PAIR, TOK, HALF, index=upto(LAST_SEQ)), whole(TT, D), whole(8, D),
                   grads_block(SEQS[0], 0), ANY),
        scratch_shapes=[pltpu.VMEM((TT, D), BF16)] + WideGrads.scratch(1) + Exchange.semaphores() + Exchange.semaphores(SIDE) +
        Bands(DOWN).later(),
        compiler_params=comm_params(collective_id), name="mid",
    )(mlp, d_h2, att, x, gz, vec, w_attn, h2, d_pre, acc)


ATTN_PLAN = {"start": ((0, 0, 3),), 6: ((0, 3, 4),), "end": ((LAST_SEQ, 4, 5), (LAST_SEQ + GRAD_STEPS, 5, None))}


def attn_back_kernel(*refs):
    refs = list(refs)
    take = lambda n: [refs.pop(0) for _ in range(n)]
    (qkv, d_o), (h1, o, d_att, part, result), (d_qkv, db, d_attn, sums, total) = take(2), take(5), take(5)
    acc, away, rows = refs.pop(0), refs.pop(0), take(3)
    a_sems, b_sems, away_sems = take(C), take(C), take(PAIR)
    first = First(Bands(WIDE), part, sums, *take(len(Bands(WIDE).first())))
    spread = Spread(Bands(DOWN), result, total, *refs)
    hosted = Background([spread.begin, first.near, first.far, spread.forward, first.relay, first.settle, first.finish,
                         spread.finish], ATTN_PLAN)
    c = Torus().at["c"]
    pushes = [Push(away.at[n], OWN_BODY, rows[2].at[n], away_sems, n) for n in range(O)]
    grads = WideGrads(
        [Exchange(a, a, rows[0].at[i], a_sems, (i,)) for i, a in enumerate((h1, o))], (0,) * O + (1,),
        pushes + [Exchange(d_att.at[c], d_att.at[1 - c], rows[2].at[O], b_sems, ())], d_attn, SEQS[0], O, *rows)
    at_step(0)(enter)
    hosted.visit("start")

    @at_step(0)
    def _():
        for move in (*grads.inputs, grads.cotangents[O]):
            move.start()

    @at_step(SEQS[0])
    def _():
        for push in pushes:
            push.start()

    j = pl.program_id(0)
    pl.when(j < SEQS[0])(lambda: attention_back(j, qkv, d_o, d_qkv, db, acc, rows[2], away, c == 0, hosted.visit))

    grads.step()
    hosted.visit("end")
    at_step(LAST_SEQ + GRAD_STEPS)(grads.finish)


def attn_back_call(qkv, d_o, h1, o, d_att, part, result, collective_id):
    return pl.pallas_call(
        attn_back_kernel, grid=(SEQS[0] + GRAD_STEPS,),
        out_shape=(sds(BF16, PAIR, O, TT, HALF), sds(F32, O, D), sds(F32, SIDE, D, HALF), Bands(WIDE).sums(),
                   Bands(DOWN).total()),
        in_specs=[along(1, O, TOK, D, index=upto(LAST_SEQ)), tok_block()] + [ANY] * 5,
        out_specs=(along(2, PAIR, O, TOK, HALF, index=upto(LAST_SEQ)), whole(O, D), grads_block(SEQS[0], O), ANY, ANY),
        scratch_shapes=[pltpu.VMEM((O, SEQ, D), F32), pltpu.VMEM((O, PAIR * TOK, HALF), BF16)] + WideGrads.scratch(2) +
        Exchange.semaphores(PAIR) + Exchange.semaphores() + Push.semaphores(O) + Bands(WIDE).first() + Spread.scratch(),
        compiler_params=comm_params(collective_id), name="attn_back",
    )(qkv, d_o, h1, o, d_att, part, result)


IN_STEPS = PAIR * O
SLOT = 40
LAST_PLAN = {"start": ((0, 0, 2),), "end": ((O, 2, None),)}


CORE_COLS = D - HALF
KEPT = 48
GRADS = ((KEPT, O * D), (KEPT, D), (KEPT, FF), (PAIR, C, UNIT, D), (SIDE, KEPT, LANES))
SHARES = PAIR * SIDE + SIDE + PAIR


def split_rows(totals, first, keep, give):
    for x in range(SIDE):
        for total, bands in totals:
            rows = jnp.concatenate([total[x, k, :n] for k, (_, n) in enumerate(BANDS[WIDE])], axis=0)
            low, high = rows[:KEPT], jnp.concatenate([rows[OWN:], rows[:KEPT - OWN]], axis=0)
            keep[x, :, bands.cols] = jnp.where(first, low, high)
            give[x, :, bands.cols] = jnp.where(first, high, low)


class Finals:
    def __init__(self, down, up, attn, outs, sems):
        self.c = Torus().at["c"]
        self.down, self.up, self.attn, self.sems = down, up, attn, sems
        self.qkv, self.out, self.up_out, self.down_out, self.pad = outs
        self.edge = pl.ds(CORE_COLS, LANES)

    def cols(self, base, width):
        return pl.ds(pl.multiple_of(base + self.c * HALF, LANES), width)

    def up_share(self, x):
        place = self.up_out.at[:, self.cols(QCOLS * x, HALF)]
        return Share(*(ref.at[x] for ref in self.up), place, self.sems, x)

    def block(self, x):
        return (self.out, 0) if x == O else (self.qkv, D * x)

    def attn_share(self, x):
        out, base = self.block(x)
        sides = (ref.at[x, :, pl.ds(0, CORE_COLS)] for ref in self.attn)
        return Share(*sides, out.at[:, self.cols(base, CORE_COLS)], self.sems, SIDE + x)

    def edge_share(self, x, padding):
        out, base = self.block(x)
        place = self.pad.at[x] if padding else out.at[:, pl.ds(base + CORE_COLS, LANES)]
        return Share(*(ref.at[x, :, self.edge] for ref in self.attn), place, self.sems, PAIR * SIDE + x)

    def down_share(self, edge):
        src = self.edge if edge else pl.ds(pl.multiple_of(self.c * LANES, LANES), CORE_COLS)
        sides = (self.down.at[pl.ds(PAIR * c, PAIR), :, :, src] for c in (self.c, 1 - self.c))
        place = self.down_out.at[:, :, :, self.edge if edge else self.cols(0, CORE_COLS)]
        return Share(*sides, place, self.sems, SHARES - PAIR + edge)

    def start_down(self):
        self.down_share(0).start()
        pl.when(self.c == 0)(lambda: self.down_share(1).start())

    def start(self):
        for x in range(SIDE):
            self.attn_share(x).start()
            pl.when(self.c == 0)(lambda: self.edge_share(x, False).start())
            pl.when(self.c == 1)(lambda: self.edge_share(x, True).start())

    def finish(self):
        for x in range(SIDE):
            for share in (self.up_share(x), self.attn_share(x), self.edge_share(x, True)):
                share.wait()
        self.down_share(0).wait()
        pl.when(self.c == 0)(lambda: self.down_share(1).sent())
        pl.when(self.c == 1)(lambda: self.down_share(1).far.wait_recv())


def last_kernel(*refs):
    refs = list(refs)
    take = lambda n: [refs.pop(0) for _ in range(n)]
    (d_half, w, x, g_res, vec), (small, acc_up, down, _), (dx, part), outs = take(5), take(SIDE), take(PAIR), take(len(GRADS))
    (acc, sums, pair_sums, block), (totals, sides), block_sem, swap_sems = take(4), (take(C), take(SIDE)), refs.pop(0), take(PAIR)
    finals = Finals(down, sides[:PAIR], sides[PAIR:], outs, take(C))
    halves = [Bands(WIDE, h) for h in WAYS]
    a, b = (First(bands, part, None, *take(len(bands.first()))) for bands in halves)
    rest_a, rest_b = (Rest(f.bands, f.own_all, None, f.own_all, *take(len(f.bands.later()) - 1)) for f in (a, b))
    rest_up = Rest(Bands(WIDE), acc_up, None, *take(len(Bands(WIDE).later())))
    spread_up, spread_a, spread_b = (
        Spread(r.bands, r.sums(), total, *take(PAIR), None) for r, total in zip((rest_up, rest_a, rest_b), totals))
    hosted = Background([rest_up.begin, a.near, rest_up.loaded, rest_up.relay], LAST_PLAN)
    first = finals.c == 0
    swap = remote(sums, pair_sums, swap_sems, (), Torus().partner())
    fetch = pltpu.make_async_copy(small, block, block_sem)
    at_step(0)(enter)
    hosted.visit("start")

    @at_step(0)
    def _():
        fetch.start()
        finals.start_down()

    @pl.when(pl.program_id(0) < IN_STEPS)
    def _():
        accumulate(acc, dot_nt(d_half[0, 0], w[0]))

    @at_step(IN_STEPS - 1)
    def _():
        rows = jnp.zeros((SUB, D), F32)
        for s in SEQ_PAIR:
            xhat, rstd = norm_stats(x[s].astype(F32))
            tokens = pl.ds(TOK * s, SEQ)
            dh = acc[tokens]
            rows = rows + jnp.concatenate([col_sum(dh * xhat), col_sum(dh), jnp.zeros((SUB - BO, D), F32)], axis=0)
            dx[s] = (g_res[tokens] + norm_back(xhat, rstd, dh * row(vec, G1))).astype(BF16)
        sums[...] = rows

    hosted.visit("end")

    @at_step(IN_STEPS)
    def _():
        swap.start()
        fetch.wait()
        swap.wait()
        both = sums[...] + pair_sums[...]
        for d in range(DEVICES):
            at = CHIP * (d // PAIR) + SLOT + OWN * (d % PAIR)
            block[at:at + BO, :OWN] = both[:BO, OWN * d:OWN * d + OWN]

        @pl.when(finals.c == 1)
        def _():
            for z in range(SIDE):
                for y in range(SIDE):
                    rows = block.at[pl.ds(CHIP * (SIDE * z + y), CHIP)]
                    put = pltpu.make_async_copy(rows, part.at[0, z, y, :, pl.ds(CORE_COLS, LANES)], block_sem)
                    put.start()
            pltpu.make_async_copy(block, small, block_sem).wait()

        def share_up():
            spread_up.finish()
            split_rows([(totals[0], Bands(WIDE))], first, *sides[:PAIR])
            for x in range(SIDE):
                finals.up_share(x).start()

        for step in (b.near, rest_up.settle, a.far, rest_up.relay_third, b.far, a.relay, rest_up.settle_third, spread_up.begin,
                     b.relay, spread_up.forward, functools.partial(a.settle, rest_a.send),
                     functools.partial(b.settle, rest_b.send), rest_a.relay, rest_b.relay, rest_a.settle, rest_b.settle,
                     share_up, rest_a.relay_third, rest_b.relay_third, rest_a.settle_third, spread_a.begin,
                     rest_b.settle_third, spread_b.begin, spread_a.forward, spread_b.forward, spread_a.finish, spread_b.finish):
            step()
        split_rows(list(zip(totals[1:], halves)), first, *sides[PAIR:])
        finals.start()
        for user in (rest_up, rest_a, rest_b, a, b, finals):
            user.finish()


def last_call(d_qkv, w_attn, x, g_res, vec, small, acc_up, down, part, collective_id):
    low = upto(IN_STEPS - 1)
    halves = [Bands(WIDE, h) for h in WAYS]
    dma = pltpu.SemaphoreType.DMA
    rings = [Bands(WIDE), *halves]
    return pl.pallas_call(
        last_kernel, grid=(IN_STEPS + 1,),
        out_shape=(sds(BF16, *SEQS), sds(F32, *part.shape), *(sds(F32, *shape) for shape in GRADS)),
        in_specs=[pl.BlockSpec((1, 1, TT, HALF), lambda j: (low(j) % PAIR, low(j) // PAIR, 0, 0)), up_tile(low),
                  whole(*SEQS), whole(TT, D), whole(8, D)] + [ANY] * SIDE,
        out_specs=(whole(*SEQS),) + (ANY,) * (len(GRADS) + 1),
        scratch_shapes=[pltpu.VMEM((TT, D), F32), pltpu.VMEM((SUB, D), F32), pltpu.VMEM((SUB, D), F32),
                        pltpu.VMEM((D, LANES), F32)] + [r.vmem(SIDE, C) for r in rings] +
        [pltpu.VMEM((SIDE, KEPT, HALF), F32)] * SIDE + [dma, dma, dma] + [dma((SHARES,))] * C + halves[0].first() * PAIR +
        halves[0].later()[1:] * PAIR + Bands(WIDE).later() + Spread.scratch()[:PAIR] * C,
        input_output_aliases={8: 1},
        compiler_params=comm_params(collective_id), name="last",
    )(d_qkv, w_attn, x, g_res, vec, small, acc_up, down, part)


BQ, BU, VEC = 3 * D // 32, 3 * D // 32 + FF // 32, 3 * D // 32 + FF // 32 + 8 * OWN


def pair_swap(a):
    return lax.ppermute(a, "fsdp", [(i, i ^ 1) for i in range(DEVICES)])


def by_core(first, a, b):
    return jnp.where(first, a, b), jnp.where(first, b, a)


def my_pieces(shards, first):
    w_qkv, b_qkv, w_out, w_up, b_up, w_down, vec_params = shards
    x = lax.axis_index("rep")
    small = jnp.concatenate([b_qkv, b_up, vec_params.reshape(-1)])
    small = jnp.pad(small, (0, OWN * LANES - VEC)).reshape(OWN, LANES)
    attn = lax.dynamic_slice_in_dim(jnp.concatenate([w_qkv, w_out], axis=1), x * D, D, 1)
    attn = jnp.concatenate([attn, small], axis=1)
    up = lax.dynamic_slice_in_dim(w_up, x * QCOLS, QCOLS, 1)
    wide = jnp.stack([attn, up]).astype(BF16)
    mine, theirs = by_core(first, wide[..., :HALF], wide[..., HALF:])
    theirs = pair_swap(theirs)
    piece = jnp.concatenate(by_core(first, mine, theirs), axis=1)
    down = lax.dynamic_slice_in_dim(w_down, x * 48, 48, 0).astype(BF16).reshape(3, 16, D)
    return piece[0], piece[1], down


def small_params(w_attn):
    small = w_attn[0, :, D:].astype(F32).reshape(DEVICES, OWN * LANES)
    vec = small[:, BU:VEC].reshape(DEVICES, 8, OWN).transpose(1, 0, 2).reshape(8, D)
    return small[:, :BQ].reshape(O, 1, D), small[:, BQ:BU].reshape(FF), vec


ROOM = 5 * LANES


def small_grads(db_qkv, db_up, sums):
    vec = sums[BO:].reshape(8 - BO, DEVICES, OWN).transpose(1, 0, 2).reshape(DEVICES, VEC - BU - BO * OWN)
    small = jnp.concatenate([db_qkv.reshape(DEVICES, BQ), db_up.reshape(DEVICES, BU - BQ), vec], axis=1)
    small = small + pair_swap(small)
    small = jnp.pad(small, ((0, 0), (0, ROOM - small.shape[1]))).reshape(DEVICES, ROOM // LANES, LANES)
    return jnp.pad(small, ((0, 0), (0, OWN - ROOM // LANES), (0, 0))).reshape(D, LANES)


def device_step(x, gz, *shards):
    first = lax.rem(lax.axis_index("fsdp"), PAIR) == 0
    attn, up, down = my_pieces(shards, first)
    w_attn, up, down = gather_call(attn, up, down, 0)
    w_attn = w_attn.reshape(SIDE, D, QCOLS)
    b_qkv, b_up, vec = small_params(w_attn)
    qkv, h1, o, att, h2, w_up = front_call(x, w_attn, b_qkv, vec, up, 1)
    w_up = w_up.reshape(SIDE, D, QCOLS)
    act, slope, part, w_down = mlp_in_call(h2, gz, w_up, b_up, vec, down, 2)
    part = part.reshape((SIDE,) * 3 + (C * UNIT, HALF))
    d_pre, db_up, mlp, d_h2, acc = mlp_out_call(act, slope, gz, w_up, w_down.reshape(FF, D), vec, part, 3)
    z, g_res, d_att, d_o, sums, part, result = mid_call(mlp, d_h2, att, x, gz, vec, w_attn, h2, d_pre, acc, 4)
    part = part.reshape((SIDE,) * 3 + (CHIP, HALF))
    d_qkv, db_qkv, part, acc, down = attn_back_call(qkv, d_o, h1, o, d_att, part, result, 5)
    small = small_grads(db_qkv, db_up, sums)
    part = part.reshape((SIDE,) * 3 + (CHIP, HALF))
    dx, _, g_qkv, g_out, g_up, g_down, edge = last_call(d_qkv, w_attn, x, g_res, vec, small, acc, down, part, 6)
    small = edge[0, :ROOM // LANES].reshape(ROOM)
    vec = jnp.concatenate([edge[0, SLOT:SLOT + BO, :OWN], small[BU:VEC - BO * OWN].reshape(8 - BO, OWN)], axis=0)
    g_qkv, g_out, g_up = (g[:OWN] for g in (g_qkv, g_out, g_up))
    return z, dx, g_qkv, small[:BQ], g_out, g_up, small[BQ:BU], g_down.reshape(FF // DEVICES, D), vec


def solution(mesh):
    batch = P(("rep", "fsdp"), None, None)
    rows, flat, cols = P("fsdp", None), P("fsdp"), P(None, "fsdp")
    shards = (rows, flat, rows, rows, flat, rows, cols)
    return jax.shard_map(device_step, mesh=mesh, in_specs=(batch, batch) + shards,
                         out_specs=(batch, batch) + shards, check_vma=False)
```

```python
import functools
import math

import jax
import jax.numpy as jnp
from jax import lax
from jax.experimental import pallas as pl
from jax.experimental.pallas import tpu as pltpu
from jax.sharding import PartitionSpec as P

HEADS = 16
LN_EPS = 1e-5
D = 1408
FF = 6144
SEQ = 257
HEAD = D // HEADS
SCALE = HEAD ** -0.5
QCOLS = 1536
HALF = 768
OWN = 44
CHIP = 2 * OWN
LANES = 128
DEVICES = 32
F32 = jnp.float32
BF16 = jnp.bfloat16
VMEM_LIMIT = 66 * 1000 * 1000
G1, C1, BO, S1, G2, C2, B2, S2 = range(8)
Q, K, V, O = range(4)
SEQS = (2, SEQ, D)
LAST_SEQ = SEQS[0] - 1
SEQ_PAIR = range(SEQS[0])
TAIL = 16
BODY = SEQ - 1
TOK = BODY + TAIL
TT = 2 * TOK
ROWS = 4 * TOK
STEP = 256


def sds(dtype, *shape):
    return jax.ShapeDtypeStruct(shape, dtype)


MESH_ID = pl.DeviceIdType.MESH
SIDE = 4
SUB = 8
PAIR = 2
C = 3
COLOURS = range(C)
COLOUR_DIMS = ("xyz", "yzx", "zxy")
FIRST, SECOND, THIRD, LAST = range(4)
WAYS = range(PAIR)
NEAR, FAR, ADDED = 0, 2, 4
WIDE, DOWN = "wide", "down"
ANY = pl.BlockSpec(memory_space=pl.ANY)
ALL = slice(None)


def duo(m):
    return pl.ds(PAIR * m, PAIR)


def toward(m):
    return 1 - PAIR * (m % PAIR)


class Torus:
    def __init__(self):
        f = lax.axis_index("fsdp")
        self.at = {"x": lax.axis_index("rep"), "z": lax.div(f, SIDE * PAIR), "y": lax.rem(lax.div(f, PAIR), SIDE),
                   "c": lax.rem(f, PAIR)}

    def shift(self, dim, by):
        return lax.rem(self.at[dim] + (SIDE + by), SIDE)

    def device(self, **moved):
        p = {**self.at, **moved}
        return (p["x"], (p["z"] * SIDE + p["y"]) * PAIR + p["c"])

    def neighbour(self, dim, by):
        return self.device(**{dim: self.shift(dim, by)})

    def partner(self):
        return self.device(c=1 - self.at["c"])


def enter():
    me = Torus()
    barrier = pltpu.get_barrier_semaphore()
    others = [me.neighbour(d, toward(m)) for d in COLOUR_DIMS[0] for m in WAYS] + [me.partner()]
    for other in others:
        pl.semaphore_signal(barrier, device_id=other, device_id_type=MESH_ID)
    pl.semaphore_wait(barrier, len(others))


def remote(src, dst, sems, slot, device):
    return pltpu.make_async_remote_copy(src_ref=src, dst_ref=dst, send_sem=sems[0].at[slot], recv_sem=sems[1].at[slot],
                                        device_id=device, device_id_type=MESH_ID)


class Gather:
    def __init__(self, kind, src, dst, hop_send, hop_recv, push_send, push_recv, local):
        self.kind, self.src, self.dst, self.local = kind, src, dst, local
        self.hops, self.pushes = (hop_send, hop_recv), (push_send, push_recv)
        self.cols, self.cut = (256, 128) if kind == WIDE else (D, HALF)
        self.parts = ((0, self.cut), (self.cut, self.cols - self.cut))

    @staticmethod
    def semaphores():
        dma = pltpu.SemaphoreType.DMA
        return [dma((C, SIDE, ADDED))] * PAIR + [dma((C, PAIR, ADDED + 1))] * PAIR + [dma((C,))]

    @staticmethod
    def shape(kind):
        return (SIDE,) * 3 + (CHIP, QCOLS) if kind == WIDE else (SIDE, SIDE, PAIR, SIDE, C, 16, D)

    @staticmethod
    def dim(k, s):
        return COLOUR_DIMS[k][min(s, THIRD)]

    def source(self, k):
        return self.src.at[:, pl.ds(self.cols * k, self.cols)] if self.kind == WIDE else self.src.at[k]

    def piece(self, me, k, s, v, half=None):
        dims = COLOUR_DIMS[k]
        at = {**me.at, **{d: ALL for d in dims[:min(s, THIRD)]}, self.dim(k, s): v}
        off, width = self.parts[s - THIRD] if s >= THIRD else (0, self.cols)
        if half is not None and s == FIRST:
            off, width = self.parts[half]
        elif half is not None:
            at[dims[0]] = duo(half)
        if self.kind == WIDE:
            cols = pl.ds(pl.multiple_of(at["c"] * HALF + self.cols * k + off, 128), width)
            return self.dst.at[at["x"], at["z"], at["y"], :, cols]
        return self.dst.at[at["z"], at["y"], at["c"], at["x"], k, :, pl.ds(off, width)]

    def hop(self, k, s, m):
        me = Torus()
        dim = self.dim(k, s)
        by = toward(m)
        if m < FAR:
            ref = self.piece(me, k, s, me.at[dim])
        else:
            ref = self.piece(me, k, s, me.shift(dim, -by), m - FAR)
        src = self.source(k) if s == FIRST and m < FAR else ref
        return remote(src, ref, self.hops, (k, s, m), me.neighbour(dim, by))

    def push(self, k, s, n):
        me = Torus()
        dim = self.dim(k, s)
        if n < FAR:
            ref = self.piece(me, k, s, me.shift(dim, -toward(n)))
        elif n < ADDED:
            ref = self.piece(me, k, s, me.shift(dim, FAR), n - FAR)
        else:
            ref = self.piece(me, k, s, me.at[dim])
        return remote(ref, ref, self.pushes, (k, s - THIRD, n), me.partner())

    def own(self, k):
        me = Torus()
        return pltpu.make_async_copy(self.source(k), self.piece(me, k, FIRST, me.at[COLOUR_DIMS[k][FIRST]]), self.local.at[k])

    def launch(self, s):
        for k in COLOURS:
            for m in WAYS:
                self.hop(k, s, m).start()
            if s >= THIRD:
                self.push(k, s, ADDED).start()

    def relay(self, s):
        for k in COLOURS:
            for m in WAYS:
                self.hop(k, s, m).wait_recv()
                self.hop(k, s, FAR + m).start()
                if s >= THIRD:
                    self.push(k, s, m).start()

    def settle(self, s):
        for k in COLOURS:
            for m in WAYS:
                self.hop(k, s, FAR + m).wait_recv()
                if s >= THIRD:
                    self.push(k, s, FAR + m).start()
            if s == FIRST:
                self.own(k).wait()

    def begin(self):
        for k in COLOURS:
            self.own(k).start()
        self.launch(FIRST)

    def sent(self, *rings):
        for k in COLOURS:
            for s in rings:
                for m in range(ADDED):
                    self.hop(k, s, m).wait_send()
                if s >= THIRD:
                    for n in range(ADDED + 1):
                        self.push(k, s, n).wait()

    def last_ring(self):
        parts = THIRD, LAST
        steps = [functools.partial(f, s) for f in (self.launch, self.relay, self.settle) for s in parts]
        return steps + [functools.partial(self.sent, *parts)]


def add_into(total, *others):
    lead = total.shape[:-2]

    def body(i, carry):
        idx = []
        for n in reversed(lead):
            idx.insert(0, lax.rem(i, n))
            i = lax.div(i, n)
        value = total[tuple(idx)]
        for other in others:
            value = value + other[tuple(idx)]
        total[tuple(idx)] = value
        return carry

    lax.fori_loop(0, math.prod(lead), body, 0)


class Ring:
    def __init__(self, s, bands, terms, passed, relay, landing, send, recv):
        self.s, self.bands, self.terms, self.passed, self.relay, self.landing = s, bands, terms, passed, relay, landing
        self.sems = (send, recv)

    def zone(self, k, way, half):
        if self.s == THIRD:
            return self.landing.at[k, way, self.bands.cuts(k)[half]]
        return self.bands.rows(self.landing.at[k, way, duo(half)], k)

    def carried(self, ref, k, way):
        if self.s == THIRD:
            return ref.at[k, way, pl.ds(0, self.bands.cuts(k)[way].size)]
        return self.bands.rows(ref.at[k, way], k)

    def hop(self, k, m):
        me = Torus()
        dim = COLOUR_DIMS[k][self.s]
        way, by = m % PAIR, toward(m)
        if m < FAR:
            src, dst = self.terms(k, me.shift(dim, FAR), way), self.carried(self.relay, k, way)
        elif m < ADDED:
            src, dst = self.terms(k, me.shift(dim, by), 1 - way), self.zone(k, way, 1 - way)
        else:
            src, dst = self.carried(self.passed, k, way), self.zone(k, way, way)
        return remote(src, dst, self.sems, (k, m), me.neighbour(dim, by))

    def start(self, k, base):
        for m in WAYS:
            self.hop(k, base + m).start()

    def arrived(self, k, base):
        for m in WAYS:
            self.hop(k, base + m).wait_recv()

    def finish(self):
        for k in COLOURS:
            for m in range(ADDED + PAIR):
                self.hop(k, m).wait_send()

    @staticmethod
    def semaphores():
        return [pltpu.SemaphoreType.DMA((C, ADDED + PAIR))] * PAIR


UNIT = 32
BANDS = {WIDE: ((0, 24), (24, UNIT), (56, UNIT)), DOWN: ((0, UNIT), (UNIT, UNIT), (2 * UNIT, UNIT))}
ORDERS = {WIDE: "xzy", DOWN: "zyx"}


class Bands:
    def __init__(self, kind, half=None):
        self.order, self.bands = ORDERS[kind], BANDS[kind]
        self.width = HALF if half is None else HALF // PAIR
        self.cols = pl.ds(self.width * (half or 0), self.width)

    def band(self, k):
        return pl.ds(*self.bands[k])

    def rows(self, ref, k):
        return ref.at[(ALL,) * (len(ref.shape) - PAIR) + (pl.ds(0, self.bands[k][1]),)]

    def cuts(self, k):
        rows = self.bands[k][1]
        cut = (rows // SUB + 1) // PAIR * SUB
        return pl.ds(0, cut), pl.ds(cut, rows - cut)

    def rest(self, k):
        return [d for d in self.order if d != COLOUR_DIMS[k][FIRST]]

    def units(self, *lead):
        return lead + (UNIT, self.width)

    def vmem(self, *lead):
        return pltpu.VMEM(self.units(*lead), F32)

    def sums(self):
        return sds(F32, *self.units(C, SIDE, SIDE))

    def result(self):
        return sds(F32, *self.units(C))

    def total(self):
        return sds(F32, *self.units(SIDE, C))

    def first(self):
        relays = [self.vmem(C, PAIR, PAIR, SIDE)] * PAIR
        dma = pltpu.SemaphoreType.DMA
        return [self.vmem(C, SIDE, SIDE), *relays, self.vmem(C, PAIR, SIDE, SIDE), *Ring.semaphores(), dma((C, C)), dma((C,))]

    def later(self):
        dma = pltpu.SemaphoreType.DMA
        return [self.vmem(C, SIDE, SIDE), self.vmem(C, PAIR, PAIR), self.vmem(C, PAIR, SIDE),
                pltpu.VMEM((C, PAIR, UNIT // PAIR, self.width), F32), self.vmem(C, PAIR),
                *Ring.semaphores(), *Ring.semaphores(), dma((C,)), dma((C,))]


class First:
    def __init__(self, bands, part, acc, own, passed, relay, landing, send, recv, load, store):
        self.bands, self.part, self.acc, self.own_all, self.passed = bands, part, acc, own, passed
        self.relay_in, self.landing, self.load_sem, self.store_sem = relay, landing, load, store
        self.ring = Ring(FIRST, bands, self.terms, passed, relay, landing, send, recv)

    def own(self, k):
        return self.bands.rows(self.own_all.at[k], k)

    def terms(self, k, v, half=None):
        b = self.bands
        at = {d: ALL for d in b.order}
        at[COLOUR_DIMS[k][FIRST]] = v
        if half is not None:
            at[b.rest(k)[0]] = duo(half)
        return self.part.at[tuple(at[d] for d in b.order) + (b.band(k), b.cols)]

    def load(self, k, m):
        me = Torus()
        dim = COLOUR_DIMS[k][FIRST]
        if m in WAYS:
            src, dst = self.terms(k, me.shift(dim, toward(m)), m), self.ring.carried(self.passed, k, m)
        else:
            src, dst = self.terms(k, me.at[dim]), self.own(k)
        return pltpu.make_async_copy(src, dst, self.load_sem.at[k, m])

    def store(self, k):
        return pltpu.make_async_copy(self.own(k), self.bands.rows(self.acc.at[k], k), self.store_sem.at[k])

    def near(self):
        for k in COLOURS:
            self.ring.start(k, NEAR)

    def far(self):
        for k in COLOURS:
            self.ring.start(k, FAR)
        for m in COLOURS:
            for k in COLOURS:
                self.load(k, m).start()

    def relay(self):
        for k in COLOURS:
            self.ring.arrived(k, NEAR)
            for m in WAYS:
                self.load(k, m).wait()
                add_into(self.ring.carried(self.passed, k, m), self.ring.carried(self.relay_in, k, m))
            self.ring.start(k, ADDED)

    def settle(self, then=None):
        for k in COLOURS:
            self.load(k, FAR).wait()
            for base in (FAR, ADDED):
                self.ring.arrived(k, base)
            add_into(self.own(k), *(self.bands.rows(self.landing.at[k, m], k) for m in WAYS))
            if then is None:
                self.store(k).start()
            else:
                then(k)

    def finish(self):
        self.ring.finish()
        if self.acc is not None:
            for k in COLOURS:
                self.store(k).wait()


class Rest:
    def __init__(self, bands, acc, result, own, relay2, in2, relay3, in3, *sems):
        self.bands, self.acc, self.own, self.result = bands, acc, own, result
        self.in2, self.in3, self.relay2, self.relay3, self.load_sem, self.store_sem = in2, in3, relay2, relay3, *sems[-2:]
        self.second = Ring(SECOND, bands, functools.partial(self.terms, acc), relay2, relay2, in2, *sems[:PAIR])
        self.third = Ring(THIRD, bands, self.final, relay3, relay3, in3, *sems[PAIR:2 * PAIR])

    def terms(self, ref, k, v, half=None):
        other = ALL if half is None else duo(half)
        first = self.bands.rest(k)[0] == COLOUR_DIMS[k][SECOND]
        return self.bands.rows(ref.at[(k, v, other) if first else (k, other, v)], k)

    def final(self, k, v, half=None):
        if half is None:
            return self.bands.rows(self.in2.at[k, 0, v], k)
        return self.in2.at[k, 0, v, self.bands.cuts(k)[half]]

    def load(self, k):
        return pltpu.make_async_copy(self.bands.rows(self.acc.at[k], k), self.bands.rows(self.own.at[k], k), self.load_sem.at[k])

    def store(self, k):
        rows = self.bands.rows
        return pltpu.make_async_copy(rows(self.in3.at[k, 0], k), rows(self.result.at[k], k), self.store_sem.at[k])

    def send(self, k):
        for base in (NEAR, FAR):
            self.second.start(k, base)

    def begin(self):
        for k in COLOURS:
            self.send(k)
        for k in COLOURS:
            self.load(k).start()

    def loaded(self):
        for k in COLOURS:
            self.load(k).wait()

    def relay(self):
        me = Torus()
        for k in COLOURS:
            self.second.arrived(k, NEAR)
            for m in WAYS:
                terms = self.terms(self.own, k, me.shift(COLOUR_DIMS[k][SECOND], toward(m)), m)
                add_into(self.second.carried(self.relay2, k, m), terms)
            self.second.start(k, ADDED)

    def settle(self):
        me = Torus()
        for k in COLOURS:
            for base in (FAR, ADDED):
                self.second.arrived(k, base)
            plus, minus = (self.bands.rows(self.in2.at[k, m], k) for m in WAYS)
            add_into(plus, minus, self.terms(self.own, k, me.at[COLOUR_DIMS[k][SECOND]]))
            for base in (NEAR, FAR):
                self.third.start(k, base)

    def relay_third(self):
        me = Torus()
        for k in COLOURS:
            self.third.arrived(k, NEAR)
            for m in WAYS:
                mine = self.third.carried(self.relay3, k, m)
                mine[...] += self.final(k, me.shift(COLOUR_DIMS[k][THIRD], toward(m)), m)[...]
            self.third.start(k, ADDED)

    def settle_third(self):
        me = Torus()
        for k in COLOURS:
            for base in (FAR, ADDED):
                self.third.arrived(k, base)
            plus, minus = (self.bands.rows(self.in3.at[k, m], k) for m in WAYS)
            plus[...] += minus[...] + self.final(k, me.at[COLOUR_DIMS[k][THIRD]])[...]
            if self.result is not None:
                self.store(k).start()

    def finish(self):
        self.second.finish()
        self.third.finish()
        if self.result is not None:
            for k in COLOURS:
                self.store(k).wait()

    def sums(self):
        return self.in3.at[:, 0]


class Spread:
    def __init__(self, bands, result, total, send, recv, local):
        self.bands, self.result, self.total, self.sems, self.local = bands, result, total, (send, recv), local

    @staticmethod
    def scratch():
        return [pltpu.SemaphoreType.DMA((C, ADDED))] * PAIR + [pltpu.SemaphoreType.DMA((C,))]

    def mine(self, k):
        return self.bands.rows(self.result.at[k], k)

    def place(self, k):
        return self.bands.rows(self.total.at[Torus().at["x"], k], k)

    def hop(self, k, m):
        me = Torus()
        by = toward(m)
        if m < FAR:
            src, dst = self.mine(k), self.place(k)
        else:
            dst = src = self.total.at[me.shift("x", -by), k, self.bands.cuts(k)[m - FAR]]
        return remote(src, dst, self.sems, (k, m), me.neighbour("x", by))

    def own(self, k):
        return pltpu.make_async_copy(self.mine(k), self.place(k), self.local.at[k])

    def begin(self):
        for k in COLOURS:
            if self.local is None:
                self.place(k)[...] = self.mine(k)[...]
            else:
                self.own(k).start()
            for m in WAYS:
                self.hop(k, m).start()

    def forward(self):
        for k in COLOURS:
            for m in WAYS:
                self.hop(k, m).wait_recv()
                self.hop(k, FAR + m).start()

    def finish(self):
        for k in COLOURS:
            for m in WAYS:
                self.hop(k, FAR + m).wait_recv()
            if self.local is not None:
                self.own(k).wait()
            for m in range(ADDED):
                self.hop(k, m).wait_send()


def comm_params(collective_id):
    return pltpu.CompilerParams(collective_id=collective_id, has_side_effects=True, vmem_limit_bytes=VMEM_LIMIT)


def gather_kernel(*refs):
    n = len(Gather.semaphores())
    a, u, d = (Gather(kind, *refs[i::C][:PAIR], *refs[PAIR * C + n * i:][:n]) for i, kind in enumerate((WIDE, WIDE, DOWN)))
    enter()
    for gather in (a, u, d):
        gather.begin()
    for step, *ring in ((a.relay, FIRST), (u.relay, FIRST), (d.relay, FIRST), (a.settle, FIRST), (a.launch, SECOND),
                        (u.settle, FIRST), (u.launch, SECOND), (a.relay, SECOND), (d.settle, FIRST), (d.launch, SECOND),
                        (u.relay, SECOND), (a.settle, SECOND), (a.launch, THIRD), (a.launch, LAST), (d.relay, SECOND),
                        (u.settle, SECOND), (a.relay, THIRD), (d.settle, SECOND), (a.relay, LAST), (a.settle, THIRD),
                        (a.settle, LAST), (u.sent, FIRST, SECOND), (d.sent, FIRST, SECOND), (a.sent, *range(SIDE))):
        step(*ring)


def gather_call(attn, up, down, collective_id):
    return pl.pallas_call(
        gather_kernel, out_shape=[sds(BF16, *Gather.shape(kind)) for kind in (WIDE, WIDE, DOWN)], in_specs=[ANY] * C,
        out_specs=[ANY] * C, scratch_shapes=Gather.semaphores() * C, compiler_params=comm_params(collective_id),
        name="gather")(attn, up, down)


class Background:
    def __init__(self, steps, plan):
        self.steps, self.plan = steps, plan

    def visit(self, place):
        for j, first, end in self.plan.get(place, ()):
            @at_step(j)
            def _():
                for step in self.steps[first:end]:
                    step()


class Share:
    def __init__(self, mine, theirs, place, sems, slot):
        self.local = pltpu.make_async_copy(mine, place, sems[PAIR].at[slot])
        self.far = remote(theirs, place, sems, slot, Torus().partner())

    def start(self):
        self.far.start()
        self.local.start()

    def sent(self):
        self.local.wait()
        self.far.wait_send()

    def wait(self):
        self.sent()
        self.far.wait_recv()


class Push:
    def __init__(self, src, tail, rows, sems, slot=0):
        body = BODY * len(SEQ_PAIR)
        tails = TAIL * len(SEQ_PAIR)
        self.copies = [
            remote(src.at[pl.ds(start, size)], rows.at[pl.ds(to, size)], sems, (slot, i), Torus().partner())
            for i, (start, to, size) in enumerate(((0, body, body), (tail, PAIR * body + tails, tails)))]

    @staticmethod
    def semaphores(n):
        return [pltpu.SemaphoreType.DMA((n, PAIR))] * PAIR

    def start(self):
        for copy in self.copies:
            copy.start()

    def wait(self):
        for copy in self.copies:
            copy.wait_recv()

    def finish(self):
        for copy in self.copies:
            copy.wait_send()


class Exchange:
    def __init__(self, mine, theirs, rows, sems, slot):
        self.moves = []
        for s in SEQ_PAIR:
            for i, (start, size) in enumerate(((0, BODY), (BODY, TAIL))):
                place = lambda n: rows.at[pl.ds(start * len(SEQ_PAIR) * PAIR + size * n, size)]
                part = pl.ds(TOK * s + start, size)
                at = slot + (PAIR * s + i,)
                local = pltpu.make_async_copy(mine.at[part], place(s), sems[2].at[at])
                far = remote(theirs.at[part], place(len(SEQ_PAIR) + s), sems, at, Torus().partner())
                self.moves.append((local, far))

    @staticmethod
    def semaphores(*lead):
        return [pltpu.SemaphoreType.DMA(lead + (2 * PAIR,))] * 3

    def start(self):
        for local, far in self.moves:
            far.start()
            local.start()

    def wait(self):
        for local, far in self.moves:
            local.wait()
            far.wait_recv()

    def finish(self):
        for _, far in self.moves:
            far.wait_send()


NT = (((1,), (1,)), ((), ()))
TN = (((0,), (0,)), ((), ()))


def dot(a, b):
    return jnp.dot(a, b, preferred_element_type=F32)


def dot_nt(a, b):
    return lax.dot_general(a, b, NT, preferred_element_type=F32)


def dot_tn(a, b):
    return lax.dot_general(a, b, TN, preferred_element_type=F32)


def zeros_but(n, axis, value):
    return tuple(value if i == axis else 0 for i in range(n))


def whole(*shape):
    return pl.BlockSpec(shape, lambda *_: (0,) * len(shape))


def along(axis, *block, index=lambda j: j):
    return pl.BlockSpec(block, lambda j: zeros_but(len(block), axis, index(j)))


def row(vec, i):
    return vec[i:i + 1]


def row_mean(t):
    return jnp.mean(t, axis=-1, keepdims=True)


def norm_stats(t):
    centered = t - row_mean(t)
    rstd = lax.rsqrt(row_mean(centered * centered) + LN_EPS)
    return centered * rstd, rstd


def norm_back(xhat, rstd, g):
    return rstd * (g - row_mean(g) - xhat * row_mean(g * xhat))


def col_sum(t):
    return jnp.sum(t, axis=0, keepdims=True)


def at_step(j):
    return pl.when(pl.program_id(0) == j)


def accumulate(ref, value):
    @at_step(0)
    def _():
        ref[...] = value

    @pl.when(pl.program_id(0) > 0)
    def _():
        ref[...] += value


def pad(t):
    return jnp.concatenate([t.astype(F32), jnp.zeros((TOK - SEQ, t.shape[1]), F32)], axis=0).astype(BF16)


WINDOW = 2 * LANES


def window(h):
    first = h * HEAD
    start = jnp.minimum(lax.div(first, LANES) * LANES, D - WINDOW)
    lane = lax.broadcasted_iota(jnp.int32, (1, WINDOW), 1) + (start - first)
    return pl.ds(pl.multiple_of(start, LANES), WINDOW), (lane >= 0) & (lane < HEAD)


def each_head(body):
    def trip(i, carry):
        for n in range(PAIR):
            body(i * PAIR + n)
        return carry

    lax.fori_loop(0, HEADS // PAIR, trip, 0)


def only(mask, t):
    return jnp.where(mask, t, jnp.zeros_like(t))


def softmax(scores):
    e = jnp.exp(scores - jnp.max(scores, axis=-1, keepdims=True))
    return e * (1.0 / jnp.sum(e, axis=-1, keepdims=True))


def attention(s, rows, o, acc, visit):
    acc[...] = jnp.zeros_like(acc)
    start = pl.multiple_of(s * TOK, TAIL)
    tokens = pl.ds(start, SEQ)

    def head(h):
        lanes, mask = window(h)
        k = only(mask, rows[K, tokens, lanes])
        v = only(mask, rows[V, tokens, lanes])
        probs = softmax(dot_nt(rows[Q, tokens, lanes], k) * SCALE).astype(BF16)
        acc[:, lanes] += dot(probs, v)

    each_head(head)
    visit("half")
    o[pl.ds(start, TOK)] = pad(acc[...])


def seq_rows(t, s):
    return t[TOK * s:TOK * s + SEQ]


def seq_tile(s):
    return pl.ds(TOK * s, TOK)


FRONT_PLAN = {"start": ((0, 0, 2),), "half": ((O, 2, 3),), "wo": ((O + 1, 3, 4),), "end": ((O + 1, 4, None),)}


def front_kernel(x, w, b, vec, _, qkv, h1, o, att, h2, up, rows, acc, *sems):
    hosted = Background(Gather(WIDE, None, up, *sems).last_ring(), FRONT_PLAN)
    j = pl.program_id(0)
    at_step(0)(enter)
    hosted.visit("start")

    @at_step(0)
    def _():
        for s in SEQ_PAIR:
            xhat, _ = norm_stats(x[s].astype(F32))
            h1[seq_tile(s)] = pad(xhat * row(vec, G1) + row(vec, C1))

    @pl.when(j < O)
    def _():
        t = (dot(h1[...], w[0]) + b[0]).astype(BF16)
        qkv[0] = t
        rows[j] = t

    pl.when(j >= O)(lambda: attention(j - O, rows, o, acc, hosted.visit))

    hosted.visit("wo")

    @at_step(O + LAST_SEQ)
    def _():
        a = dot(o[...], w[0]) + row(vec, BO)
        att[...] = a
        for s in SEQ_PAIR:
            xhat, _ = norm_stats(x[s].astype(F32) + row(vec, S1) * seq_rows(a, s))
            h2[seq_tile(s)] = pad(xhat * row(vec, G2) + row(vec, C2))

    hosted.visit("end")


def upto(n):
    return lambda j: jnp.minimum(j, n)


def front_call(x, w_attn, b_qkv, vec, up, collective_id):
    return pl.pallas_call(
        front_kernel, grid=(O + PAIR,),
        out_shape=(sds(BF16, O, TT, D), sds(BF16, TT, D), sds(BF16, TT, D), sds(F32, TT, D), sds(BF16, TT, D),
                   sds(BF16, *Gather.shape(WIDE))),
        in_specs=[whole(*SEQS), along(0, 1, D, D, index=upto(O)), along(0, 1, 1, D, index=upto(V)), whole(8, D), ANY],
        out_specs=(along(0, 1, TT, D, index=upto(V)),) + (whole(TT, D),) * SIDE + (ANY,),
        scratch_shapes=[pltpu.VMEM((O, TT, D), BF16), pltpu.VMEM((SEQ, D), F32)] + Gather.semaphores(),
        input_output_aliases={SIDE: SIDE + 1},
        compiler_params=comm_params(collective_id), name="front",
    )(x, w_attn, b_qkv, vec, up)


def w_out_block():
    return pl.BlockSpec((1, D, D), lambda j: (O, 0, 0), pipeline_mode=pl.Buffered(1))


TILES = FF // HALF
OWN_BODY = BODY * len(SEQ_PAIR)
TAILS = ROWS - TAIL * PAIR * len(SEQ_PAIR)


def put_rows(ref, tail, s, t):
    ref[pl.ds(pl.multiple_of(BODY * s, BODY), BODY)] = t[:BODY]
    ref[pl.ds(pl.multiple_of(tail + TAIL * s, TAIL), TAIL)] = t[BODY:]


DOWN_PLAN = {"start": ((0, 0, 2),), "end": ((TILES - PAIR, 2, 3), (TILES + 2, 3, 4), (2 * TILES - 1, 4, None))}


def mlp_in_kernel(h2, gz, w_up, b_up, vec, _, act, slope, d_down, down, a_rows, b_rows, b_away, *sems):
    a_sems, b_sems, sems = sems[:PAIR], sems[PAIR:2 * PAIR], sems[2 * PAIR:]
    hosted = Background(Gather(DOWN, None, down, *sems).last_ring(), DOWN_PLAN)
    j = pl.program_id(0)
    away = Push(b_away, OWN_BODY, b_rows, b_sems, 0)
    tile = lambda n: Push(a_rows.at[n], TAILS, a_rows.at[n], a_sems, n)
    at_step(0)(enter)
    hosted.visit("start")

    @at_step(0)
    def _():
        first = Torus().at["c"] == 0
        for s in SEQ_PAIR:
            d = pad(gz[s].astype(F32) * row(vec, S2))
            left, right = d[:, :HALF], d[:, D - HALF:]
            put_rows(b_rows, TAILS, s, jnp.where(first, left, right))
            put_rows(b_away, OWN_BODY, s, jnp.where(first, right, left))

    at_step(1)(away.start)
    for n in range(TILES):
        at_step(n + 1)(tile(n).start)

    @pl.when(j < TILES)
    def _():
        u = dot(h2[...], w_up[0]) + b_up[0]
        phi = 0.5 * (1.0 + lax.erf(u * math.sqrt(0.5)))
        slope[...] = phi + u * (jnp.exp(-0.5 * u * u) * math.sqrt(0.5 / math.pi))
        place = lax.rem(lax.broadcasted_iota(jnp.int32, (TT, 1), 0), TOK)
        a = only(place < SEQ, u * phi).astype(BF16)
        act[...] = a
        for s in SEQ_PAIR:
            put_rows(a_rows.at[j], TAILS, s, a[TOK * s:TOK * s + TOK])

    at_step(TILES)(away.wait)
    for n in range(TILES):
        at_step(TILES + n)(tile(n).wait)

    @pl.when(j >= TILES)
    def _():
        d_down[...] = dot_tn(a_rows[j - TILES], b_rows[...])

    hosted.visit("end")

    @at_step(2 * TILES - 1)
    def _():
        away.finish()
        for n in range(TILES):
            tile(n).finish()


def mlp_in_call(h2, gz, w_up, b_up, vec, down, collective_id):
    low = lambda j: jnp.minimum(j, TILES - 1)
    high = lambda j: jnp.maximum(j - TILES, 0)
    return pl.pallas_call(
        mlp_in_kernel, grid=(2 * TILES,),
        out_shape=(sds(BF16, TT, FF), sds(F32, TT, FF), sds(F32, FF, HALF), sds(BF16, *Gather.shape(DOWN))),
        in_specs=[whole(TT, D), whole(*SEQS), up_tile(low), along(0, 1, 1, HALF, index=low), whole(8, D), ANY],
        out_specs=(along(1, TT, HALF, index=low), along(1, TT, HALF, index=low),
                   along(0, HALF, HALF, index=high), ANY),
        scratch_shapes=[pltpu.VMEM((TILES, ROWS, HALF), BF16), pltpu.VMEM((ROWS, HALF), BF16),
                        pltpu.VMEM((PAIR * TOK, HALF), BF16)] + Push.semaphores(TILES) + Push.semaphores(1) +
        Gather.semaphores(),
        input_output_aliases={SIDE + 1: O},
        compiler_params=comm_params(collective_id), name="mlp_in",
    )(h2, gz, w_up, b_up.reshape(TILES, 1, HALF), vec, down)


def up_tile(index=lambda j: j):
    return pl.BlockSpec((1, D, HALF), lambda j: (index(j) // PAIR, 0, index(j) % PAIR))


MLP_PLAN = {"start": ((0, 0, 2),), "end": ((3, 2, 3), (TILES - 1, 3, None))}


def mlp_out_kernel(act, slope, gz, w_up, w_down, vec, part, d_pre, db_up, mlp, d_h2, sums, dm, *scratch):
    first = First(Bands(DOWN), part, sums, *scratch)
    hosted = Background([first.near, first.far, first.relay, first.settle, first.finish], MLP_PLAN)
    at_step(0)(enter)
    hosted.visit("start")

    @at_step(0)
    def _():
        for s in SEQ_PAIR:
            dm[seq_tile(s)] = pad(gz[s].astype(F32) * row(vec, S2))

    accumulate(mlp, dot(act[...], w_down[...]))
    d = dot_nt(dm[...], w_down[...]) * slope[...]
    db_up[0] = col_sum(d)
    d = d.astype(BF16)
    d_pre[0, 0] = d
    accumulate(d_h2, dot_nt(d, w_up[0]))
    hosted.visit("end")


def mlp_out_call(act, slope, gz, w_up, w_down, vec, part, collective_id):
    return pl.pallas_call(
        mlp_out_kernel, grid=(TILES,),
        out_shape=(sds(BF16, PAIR, SIDE, TT, HALF), sds(F32, TILES, 1, HALF), sds(F32, TT, D), sds(F32, TT, D),
                   Bands(DOWN).sums()),
        in_specs=[along(1, TT, HALF), along(1, TT, HALF), whole(*SEQS), up_tile(), along(0, HALF, D), whole(8, D), ANY],
        out_specs=(pl.BlockSpec((1, 1, TT, HALF), lambda j: (j % PAIR, j // PAIR, 0, 0)), along(0, 1, 1, HALF),
                   whole(TT, D), whole(TT, D), ANY),
        scratch_shapes=[pltpu.VMEM((TT, D), BF16)] + Bands(DOWN).first(),
        compiler_params=comm_params(collective_id), name="mlp_out",
    )(act, slope, gz, w_up, w_down, vec, part)


def halves_of(t):
    t = pad(t)
    return t[:, :HALF], jnp.concatenate([t[:, HALF:], jnp.zeros((TOK, QCOLS - D), BF16)], axis=1)


def mid(mlp, d_h2, att, x, gz, vec, w_out, z, g_res, d_att, d_o, sums, da_rows):
    a = att[:SEQ]
    y = x[0].astype(F32) + row(vec, S1) * a
    m = mlp[:SEQ] + row(vec, B2)
    g = gz[0].astype(F32)
    z[0] = (y + row(vec, S2) * m).astype(BF16)
    xhat, rstd = norm_stats(y)
    dh = d_h2[:SEQ]
    gr = g + norm_back(xhat, rstd, dh * row(vec, G2))
    g_res[:SEQ] = gr
    da = gr * row(vec, S1)
    terms = (da, gr * a, dh * xhat, dh, g * row(vec, S2), g * m)
    accumulate(sums, jnp.concatenate([jnp.zeros((BO, D), F32)] + [col_sum(t) for t in terms], axis=0))
    for i, t in enumerate(halves_of(da)):
        d_att[i] = t
    da_rows[pl.ds(pl.multiple_of(pl.program_id(0) * TOK, TAIL), TOK)] = pad(da)

    @at_step(LAST_SEQ)
    def _():
        d_o[...] = dot_nt(da_rows[...], w_out[0]).astype(BF16)


def attention_back(s, qkv, d_o, d_qkv, db, acc, b_rows, away, first, visit):
    acc[...] = jnp.zeros_like(acc)

    def head(h):
        lanes, mask = window(h)
        q, k, v = (only(mask, qkv[i, :SEQ, lanes]) for i in (Q, K, V))
        do = only(mask, d_o[:SEQ, lanes])
        scores = dot_nt(k, q) * SCALE
        e = jnp.exp(scores - jnp.max(scores, axis=0, keepdims=True))
        probs = e * (1.0 / col_sum(e))
        acc[V, :, lanes] += dot(probs.astype(BF16), do)
        dp = dot_nt(v, do)
        ds = probs * (dp - col_sum(dp * probs))
        ds = (ds * SCALE).astype(BF16)
        acc[K, :, lanes] += dot(ds, q)
        acc[Q, :, lanes] += dot_tn(ds, k)

    each_head(head)
    visit("half")
    accumulate(db, jnp.concatenate([col_sum(acc[i]) for i in (Q, K, V)], axis=0))
    for n in (Q, K, V):
        left, right = halves_of(acc[n])
        d_qkv[0, n] = left
        d_qkv[1, n] = right
        put_rows(b_rows.at[n], TAILS, s, jnp.where(first, left, right))
        put_rows(away.at[n], OWN_BODY, s, jnp.where(first, right, left))


PER = HALF // STEP


class WideGrads:
    def __init__(self, inputs, a_of, cotangents, out, base, lead, a_rows, a_cols, b_rows):
        self.inputs, self.a_of, self.cotangents, self.out, self.base, self.lead = inputs, a_of, cotangents, out, base, lead
        self.a_rows, self.a_cols, self.b_rows = a_rows, a_cols, b_rows

    @staticmethod
    def scratch(inputs):
        return [pltpu.VMEM((inputs, ROWS, D), BF16), pltpu.VMEM((inputs, D, ROWS), BF16), pltpu.VMEM((SIDE, ROWS, HALF), BF16)]

    def step(self):
        j = pl.program_id(0)
        done = []
        for t in range(SIDE):
            n = (t + self.lead) % SIDE

            @at_step(self.base + PER * t)
            def _():
                i = self.a_of[n]
                if i not in done:
                    self.inputs[i].wait()
                    self.a_cols[i] = self.a_rows[i].T
                    done.append(i)
                self.cotangents[n].wait()

        @pl.when(j >= self.base)
        def _():
            n = lax.rem(lax.div(j - self.base, PER) + self.lead, SIDE)
            cols = pl.ds(pl.multiple_of(lax.rem(j - self.base, PER) * STEP, STEP), STEP)
            i = 0 if len(self.inputs) == 1 else lax.div(n, O)
            self.out[0] = dot(self.a_cols[i], self.b_rows[n, :, cols])

    def finish(self):
        for move in (*self.inputs, *self.cotangents):
            move.finish()


def grads_block(base, lead):
    def index(j):
        n = jnp.maximum(j - base, 0)
        return (n // PER + lead) % SIDE, 0, n % PER

    return pl.BlockSpec((1, D, STEP), index)


GRAD_STEPS = PER * SIDE


def tok_block():
    return along(0, TOK, D, index=upto(LAST_SEQ))


def seq_block():
    return along(0, 1, SEQ, D, index=upto(LAST_SEQ))


MID_PLAN = {"start": ((0, 0, 1),), "end": ((1, 1, 3), (8, 3, 4), (11, 4, 5), (LAST_SEQ + GRAD_STEPS, 5, None))}


def mid_kernel(*refs):
    refs = list(refs)
    take = lambda n: [refs.pop(0) for _ in range(n)]
    ins, (h2, d_pre, acc), outs, (d_up, result), da_rows = take(7), take(3), take(5), take(2), refs.pop(0)
    rows, a_sems, b_sems = take(3), take(C), take(C)
    rest = Rest(Bands(DOWN), acc, result, *refs)
    hosted = Background([rest.begin, rest.loaded, rest.relay, rest.settle, rest.relay_third, rest.settle_third, rest.finish],
                        MID_PLAN)
    c = Torus().at["c"]
    grads = WideGrads(
        [Exchange(h2, h2, rows[0].at[0], a_sems, ())], (0,) * SIDE,
        [Exchange(d_pre.at[c, n], d_pre.at[1 - c, n], rows[2].at[n], b_sems, (n,)) for n in range(SIDE)], d_up, SEQS[0], 0, *rows)
    at_step(0)(enter)
    hosted.visit("start")

    @at_step(0)
    def _():
        for move in (*grads.inputs, *grads.cotangents):
            move.start()

    pl.when(pl.program_id(0) < SEQS[0])(lambda: mid(*ins, *outs, da_rows))
    grads.step()
    hosted.visit("end")
    at_step(LAST_SEQ + GRAD_STEPS)(grads.finish)


def mid_call(mlp, d_h2, att, x, gz, vec, w_attn, h2, d_pre, acc, collective_id):
    return pl.pallas_call(
        mid_kernel, grid=(SEQS[0] + GRAD_STEPS,),
        out_shape=(sds(BF16, *SEQS), sds(F32, TT, D), sds(BF16, PAIR, TT, HALF), sds(BF16, TT, D), sds(F32, 8, D),
                   sds(F32, SIDE, D, HALF), Bands(DOWN).result()),
        in_specs=[tok_block()] * O + [seq_block()] * PAIR + [whole(8, D), w_out_block()] + [ANY] * O,
        out_specs=(seq_block(), tok_block(), along(1, PAIR, TOK, HALF, index=upto(LAST_SEQ)), whole(TT, D), whole(8, D),
                   grads_block(SEQS[0], 0), ANY),
        scratch_shapes=[pltpu.VMEM((TT, D), BF16)] + WideGrads.scratch(1) + Exchange.semaphores() + Exchange.semaphores(SIDE) +
        Bands(DOWN).later(),
        compiler_params=comm_params(collective_id), name="mid",
    )(mlp, d_h2, att, x, gz, vec, w_attn, h2, d_pre, acc)


ATTN_PLAN = {"start": ((0, 0, 3),), "half": ((0, 3, 4),), "end": ((LAST_SEQ, 4, 5), (LAST_SEQ + GRAD_STEPS, 5, None))}


def attn_back_kernel(*refs):
    refs = list(refs)
    take = lambda n: [refs.pop(0) for _ in range(n)]
    (qkv, d_o), (h1, o, d_att, part, result), (d_qkv, db, d_attn, sums, total) = take(2), take(5), take(5)
    acc, away, rows = refs.pop(0), refs.pop(0), take(3)
    a_sems, b_sems, away_sems = take(C), take(C), take(PAIR)
    first = First(Bands(WIDE), part, sums, *take(len(Bands(WIDE).first())))
    spread = Spread(Bands(DOWN), result, total, *refs)
    hosted = Background([spread.begin, first.near, first.far, spread.forward, first.relay, first.settle, first.finish,
                         spread.finish], ATTN_PLAN)
    c = Torus().at["c"]
    pushes = [Push(away.at[n], OWN_BODY, rows[2].at[n], away_sems, n) for n in range(O)]
    grads = WideGrads(
        [Exchange(a, a, rows[0].at[i], a_sems, (i,)) for i, a in enumerate((h1, o))], (0,) * O + (1,),
        pushes + [Exchange(d_att.at[c], d_att.at[1 - c], rows[2].at[O], b_sems, ())], d_attn, SEQS[0], O, *rows)
    at_step(0)(enter)
    hosted.visit("start")

    @at_step(0)
    def _():
        for move in (*grads.inputs, grads.cotangents[O]):
            move.start()

    @at_step(SEQS[0])
    def _():
        for push in pushes:
            push.start()

    j = pl.program_id(0)
    pl.when(j < SEQS[0])(lambda: attention_back(j, qkv, d_o, d_qkv, db, acc, rows[2], away, c == 0, hosted.visit))

    grads.step()
    hosted.visit("end")
    at_step(LAST_SEQ + GRAD_STEPS)(grads.finish)


def attn_back_call(qkv, d_o, h1, o, d_att, part, result, collective_id):
    return pl.pallas_call(
        attn_back_kernel, grid=(SEQS[0] + GRAD_STEPS,),
        out_shape=(sds(BF16, PAIR, O, TT, HALF), sds(F32, O, D), sds(F32, SIDE, D, HALF), Bands(WIDE).sums(),
                   Bands(DOWN).total()),
        in_specs=[along(1, O, TOK, D, index=upto(LAST_SEQ)), tok_block()] + [ANY] * 5,
        out_specs=(along(2, PAIR, O, TOK, HALF, index=upto(LAST_SEQ)), whole(O, D), grads_block(SEQS[0], O), ANY, ANY),
        scratch_shapes=[pltpu.VMEM((O, SEQ, D), F32), pltpu.VMEM((O, PAIR * TOK, HALF), BF16)] + WideGrads.scratch(2) +
        Exchange.semaphores(PAIR) + Exchange.semaphores() + Push.semaphores(O) + Bands(WIDE).first() + Spread.scratch(),
        compiler_params=comm_params(collective_id), name="attn_back",
    )(qkv, d_o, h1, o, d_att, part, result)


IN_STEPS = PAIR * O
SLOT = 40
LAST_PLAN = {"start": ((0, 0, 2),), "end": ((O, 2, None),)}


CORE_COLS = D - HALF
KEPT = 48
GRADS = ((KEPT, O * D), (KEPT, D), (KEPT, FF), (PAIR, C, UNIT, D), (SIDE, KEPT, LANES))
SHARES = PAIR * SIDE + SIDE + PAIR


def split_rows(totals, first, keep, give):
    for x in range(SIDE):
        for total, bands in totals:
            rows = jnp.concatenate([total[x, k, :n] for k, (_, n) in enumerate(BANDS[WIDE])], axis=0)
            low, high = rows[:KEPT], jnp.concatenate([rows[OWN:], rows[:KEPT - OWN]], axis=0)
            keep[x, :, bands.cols] = jnp.where(first, low, high)
            give[x, :, bands.cols] = jnp.where(first, high, low)


class Finals:
    def __init__(self, down, up, attn, outs, sems):
        self.c = Torus().at["c"]
        self.down, self.up, self.attn, self.sems = down, up, attn, sems
        self.qkv, self.out, self.up_out, self.down_out, self.pad = outs
        self.edge = pl.ds(CORE_COLS, LANES)

    def cols(self, base, width):
        return pl.ds(pl.multiple_of(base + self.c * HALF, LANES), width)

    def up_share(self, x):
        place = self.up_out.at[:, self.cols(QCOLS * x, HALF)]
        return Share(*(ref.at[x] for ref in self.up), place, self.sems, x)

    def block(self, x):
        return (self.out, 0) if x == O else (self.qkv, D * x)

    def attn_share(self, x):
        out, base = self.block(x)
        sides = (ref.at[x, :, pl.ds(0, CORE_COLS)] for ref in self.attn)
        return Share(*sides, out.at[:, self.cols(base, CORE_COLS)], self.sems, SIDE + x)

    def edge_share(self, x, padding):
        out, base = self.block(x)
        place = self.pad.at[x] if padding else out.at[:, pl.ds(base + CORE_COLS, LANES)]
        return Share(*(ref.at[x, :, self.edge] for ref in self.attn), place, self.sems, PAIR * SIDE + x)

    def down_share(self, edge):
        src = self.edge if edge else pl.ds(pl.multiple_of(self.c * LANES, LANES), CORE_COLS)
        sides = (self.down.at[pl.ds(PAIR * c, PAIR), :, :, src] for c in (self.c, 1 - self.c))
        place = self.down_out.at[:, :, :, self.edge if edge else self.cols(0, CORE_COLS)]
        return Share(*sides, place, self.sems, SHARES - PAIR + edge)

    def start_down(self):
        self.down_share(0).start()
        pl.when(self.c == 0)(lambda: self.down_share(1).start())

    def start(self):
        for x in range(SIDE):
            self.attn_share(x).start()
            pl.when(self.c == 0)(lambda: self.edge_share(x, False).start())
            pl.when(self.c == 1)(lambda: self.edge_share(x, True).start())

    def finish(self):
        for x in range(SIDE):
            for share in (self.up_share(x), self.attn_share(x), self.edge_share(x, True)):
                share.wait()
        self.down_share(0).wait()
        pl.when(self.c == 0)(lambda: self.down_share(1).sent())
        pl.when(self.c == 1)(lambda: self.down_share(1).far.wait_recv())


def last_kernel(*refs):
    refs = list(refs)
    take = lambda n: [refs.pop(0) for _ in range(n)]
    (d_half, w, x, g_res, vec), (small, acc_up, down, _), (dx, part), outs = take(5), take(SIDE), take(PAIR), take(len(GRADS))
    (acc, sums, pair_sums, block), (totals, sides), block_sem, swap_sems = take(4), (take(C), take(SIDE)), refs.pop(0), take(PAIR)
    finals = Finals(down, sides[:PAIR], sides[PAIR:], outs, take(C))
    halves = [Bands(WIDE, h) for h in WAYS]
    a, b = (First(bands, part, None, *take(len(bands.first()))) for bands in halves)
    rest_a, rest_b = (Rest(f.bands, f.own_all, None, f.own_all, *take(len(f.bands.later()) - 1)) for f in (a, b))
    rest_up = Rest(Bands(WIDE), acc_up, None, *take(len(Bands(WIDE).later())))
    spread_up, spread_a, spread_b = (
        Spread(r.bands, r.sums(), total, *take(PAIR), None) for r, total in zip((rest_up, rest_a, rest_b), totals))
    hosted = Background([rest_up.begin, a.near, rest_up.loaded, rest_up.relay], LAST_PLAN)
    first = finals.c == 0
    swap = remote(sums, pair_sums, swap_sems, (), Torus().partner())
    fetch = pltpu.make_async_copy(small, block, block_sem)
    at_step(0)(enter)
    hosted.visit("start")

    @at_step(0)
    def _():
        fetch.start()
        finals.start_down()

    @pl.when(pl.program_id(0) < IN_STEPS)
    def _():
        accumulate(acc, dot_nt(d_half[0, 0], w[0]))

    @at_step(IN_STEPS - 1)
    def _():
        rows = jnp.zeros((SUB, D), F32)
        for s in SEQ_PAIR:
            xhat, rstd = norm_stats(x[s].astype(F32))
            tokens = pl.ds(TOK * s, SEQ)
            dh = acc[tokens]
            rows = rows + jnp.concatenate([col_sum(dh * xhat), col_sum(dh), jnp.zeros((SUB - BO, D), F32)], axis=0)
            dx[s] = (g_res[tokens] + norm_back(xhat, rstd, dh * row(vec, G1))).astype(BF16)
        sums[...] = rows

    hosted.visit("end")

    @at_step(IN_STEPS)
    def _():
        swap.start()
        fetch.wait()
        swap.wait()
        both = sums[...] + pair_sums[...]
        for d in range(DEVICES):
            at = CHIP * (d // PAIR) + SLOT + OWN * (d % PAIR)
            block[at:at + BO, :OWN] = both[:BO, OWN * d:OWN * d + OWN]

        @pl.when(finals.c == 1)
        def _():
            for z in range(SIDE):
                for y in range(SIDE):
                    rows = block.at[pl.ds(CHIP * (SIDE * z + y), CHIP)]
                    put = pltpu.make_async_copy(rows, part.at[0, z, y, :, pl.ds(CORE_COLS, LANES)], block_sem)
                    put.start()
            pltpu.make_async_copy(block, small, block_sem).wait()

        def share_up():
            spread_up.finish()
            split_rows([(totals[0], Bands(WIDE))], first, *sides[:PAIR])
            for x in range(SIDE):
                finals.up_share(x).start()

        for step in (b.near, rest_up.settle, a.far, rest_up.relay_third, b.far, a.relay, rest_up.settle_third, spread_up.begin,
                     b.relay, spread_up.forward, functools.partial(a.settle, rest_a.send),
                     functools.partial(b.settle, rest_b.send), rest_a.relay, rest_b.relay, rest_a.settle, rest_b.settle,
                     share_up, rest_a.relay_third, rest_b.relay_third, rest_a.settle_third, spread_a.begin,
                     rest_b.settle_third, spread_b.begin, spread_a.forward, spread_b.forward, spread_a.finish, spread_b.finish):
            step()
        split_rows(list(zip(totals[1:], halves)), first, *sides[PAIR:])
        finals.start()
        for user in (rest_up, rest_a, rest_b, a, b, finals):
            user.finish()


def last_call(d_qkv, w_attn, x, g_res, vec, small, acc_up, down, part, collective_id):
    low = upto(IN_STEPS - 1)
    halves = [Bands(WIDE, h) for h in WAYS]
    dma = pltpu.SemaphoreType.DMA
    rings = [Bands(WIDE), *halves]
    return pl.pallas_call(
        last_kernel, grid=(IN_STEPS + 1,),
        out_shape=(sds(BF16, *SEQS), sds(F32, *part.shape), *(sds(F32, *shape) for shape in GRADS)),
        in_specs=[pl.BlockSpec((1, 1, TT, HALF), lambda j: (low(j) % PAIR, low(j) // PAIR, 0, 0)), up_tile(low),
                  whole(*SEQS), whole(TT, D), whole(8, D)] + [ANY] * SIDE,
        out_specs=(whole(*SEQS),) + (ANY,) * (len(GRADS) + 1),
        scratch_shapes=[pltpu.VMEM((TT, D), F32), pltpu.VMEM((SUB, D), F32), pltpu.VMEM((SUB, D), F32),
                        pltpu.VMEM((D, LANES), F32)] + [r.vmem(SIDE, C) for r in rings] +
        [pltpu.VMEM((SIDE, KEPT, HALF), F32)] * SIDE + [dma, dma, dma] + [dma((SHARES,))] * C + halves[0].first() * PAIR +
        halves[0].later()[1:] * PAIR + Bands(WIDE).later() + Spread.scratch()[:PAIR] * C,
        input_output_aliases={8: 1},
        compiler_params=comm_params(collective_id), name="last",
    )(d_qkv, w_attn, x, g_res, vec, small, acc_up, down, part)


BQ, BU, VEC = 3 * D // 32, 3 * D // 32 + FF // 32, 3 * D // 32 + FF // 32 + 8 * OWN


def pair_swap(a):
    return lax.ppermute(a, "fsdp", [(i, i ^ 1) for i in range(DEVICES)])


def by_core(first, a, b):
    return jnp.where(first, a, b), jnp.where(first, b, a)


def my_pieces(shards, first):
    w_qkv, b_qkv, w_out, w_up, b_up, w_down, vec_params = shards
    x = lax.axis_index("rep")
    small = jnp.concatenate([b_qkv, b_up, vec_params.reshape(-1)])
    small = jnp.pad(small, (0, OWN * LANES - VEC)).reshape(OWN, LANES)
    attn = lax.dynamic_slice_in_dim(jnp.concatenate([w_qkv, w_out], axis=1), x * D, D, 1)
    attn = jnp.concatenate([attn, small], axis=1)
    up = lax.dynamic_slice_in_dim(w_up, x * QCOLS, QCOLS, 1)
    wide = jnp.stack([attn, up]).astype(BF16)
    mine, theirs = by_core(first, wide[..., :HALF], wide[..., HALF:])
    theirs = pair_swap(theirs)
    piece = jnp.concatenate(by_core(first, mine, theirs), axis=1)
    down = lax.dynamic_slice_in_dim(w_down, x * 48, 48, 0).astype(BF16).reshape(3, 16, D)
    return piece[0], piece[1], down


def small_params(w_attn):
    small = w_attn[0, :, D:].astype(F32).reshape(DEVICES, OWN * LANES)
    vec = small[:, BU:VEC].reshape(DEVICES, 8, OWN).transpose(1, 0, 2).reshape(8, D)
    return small[:, :BQ].reshape(O, 1, D), small[:, BQ:BU].reshape(FF), vec


ROOM = 5 * LANES


def small_grads(db_qkv, db_up, sums):
    vec = sums[BO:].reshape(8 - BO, DEVICES, OWN).transpose(1, 0, 2).reshape(DEVICES, VEC - BU - BO * OWN)
    small = jnp.concatenate([db_qkv.reshape(DEVICES, BQ), db_up.reshape(DEVICES, BU - BQ), vec], axis=1)
    small = small + pair_swap(small)
    small = jnp.pad(small, ((0, 0), (0, ROOM - small.shape[1]))).reshape(DEVICES, ROOM // LANES, LANES)
    return jnp.pad(small, ((0, 0), (0, OWN - ROOM // LANES), (0, 0))).reshape(D, LANES)


def device_step(x, gz, *shards):
    first = lax.rem(lax.axis_index("fsdp"), PAIR) == 0
    attn, up, down = my_pieces(shards, first)
    w_attn, up, down = gather_call(attn, up, down, 0)
    w_attn = w_attn.reshape(SIDE, D, QCOLS)
    b_qkv, b_up, vec = small_params(w_attn)
    qkv, h1, o, att, h2, w_up = front_call(x, w_attn, b_qkv, vec, up, 1)
    w_up = w_up.reshape(SIDE, D, QCOLS)
    act, slope, part, w_down = mlp_in_call(h2, gz, w_up, b_up, vec, down, 2)
    part = part.reshape((SIDE,) * 3 + (C * UNIT, HALF))
    d_pre, db_up, mlp, d_h2, acc = mlp_out_call(act, slope, gz, w_up, w_down.reshape(FF, D), vec, part, 3)
    z, g_res, d_att, d_o, sums, part, result = mid_call(mlp, d_h2, att, x, gz, vec, w_attn, h2, d_pre, acc, 4)
    part = part.reshape((SIDE,) * 3 + (CHIP, HALF))
    d_qkv, db_qkv, part, acc, down = attn_back_call(qkv, d_o, h1, o, d_att, part, result, 5)
    small = small_grads(db_qkv, db_up, sums)
    part = part.reshape((SIDE,) * 3 + (CHIP, HALF))
    dx, _, g_qkv, g_out, g_up, g_down, edge = last_call(d_qkv, w_attn, x, g_res, vec, small, acc, down, part, 6)
    small = edge[0, :ROOM // LANES].reshape(ROOM)
    vec = jnp.concatenate([edge[0, SLOT:SLOT + BO, :OWN], small[BU:VEC - BO * OWN].reshape(8 - BO, OWN)], axis=0)
    g_qkv, g_out, g_up = (g[:OWN] for g in (g_qkv, g_out, g_up))
    return z, dx, g_qkv, small[:BQ], g_out, g_up, small[BQ:BU], g_down.reshape(FF // DEVICES, D), vec


def solution(mesh):
    batch = P(("rep", "fsdp"), None, None)
    rows, flat, cols = P("fsdp", None), P("fsdp"), P(None, "fsdp")
    shards = (rows, flat, rows, rows, flat, rows, cols)
    return jax.shard_map(device_step, mesh=mesh, in_specs=(batch, batch) + shards,
                         out_specs=(batch, batch) + shards, check_vma=False)
```

```python
import functools
import math

import jax
import jax.numpy as jnp
from jax import lax
from jax.experimental import pallas as pl
from jax.experimental.pallas import tpu as pltpu
from jax.sharding import PartitionSpec as P

HEADS = 16
LN_EPS = 1e-5
D = 1408
FF = 6144
SEQ = 257
HEAD = D // HEADS
SCALE = HEAD ** -0.5
QCOLS = 1536
HALF = 768
OWN = 44
CHIP = 2 * OWN
LANES = 128
DEVICES = 32
F32 = jnp.float32
BF16 = jnp.bfloat16
VMEM_LIMIT = 66 * 1000 * 1000
G1, C1, BO, S1, G2, C2, B2, S2 = range(8)
Q, K, V, O = range(4)
SEQS = (2, SEQ, D)
LAST_SEQ = SEQS[0] - 1
SEQ_PAIR = range(SEQS[0])
TAIL = 16
BODY = SEQ - 1
TOK = BODY + TAIL
TT = 2 * TOK
ROWS = 4 * TOK
STEP = 256


def sds(dtype, *shape):
    return jax.ShapeDtypeStruct(shape, dtype)


MESH_ID = pl.DeviceIdType.MESH
SIDE = 4
SUB = 8
PAIR = 2
C = 3
COLOURS = range(C)
COLOUR_DIMS = ("xyz", "yzx", "zxy")
FIRST, SECOND, THIRD, LAST = range(4)
WAYS = range(PAIR)
NEAR, FAR, ADDED = 0, 2, 4
WIDE, DOWN = "wide", "down"
ANY = pl.BlockSpec(memory_space=pl.ANY)
ALL = slice(None)


def duo(m):
    return pl.ds(PAIR * m, PAIR)


def toward(m):
    return 1 - PAIR * (m % PAIR)


class Torus:
    def __init__(self):
        f = lax.axis_index("fsdp")
        self.at = {"x": lax.axis_index("rep"), "z": lax.div(f, SIDE * PAIR), "y": lax.rem(lax.div(f, PAIR), SIDE),
                   "c": lax.rem(f, PAIR)}

    def shift(self, dim, by):
        return lax.rem(self.at[dim] + (SIDE + by), SIDE)

    def device(self, **moved):
        p = {**self.at, **moved}
        return (p["x"], (p["z"] * SIDE + p["y"]) * PAIR + p["c"])

    def neighbour(self, dim, by):
        return self.device(**{dim: self.shift(dim, by)})

    def partner(self):
        return self.device(c=1 - self.at["c"])


def enter():
    me = Torus()
    barrier = pltpu.get_barrier_semaphore()
    others = [me.neighbour(d, toward(m)) for d in COLOUR_DIMS[0] for m in WAYS] + [me.partner()]
    for other in others:
        pl.semaphore_signal(barrier, device_id=other, device_id_type=MESH_ID)
    pl.semaphore_wait(barrier, len(others))


def remote(src, dst, sems, slot, device):
    return pltpu.make_async_remote_copy(src_ref=src, dst_ref=dst, send_sem=sems[0].at[slot], recv_sem=sems[1].at[slot],
                                        device_id=device, device_id_type=MESH_ID)


class Gather:
    def __init__(self, kind, src, dst, hop_send, hop_recv, push_send, push_recv, local):
        self.kind, self.src, self.dst, self.local = kind, src, dst, local
        self.hops, self.pushes = (hop_send, hop_recv), (push_send, push_recv)
        self.cols, self.cut = (256, 128) if kind == WIDE else (D, HALF)

    @staticmethod
    def semaphores():
        dma = pltpu.SemaphoreType.DMA
        return [dma((C, C, ADDED))] * PAIR + [dma((C, ADDED + 1))] * PAIR + [dma((C,))]

    @staticmethod
    def shape(kind):
        return (SIDE,) * 3 + (CHIP, QCOLS) if kind == WIDE else (SIDE, SIDE, PAIR, SIDE, C, 16, D)

    def source(self, k):
        return self.src.at[:, pl.ds(self.cols * k, self.cols)] if self.kind == WIDE else self.src.at[k]

    def piece(self, me, k, s, v, half=None):
        dims = COLOUR_DIMS[k]
        at = {**me.at, **{d: ALL for d in dims[:s]}, dims[s]: v}
        off, width = 0, self.cols
        if half is not None and s == FIRST:
            off, width = self.cut * half, (self.cut, self.cols - self.cut)[half]
        elif half is not None:
            at[dims[0]] = duo(half)
        if self.kind == WIDE:
            cols = pl.ds(pl.multiple_of(at["c"] * HALF + self.cols * k + off, 128), width)
            return self.dst.at[at["x"], at["z"], at["y"], :, cols]
        return self.dst.at[at["z"], at["y"], at["c"], at["x"], k, :, pl.ds(off, width)]

    def hop(self, k, s, m):
        me = Torus()
        dim = COLOUR_DIMS[k][s]
        by = toward(m)
        if m < FAR:
            ref = self.piece(me, k, s, me.at[dim])
        else:
            ref = self.piece(me, k, s, me.shift(dim, -by), m - FAR)
        src = self.source(k) if s == FIRST and m < FAR else ref
        return remote(src, ref, self.hops, (k, s, m), me.neighbour(dim, by))

    def push(self, k, n):
        me = Torus()
        dim = COLOUR_DIMS[k][THIRD]
        if n < FAR:
            ref = self.piece(me, k, THIRD, me.shift(dim, -toward(n)))
        elif n < ADDED:
            ref = self.piece(me, k, THIRD, me.shift(dim, FAR), n - FAR)
        else:
            ref = self.piece(me, k, THIRD, me.at[dim])
        return remote(ref, ref, self.pushes, (k, n), me.partner())

    def own(self, k):
        me = Torus()
        return pltpu.make_async_copy(self.source(k), self.piece(me, k, FIRST, me.at[COLOUR_DIMS[k][FIRST]]), self.local.at[k])

    def launch(self, s):
        for k in COLOURS:
            for m in WAYS:
                self.hop(k, s, m).start()
            if s == THIRD:
                self.push(k, ADDED).start()

    def relay(self, s):
        for k in COLOURS:
            for m in WAYS:
                self.hop(k, s, m).wait_recv()
                self.hop(k, s, FAR + m).start()
                if s == THIRD:
                    self.push(k, m).start()

    def settle(self, s):
        for k in COLOURS:
            for m in WAYS:
                self.hop(k, s, FAR + m).wait_recv()
                if s == THIRD:
                    self.push(k, FAR + m).start()
            if s == FIRST:
                self.own(k).wait()

    def begin(self):
        for k in COLOURS:
            self.own(k).start()
        self.launch(FIRST)

    def sent(self, *rings):
        for k in COLOURS:
            for s in rings:
                for m in range(ADDED):
                    self.hop(k, s, m).wait_send()
            if THIRD in rings:
                for n in range(ADDED + 1):
                    self.push(k, n).wait()

    def last_ring(self):
        return [functools.partial(f, THIRD) for f in (self.launch, self.relay, self.settle, self.sent)]


def add_into(total, *others):
    lead = total.shape[:-2]

    def body(i, carry):
        idx = []
        for n in reversed(lead):
            idx.insert(0, lax.rem(i, n))
            i = lax.div(i, n)
        value = total[tuple(idx)]
        for other in others:
            value = value + other[tuple(idx)]
        total[tuple(idx)] = value
        return carry

    lax.fori_loop(0, math.prod(lead), body, 0)


class Ring:
    def __init__(self, s, bands, terms, passed, relay, landing, send, recv):
        self.s, self.bands, self.terms, self.passed, self.relay, self.landing = s, bands, terms, passed, relay, landing
        self.sems = (send, recv)

    def zone(self, k, way, half):
        if self.s == THIRD:
            return self.landing.at[k, way, self.bands.cuts(k)[half]]
        return self.bands.rows(self.landing.at[k, way, duo(half)], k)

    def carried(self, ref, k, way):
        if self.s == THIRD:
            return ref.at[k, way, pl.ds(0, self.bands.cuts(k)[way].size)]
        return self.bands.rows(ref.at[k, way], k)

    def hop(self, k, m):
        me = Torus()
        dim = COLOUR_DIMS[k][self.s]
        way, by = m % PAIR, toward(m)
        if m < FAR:
            src, dst = self.terms(k, me.shift(dim, FAR), way), self.carried(self.relay, k, way)
        elif m < ADDED:
            src, dst = self.terms(k, me.shift(dim, by), 1 - way), self.zone(k, way, 1 - way)
        else:
            src, dst = self.carried(self.passed, k, way), self.zone(k, way, way)
        return remote(src, dst, self.sems, (k, m), me.neighbour(dim, by))

    def start(self, k, base):
        for m in WAYS:
            self.hop(k, base + m).start()

    def arrived(self, k, base):
        for m in WAYS:
            self.hop(k, base + m).wait_recv()

    def finish(self):
        for k in COLOURS:
            for m in range(ADDED + PAIR):
                self.hop(k, m).wait_send()

    @staticmethod
    def semaphores():
        return [pltpu.SemaphoreType.DMA((C, ADDED + PAIR))] * PAIR


UNIT = 32
BANDS = {WIDE: ((0, 24), (24, UNIT), (56, UNIT)), DOWN: ((0, UNIT), (UNIT, UNIT), (2 * UNIT, UNIT))}
ORDERS = {WIDE: "xzy", DOWN: "zyx"}


class Bands:
    def __init__(self, kind, half=None):
        self.order, self.bands = ORDERS[kind], BANDS[kind]
        self.width = HALF if half is None else HALF // PAIR
        self.cols = pl.ds(self.width * (half or 0), self.width)

    def band(self, k):
        return pl.ds(*self.bands[k])

    def rows(self, ref, k):
        return ref.at[(ALL,) * (len(ref.shape) - PAIR) + (pl.ds(0, self.bands[k][1]),)]

    def cuts(self, k):
        rows = self.bands[k][1]
        cut = (rows // SUB + 1) // PAIR * SUB
        return pl.ds(0, cut), pl.ds(cut, rows - cut)

    def rest(self, k):
        return [d for d in self.order if d != COLOUR_DIMS[k][FIRST]]

    def units(self, *lead):
        return lead + (UNIT, self.width)

    def vmem(self, *lead):
        return pltpu.VMEM(self.units(*lead), F32)

    def sums(self):
        return sds(F32, *self.units(C, SIDE, SIDE))

    def result(self):
        return sds(F32, *self.units(C))

    def total(self):
        return sds(F32, *self.units(SIDE, C))

    def first(self):
        relays = [self.vmem(C, PAIR, PAIR, SIDE)] * PAIR
        dma = pltpu.SemaphoreType.DMA
        return [self.vmem(C, SIDE, SIDE), *relays, self.vmem(C, PAIR, SIDE, SIDE), *Ring.semaphores(), dma((C, C)), dma((C,))]

    def later(self):
        dma = pltpu.SemaphoreType.DMA
        return [self.vmem(C, SIDE, SIDE), self.vmem(C, PAIR, PAIR), self.vmem(C, PAIR, SIDE),
                pltpu.VMEM((C, PAIR, UNIT // PAIR, self.width), F32), self.vmem(C, PAIR),
                *Ring.semaphores(), *Ring.semaphores(), dma((C,)), dma((C,))]


class First:
    def __init__(self, bands, part, acc, own, passed, relay, landing, send, recv, load, store):
        self.bands, self.part, self.acc, self.own_all, self.passed = bands, part, acc, own, passed
        self.relay_in, self.landing, self.load_sem, self.store_sem = relay, landing, load, store
        self.ring = Ring(FIRST, bands, self.terms, passed, relay, landing, send, recv)

    def own(self, k):
        return self.bands.rows(self.own_all.at[k], k)

    def terms(self, k, v, half=None):
        b = self.bands
        at = {d: ALL for d in b.order}
        at[COLOUR_DIMS[k][FIRST]] = v
        if half is not None:
            at[b.rest(k)[0]] = duo(half)
        return self.part.at[tuple(at[d] for d in b.order) + (b.band(k), b.cols)]

    def load(self, k, m):
        me = Torus()
        dim = COLOUR_DIMS[k][FIRST]
        if m in WAYS:
            src, dst = self.terms(k, me.shift(dim, toward(m)), m), self.ring.carried(self.passed, k, m)
        else:
            src, dst = self.terms(k, me.at[dim]), self.own(k)
        return pltpu.make_async_copy(src, dst, self.load_sem.at[k, m])

    def store(self, k):
        return pltpu.make_async_copy(self.own(k), self.bands.rows(self.acc.at[k], k), self.store_sem.at[k])

    def near(self):
        for k in COLOURS:
            self.ring.start(k, NEAR)

    def far(self):
        for k in COLOURS:
            self.ring.start(k, FAR)
        for m in COLOURS:
            for k in COLOURS:
                self.load(k, m).start()

    def relay(self):
        for k in COLOURS:
            self.ring.arrived(k, NEAR)
            for m in WAYS:
                self.load(k, m).wait()
                add_into(self.ring.carried(self.passed, k, m), self.ring.carried(self.relay_in, k, m))
            self.ring.start(k, ADDED)

    def settle(self, then=None):
        for k in COLOURS:
            self.load(k, FAR).wait()
            for base in (FAR, ADDED):
                self.ring.arrived(k, base)
            add_into(self.own(k), *(self.bands.rows(self.landing.at[k, m], k) for m in WAYS))
            if then is None:
                self.store(k).start()
            else:
                then(k)

    def finish(self):
        self.ring.finish()
        if self.acc is not None:
            for k in COLOURS:
                self.store(k).wait()


class Rest:
    def __init__(self, bands, acc, result, own, relay2, in2, relay3, in3, *sems):
        self.bands, self.acc, self.own, self.result = bands, acc, own, result
        self.in2, self.in3, self.relay2, self.relay3, self.load_sem, self.store_sem = in2, in3, relay2, relay3, *sems[-2:]
        self.second = Ring(SECOND, bands, functools.partial(self.terms, acc), relay2, relay2, in2, *sems[:PAIR])
        self.third = Ring(THIRD, bands, self.final, relay3, relay3, in3, *sems[PAIR:2 * PAIR])

    def terms(self, ref, k, v, half=None):
        other = ALL if half is None else duo(half)
        first = self.bands.rest(k)[0] == COLOUR_DIMS[k][SECOND]
        return self.bands.rows(ref.at[(k, v, other) if first else (k, other, v)], k)

    def final(self, k, v, half=None):
        if half is None:
            return self.bands.rows(self.in2.at[k, 0, v], k)
        return self.in2.at[k, 0, v, self.bands.cuts(k)[half]]

    def load(self, k):
        return pltpu.make_async_copy(self.bands.rows(self.acc.at[k], k), self.bands.rows(self.own.at[k], k), self.load_sem.at[k])

    def store(self, k):
        rows = self.bands.rows
        return pltpu.make_async_copy(rows(self.in3.at[k, 0], k), rows(self.result.at[k], k), self.store_sem.at[k])

    def send(self, k):
        for base in (NEAR, FAR):
            self.second.start(k, base)

    def begin(self):
        for k in COLOURS:
            self.send(k)
        for k in COLOURS:
            self.load(k).start()

    def loaded(self):
        for k in COLOURS:
            self.load(k).wait()

    def relay(self):
        me = Torus()
        for k in COLOURS:
            self.second.arrived(k, NEAR)
            for m in WAYS:
                terms = self.terms(self.own, k, me.shift(COLOUR_DIMS[k][SECOND], toward(m)), m)
                add_into(self.second.carried(self.relay2, k, m), terms)
            self.second.start(k, ADDED)

    def settle(self):
        me = Torus()
        for k in COLOURS:
            for base in (FAR, ADDED):
                self.second.arrived(k, base)
            plus, minus = (self.bands.rows(self.in2.at[k, m], k) for m in WAYS)
            add_into(plus, minus, self.terms(self.own, k, me.at[COLOUR_DIMS[k][SECOND]]))
            for base in (NEAR, FAR):
                self.third.start(k, base)

    def relay_third(self):
        me = Torus()
        for k in COLOURS:
            self.third.arrived(k, NEAR)
            for m in WAYS:
                mine = self.third.carried(self.relay3, k, m)
                mine[...] += self.final(k, me.shift(COLOUR_DIMS[k][THIRD], toward(m)), m)[...]
            self.third.start(k, ADDED)

    def settle_third(self):
        me = Torus()
        for k in COLOURS:
            for base in (FAR, ADDED):
                self.third.arrived(k, base)
            plus, minus = (self.bands.rows(self.in3.at[k, m], k) for m in WAYS)
            plus[...] += minus[...] + self.final(k, me.at[COLOUR_DIMS[k][THIRD]])[...]
            if self.result is not None:
                self.store(k).start()

    def finish(self):
        self.second.finish()
        self.third.finish()
        if self.result is not None:
            for k in COLOURS:
                self.store(k).wait()

    def sums(self):
        return self.in3.at[:, 0]


class Spread:
    def __init__(self, bands, result, total, send, recv, local):
        self.bands, self.result, self.total, self.sems, self.local = bands, result, total, (send, recv), local

    @staticmethod
    def scratch():
        return [pltpu.SemaphoreType.DMA((C, ADDED))] * PAIR + [pltpu.SemaphoreType.DMA((C,))]

    def mine(self, k):
        return self.bands.rows(self.result.at[k], k)

    def place(self, k):
        return self.bands.rows(self.total.at[Torus().at["x"], k], k)

    def hop(self, k, m):
        me = Torus()
        by = toward(m)
        if m < FAR:
            src, dst = self.mine(k), self.place(k)
        else:
            dst = src = self.total.at[me.shift("x", -by), k, self.bands.cuts(k)[m - FAR]]
        return remote(src, dst, self.sems, (k, m), me.neighbour("x", by))

    def own(self, k):
        return pltpu.make_async_copy(self.mine(k), self.place(k), self.local.at[k])

    def begin(self):
        for k in COLOURS:
            if self.local is None:
                self.place(k)[...] = self.mine(k)[...]
            else:
                self.own(k).start()
            for m in WAYS:
                self.hop(k, m).start()

    def forward(self):
        for k in COLOURS:
            for m in WAYS:
                self.hop(k, m).wait_recv()
                self.hop(k, FAR + m).start()

    def finish(self):
        for k in COLOURS:
            for m in WAYS:
                self.hop(k, FAR + m).wait_recv()
            if self.local is not None:
                self.own(k).wait()
            for m in range(ADDED):
                self.hop(k, m).wait_send()


def comm_params(collective_id):
    return pltpu.CompilerParams(collective_id=collective_id, has_side_effects=True, vmem_limit_bytes=VMEM_LIMIT)


def gather_kernel(*refs):
    n = len(Gather.semaphores())
    a, u, d = (Gather(kind, *refs[i::C][:PAIR], *refs[PAIR * C + n * i:][:n]) for i, kind in enumerate((WIDE, WIDE, DOWN)))
    enter()
    for gather in (a, u, d):
        gather.begin()
    for step, *ring in ((a.relay, FIRST), (u.relay, FIRST), (d.relay, FIRST), (a.settle, FIRST), (a.launch, SECOND),
                        (u.settle, FIRST), (u.launch, SECOND), (a.relay, SECOND), (d.settle, FIRST), (d.launch, SECOND),
                        (u.relay, SECOND), (a.settle, SECOND), (a.launch, THIRD), (d.relay, SECOND), (u.settle, SECOND),
                        (a.relay, THIRD), (d.settle, SECOND), (a.settle, THIRD), (u.sent, FIRST, SECOND),
                        (d.sent, FIRST, SECOND), (a.sent, FIRST, SECOND, THIRD)):
        step(*ring)


def gather_call(attn, up, down, collective_id):
    return pl.pallas_call(
        gather_kernel, out_shape=[sds(BF16, *Gather.shape(kind)) for kind in (WIDE, WIDE, DOWN)], in_specs=[ANY] * C,
        out_specs=[ANY] * C, scratch_shapes=Gather.semaphores() * C, compiler_params=comm_params(collective_id),
        name="gather")(attn, up, down)


class Background:
    def __init__(self, steps, plan):
        self.steps, self.plan = steps, plan

    def visit(self, place):
        for j, first, end in self.plan.get(place, ()):
            @at_step(j)
            def _():
                for step in self.steps[first:end]:
                    step()


class Share:
    def __init__(self, mine, theirs, place, sems, slot):
        self.local = pltpu.make_async_copy(mine, place, sems[PAIR].at[slot])
        self.far = remote(theirs, place, sems, slot, Torus().partner())

    def start(self):
        self.far.start()
        self.local.start()

    def sent(self):
        self.local.wait()
        self.far.wait_send()

    def wait(self):
        self.sent()
        self.far.wait_recv()


class Push:
    def __init__(self, src, tail, rows, sems, slot=0):
        body = BODY * len(SEQ_PAIR)
        tails = TAIL * len(SEQ_PAIR)
        self.copies = [
            remote(src.at[pl.ds(start, size)], rows.at[pl.ds(to, size)], sems, (slot, i), Torus().partner())
            for i, (start, to, size) in enumerate(((0, body, body), (tail, PAIR * body + tails, tails)))]

    @staticmethod
    def semaphores(n):
        return [pltpu.SemaphoreType.DMA((n, PAIR))] * PAIR

    def start(self):
        for copy in self.copies:
            copy.start()

    def wait(self):
        for copy in self.copies:
            copy.wait_recv()

    def finish(self):
        for copy in self.copies:
            copy.wait_send()


class Exchange:
    def __init__(self, mine, theirs, rows, sems, slot):
        self.moves = []
        for s in SEQ_PAIR:
            for i, (start, size) in enumerate(((0, BODY), (BODY, TAIL))):
                place = lambda n: rows.at[pl.ds(start * len(SEQ_PAIR) * PAIR + size * n, size)]
                part = pl.ds(TOK * s + start, size)
                at = slot + (PAIR * s + i,)
                local = pltpu.make_async_copy(mine.at[part], place(s), sems[2].at[at])
                far = remote(theirs.at[part], place(len(SEQ_PAIR) + s), sems, at, Torus().partner())
                self.moves.append((local, far))

    @staticmethod
    def semaphores(*lead):
        return [pltpu.SemaphoreType.DMA(lead + (2 * PAIR,))] * 3

    def start(self):
        for local, far in self.moves:
            far.start()
            local.start()

    def wait(self):
        for local, far in self.moves:
            local.wait()
            far.wait_recv()

    def finish(self):
        for _, far in self.moves:
            far.wait_send()


NT = (((1,), (1,)), ((), ()))
TN = (((0,), (0,)), ((), ()))


def dot(a, b):
    return jnp.dot(a, b, preferred_element_type=F32)


def dot_nt(a, b):
    return lax.dot_general(a, b, NT, preferred_element_type=F32)


def dot_tn(a, b):
    return lax.dot_general(a, b, TN, preferred_element_type=F32)


def zeros_but(n, axis, value):
    return tuple(value if i == axis else 0 for i in range(n))


def whole(*shape):
    return pl.BlockSpec(shape, lambda *_: (0,) * len(shape))


def along(axis, *block, index=lambda j: j):
    return pl.BlockSpec(block, lambda j: zeros_but(len(block), axis, index(j)))


def row(vec, i):
    return vec[i:i + 1]


def row_mean(t):
    return jnp.mean(t, axis=-1, keepdims=True)


def norm_stats(t):
    centered = t - row_mean(t)
    rstd = lax.rsqrt(row_mean(centered * centered) + LN_EPS)
    return centered * rstd, rstd


def norm_back(xhat, rstd, g):
    return rstd * (g - row_mean(g) - xhat * row_mean(g * xhat))


def col_sum(t):
    return jnp.sum(t, axis=0, keepdims=True)


def at_step(j):
    return pl.when(pl.program_id(0) == j)


def accumulate(ref, value):
    @at_step(0)
    def _():
        ref[...] = value

    @pl.when(pl.program_id(0) > 0)
    def _():
        ref[...] += value


def pad(t):
    return jnp.concatenate([t.astype(F32), jnp.zeros((TOK - SEQ, t.shape[1]), F32)], axis=0).astype(BF16)


WINDOW = 2 * LANES


def window(h):
    first = h * HEAD
    start = jnp.minimum(lax.div(first, LANES) * LANES, D - WINDOW)
    lane = lax.broadcasted_iota(jnp.int32, (1, WINDOW), 1) + (start - first)
    return pl.ds(pl.multiple_of(start, LANES), WINDOW), (lane >= 0) & (lane < HEAD)


def each_head(body):
    lax.fori_loop(0, HEADS, lambda h, carry: (body(h), carry)[1], 0)


def each_seq(body):
    def trip(s, carry):
        start = pl.multiple_of(s * TOK, TAIL)
        body(s, pl.ds(start, TOK), pl.ds(start, SEQ))
        return carry

    lax.fori_loop(0, len(SEQ_PAIR), trip, 0)


def only(mask, t):
    return jnp.where(mask, t, jnp.zeros_like(t))


def softmax(scores):
    e = jnp.exp(scores - jnp.max(scores, axis=-1, keepdims=True))
    return e * (1.0 / jnp.sum(e, axis=-1, keepdims=True))


def attention(s, rows, o, acc, visit):
    acc[...] = jnp.zeros_like(acc)
    start = pl.multiple_of(s * TOK, TAIL)
    tokens = pl.ds(start, SEQ)

    def head(h):
        lanes, mask = window(h)
        k = only(mask, rows[K, tokens, lanes])
        v = only(mask, rows[V, tokens, lanes])
        probs = softmax(dot_nt(rows[Q, tokens, lanes], k) * SCALE).astype(BF16)
        acc[:, lanes] += dot(probs, v)

    each_head(head)
    visit("half")
    o[pl.ds(start, TOK)] = pad(acc[...])


FRONT_PLAN = {"start": ((0, 0, 1),), "half": ((O + 1, 1, 2),), "end": ((O + 1, 2, None),)}


def front_kernel(x, w, b, vec, _, qkv, h1, o, att, h2, up, rows, lhs, acc, *sems):
    hosted = Background(Gather(WIDE, None, up, *sems).last_ring(), FRONT_PLAN)
    j = pl.program_id(0)
    at_step(0)(enter)
    hosted.visit("start")

    @at_step(0)
    def _():
        def norm(s, tile, tokens):
            xhat, _ = norm_stats(x[s].astype(F32))
            h1[tile] = pad(xhat * row(vec, G1) + row(vec, C1))

        each_seq(norm)
        lhs[...] = h1[...]

    @pl.when(j >= O)
    def _():
        attention(j - O, rows, o, acc, hosted.visit)
        lhs[...] = o[...]

    @pl.when((j < O) | (j == O + LAST_SEQ))
    def _():
        bias = jnp.where(j < O, b[0], row(vec, BO))

        def product(s, tile, tokens):
            att[tile] = dot(lhs[tile], w[0]) + bias

        each_seq(product)

    @pl.when(j < O)
    def _():
        t = att[...].astype(BF16)
        qkv[0] = t
        rows[j] = t

    @at_step(O + LAST_SEQ)
    def _():
        def norm(s, tile, tokens):
            xhat, _ = norm_stats(x[s].astype(F32) + row(vec, S1) * att[tokens])
            h2[tile] = pad(xhat * row(vec, G2) + row(vec, C2))

        each_seq(norm)

    hosted.visit("end")


def upto(n):
    return lambda j: jnp.minimum(j, n)


def front_call(x, w_attn, b_qkv, vec, up, collective_id):
    return pl.pallas_call(
        front_kernel, grid=(O + PAIR,),
        out_shape=(sds(BF16, O, TT, D), sds(BF16, TT, D), sds(BF16, TT, D), sds(F32, TT, D), sds(BF16, TT, D),
                   sds(BF16, *Gather.shape(WIDE))),
        in_specs=[whole(*SEQS), along(0, 1, D, D, index=upto(O)), along(0, 1, 1, D, index=upto(V)), whole(8, D), ANY],
        out_specs=(along(0, 1, TT, D, index=upto(V)),) + (whole(TT, D),) * SIDE + (ANY,),
        scratch_shapes=[pltpu.VMEM((O, TT, D), BF16), pltpu.VMEM((TT, D), BF16), pltpu.VMEM((SEQ, D), F32)] + Gather.semaphores(),
        input_output_aliases={SIDE: SIDE + 1},
        compiler_params=comm_params(collective_id), name="front",
    )(x, w_attn, b_qkv, vec, up)


def w_out_block():
    return pl.BlockSpec((1, D, D), lambda j: (O, 0, 0), pipeline_mode=pl.Buffered(1))


TILES = FF // HALF
OWN_BODY = BODY * len(SEQ_PAIR)
TAILS = ROWS - TAIL * PAIR * len(SEQ_PAIR)


def put_rows(ref, tail, s, t):
    ref[pl.ds(pl.multiple_of(BODY * s, BODY), BODY)] = t[:BODY]
    ref[pl.ds(pl.multiple_of(tail + TAIL * s, TAIL), TAIL)] = t[BODY:]


DOWN_PLAN = {"start": ((0, 0, 1),), "end": ((TILES + 2, 1, 2), (2 * TILES - 1, 2, None))}


def mlp_in_kernel(h2, gz, w_up, b_up, vec, _, act, slope, d_down, down, a_rows, b_rows, b_away, *sems):
    a_sems, b_sems, sems = sems[:PAIR], sems[PAIR:2 * PAIR], sems[2 * PAIR:]
    hosted = Background(Gather(DOWN, None, down, *sems).last_ring(), DOWN_PLAN)
    j = pl.program_id(0)
    away = Push(b_away, OWN_BODY, b_rows, b_sems, 0)
    tile = lambda n: Push(a_rows.at[n], TAILS, a_rows.at[n], a_sems, n)
    at_step(0)(enter)
    hosted.visit("start")

    @at_step(0)
    def _():
        first = Torus().at["c"] == 0
        def scale(s, tile, tokens):
            d = pad(gz[s].astype(F32) * row(vec, S2))
            left, right = d[:, :HALF], d[:, D - HALF:]
            put_rows(b_rows, TAILS, s, jnp.where(first, left, right))
            put_rows(b_away, OWN_BODY, s, jnp.where(first, right, left))

        each_seq(scale)

    at_step(1)(away.start)
    for n in range(TILES):
        at_step(n + 1)(tile(n).start)

    @pl.when(j < TILES)
    def _():
        u = dot(h2[...], w_up[0]) + b_up[0]
        phi = 0.5 * (1.0 + lax.erf(u * math.sqrt(0.5)))
        slope[...] = phi + u * (jnp.exp(-0.5 * u * u) * math.sqrt(0.5 / math.pi))
        place = lax.rem(lax.broadcasted_iota(jnp.int32, (TT, 1), 0), TOK)
        a = only(place < SEQ, u * phi).astype(BF16)
        act[...] = a
        for s in SEQ_PAIR:
            put_rows(a_rows.at[j], TAILS, s, a[TOK * s:TOK * s + TOK])

    at_step(TILES)(away.wait)
    for n in range(TILES):
        at_step(TILES + n)(tile(n).wait)

    @pl.when(j >= TILES)
    def _():
        d_down[...] = dot_tn(a_rows[j - TILES], b_rows[...])

    hosted.visit("end")

    @at_step(2 * TILES - 1)
    def _():
        away.finish()
        for n in range(TILES):
            tile(n).finish()


def mlp_in_call(h2, gz, w_up, b_up, vec, down, collective_id):
    low = lambda j: jnp.minimum(j, TILES - 1)
    high = lambda j: jnp.maximum(j - TILES, 0)
    return pl.pallas_call(
        mlp_in_kernel, grid=(2 * TILES,),
        out_shape=(sds(BF16, TT, FF), sds(F32, TT, FF), sds(F32, FF, HALF), sds(BF16, *Gather.shape(DOWN))),
        in_specs=[whole(TT, D), whole(*SEQS), up_tile(low), along(0, 1, 1, HALF, index=low), whole(8, D), ANY],
        out_specs=(along(1, TT, HALF, index=low), along(1, TT, HALF, index=low),
                   along(0, HALF, HALF, index=high), ANY),
        scratch_shapes=[pltpu.VMEM((TILES, ROWS, HALF), BF16), pltpu.VMEM((ROWS, HALF), BF16),
                        pltpu.VMEM((PAIR * TOK, HALF), BF16)] + Push.semaphores(TILES) + Push.semaphores(1) +
        Gather.semaphores(),
        input_output_aliases={SIDE + 1: O},
        compiler_params=comm_params(collective_id), name="mlp_in",
    )(h2, gz, w_up, b_up.reshape(TILES, 1, HALF), vec, down)


def up_tile(index=lambda j: j):
    return pl.BlockSpec((1, D, HALF), lambda j: (index(j) // PAIR, 0, index(j) % PAIR))


MLP_PLAN = {"start": ((0, 0, 1),), "end": ((1, 1, 2), (3, 2, 3), (TILES - 1, 3, None))}


def mlp_out_kernel(act, slope, gz, w_up, w_down, vec, part, d_pre, db_up, mlp, d_h2, sums, dm, *scratch):
    first = First(Bands(DOWN), part, sums, *scratch)
    hosted = Background([first.near, first.far, first.relay, first.settle, first.finish], MLP_PLAN)
    at_step(0)(enter)
    hosted.visit("start")

    @at_step(0)
    def _():
        def scale(s, tile, tokens):
            dm[tile] = pad(gz[s].astype(F32) * row(vec, S2))

        each_seq(scale)

    accumulate(mlp, dot(act[...], w_down[...]))
    d = dot_nt(dm[...], w_down[...]) * slope[...]
    db_up[0] = col_sum(d)
    d = d.astype(BF16)
    d_pre[0, 0] = d
    accumulate(d_h2, dot_nt(d, w_up[0]))
    hosted.visit("end")


def mlp_out_call(act, slope, gz, w_up, w_down, vec, part, collective_id):
    return pl.pallas_call(
        mlp_out_kernel, grid=(TILES,),
        out_shape=(sds(BF16, PAIR, SIDE, TT, HALF), sds(F32, TILES, 1, HALF), sds(F32, TT, D), sds(F32, TT, D),
                   Bands(DOWN).sums()),
        in_specs=[along(1, TT, HALF), along(1, TT, HALF), whole(*SEQS), up_tile(), along(0, HALF, D), whole(8, D), ANY],
        out_specs=(pl.BlockSpec((1, 1, TT, HALF), lambda j: (j % PAIR, j // PAIR, 0, 0)), along(0, 1, 1, HALF),
                   whole(TT, D), whole(TT, D), ANY),
        scratch_shapes=[pltpu.VMEM((TT, D), BF16)] + Bands(DOWN).first(),
        compiler_params=comm_params(collective_id), name="mlp_out",
    )(act, slope, gz, w_up, w_down, vec, part)


def halves_of(t):
    t = pad(t)
    return t[:, :HALF], jnp.concatenate([t[:, HALF:], jnp.zeros((TOK, QCOLS - D), BF16)], axis=1)


def mid(mlp, d_h2, att, x, gz, vec, w_out, z, g_res, d_att, d_o, sums):
    a = att[:SEQ]
    y = x[0].astype(F32) + row(vec, S1) * a
    m = mlp[:SEQ] + row(vec, B2)
    g = gz[0].astype(F32)
    z[0] = (y + row(vec, S2) * m).astype(BF16)
    xhat, rstd = norm_stats(y)
    dh = d_h2[:SEQ]
    gr = g + norm_back(xhat, rstd, dh * row(vec, G2))
    g_res[:SEQ] = gr
    da = gr * row(vec, S1)
    terms = (da, gr * a, dh * xhat, dh, g * row(vec, S2), g * m)
    accumulate(sums, jnp.concatenate([jnp.zeros((BO, D), F32)] + [col_sum(t) for t in terms], axis=0))
    for i, t in enumerate(halves_of(da)):
        d_att[i] = t
    d_o[...] = dot_nt(pad(da), w_out[0]).astype(BF16)


def attention_back(s, qkv, d_o, d_qkv, db, acc, b_rows, away, first, visit):
    acc[...] = jnp.zeros_like(acc)

    def head(h):
        lanes, mask = window(h)
        q, k, v = (only(mask, qkv[i, :SEQ, lanes]) for i in (Q, K, V))
        do = only(mask, d_o[:SEQ, lanes])
        scores = dot_nt(k, q) * SCALE
        e = jnp.exp(scores - jnp.max(scores, axis=0, keepdims=True))
        probs = e * (1.0 / col_sum(e))
        acc[V, :, lanes] += dot(probs.astype(BF16), do)
        dp = dot_nt(v, do)
        ds = probs * (dp - col_sum(dp * probs))
        ds = (ds * SCALE).astype(BF16)
        acc[K, :, lanes] += dot(ds, q)
        acc[Q, :, lanes] += dot_tn(ds, k)

    each_head(head)
    visit("half")
    accumulate(db, jnp.concatenate([col_sum(acc[i]) for i in (Q, K, V)], axis=0))
    for n in (Q, K, V):
        left, right = halves_of(acc[n])
        d_qkv[0, n] = left
        d_qkv[1, n] = right
        put_rows(b_rows.at[n], TAILS, s, jnp.where(first, left, right))
        put_rows(away.at[n], OWN_BODY, s, jnp.where(first, right, left))


PER = HALF // STEP


class WideGrads:
    def __init__(self, inputs, a_of, cotangents, out, base, lead, a_rows, a_cols, b_rows):
        self.inputs, self.a_of, self.cotangents, self.out, self.base, self.lead = inputs, a_of, cotangents, out, base, lead
        self.a_rows, self.a_cols, self.b_rows = a_rows, a_cols, b_rows

    @staticmethod
    def scratch(inputs):
        return [pltpu.VMEM((inputs, ROWS, D), BF16), pltpu.VMEM((inputs, D, ROWS), BF16), pltpu.VMEM((SIDE, ROWS, HALF), BF16)]

    def turn(self, i):
        def trip(n, carry):
            lanes = pl.ds(pl.multiple_of(n * LANES, LANES), LANES)
            self.a_cols[i, lanes] = self.a_rows[i, :, lanes].T
            return carry

        lax.fori_loop(0, D // LANES, trip, 0)

    def step(self):
        j = pl.program_id(0)
        done = []
        for t in range(SIDE):
            n = (t + self.lead) % SIDE

            @at_step(self.base + PER * t)
            def _():
                i = self.a_of[n]
                if i not in done:
                    self.inputs[i].wait()
                    self.turn(i)
                    done.append(i)
                self.cotangents[n].wait()

        @pl.when(j >= self.base)
        def _():
            n = lax.rem(lax.div(j - self.base, PER) + self.lead, SIDE)
            cols = pl.ds(pl.multiple_of(lax.rem(j - self.base, PER) * STEP, STEP), STEP)
            i = 0 if len(self.inputs) == 1 else lax.div(n, O)
            self.out[0] = dot(self.a_cols[i], self.b_rows[n, :, cols])

    def finish(self):
        for move in (*self.inputs, *self.cotangents):
            move.finish()


def grads_block(base, lead):
    def index(j):
        n = jnp.maximum(j - base, 0)
        return (n // PER + lead) % SIDE, 0, n % PER

    return pl.BlockSpec((1, D, STEP), index)


GRAD_STEPS = PER * SIDE


def tok_block():
    return along(0, TOK, D, index=upto(LAST_SEQ))


def seq_block():
    return along(0, 1, SEQ, D, index=upto(LAST_SEQ))


MID_PLAN = {"start": ((0, 0, 1),), "end": ((1, 1, 3), (8, 3, 4), (11, 4, 5), (LAST_SEQ + GRAD_STEPS, 5, None))}


def mid_kernel(*refs):
    refs = list(refs)
    take = lambda n: [refs.pop(0) for _ in range(n)]
    ins, (h2, d_pre, acc), outs, (d_up, result) = take(7), take(3), take(5), take(2)
    rows, a_sems, b_sems = take(3), take(C), take(C)
    rest = Rest(Bands(DOWN), acc, result, *refs)
    hosted = Background([rest.begin, rest.loaded, rest.relay, rest.settle, rest.relay_third, rest.settle_third, rest.finish],
                        MID_PLAN)
    c = Torus().at["c"]
    grads = WideGrads(
        [Exchange(h2, h2, rows[0].at[0], a_sems, ())], (0,) * SIDE,
        [Exchange(d_pre.at[c, n], d_pre.at[1 - c, n], rows[2].at[n], b_sems, (n,)) for n in range(SIDE)], d_up, SEQS[0], 0, *rows)
    at_step(0)(enter)
    hosted.visit("start")

    @at_step(0)
    def _():
        for move in (*grads.inputs, *grads.cotangents):
            move.start()

    pl.when(pl.program_id(0) < SEQS[0])(lambda: mid(*ins, *outs))
    grads.step()
    hosted.visit("end")
    at_step(LAST_SEQ + GRAD_STEPS)(grads.finish)


def mid_call(mlp, d_h2, att, x, gz, vec, w_attn, h2, d_pre, acc, collective_id):
    return pl.pallas_call(
        mid_kernel, grid=(SEQS[0] + GRAD_STEPS,),
        out_shape=(sds(BF16, *SEQS), sds(F32, TT, D), sds(BF16, PAIR, TT, HALF), sds(BF16, TT, D), sds(F32, 8, D),
                   sds(F32, SIDE, D, HALF), Bands(DOWN).result()),
        in_specs=[tok_block()] * O + [seq_block()] * PAIR + [whole(8, D), w_out_block()] + [ANY] * O,
        out_specs=(seq_block(), tok_block(), along(1, PAIR, TOK, HALF, index=upto(LAST_SEQ)), tok_block(), whole(8, D),
                   grads_block(SEQS[0], 0), ANY),
        scratch_shapes=WideGrads.scratch(1) + Exchange.semaphores() + Exchange.semaphores(SIDE) +
        Bands(DOWN).later(),
        compiler_params=comm_params(collective_id), name="mid",
    )(mlp, d_h2, att, x, gz, vec, w_attn, h2, d_pre, acc)


ATTN_PLAN = {"start": ((0, 0, 2),), "half": ((0, 2, 4),), "end": ((SIDE, 4, 5), (LAST_SEQ + GRAD_STEPS, 5, None))}


def attn_back_kernel(*refs):
    refs = list(refs)
    take = lambda n: [refs.pop(0) for _ in range(n)]
    (qkv, d_o), (h1, o, d_att, part, result), (d_qkv, db, d_attn, sums, total) = take(2), take(5), take(5)
    acc, away, rows = refs.pop(0), refs.pop(0), take(3)
    a_sems, b_sems, away_sems = take(C), take(C), take(PAIR)
    first = First(Bands(WIDE), part, sums, *take(len(Bands(WIDE).first())))
    spread = Spread(Bands(DOWN), result, total, *refs)
    hosted = Background([spread.begin, first.near, first.far, spread.forward, first.relay, first.settle, first.finish,
                         spread.finish], ATTN_PLAN)
    c = Torus().at["c"]
    pushes = [Push(away.at[n], OWN_BODY, rows[2].at[n], away_sems, n) for n in range(O)]
    grads = WideGrads(
        [Exchange(a, a, rows[0].at[i], a_sems, (i,)) for i, a in enumerate((h1, o))], (0,) * O + (1,),
        pushes + [Exchange(d_att.at[c], d_att.at[1 - c], rows[2].at[O], b_sems, ())], d_attn, SEQS[0], O, *rows)
    at_step(0)(enter)
    hosted.visit("start")

    @at_step(0)
    def _():
        for move in (*grads.inputs, grads.cotangents[O]):
            move.start()

    @at_step(SEQS[0])
    def _():
        for push in pushes:
            push.start()

    j = pl.program_id(0)
    pl.when(j < SEQS[0])(lambda: attention_back(j, qkv, d_o, d_qkv, db, acc, rows[2], away, c == 0, hosted.visit))

    grads.step()
    hosted.visit("end")
    at_step(LAST_SEQ + GRAD_STEPS)(grads.finish)


def attn_back_call(qkv, d_o, h1, o, d_att, part, result, collective_id):
    return pl.pallas_call(
        attn_back_kernel, grid=(SEQS[0] + GRAD_STEPS,),
        out_shape=(sds(BF16, PAIR, O, TT, HALF), sds(F32, O, D), sds(F32, SIDE, D, HALF), Bands(WIDE).sums(),
                   Bands(DOWN).total()),
        in_specs=[along(1, O, TOK, D, index=upto(LAST_SEQ)), tok_block()] + [ANY] * 5,
        out_specs=(along(2, PAIR, O, TOK, HALF, index=upto(LAST_SEQ)), whole(O, D), grads_block(SEQS[0], O), ANY, ANY),
        scratch_shapes=[pltpu.VMEM((O, SEQ, D), F32), pltpu.VMEM((O, PAIR * TOK, HALF), BF16)] + WideGrads.scratch(2) +
        Exchange.semaphores(PAIR) + Exchange.semaphores() + Push.semaphores(O) + Bands(WIDE).first() + Spread.scratch(),
        compiler_params=comm_params(collective_id), name="attn_back",
    )(qkv, d_o, h1, o, d_att, part, result)


IN_STEPS = PAIR * O
SLOT = 40
LAST_PLAN = {"start": ((0, 0, 2),), "end": ((O, 2, None),)}


CORE_COLS = D - HALF
KEPT = 48
GRADS = ((KEPT, O * D), (KEPT, D), (KEPT, FF), (PAIR, C, UNIT, D), (SIDE, KEPT, LANES))
SHARES = PAIR * SIDE + SIDE + PAIR


def split_rows(totals, first, keep, give):
    for x in range(SIDE):
        for total, bands in totals:
            rows = jnp.concatenate([total[x, k, :n] for k, (_, n) in enumerate(BANDS[WIDE])], axis=0)
            low, high = rows[:KEPT], jnp.concatenate([rows[OWN:], rows[:KEPT - OWN]], axis=0)
            keep[x, :, bands.cols] = jnp.where(first, low, high)
            give[x, :, bands.cols] = jnp.where(first, high, low)


class Finals:
    def __init__(self, down, up, attn, outs, sems):
        self.c = Torus().at["c"]
        self.down, self.up, self.attn, self.sems = down, up, attn, sems
        self.qkv, self.out, self.up_out, self.down_out, self.pad = outs
        self.edge = pl.ds(CORE_COLS, LANES)

    def cols(self, base, width):
        return pl.ds(pl.multiple_of(base + self.c * HALF, LANES), width)

    def up_share(self, x):
        place = self.up_out.at[:, self.cols(QCOLS * x, HALF)]
        return Share(*(ref.at[x] for ref in self.up), place, self.sems, x)

    def block(self, x):
        return (self.out, 0) if x == O else (self.qkv, D * x)

    def attn_share(self, x):
        out, base = self.block(x)
        sides = (ref.at[x, :, pl.ds(0, CORE_COLS)] for ref in self.attn)
        return Share(*sides, out.at[:, self.cols(base, CORE_COLS)], self.sems, SIDE + x)

    def edge_share(self, x, padding):
        out, base = self.block(x)
        place = self.pad.at[x] if padding else out.at[:, pl.ds(base + CORE_COLS, LANES)]
        return Share(*(ref.at[x, :, self.edge] for ref in self.attn), place, self.sems, PAIR * SIDE + x)

    def down_share(self, edge):
        src = self.edge if edge else pl.ds(pl.multiple_of(self.c * LANES, LANES), CORE_COLS)
        sides = (self.down.at[pl.ds(PAIR * c, PAIR), :, :, src] for c in (self.c, 1 - self.c))
        place = self.down_out.at[:, :, :, self.edge if edge else self.cols(0, CORE_COLS)]
        return Share(*sides, place, self.sems, SHARES - PAIR + edge)

    def start_down(self):
        self.down_share(0).start()
        pl.when(self.c == 0)(lambda: self.down_share(1).start())

    def start(self):
        for x in range(SIDE):
            self.attn_share(x).start()
            pl.when(self.c == 0)(lambda: self.edge_share(x, False).start())
            pl.when(self.c == 1)(lambda: self.edge_share(x, True).start())

    def finish(self):
        for x in range(SIDE):
            for share in (self.up_share(x), self.attn_share(x), self.edge_share(x, True)):
                share.wait()
        self.down_share(0).wait()
        pl.when(self.c == 0)(lambda: self.down_share(1).sent())
        pl.when(self.c == 1)(lambda: self.down_share(1).far.wait_recv())


def last_kernel(*refs):
    refs = list(refs)
    take = lambda n: [refs.pop(0) for _ in range(n)]
    (d_half, w, x, g_res, vec), (small, acc_up, down, _), (dx, part), outs = take(5), take(SIDE), take(PAIR), take(len(GRADS))
    (acc, sums, pair_sums, block), (totals, sides), block_sem, swap_sems = take(4), (take(C), take(SIDE)), refs.pop(0), take(PAIR)
    finals = Finals(down, sides[:PAIR], sides[PAIR:], outs, take(C))
    halves = [Bands(WIDE, h) for h in WAYS]
    a, b = (First(bands, part, None, *take(len(bands.first()))) for bands in halves)
    rest_a, rest_b = (Rest(f.bands, f.own_all, None, f.own_all, *take(len(f.bands.later()) - 1)) for f in (a, b))
    rest_up = Rest(Bands(WIDE), acc_up, None, *take(len(Bands(WIDE).later())))
    spread_up, spread_a, spread_b = (
        Spread(r.bands, r.sums(), total, *take(PAIR), None) for r, total in zip((rest_up, rest_a, rest_b), totals))
    hosted = Background([rest_up.begin, a.near, rest_up.loaded, rest_up.relay], LAST_PLAN)
    first = finals.c == 0
    swap = remote(sums, pair_sums, swap_sems, (), Torus().partner())
    fetch = pltpu.make_async_copy(small, block, block_sem)
    at_step(0)(enter)
    hosted.visit("start")

    @at_step(0)
    def _():
        fetch.start()
        finals.start_down()

    @pl.when(pl.program_id(0) < IN_STEPS)
    def _():
        each_seq(lambda s, tile, tokens: accumulate(acc.at[tile], dot_nt(d_half[0, 0, tile], w[0])))

    @at_step(IN_STEPS - 1)
    def _():
        sums[...] = jnp.zeros_like(sums)

        def back(s, tile, tokens):
            xhat, rstd = norm_stats(x[s].astype(F32))
            dh = acc[tokens]
            sums[:BO] += jnp.concatenate([col_sum(dh * xhat), col_sum(dh)], axis=0)
            dx[s] = (g_res[tokens] + norm_back(xhat, rstd, dh * row(vec, G1))).astype(BF16)

        each_seq(back)

    hosted.visit("end")

    @at_step(IN_STEPS)
    def _():
        swap.start()
        fetch.wait()
        swap.wait()
        both = sums[...] + pair_sums[...]
        for d in range(DEVICES):
            at = CHIP * (d // PAIR) + SLOT + OWN * (d % PAIR)
            block[at:at + BO, :OWN] = both[:BO, OWN * d:OWN * d + OWN]

        @pl.when(finals.c == 1)
        def _():
            for z in range(SIDE):
                for y in range(SIDE):
                    rows = block.at[pl.ds(CHIP * (SIDE * z + y), CHIP)]
                    put = pltpu.make_async_copy(rows, part.at[0, z, y, :, pl.ds(CORE_COLS, LANES)], block_sem)
                    put.start()
            pltpu.make_async_copy(block, small, block_sem).wait()

        def share_up():
            spread_up.finish()
            split_rows([(totals[0], Bands(WIDE))], first, *sides[:PAIR])
            for x in range(SIDE):
                finals.up_share(x).start()

        for step in (b.near, rest_up.settle, a.far, rest_up.relay_third, b.far, a.relay, rest_up.settle_third, spread_up.begin,
                     b.relay, spread_up.forward, functools.partial(a.settle, rest_a.send),
                     functools.partial(b.settle, rest_b.send), rest_a.relay, rest_b.relay, rest_a.settle, rest_b.settle,
                     share_up, rest_a.relay_third, rest_b.relay_third, rest_a.settle_third, spread_a.begin,
                     rest_b.settle_third, spread_b.begin, spread_a.forward, spread_b.forward, spread_a.finish, spread_b.finish):
            step()
        split_rows(list(zip(totals[1:], halves)), first, *sides[PAIR:])
        finals.start()
        for user in (rest_up, rest_a, rest_b, a, b, finals):
            user.finish()


def last_call(d_qkv, w_attn, x, g_res, vec, small, acc_up, down, part, collective_id):
    low = upto(IN_STEPS - 1)
    halves = [Bands(WIDE, h) for h in WAYS]
    dma = pltpu.SemaphoreType.DMA
    rings = [Bands(WIDE), *halves]
    return pl.pallas_call(
        last_kernel, grid=(IN_STEPS + 1,),
        out_shape=(sds(BF16, *SEQS), sds(F32, *part.shape), *(sds(F32, *shape) for shape in GRADS)),
        in_specs=[pl.BlockSpec((1, 1, TT, HALF), lambda j: (low(j) % PAIR, low(j) // PAIR, 0, 0)), up_tile(low),
                  whole(*SEQS), whole(TT, D), whole(8, D)] + [ANY] * SIDE,
        out_specs=(whole(*SEQS),) + (ANY,) * (len(GRADS) + 1),
        scratch_shapes=[pltpu.VMEM((TT, D), F32), pltpu.VMEM((SUB, D), F32), pltpu.VMEM((SUB, D), F32),
                        pltpu.VMEM((D, LANES), F32)] + [r.vmem(SIDE, C) for r in rings] +
        [pltpu.VMEM((SIDE, KEPT, HALF), F32)] * SIDE + [dma, dma, dma] + [dma((SHARES,))] * C + halves[0].first() * PAIR +
        halves[0].later()[1:] * PAIR + Bands(WIDE).later() + Spread.scratch()[:PAIR] * C,
        input_output_aliases={8: 1},
        compiler_params=comm_params(collective_id), name="last",
    )(d_qkv, w_attn, x, g_res, vec, small, acc_up, down, part)


BQ, BU, VEC = 3 * D // 32, 3 * D // 32 + FF // 32, 3 * D // 32 + FF // 32 + 8 * OWN


def pair_swap(a):
    return lax.ppermute(a, "fsdp", [(i, i ^ 1) for i in range(DEVICES)])


def by_core(first, a, b):
    return jnp.where(first, a, b), jnp.where(first, b, a)


def my_pieces(shards, first):
    w_qkv, b_qkv, w_out, w_up, b_up, w_down, vec_params = shards
    x = lax.axis_index("rep")
    small = jnp.concatenate([b_qkv, b_up, vec_params.reshape(-1)])
    small = jnp.pad(small, (0, OWN * LANES - VEC)).reshape(OWN, LANES)
    attn = lax.dynamic_slice_in_dim(jnp.concatenate([w_qkv, w_out], axis=1), x * D, D, 1)
    attn = jnp.concatenate([attn, small], axis=1)
    up = lax.dynamic_slice_in_dim(w_up, x * QCOLS, QCOLS, 1)
    wide = jnp.stack([attn, up]).astype(BF16)
    mine, theirs = by_core(first, wide[..., :HALF], wide[..., HALF:])
    theirs = pair_swap(theirs)
    piece = jnp.concatenate(by_core(first, mine, theirs), axis=1)
    down = lax.dynamic_slice_in_dim(w_down, x * 48, 48, 0).astype(BF16).reshape(3, 16, D)
    return piece[0], piece[1], down


def small_params(w_attn):
    small = w_attn[0, :, D:].astype(F32).reshape(DEVICES, OWN * LANES)
    vec = small[:, BU:VEC].reshape(DEVICES, 8, OWN).transpose(1, 0, 2).reshape(8, D)
    return small[:, :BQ].reshape(O, 1, D), small[:, BQ:BU].reshape(FF), vec


ROOM = 5 * LANES


def small_grads(db_qkv, db_up, sums):
    vec = sums[BO:].reshape(8 - BO, DEVICES, OWN).transpose(1, 0, 2).reshape(DEVICES, VEC - BU - BO * OWN)
    small = jnp.concatenate([db_qkv.reshape(DEVICES, BQ), db_up.reshape(DEVICES, BU - BQ), vec], axis=1)
    small = small + pair_swap(small)
    small = jnp.pad(small, ((0, 0), (0, ROOM - small.shape[1]))).reshape(DEVICES, ROOM // LANES, LANES)
    return jnp.pad(small, ((0, 0), (0, OWN - ROOM // LANES), (0, 0))).reshape(D, LANES)


def device_step(x, gz, *shards):
    first = lax.rem(lax.axis_index("fsdp"), PAIR) == 0
    attn, up, down = my_pieces(shards, first)
    w_attn, up, down = gather_call(attn, up, down, 0)
    w_attn = w_attn.reshape(SIDE, D, QCOLS)
    b_qkv, b_up, vec = small_params(w_attn)
    qkv, h1, o, att, h2, w_up = front_call(x, w_attn, b_qkv, vec, up, 1)
    w_up = w_up.reshape(SIDE, D, QCOLS)
    act, slope, part, w_down = mlp_in_call(h2, gz, w_up, b_up, vec, down, 2)
    part = part.reshape((SIDE,) * 3 + (C * UNIT, HALF))
    d_pre, db_up, mlp, d_h2, acc = mlp_out_call(act, slope, gz, w_up, w_down.reshape(FF, D), vec, part, 3)
    z, g_res, d_att, d_o, sums, part, result = mid_call(mlp, d_h2, att, x, gz, vec, w_attn, h2, d_pre, acc, 4)
    part = part.reshape((SIDE,) * 3 + (CHIP, HALF))
    d_qkv, db_qkv, part, acc, down = attn_back_call(qkv, d_o, h1, o, d_att, part, result, 5)
    small = small_grads(db_qkv, db_up, sums)
    part = part.reshape((SIDE,) * 3 + (CHIP, HALF))
    dx, _, g_qkv, g_out, g_up, g_down, edge = last_call(d_qkv, w_attn, x, g_res, vec, small, acc, down, part, 6)
    small = edge[0, :ROOM // LANES].reshape(ROOM)
    vec = jnp.concatenate([edge[0, SLOT:SLOT + BO, :OWN], small[BU:VEC - BO * OWN].reshape(8 - BO, OWN)], axis=0)
    g_qkv, g_out, g_up = (g[:OWN] for g in (g_qkv, g_out, g_up))
    return z, dx, g_qkv, small[:BQ], g_out, g_up, small[BQ:BU], g_down.reshape(FF // DEVICES, D), vec


def solution(mesh):
    batch = P(("rep", "fsdp"), None, None)
    rows, flat, cols = P("fsdp", None), P("fsdp"), P(None, "fsdp")
    shards = (rows, flat, rows, rows, flat, rows, cols)
    return jax.shard_map(device_step, mesh=mesh, in_specs=(batch, batch) + shards,
                         out_specs=(batch, batch) + shards, check_vma=False)
```

```python
import functools
import math

import jax
import jax.numpy as jnp
from jax import lax
from jax.experimental import pallas as pl
from jax.experimental.pallas import tpu as pltpu
from jax.sharding import PartitionSpec as P

HEADS = 16
LN_EPS = 1e-5
D = 1408
FF = 6144
SEQ = 257
HEAD = D // HEADS
SCALE = HEAD ** -0.5
QCOLS = 1536
HALF = 768
OWN = 44
CHIP = 2 * OWN
LANES = 128
DEVICES = 32
F32 = jnp.float32
BF16 = jnp.bfloat16
VMEM_LIMIT = 66 * 1000 * 1000
G1, C1, BO, S1, G2, C2, B2, S2 = range(8)
Q, K, V, O = range(4)
SEQS = (2, SEQ, D)
LAST_SEQ = SEQS[0] - 1
SEQ_PAIR = range(SEQS[0])
TAIL = 16
BODY = SEQ - 1
TOK = BODY + TAIL
TT = 2 * TOK
ROWS = 4 * TOK
STEP = 256


def sds(dtype, *shape):
    return jax.ShapeDtypeStruct(shape, dtype)


MESH_ID = pl.DeviceIdType.MESH
SIDE = 4
SUB = 8
PAIR = 2
C = 3
COLOURS = range(C)
COLOUR_DIMS = ("xyz", "yzx", "zxy")
FIRST, SECOND, THIRD, LAST = range(4)
WAYS = range(PAIR)
NEAR, FAR, ADDED = 0, 2, 4
WIDE, DOWN = "wide", "down"
ANY = pl.BlockSpec(memory_space=pl.ANY)
ALL = slice(None)


def duo(m):
    return pl.ds(PAIR * m, PAIR)


def toward(m):
    return 1 - PAIR * (m % PAIR)


class Torus:
    def __init__(self):
        f = lax.axis_index("fsdp")
        self.at = {"x": lax.axis_index("rep"), "z": lax.div(f, SIDE * PAIR), "y": lax.rem(lax.div(f, PAIR), SIDE),
                   "c": lax.rem(f, PAIR)}

    def shift(self, dim, by):
        return lax.rem(self.at[dim] + (SIDE + by), SIDE)

    def device(self, **moved):
        p = {**self.at, **moved}
        return (p["x"], (p["z"] * SIDE + p["y"]) * PAIR + p["c"])

    def neighbour(self, dim, by):
        return self.device(**{dim: self.shift(dim, by)})

    def partner(self):
        return self.device(c=1 - self.at["c"])


def enter():
    me = Torus()
    barrier = pltpu.get_barrier_semaphore()
    others = [me.neighbour(d, toward(m)) for d in COLOUR_DIMS[0] for m in WAYS] + [me.partner()]
    for other in others:
        pl.semaphore_signal(barrier, device_id=other, device_id_type=MESH_ID)
    pl.semaphore_wait(barrier, len(others))


def remote(src, dst, sems, slot, device):
    return pltpu.make_async_remote_copy(src_ref=src, dst_ref=dst, send_sem=sems[0].at[slot], recv_sem=sems[1].at[slot],
                                        device_id=device, device_id_type=MESH_ID)


class Gather:
    def __init__(self, kind, src, dst, hop_send, hop_recv, push_send, push_recv, local):
        self.kind, self.src, self.dst, self.local = kind, src, dst, local
        self.hops, self.pushes = (hop_send, hop_recv), (push_send, push_recv)
        self.cols, self.cut = (256, 128) if kind == WIDE else (D, HALF)

    @staticmethod
    def semaphores():
        dma = pltpu.SemaphoreType.DMA
        return [dma((C, C, ADDED))] * PAIR + [dma((C, ADDED + 1))] * PAIR + [dma((C,))]

    @staticmethod
    def shape(kind):
        return (SIDE,) * 3 + (CHIP, QCOLS) if kind == WIDE else (SIDE, SIDE, PAIR, SIDE, C, 16, D)

    def source(self, k):
        return self.src.at[:, pl.ds(self.cols * k, self.cols)] if self.kind == WIDE else self.src.at[k]

    def piece(self, me, k, s, v, half=None):
        dims = COLOUR_DIMS[k]
        at = {**me.at, **{d: ALL for d in dims[:s]}, dims[s]: v}
        off, width = 0, self.cols
        if half is not None and s == FIRST:
            off, width = self.cut * half, (self.cut, self.cols - self.cut)[half]
        elif half is not None:
            at[dims[0]] = duo(half)
        if self.kind == WIDE:
            cols = pl.ds(pl.multiple_of(at["c"] * HALF + self.cols * k + off, 128), width)
            return self.dst.at[at["x"], at["z"], at["y"], :, cols]
        return self.dst.at[at["z"], at["y"], at["c"], at["x"], k, :, pl.ds(off, width)]

    def hop(self, k, s, m):
        me = Torus()
        dim = COLOUR_DIMS[k][s]
        by = toward(m)
        if m < FAR:
            ref = self.piece(me, k, s, me.at[dim])
        else:
            ref = self.piece(me, k, s, me.shift(dim, -by), m - FAR)
        src = self.source(k) if s == FIRST and m < FAR else ref
        return remote(src, ref, self.hops, (k, s, m), me.neighbour(dim, by))

    def push(self, k, n):
        me = Torus()
        dim = COLOUR_DIMS[k][THIRD]
        if n < FAR:
            ref = self.piece(me, k, THIRD, me.shift(dim, -toward(n)))
        elif n < ADDED:
            ref = self.piece(me, k, THIRD, me.shift(dim, FAR), n - FAR)
        else:
            ref = self.piece(me, k, THIRD, me.at[dim])
        return remote(ref, ref, self.pushes, (k, n), me.partner())

    def own(self, k):
        me = Torus()
        return pltpu.make_async_copy(self.source(k), self.piece(me, k, FIRST, me.at[COLOUR_DIMS[k][FIRST]]), self.local.at[k])

    def launch(self, s):
        for k in COLOURS:
            for m in WAYS:
                self.hop(k, s, m).start()
            if s == THIRD:
                self.push(k, ADDED).start()

    def relay(self, s):
        for k in COLOURS:
            for m in WAYS:
                self.hop(k, s, m).wait_recv()
                self.hop(k, s, FAR + m).start()
                if s == THIRD:
                    self.push(k, m).start()

    def settle(self, s):
        for k in COLOURS:
            for m in WAYS:
                self.hop(k, s, FAR + m).wait_recv()
                if s == THIRD:
                    self.push(k, FAR + m).start()
            if s == FIRST:
                self.own(k).wait()

    def begin(self):
        for k in COLOURS:
            self.own(k).start()
        self.launch(FIRST)

    def sent(self, *rings):
        for k in COLOURS:
            for s in rings:
                for m in range(ADDED):
                    self.hop(k, s, m).wait_send()
            if THIRD in rings:
                for n in range(ADDED + 1):
                    self.push(k, n).wait()

    def last_ring(self):
        return [functools.partial(f, THIRD) for f in (self.launch, self.relay, self.settle, self.sent)]


def add_into(total, *others):
    lead = total.shape[:-2]

    def body(i, carry):
        idx = []
        for n in reversed(lead):
            idx.insert(0, lax.rem(i, n))
            i = lax.div(i, n)
        value = total[tuple(idx)]
        for other in others:
            value = value + other[tuple(idx)]
        total[tuple(idx)] = value
        return carry

    lax.fori_loop(0, math.prod(lead), body, 0)


class Ring:
    def __init__(self, s, bands, terms, passed, relay, landing, send, recv):
        self.s, self.bands, self.terms, self.passed, self.relay, self.landing = s, bands, terms, passed, relay, landing
        self.sems = (send, recv)

    def zone(self, k, way, half):
        if self.s == THIRD:
            return self.landing.at[k, way, self.bands.cuts(k)[half]]
        return self.bands.rows(self.landing.at[k, way, duo(half)], k)

    def carried(self, ref, k, way):
        if self.s == THIRD:
            return ref.at[k, way, pl.ds(0, self.bands.cuts(k)[way].size)]
        return self.bands.rows(ref.at[k, way], k)

    def hop(self, k, m):
        me = Torus()
        dim = COLOUR_DIMS[k][self.s]
        way, by = m % PAIR, toward(m)
        if m < FAR:
            src, dst = self.terms(k, me.shift(dim, FAR), way), self.carried(self.relay, k, way)
        elif m < ADDED:
            src, dst = self.terms(k, me.shift(dim, by), 1 - way), self.zone(k, way, 1 - way)
        else:
            src, dst = self.carried(self.passed, k, way), self.zone(k, way, way)
        return remote(src, dst, self.sems, (k, m), me.neighbour(dim, by))

    def start(self, k, base):
        for m in WAYS:
            self.hop(k, base + m).start()

    def arrived(self, k, base):
        for m in WAYS:
            self.hop(k, base + m).wait_recv()

    def finish(self):
        for k in COLOURS:
            for m in range(ADDED + PAIR):
                self.hop(k, m).wait_send()

    @staticmethod
    def semaphores():
        return [pltpu.SemaphoreType.DMA((C, ADDED + PAIR))] * PAIR


UNIT = 32
BANDS = {WIDE: ((0, 24), (24, UNIT), (56, UNIT)), DOWN: ((0, UNIT), (UNIT, UNIT), (2 * UNIT, UNIT))}
ORDERS = {WIDE: "xzy", DOWN: "zyx"}


class Bands:
    def __init__(self, kind, half=None):
        self.order, self.bands = ORDERS[kind], BANDS[kind]
        self.width = HALF if half is None else HALF // PAIR
        self.cols = pl.ds(self.width * (half or 0), self.width)

    def band(self, k):
        return pl.ds(*self.bands[k])

    def rows(self, ref, k):
        return ref.at[(ALL,) * (len(ref.shape) - PAIR) + (pl.ds(0, self.bands[k][1]),)]

    def cuts(self, k):
        rows = self.bands[k][1]
        cut = (rows // SUB + 1) // PAIR * SUB
        return pl.ds(0, cut), pl.ds(cut, rows - cut)

    def rest(self, k):
        return [d for d in self.order if d != COLOUR_DIMS[k][FIRST]]

    def units(self, *lead):
        return lead + (UNIT, self.width)

    def vmem(self, *lead):
        return pltpu.VMEM(self.units(*lead), F32)

    def sums(self):
        return sds(F32, *self.units(C, SIDE, SIDE))

    def result(self):
        return sds(F32, *self.units(C))

    def total(self):
        return sds(F32, *self.units(SIDE, C))

    def first(self):
        relays = [self.vmem(C, PAIR, PAIR, SIDE)] * PAIR
        dma = pltpu.SemaphoreType.DMA
        return [self.vmem(C, SIDE, SIDE), *relays, self.vmem(C, PAIR, SIDE, SIDE), *Ring.semaphores(), dma((C, C)), dma((C,))]

    def later(self):
        dma = pltpu.SemaphoreType.DMA
        return [self.vmem(C, SIDE, SIDE), self.vmem(C, PAIR, PAIR), self.vmem(C, PAIR, SIDE),
                pltpu.VMEM((C, PAIR, UNIT // PAIR, self.width), F32), self.vmem(C, PAIR),
                *Ring.semaphores(), *Ring.semaphores(), dma((C,)), dma((C,))]


class First:
    def __init__(self, bands, part, acc, own, passed, relay, landing, send, recv, load, store):
        self.bands, self.part, self.acc, self.own_all, self.passed = bands, part, acc, own, passed
        self.relay_in, self.landing, self.load_sem, self.store_sem = relay, landing, load, store
        self.ring = Ring(FIRST, bands, self.terms, passed, relay, landing, send, recv)

    def own(self, k):
        return self.bands.rows(self.own_all.at[k], k)

    def terms(self, k, v, half=None):
        b = self.bands
        at = {d: ALL for d in b.order}
        at[COLOUR_DIMS[k][FIRST]] = v
        if half is not None:
            at[b.rest(k)[0]] = duo(half)
        return self.part.at[tuple(at[d] for d in b.order) + (b.band(k), b.cols)]

    def load(self, k, m):
        me = Torus()
        dim = COLOUR_DIMS[k][FIRST]
        if m in WAYS:
            src, dst = self.terms(k, me.shift(dim, toward(m)), m), self.ring.carried(self.passed, k, m)
        else:
            src, dst = self.terms(k, me.at[dim]), self.own(k)
        return pltpu.make_async_copy(src, dst, self.load_sem.at[k, m])

    def store(self, k):
        return pltpu.make_async_copy(self.own(k), self.bands.rows(self.acc.at[k], k), self.store_sem.at[k])

    def near(self):
        for k in COLOURS:
            self.ring.start(k, NEAR)

    def far(self):
        for k in COLOURS:
            self.ring.start(k, FAR)
        for m in COLOURS:
            for k in COLOURS:
                self.load(k, m).start()

    def relay(self):
        for k in COLOURS:
            self.ring.arrived(k, NEAR)
            for m in WAYS:
                self.load(k, m).wait()
                add_into(self.ring.carried(self.passed, k, m), self.ring.carried(self.relay_in, k, m))
            self.ring.start(k, ADDED)

    def settle(self, then=None):
        for k in COLOURS:
            self.load(k, FAR).wait()
            for base in (FAR, ADDED):
                self.ring.arrived(k, base)
            add_into(self.own(k), *(self.bands.rows(self.landing.at[k, m], k) for m in WAYS))
            if then is None:
                self.store(k).start()
            else:
                then(k)

    def finish(self):
        self.ring.finish()
        if self.acc is not None:
            for k in COLOURS:
                self.store(k).wait()


class Rest:
    def __init__(self, bands, acc, result, own, relay2, in2, relay3, in3, *sems):
        self.bands, self.acc, self.own, self.result = bands, acc, own, result
        self.in2, self.in3, self.relay2, self.relay3, self.load_sem, self.store_sem = in2, in3, relay2, relay3, *sems[-2:]
        self.second = Ring(SECOND, bands, functools.partial(self.terms, acc), relay2, relay2, in2, *sems[:PAIR])
        self.third = Ring(THIRD, bands, self.final, relay3, relay3, in3, *sems[PAIR:2 * PAIR])

    def terms(self, ref, k, v, half=None):
        other = ALL if half is None else duo(half)
        first = self.bands.rest(k)[0] == COLOUR_DIMS[k][SECOND]
        return self.bands.rows(ref.at[(k, v, other) if first else (k, other, v)], k)

    def final(self, k, v, half=None):
        if half is None:
            return self.bands.rows(self.in2.at[k, 0, v], k)
        return self.in2.at[k, 0, v, self.bands.cuts(k)[half]]

    def load(self, k):
        return pltpu.make_async_copy(self.bands.rows(self.acc.at[k], k), self.bands.rows(self.own.at[k], k), self.load_sem.at[k])

    def store(self, k):
        rows = self.bands.rows
        return pltpu.make_async_copy(rows(self.in3.at[k, 0], k), rows(self.result.at[k], k), self.store_sem.at[k])

    def send(self, k):
        for base in (NEAR, FAR):
            self.second.start(k, base)

    def begin(self):
        for k in COLOURS:
            self.send(k)
        for k in COLOURS:
            self.load(k).start()

    def loaded(self):
        for k in COLOURS:
            self.load(k).wait()

    def relay(self):
        me = Torus()
        for k in COLOURS:
            self.second.arrived(k, NEAR)
            for m in WAYS:
                terms = self.terms(self.own, k, me.shift(COLOUR_DIMS[k][SECOND], toward(m)), m)
                add_into(self.second.carried(self.relay2, k, m), terms)
            self.second.start(k, ADDED)

    def settle(self):
        me = Torus()
        for k in COLOURS:
            for base in (FAR, ADDED):
                self.second.arrived(k, base)
            plus, minus = (self.bands.rows(self.in2.at[k, m], k) for m in WAYS)
            add_into(plus, minus, self.terms(self.own, k, me.at[COLOUR_DIMS[k][SECOND]]))
            for base in (NEAR, FAR):
                self.third.start(k, base)

    def relay_third(self):
        me = Torus()
        for k in COLOURS:
            self.third.arrived(k, NEAR)
            for m in WAYS:
                mine = self.third.carried(self.relay3, k, m)
                mine[...] += self.final(k, me.shift(COLOUR_DIMS[k][THIRD], toward(m)), m)[...]
            self.third.start(k, ADDED)

    def settle_third(self):
        me = Torus()
        for k in COLOURS:
            for base in (FAR, ADDED):
                self.third.arrived(k, base)
            plus, minus = (self.bands.rows(self.in3.at[k, m], k) for m in WAYS)
            plus[...] += minus[...] + self.final(k, me.at[COLOUR_DIMS[k][THIRD]])[...]
            if self.result is not None:
                self.store(k).start()

    def finish(self):
        self.second.finish()
        self.third.finish()
        if self.result is not None:
            for k in COLOURS:
                self.store(k).wait()

    def sums(self):
        return self.in3.at[:, 0]


class Spread:
    def __init__(self, bands, result, total, send, recv, local):
        self.bands, self.result, self.total, self.sems, self.local = bands, result, total, (send, recv), local

    @staticmethod
    def scratch():
        return [pltpu.SemaphoreType.DMA((C, ADDED))] * PAIR + [pltpu.SemaphoreType.DMA((C,))]

    def mine(self, k):
        return self.bands.rows(self.result.at[k], k)

    def place(self, k):
        return self.bands.rows(self.total.at[Torus().at["x"], k], k)

    def hop(self, k, m):
        me = Torus()
        by = toward(m)
        if m < FAR:
            src, dst = self.mine(k), self.place(k)
        else:
            dst = src = self.total.at[me.shift("x", -by), k, self.bands.cuts(k)[m - FAR]]
        return remote(src, dst, self.sems, (k, m), me.neighbour("x", by))

    def own(self, k):
        return pltpu.make_async_copy(self.mine(k), self.place(k), self.local.at[k])

    def begin(self):
        for k in COLOURS:
            if self.local is None:
                self.place(k)[...] = self.mine(k)[...]
            else:
                self.own(k).start()
            for m in WAYS:
                self.hop(k, m).start()

    def forward(self):
        for k in COLOURS:
            for m in WAYS:
                self.hop(k, m).wait_recv()
                self.hop(k, FAR + m).start()

    def finish(self):
        for k in COLOURS:
            for m in WAYS:
                self.hop(k, FAR + m).wait_recv()
            if self.local is not None:
                self.own(k).wait()
            for m in range(ADDED):
                self.hop(k, m).wait_send()


def comm_params(collective_id):
    return pltpu.CompilerParams(collective_id=collective_id, has_side_effects=True, vmem_limit_bytes=VMEM_LIMIT)


def gather_kernel(*refs):
    n = len(Gather.semaphores())
    a, u, d = (Gather(kind, *refs[i::C][:PAIR], *refs[PAIR * C + n * i:][:n]) for i, kind in enumerate((WIDE, WIDE, DOWN)))
    enter()
    for gather in (a, u, d):
        gather.begin()
    for step, *ring in ((a.relay, FIRST), (u.relay, FIRST), (d.relay, FIRST), (a.settle, FIRST), (a.launch, SECOND),
                        (u.settle, FIRST), (u.launch, SECOND), (a.relay, SECOND), (d.settle, FIRST), (d.launch, SECOND),
                        (u.relay, SECOND), (a.settle, SECOND), (a.launch, THIRD), (d.relay, SECOND), (u.settle, SECOND),
                        (a.relay, THIRD), (d.settle, SECOND), (a.settle, THIRD), (u.sent, FIRST, SECOND),
                        (d.sent, FIRST, SECOND), (a.sent, FIRST, SECOND, THIRD)):
        step(*ring)


def gather_call(attn, up, down, collective_id):
    return pl.pallas_call(
        gather_kernel, out_shape=[sds(BF16, *Gather.shape(kind)) for kind in (WIDE, WIDE, DOWN)], in_specs=[ANY] * C,
        out_specs=[ANY] * C, scratch_shapes=Gather.semaphores() * C, compiler_params=comm_params(collective_id),
        name="gather")(attn, up, down)


class Background:
    def __init__(self, steps, plan):
        self.steps, self.plan = steps, plan

    def visit(self, place):
        for j, first, end in self.plan.get(place, ()):
            @at_step(j)
            def _():
                for step in self.steps[first:end]:
                    step()


class Feed:
    def __init__(self, block, steps, buffers, sems):
        self.block, self.steps, self.buffers, self.sems = block, steps, buffers, sems

    @staticmethod
    def scratch(dtype, *shape):
        return [pltpu.VMEM((PAIR,) + shape, dtype), pltpu.SemaphoreType.DMA((PAIR,))]

    def copy(self, j):
        slot = lax.rem(j, PAIR)
        return pltpu.make_async_copy(self.block(j), self.buffers.at[slot], self.sems.at[slot])

    def get(self, j):
        pl.when(j + 1 < self.steps)(lambda: self.copy(j + 1).start())
        self.copy(j).wait()
        return self.buffers.at[lax.rem(j, PAIR)]


def first_feeds(*feeds):
    @at_step(0)
    def _():
        for feed in feeds:
            feed.copy(0).start()


class Share:
    def __init__(self, mine, theirs, place, sems, slot):
        self.local = pltpu.make_async_copy(mine, place, sems[PAIR].at[slot])
        self.far = remote(theirs, place, sems, slot, Torus().partner())

    def start(self):
        self.far.start()
        self.local.start()

    def sent(self):
        self.local.wait()
        self.far.wait_send()

    def wait(self):
        self.sent()
        self.far.wait_recv()


class Push:
    def __init__(self, src, tail, rows, sems, slot=0):
        body = BODY * len(SEQ_PAIR)
        tails = TAIL * len(SEQ_PAIR)
        self.copies = [
            remote(src.at[pl.ds(start, size)], rows.at[pl.ds(to, size)], sems, (slot, i), Torus().partner())
            for i, (start, to, size) in enumerate(((0, body, body), (tail, PAIR * body + tails, tails)))]

    @staticmethod
    def semaphores(n):
        return [pltpu.SemaphoreType.DMA((n, PAIR))] * PAIR

    def start(self):
        for copy in self.copies:
            copy.start()

    def wait(self):
        for copy in self.copies:
            copy.wait_recv()

    def finish(self):
        for copy in self.copies:
            copy.wait_send()


class Exchange:
    def __init__(self, mine, theirs, rows, sems, slot):
        self.moves = []
        for s in SEQ_PAIR:
            for i, (start, size) in enumerate(((0, BODY), (BODY, TAIL))):
                place = lambda n: rows.at[pl.ds(start * len(SEQ_PAIR) * PAIR + size * n, size)]
                part = pl.ds(TOK * s + start, size)
                at = slot + (PAIR * s + i,)
                local = pltpu.make_async_copy(mine.at[part], place(s), sems[2].at[at])
                far = remote(theirs.at[part], place(len(SEQ_PAIR) + s), sems, at, Torus().partner())
                self.moves.append((local, far))

    @staticmethod
    def semaphores(*lead):
        return [pltpu.SemaphoreType.DMA(lead + (2 * PAIR,))] * 3

    def start(self):
        for local, far in self.moves:
            far.start()
            local.start()

    def wait(self):
        for local, far in self.moves:
            local.wait()
            far.wait_recv()

    def finish(self):
        for _, far in self.moves:
            far.wait_send()


NT = (((1,), (1,)), ((), ()))
TN = (((0,), (0,)), ((), ()))


def dot(a, b):
    return jnp.dot(a, b, preferred_element_type=F32)


def dot_nt(a, b):
    return lax.dot_general(a, b, NT, preferred_element_type=F32)


def dot_tn(a, b):
    return lax.dot_general(a, b, TN, preferred_element_type=F32)


def zeros_but(n, axis, value):
    return tuple(value if i == axis else 0 for i in range(n))


def whole(*shape):
    return pl.BlockSpec(shape, lambda *_: (0,) * len(shape))


def along(axis, *block, index=lambda j: j):
    return pl.BlockSpec(block, lambda j: zeros_but(len(block), axis, index(j)))


def row(vec, i):
    return vec[i:i + 1]


def row_mean(t):
    return jnp.mean(t, axis=-1, keepdims=True)


def norm_stats(t):
    centered = t - row_mean(t)
    rstd = lax.rsqrt(row_mean(centered * centered) + LN_EPS)
    return centered * rstd, rstd


def norm_back(xhat, rstd, g):
    return rstd * (g - row_mean(g) - xhat * row_mean(g * xhat))


def col_sum(t):
    return jnp.sum(t, axis=0, keepdims=True)


def at_step(j):
    return pl.when(pl.program_id(0) == j)


def accumulate(ref, value):
    @at_step(0)
    def _():
        ref[...] = value

    @pl.when(pl.program_id(0) > 0)
    def _():
        ref[...] += value


def pad(t):
    return jnp.concatenate([t.astype(F32), jnp.zeros((TOK - SEQ, t.shape[1]), F32)], axis=0).astype(BF16)


WINDOW = 2 * LANES


def window(h):
    first = h * HEAD
    start = jnp.minimum(lax.div(first, LANES) * LANES, D - WINDOW)
    lane = lax.broadcasted_iota(jnp.int32, (1, WINDOW), 1) + (start - first)
    return pl.ds(pl.multiple_of(start, LANES), WINDOW), (lane >= 0) & (lane < HEAD)


def each_head(body):
    def trip(i, carry):
        for n in range(PAIR):
            body(i * PAIR + n)
        return carry

    lax.fori_loop(0, HEADS // PAIR, trip, 0)


def each_seq(body):
    def trip(s, carry):
        start = pl.multiple_of(s * TOK, TAIL)
        body(s, pl.ds(start, TOK), pl.ds(start, SEQ))
        return carry

    lax.fori_loop(0, len(SEQ_PAIR), trip, 0)


def only(mask, t):
    return jnp.where(mask, t, jnp.zeros_like(t))


def softmax(scores):
    e = jnp.exp(scores - jnp.max(scores, axis=-1, keepdims=True))
    return e * (1.0 / jnp.sum(e, axis=-1, keepdims=True))


def attention(s, rows, o, acc, visit):
    acc[...] = jnp.zeros_like(acc)
    start = pl.multiple_of(s * TOK, TAIL)
    tokens = pl.ds(start, SEQ)

    def head(h):
        lanes, mask = window(h)
        k = only(mask, rows[K, tokens, lanes])
        v = only(mask, rows[V, tokens, lanes])
        probs = softmax(dot_nt(rows[Q, tokens, lanes], k) * SCALE).astype(BF16)
        acc[:, lanes] += dot(probs, v)

    each_head(head)
    visit("half")
    o[pl.ds(start, TOK)] = pad(acc[...])


FRONT_PLAN = {"start": ((0, 0, 1),), "half": ((O + 1, 1, 2),), "end": ((O + 1, 2, None),)}


def front_kernel(x_in, w_in, b, vec, _, qkv, h1, o, att, h2, up, rows, lhs, acc, x, x_sem, w_rows, w_sems, *sems):
    hosted = Background(Gather(WIDE, None, up, *sems).last_ring(), FRONT_PLAN)
    j = pl.program_id(0)
    weights = Feed(lambda n: w_in.at[n, :, pl.ds(0, D)], SIDE, w_rows, w_sems)
    fetch = pltpu.make_async_copy(x_in, x, x_sem)
    at_step(0)(fetch.start)
    first_feeds(weights)
    at_step(0)(enter)
    hosted.visit("start")

    @at_step(0)
    def _():
        fetch.wait()

        def norm(s, tile, tokens):
            xhat, _ = norm_stats(x[s].astype(F32))
            h1[tile] = pad(xhat * row(vec, G1) + row(vec, C1))

        each_seq(norm)
        lhs[...] = h1[...]

    @pl.when(j >= O)
    def _():
        attention(j - O, rows, o, acc, hosted.visit)
        lhs[...] = o[...]

    @pl.when((j < O) | (j == O + LAST_SEQ))
    def _():
        bias = jnp.where(j < O, b[0], row(vec, BO))
        w = weights.get(jnp.minimum(j, O))

        def product(s, tile, tokens):
            att[tile] = dot(lhs[tile], w[...]) + bias

        each_seq(product)

    @pl.when(j < O)
    def _():
        t = att[...].astype(BF16)
        qkv[0] = t
        rows[j] = t

    @at_step(O + LAST_SEQ)
    def _():
        def norm(s, tile, tokens):
            xhat, _ = norm_stats(x[s].astype(F32) + row(vec, S1) * att[tokens])
            h2[tile] = pad(xhat * row(vec, G2) + row(vec, C2))

        each_seq(norm)

    hosted.visit("end")


def upto(n):
    return lambda j: jnp.minimum(j, n)


def front_call(x, w_attn, b_qkv, vec, up, collective_id):
    return pl.pallas_call(
        front_kernel, grid=(O + PAIR,),
        out_shape=(sds(BF16, O, TT, D), sds(BF16, TT, D), sds(BF16, TT, D), sds(F32, TT, D), sds(BF16, TT, D),
                   sds(BF16, *Gather.shape(WIDE))),
        in_specs=[ANY, ANY, along(0, 1, 1, D, index=upto(V)), whole(8, D), ANY],
        out_specs=(along(0, 1, TT, D, index=upto(V)),) + (whole(TT, D),) * SIDE + (ANY,),
        scratch_shapes=[pltpu.VMEM((O, TT, D), BF16), pltpu.VMEM((TT, D), BF16), pltpu.VMEM((SEQ, D), F32),
                        pltpu.VMEM(SEQS, BF16), pltpu.SemaphoreType.DMA] + Feed.scratch(BF16, D, D) + Gather.semaphores(),
        input_output_aliases={SIDE: SIDE + 1},
        compiler_params=comm_params(collective_id), name="front",
    )(x, w_attn, b_qkv, vec, up)


def w_out_block():
    return pl.BlockSpec((1, D, D), lambda j: (O, 0, 0), pipeline_mode=pl.Buffered(1))


TILES = FF // HALF
OWN_BODY = BODY * len(SEQ_PAIR)
TAILS = ROWS - TAIL * PAIR * len(SEQ_PAIR)


def put_rows(ref, tail, s, t):
    ref[pl.ds(pl.multiple_of(BODY * s, BODY), BODY)] = t[:BODY]
    ref[pl.ds(pl.multiple_of(tail + TAIL * s, TAIL), TAIL)] = t[BODY:]


DOWN_PLAN = {"start": ((0, 0, 1),), "end": ((TILES + 2, 1, 2), (2 * TILES - 1, 2, None))}


def mlp_in_kernel(h2, gz, w_up, b_up, vec, _, act, slope, d_down, down, a_rows, b_rows, b_away, *sems):
    a_sems, b_sems, sems = sems[:PAIR], sems[PAIR:2 * PAIR], sems[2 * PAIR:]
    hosted = Background(Gather(DOWN, None, down, *sems).last_ring(), DOWN_PLAN)
    j = pl.program_id(0)
    away = Push(b_away, OWN_BODY, b_rows, b_sems, 0)
    tile = lambda n: Push(a_rows.at[n], TAILS, a_rows.at[n], a_sems, n)
    at_step(0)(enter)
    hosted.visit("start")

    @at_step(0)
    def _():
        first = Torus().at["c"] == 0
        def scale(s, tile, tokens):
            d = pad(gz[s].astype(F32) * row(vec, S2))
            left, right = d[:, :HALF], d[:, D - HALF:]
            put_rows(b_rows, TAILS, s, jnp.where(first, left, right))
            put_rows(b_away, OWN_BODY, s, jnp.where(first, right, left))

        each_seq(scale)

    at_step(1)(away.start)
    for n in range(TILES):
        at_step(n + 1)(tile(n).start)

    @pl.when(j < TILES)
    def _():
        u = dot(h2[...], w_up[0]) + b_up[0]
        phi = 0.5 * (1.0 + lax.erf(u * math.sqrt(0.5)))
        slope[...] = phi + u * (jnp.exp(-0.5 * u * u) * math.sqrt(0.5 / math.pi))
        place = lax.rem(lax.broadcasted_iota(jnp.int32, (TT, 1), 0), TOK)
        a = only(place < SEQ, u * phi).astype(BF16)
        act[...] = a
        for s in SEQ_PAIR:
            put_rows(a_rows.at[j], TAILS, s, a[TOK * s:TOK * s + TOK])

    at_step(TILES)(away.wait)
    for n in range(TILES):
        at_step(TILES + n)(tile(n).wait)

    @pl.when(j >= TILES)
    def _():
        d_down[...] = dot_tn(a_rows[j - TILES], b_rows[...])

    hosted.visit("end")

    @at_step(2 * TILES - 1)
    def _():
        away.finish()
        for n in range(TILES):
            tile(n).finish()


def mlp_in_call(h2, gz, w_up, b_up, vec, down, collective_id):
    low = lambda j: jnp.minimum(j, TILES - 1)
    high = lambda j: jnp.maximum(j - TILES, 0)
    return pl.pallas_call(
        mlp_in_kernel, grid=(2 * TILES,),
        out_shape=(sds(BF16, TT, FF), sds(F32, TT, FF), sds(F32, FF, HALF), sds(BF16, *Gather.shape(DOWN))),
        in_specs=[whole(TT, D), whole(*SEQS), up_tile(low), along(0, 1, 1, HALF, index=low), whole(8, D), ANY],
        out_specs=(along(1, TT, HALF, index=low), along(1, TT, HALF, index=low),
                   along(0, HALF, HALF, index=high), ANY),
        scratch_shapes=[pltpu.VMEM((TILES, ROWS, HALF), BF16), pltpu.VMEM((ROWS, HALF), BF16),
                        pltpu.VMEM((PAIR * TOK, HALF), BF16)] + Push.semaphores(TILES) + Push.semaphores(1) +
        Gather.semaphores(),
        input_output_aliases={SIDE + 1: O},
        compiler_params=comm_params(collective_id), name="mlp_in",
    )(h2, gz, w_up, b_up.reshape(TILES, 1, HALF), vec, down)


def up_tile(index=lambda j: j):
    return pl.BlockSpec((1, D, HALF), lambda j: (index(j) // PAIR, 0, index(j) % PAIR))


MLP_PLAN = {"start": ((0, 0, 1),), "end": ((1, 1, 2), (3, 2, 3), (TILES - 1, 3, None))}


def mlp_out_kernel(act_in, slope_in, gz, up_in, down_in, vec, part, d_pre, db_up, mlp, d_h2, sums, dm, *scratch):
    scratch, tiles = scratch[:-8], scratch[-8:]
    first = First(Bands(DOWN), part, sums, *scratch)
    hosted = Background([first.near, first.far, first.relay, first.settle, first.finish], MLP_PLAN)
    j = pl.program_id(0)
    cols = lambda n: pl.ds(pl.multiple_of(n * HALF, HALF), HALF)
    blocks = (lambda n: act_in.at[:, cols(n)], lambda n: slope_in.at[:, cols(n)],
              lambda n: up_in.at[lax.div(n, PAIR), :, cols(lax.rem(n, PAIR))], lambda n: down_in.at[cols(n)])
    feeds = [Feed(block, TILES, *tiles[PAIR * i:][:PAIR]) for i, block in enumerate(blocks)]
    first_feeds(*feeds)
    at_step(0)(enter)
    hosted.visit("start")

    @at_step(0)
    def _():
        def scale(s, tile, tokens):
            dm[tile] = pad(gz[s].astype(F32) * row(vec, S2))

        each_seq(scale)

    act, slope, w_up, w_down = (feed.get(j) for feed in feeds)
    db_up[0] = jnp.zeros((1, HALF), F32)

    def back(s, tile, tokens):
        accumulate(mlp.at[tile], dot(act[tile], w_down[...]))
        d = dot_nt(dm[tile], w_down[...]) * slope[tile]
        db_up[0] += col_sum(d)
        d = d.astype(BF16)
        d_pre[0, 0, tile] = d
        accumulate(d_h2.at[tile], dot_nt(d, w_up[...]))

    each_seq(back)
    hosted.visit("end")


def mlp_out_call(act, slope, gz, w_up, w_down, vec, part, collective_id):
    return pl.pallas_call(
        mlp_out_kernel, grid=(TILES,),
        out_shape=(sds(BF16, PAIR, SIDE, TT, HALF), sds(F32, TILES, 1, HALF), sds(F32, TT, D), sds(F32, TT, D),
                   Bands(DOWN).sums()),
        in_specs=[ANY, ANY, whole(*SEQS), ANY, ANY, whole(8, D), ANY],
        out_specs=(pl.BlockSpec((1, 1, TT, HALF), lambda j: (j % PAIR, j // PAIR, 0, 0)), along(0, 1, 1, HALF),
                   whole(TT, D), whole(TT, D), ANY),
        scratch_shapes=[pltpu.VMEM((TT, D), BF16)] + Bands(DOWN).first() + Feed.scratch(BF16, TT, HALF) +
        Feed.scratch(F32, TT, HALF) + Feed.scratch(BF16, D, HALF) + Feed.scratch(BF16, HALF, D),
        compiler_params=comm_params(collective_id), name="mlp_out",
    )(act, slope, gz, w_up, w_down, vec, part)


def halves_of(t):
    t = pad(t)
    return t[:, :HALF], jnp.concatenate([t[:, HALF:], jnp.zeros((TOK, QCOLS - D), BF16)], axis=1)


def mid(mlp, d_h2, att, x, gz, vec, w_out, z, g_res, d_att, d_o, sums):
    a = att[:SEQ]
    y = x[0].astype(F32) + row(vec, S1) * a
    m = mlp[:SEQ] + row(vec, B2)
    g = gz[0].astype(F32)
    z[0] = (y + row(vec, S2) * m).astype(BF16)
    xhat, rstd = norm_stats(y)
    dh = d_h2[:SEQ]
    gr = g + norm_back(xhat, rstd, dh * row(vec, G2))
    g_res[:SEQ] = gr
    da = gr * row(vec, S1)
    terms = (da, gr * a, dh * xhat, dh, g * row(vec, S2), g * m)
    accumulate(sums, jnp.concatenate([jnp.zeros((BO, D), F32)] + [col_sum(t) for t in terms], axis=0))
    for i, t in enumerate(halves_of(da)):
        d_att[i] = t
    d_o[...] = dot_nt(pad(da), w_out[0]).astype(BF16)


def attention_back(s, qkv, d_o, d_qkv, db, acc, b_rows, away, first, visit):
    acc[...] = jnp.zeros_like(acc)

    def head(h):
        lanes, mask = window(h)
        q, k, v = (only(mask, qkv[i, :SEQ, lanes]) for i in (Q, K, V))
        do = only(mask, d_o[:SEQ, lanes])
        scores = dot_nt(k, q) * SCALE
        e = jnp.exp(scores - jnp.max(scores, axis=0, keepdims=True))
        probs = e * (1.0 / col_sum(e))
        acc[V, :, lanes] += dot(probs.astype(BF16), do)
        dp = dot_nt(v, do)
        ds = probs * (dp - col_sum(dp * probs))
        ds = (ds * SCALE).astype(BF16)
        acc[K, :, lanes] += dot(ds, q)
        acc[Q, :, lanes] += dot_tn(ds, k)

    each_head(head)
    visit("half")
    accumulate(db, jnp.concatenate([col_sum(acc[i]) for i in (Q, K, V)], axis=0))
    for n in (Q, K, V):
        left, right = halves_of(acc[n])
        d_qkv[0, n] = left
        d_qkv[1, n] = right
        put_rows(b_rows.at[n], TAILS, s, jnp.where(first, left, right))
        put_rows(away.at[n], OWN_BODY, s, jnp.where(first, right, left))


PER = HALF // STEP


class WideGrads:
    def __init__(self, inputs, a_of, cotangents, out, base, lead, a_rows, a_cols, b_rows):
        self.inputs, self.a_of, self.cotangents, self.out, self.base, self.lead = inputs, a_of, cotangents, out, base, lead
        self.a_rows, self.a_cols, self.b_rows = a_rows, a_cols, b_rows

    @staticmethod
    def scratch(inputs):
        return [pltpu.VMEM((inputs, ROWS, D), BF16), pltpu.VMEM((inputs, D, ROWS), BF16), pltpu.VMEM((SIDE, ROWS, HALF), BF16)]

    def turn(self, i):
        def trip(n, carry):
            lanes = pl.ds(pl.multiple_of(n * LANES, LANES), LANES)
            self.a_cols[i, lanes] = self.a_rows[i, :, lanes].T
            return carry

        lax.fori_loop(0, D // LANES, trip, 0)

    def step(self):
        j = pl.program_id(0)
        done = []
        for t in range(SIDE):
            n = (t + self.lead) % SIDE

            @at_step(self.base + PER * t)
            def _():
                i = self.a_of[n]
                if i not in done:
                    self.inputs[i].wait()
                    self.turn(i)
                    done.append(i)
                self.cotangents[n].wait()

        @pl.when(j >= self.base)
        def _():
            n = lax.rem(lax.div(j - self.base, PER) + self.lead, SIDE)
            cols = pl.ds(pl.multiple_of(lax.rem(j - self.base, PER) * STEP, STEP), STEP)
            i = 0 if len(self.inputs) == 1 else lax.div(n, O)
            self.out[0] = dot(self.a_cols[i], self.b_rows[n, :, cols])

    def finish(self):
        for move in (*self.inputs, *self.cotangents):
            move.finish()


def grads_block(base, lead):
    def index(j):
        n = jnp.maximum(j - base, 0)
        return (n // PER + lead) % SIDE, 0, n % PER

    return pl.BlockSpec((1, D, STEP), index)


GRAD_STEPS = PER * SIDE


def tok_block():
    return along(0, TOK, D, index=upto(LAST_SEQ))


def seq_block():
    return along(0, 1, SEQ, D, index=upto(LAST_SEQ))


MID_PLAN = {"start": ((0, 0, 1),), "end": ((1, 1, 3), (8, 3, 4), (11, 4, 5), (LAST_SEQ + GRAD_STEPS, 5, None))}


def mid_kernel(*refs):
    refs = list(refs)
    take = lambda n: [refs.pop(0) for _ in range(n)]
    ins, (h2, d_pre, acc), outs, (d_up, result) = take(7), take(3), take(5), take(2)
    rows, a_sems, b_sems = take(3), take(C), take(C)
    rest = Rest(Bands(DOWN), acc, result, *refs)
    hosted = Background([rest.begin, rest.loaded, rest.relay, rest.settle, rest.relay_third, rest.settle_third, rest.finish],
                        MID_PLAN)
    c = Torus().at["c"]
    grads = WideGrads(
        [Exchange(h2, h2, rows[0].at[0], a_sems, ())], (0,) * SIDE,
        [Exchange(d_pre.at[c, n], d_pre.at[1 - c, n], rows[2].at[n], b_sems, (n,)) for n in range(SIDE)], d_up, SEQS[0], 0, *rows)
    at_step(0)(enter)
    hosted.visit("start")

    @at_step(0)
    def _():
        for move in (*grads.inputs, *grads.cotangents):
            move.start()

    pl.when(pl.program_id(0) < SEQS[0])(lambda: mid(*ins, *outs))
    grads.step()
    hosted.visit("end")
    at_step(LAST_SEQ + GRAD_STEPS)(grads.finish)


def mid_call(mlp, d_h2, att, x, gz, vec, w_attn, h2, d_pre, acc, collective_id):
    return pl.pallas_call(
        mid_kernel, grid=(SEQS[0] + GRAD_STEPS,),
        out_shape=(sds(BF16, *SEQS), sds(F32, TT, D), sds(BF16, PAIR, TT, HALF), sds(BF16, TT, D), sds(F32, 8, D),
                   sds(F32, SIDE, D, HALF), Bands(DOWN).result()),
        in_specs=[tok_block()] * O + [seq_block()] * PAIR + [whole(8, D), w_out_block()] + [ANY] * O,
        out_specs=(seq_block(), tok_block(), along(1, PAIR, TOK, HALF, index=upto(LAST_SEQ)), tok_block(), whole(8, D),
                   grads_block(SEQS[0], 0), ANY),
        scratch_shapes=WideGrads.scratch(1) + Exchange.semaphores() + Exchange.semaphores(SIDE) +
        Bands(DOWN).later(),
        compiler_params=comm_params(collective_id), name="mid",
    )(mlp, d_h2, att, x, gz, vec, w_attn, h2, d_pre, acc)


ATTN_PLAN = {"start": ((0, 0, 2),), "half": ((0, 2, 4),), "end": ((SIDE, 4, 5), (LAST_SEQ + GRAD_STEPS, 5, None))}


def attn_back_kernel(*refs):
    refs = list(refs)
    take = lambda n: [refs.pop(0) for _ in range(n)]
    (qkv_in, do_in), (h1, o, d_att, part, result), (d_qkv, db, d_attn, sums, total) = take(2), take(5), take(5)
    acc, away, rows, tiles = refs.pop(0), refs.pop(0), take(3), take(SIDE)
    tokens = lambda n: pl.ds(pl.multiple_of(n * TOK, TAIL), TOK)
    feeds = [Feed(lambda n: qkv_in.at[:, tokens(n)], SEQS[0], *tiles[:PAIR]),
             Feed(lambda n: do_in.at[tokens(n)], SEQS[0], *tiles[PAIR:])]
    first_feeds(*feeds)
    a_sems, b_sems, away_sems = take(C), take(C), take(PAIR)
    first = First(Bands(WIDE), part, sums, *take(len(Bands(WIDE).first())))
    spread = Spread(Bands(DOWN), result, total, *refs)
    hosted = Background([spread.begin, first.near, first.far, spread.forward, first.relay, first.settle, first.finish,
                         spread.finish], ATTN_PLAN)
    c = Torus().at["c"]
    pushes = [Push(away.at[n], OWN_BODY, rows[2].at[n], away_sems, n) for n in range(O)]
    grads = WideGrads(
        [Exchange(a, a, rows[0].at[i], a_sems, (i,)) for i, a in enumerate((h1, o))], (0,) * O + (1,),
        pushes + [Exchange(d_att.at[c], d_att.at[1 - c], rows[2].at[O], b_sems, ())], d_attn, SEQS[0], O, *rows)
    at_step(0)(enter)
    hosted.visit("start")

    @at_step(0)
    def _():
        for move in (*grads.inputs, grads.cotangents[O]):
            move.start()

    @at_step(SEQS[0])
    def _():
        for push in pushes:
            push.start()

    j = pl.program_id(0)

    @pl.when(j < SEQS[0])
    def _():
        qkv, d_o = (feed.get(j) for feed in feeds)
        attention_back(j, qkv, d_o, d_qkv, db, acc, rows[2], away, c == 0, hosted.visit)


    grads.step()
    hosted.visit("end")
    at_step(LAST_SEQ + GRAD_STEPS)(grads.finish)


def attn_back_call(qkv, d_o, h1, o, d_att, part, result, collective_id):
    return pl.pallas_call(
        attn_back_kernel, grid=(SEQS[0] + GRAD_STEPS,),
        out_shape=(sds(BF16, PAIR, O, TT, HALF), sds(F32, O, D), sds(F32, SIDE, D, HALF), Bands(WIDE).sums(),
                   Bands(DOWN).total()),
        in_specs=[ANY] * 7,
        out_specs=(along(2, PAIR, O, TOK, HALF, index=upto(LAST_SEQ)), whole(O, D), grads_block(SEQS[0], O), ANY, ANY),
        scratch_shapes=[pltpu.VMEM((O, SEQ, D), F32), pltpu.VMEM((O, PAIR * TOK, HALF), BF16)] + WideGrads.scratch(2) +
        Feed.scratch(BF16, O, TOK, D) + Feed.scratch(BF16, TOK, D) + Exchange.semaphores(PAIR) + Exchange.semaphores() + Push.semaphores(O) + Bands(WIDE).first() + Spread.scratch(),
        compiler_params=comm_params(collective_id), name="attn_back",
    )(qkv, d_o, h1, o, d_att, part, result)


IN_STEPS = PAIR * O
SLOT = 40
LAST_PLAN = {"start": ((0, 0, 2),), "end": ((O, 2, None),)}


CORE_COLS = D - HALF
KEPT = 48
GRADS = ((KEPT, O * D), (KEPT, D), (KEPT, FF), (PAIR, C, UNIT, D), (SIDE, KEPT, LANES))
SHARES = PAIR * SIDE + SIDE + PAIR


def split_rows(totals, first, keep, give):
    for x in range(SIDE):
        for total, bands in totals:
            rows = jnp.concatenate([total[x, k, :n] for k, (_, n) in enumerate(BANDS[WIDE])], axis=0)
            low, high = rows[:KEPT], jnp.concatenate([rows[OWN:], rows[:KEPT - OWN]], axis=0)
            keep[x, :, bands.cols] = jnp.where(first, low, high)
            give[x, :, bands.cols] = jnp.where(first, high, low)


class Finals:
    def __init__(self, down, up, attn, outs, sems):
        self.c = Torus().at["c"]
        self.down, self.up, self.attn, self.sems = down, up, attn, sems
        self.qkv, self.out, self.up_out, self.down_out, self.pad = outs
        self.edge = pl.ds(CORE_COLS, LANES)

    def cols(self, base, width):
        return pl.ds(pl.multiple_of(base + self.c * HALF, LANES), width)

    def up_share(self, x):
        place = self.up_out.at[:, self.cols(QCOLS * x, HALF)]
        return Share(*(ref.at[x] for ref in self.up), place, self.sems, x)

    def block(self, x):
        return (self.out, 0) if x == O else (self.qkv, D * x)

    def attn_share(self, x):
        out, base = self.block(x)
        sides = (ref.at[x, :, pl.ds(0, CORE_COLS)] for ref in self.attn)
        return Share(*sides, out.at[:, self.cols(base, CORE_COLS)], self.sems, SIDE + x)

    def edge_share(self, x, padding):
        out, base = self.block(x)
        place = self.pad.at[x] if padding else out.at[:, pl.ds(base + CORE_COLS, LANES)]
        return Share(*(ref.at[x, :, self.edge] for ref in self.attn), place, self.sems, PAIR * SIDE + x)

    def down_share(self, edge):
        src = self.edge if edge else pl.ds(pl.multiple_of(self.c * LANES, LANES), CORE_COLS)
        sides = (self.down.at[pl.ds(PAIR * c, PAIR), :, :, src] for c in (self.c, 1 - self.c))
        place = self.down_out.at[:, :, :, self.edge if edge else self.cols(0, CORE_COLS)]
        return Share(*sides, place, self.sems, SHARES - PAIR + edge)

    def start_down(self):
        self.down_share(0).start()
        pl.when(self.c == 0)(lambda: self.down_share(1).start())

    def start(self):
        for x in range(SIDE):
            self.attn_share(x).start()
            pl.when(self.c == 0)(lambda: self.edge_share(x, False).start())
            pl.when(self.c == 1)(lambda: self.edge_share(x, True).start())

    def finish(self):
        for x in range(SIDE):
            for share in (self.up_share(x), self.attn_share(x), self.edge_share(x, True)):
                share.wait()
        self.down_share(0).wait()
        pl.when(self.c == 0)(lambda: self.down_share(1).sent())
        pl.when(self.c == 1)(lambda: self.down_share(1).far.wait_recv())


def last_kernel(*refs):
    refs = list(refs)
    take = lambda n: [refs.pop(0) for _ in range(n)]
    (d_qkv, w_attn, x_in, g_in, vec), (small, acc_up, down, _), (dx, part) = take(5), take(SIDE), take(PAIR)
    outs, (x, g_res, x_sem, g_sem), tiles = take(len(GRADS)), take(SIDE), take(SIDE)
    j = pl.program_id(0)
    fetches = [pltpu.make_async_copy(*move) for move in ((x_in, x, x_sem), (g_in, g_res, g_sem))]
    feeds = [Feed(lambda n: d_qkv.at[lax.rem(n, PAIR), lax.div(n, PAIR)], IN_STEPS, *tiles[:PAIR]),
             Feed(lambda n: w_attn.at[lax.div(n, PAIR), :, pl.ds(pl.multiple_of(lax.rem(n, PAIR) * HALF, HALF), HALF)],
                  IN_STEPS, *tiles[PAIR:])]
    first_feeds(*feeds)
    (acc, sums, pair_sums, block), (totals, sides), block_sem, swap_sems = take(4), (take(C), take(SIDE)), refs.pop(0), take(PAIR)
    finals = Finals(down, sides[:PAIR], sides[PAIR:], outs, take(C))
    halves = [Bands(WIDE, h) for h in WAYS]
    a, b = (First(bands, part, None, *take(len(bands.first()))) for bands in halves)
    rest_a, rest_b = (Rest(f.bands, f.own_all, None, f.own_all, *take(len(f.bands.later()) - 1)) for f in (a, b))
    rest_up = Rest(Bands(WIDE), acc_up, None, *take(len(Bands(WIDE).later())))
    spread_up, spread_a, spread_b = (
        Spread(r.bands, r.sums(), total, *take(PAIR), None) for r, total in zip((rest_up, rest_a, rest_b), totals))
    hosted = Background([rest_up.begin, a.near, rest_up.loaded, rest_up.relay], LAST_PLAN)
    first = finals.c == 0
    swap = remote(sums, pair_sums, swap_sems, (), Torus().partner())
    fetch = pltpu.make_async_copy(small, block, block_sem)
    at_step(0)(enter)
    hosted.visit("start")

    @at_step(0)
    def _():
        for move in (fetch, *fetches):
            move.start()
        finals.start_down()

    @pl.when(j < IN_STEPS)
    def _():
        d_half, w = (feed.get(j) for feed in feeds)
        each_seq(lambda s, tile, tokens: accumulate(acc.at[tile], dot_nt(d_half[tile], w[...])))

    @at_step(IN_STEPS - 1)
    def _():
        for move in fetches:
            move.wait()
        sums[...] = jnp.zeros_like(sums)

        def back(s, tile, tokens):
            xhat, rstd = norm_stats(x[s].astype(F32))
            dh = acc[tokens]
            sums[:BO] += jnp.concatenate([col_sum(dh * xhat), col_sum(dh)], axis=0)
            dx[s] = (g_res[tokens] + norm_back(xhat, rstd, dh * row(vec, G1))).astype(BF16)

        each_seq(back)

    hosted.visit("end")

    @at_step(IN_STEPS)
    def _():
        swap.start()
        fetch.wait()
        swap.wait()
        both = sums[...] + pair_sums[...]
        for d in range(DEVICES):
            at = CHIP * (d // PAIR) + SLOT + OWN * (d % PAIR)
            block[at:at + BO, :OWN] = both[:BO, OWN * d:OWN * d + OWN]

        @pl.when(finals.c == 1)
        def _():
            for z in range(SIDE):
                for y in range(SIDE):
                    rows = block.at[pl.ds(CHIP * (SIDE * z + y), CHIP)]
                    put = pltpu.make_async_copy(rows, part.at[0, z, y, :, pl.ds(CORE_COLS, LANES)], block_sem)
                    put.start()
            pltpu.make_async_copy(block, small, block_sem).wait()

        def share_up():
            spread_up.finish()
            split_rows([(totals[0], Bands(WIDE))], first, *sides[:PAIR])
            for x in range(SIDE):
                finals.up_share(x).start()

        for step in (b.near, rest_up.settle, a.far, rest_up.relay_third, b.far, a.relay, rest_up.settle_third, spread_up.begin,
                     b.relay, spread_up.forward, functools.partial(a.settle, rest_a.send),
                     functools.partial(b.settle, rest_b.send), rest_a.relay, rest_b.relay, rest_a.settle, rest_b.settle,
                     share_up, rest_a.relay_third, rest_b.relay_third, rest_a.settle_third, spread_a.begin,
                     rest_b.settle_third, spread_b.begin, spread_a.forward, spread_b.forward, spread_a.finish, spread_b.finish):
            step()
        split_rows(list(zip(totals[1:], halves)), first, *sides[PAIR:])
        finals.start()
        for user in (rest_up, rest_a, rest_b, a, b, finals):
            user.finish()


def last_call(d_qkv, w_attn, x, g_res, vec, small, acc_up, down, part, collective_id):
    halves = [Bands(WIDE, h) for h in WAYS]
    dma = pltpu.SemaphoreType.DMA
    rings = [Bands(WIDE), *halves]
    return pl.pallas_call(
        last_kernel, grid=(IN_STEPS + 1,),
        out_shape=(sds(BF16, *SEQS), sds(F32, *part.shape), *(sds(F32, *shape) for shape in GRADS)),
        in_specs=[ANY] * SIDE + [whole(8, D)] + [ANY] * SIDE,
        out_specs=(whole(*SEQS),) + (ANY,) * (len(GRADS) + 1),
        scratch_shapes=[pltpu.VMEM(SEQS, BF16), pltpu.VMEM((TT, D), F32), dma, dma] + Feed.scratch(BF16, TT, HALF) +
        Feed.scratch(BF16, D, HALF) + [pltpu.VMEM((TT, D), F32), pltpu.VMEM((SUB, D), F32), pltpu.VMEM((SUB, D), F32),
                        pltpu.VMEM((D, LANES), F32)] + [r.vmem(SIDE, C) for r in rings] +
        [pltpu.VMEM((SIDE, KEPT, HALF), F32)] * SIDE + [dma, dma, dma] + [dma((SHARES,))] * C + halves[0].first() * PAIR +
        halves[0].later()[1:] * PAIR + Bands(WIDE).later() + Spread.scratch()[:PAIR] * C,
        input_output_aliases={8: 1},
        compiler_params=comm_params(collective_id), name="last",
    )(d_qkv, w_attn, x, g_res, vec, small, acc_up, down, part)


BQ, BU, VEC = 3 * D // 32, 3 * D // 32 + FF // 32, 3 * D // 32 + FF // 32 + 8 * OWN


def pair_swap(a):
    return lax.ppermute(a, "fsdp", [(i, i ^ 1) for i in range(DEVICES)])


def by_core(first, a, b):
    return jnp.where(first, a, b), jnp.where(first, b, a)


def my_pieces(shards, first):
    w_qkv, b_qkv, w_out, w_up, b_up, w_down, vec_params = shards
    x = lax.axis_index("rep")
    small = jnp.concatenate([b_qkv, b_up, vec_params.reshape(-1)])
    small = jnp.pad(small, (0, OWN * LANES - VEC)).reshape(OWN, LANES)
    attn = lax.dynamic_slice_in_dim(jnp.concatenate([w_qkv, w_out], axis=1), x * D, D, 1)
    attn = jnp.concatenate([attn, small], axis=1)
    up = lax.dynamic_slice_in_dim(w_up, x * QCOLS, QCOLS, 1)
    wide = jnp.stack([attn, up]).astype(BF16)
    mine, theirs = by_core(first, wide[..., :HALF], wide[..., HALF:])
    theirs = pair_swap(theirs)
    piece = jnp.concatenate(by_core(first, mine, theirs), axis=1)
    down = lax.dynamic_slice_in_dim(w_down, x * 48, 48, 0).astype(BF16).reshape(3, 16, D)
    return piece[0], piece[1], down


def small_params(w_attn):
    small = w_attn[0, :, D:].astype(F32).reshape(DEVICES, OWN * LANES)
    vec = small[:, BU:VEC].reshape(DEVICES, 8, OWN).transpose(1, 0, 2).reshape(8, D)
    return small[:, :BQ].reshape(O, 1, D), small[:, BQ:BU].reshape(FF), vec


ROOM = 5 * LANES


def small_grads(db_qkv, db_up, sums):
    vec = sums[BO:].reshape(8 - BO, DEVICES, OWN).transpose(1, 0, 2).reshape(DEVICES, VEC - BU - BO * OWN)
    small = jnp.concatenate([db_qkv.reshape(DEVICES, BQ), db_up.reshape(DEVICES, BU - BQ), vec], axis=1)
    small = small + pair_swap(small)
    small = jnp.pad(small, ((0, 0), (0, ROOM - small.shape[1]))).reshape(DEVICES, ROOM // LANES, LANES)
    return jnp.pad(small, ((0, 0), (0, OWN - ROOM // LANES), (0, 0))).reshape(D, LANES)


def device_step(x, gz, *shards):
    first = lax.rem(lax.axis_index("fsdp"), PAIR) == 0
    attn, up, down = my_pieces(shards, first)
    w_attn, up, down = gather_call(attn, up, down, 0)
    w_attn = w_attn.reshape(SIDE, D, QCOLS)
    b_qkv, b_up, vec = small_params(w_attn)
    qkv, h1, o, att, h2, w_up = front_call(x, w_attn, b_qkv, vec, up, 1)
    w_up = w_up.reshape(SIDE, D, QCOLS)
    act, slope, part, w_down = mlp_in_call(h2, gz, w_up, b_up, vec, down, 2)
    part = part.reshape((SIDE,) * 3 + (C * UNIT, HALF))
    d_pre, db_up, mlp, d_h2, acc = mlp_out_call(act, slope, gz, w_up, w_down.reshape(FF, D), vec, part, 3)
    z, g_res, d_att, d_o, sums, part, result = mid_call(mlp, d_h2, att, x, gz, vec, w_attn, h2, d_pre, acc, 4)
    part = part.reshape((SIDE,) * 3 + (CHIP, HALF))
    d_qkv, db_qkv, part, acc, down = attn_back_call(qkv, d_o, h1, o, d_att, part, result, 5)
    small = small_grads(db_qkv, db_up, sums)
    part = part.reshape((SIDE,) * 3 + (CHIP, HALF))
    dx, _, g_qkv, g_out, g_up, g_down, edge = last_call(d_qkv, w_attn, x, g_res, vec, small, acc, down, part, 6)
    small = edge[0, :ROOM // LANES].reshape(ROOM)
    vec = jnp.concatenate([edge[0, SLOT:SLOT + BO, :OWN], small[BU:VEC - BO * OWN].reshape(8 - BO, OWN)], axis=0)
    g_qkv, g_out, g_up = (g[:OWN] for g in (g_qkv, g_out, g_up))
    return z, dx, g_qkv, small[:BQ], g_out, g_up, small[BQ:BU], g_down.reshape(FF // DEVICES, D), vec


def solution(mesh):
    batch = P(("rep", "fsdp"), None, None)
    rows, flat, cols = P("fsdp", None), P("fsdp"), P(None, "fsdp")
    shards = (rows, flat, rows, rows, flat, rows, cols)
    return jax.shard_map(device_step, mesh=mesh, in_specs=(batch, batch) + shards,
                         out_specs=(batch, batch) + shards, check_vma=False)
```

```python
import functools
import math

import jax
import jax.numpy as jnp
from jax import lax
from jax.experimental import pallas as pl
from jax.experimental.pallas import tpu as pltpu
from jax.sharding import PartitionSpec as P

HEADS = 16
LN_EPS = 1e-5
D = 1408
FF = 6144
SEQ = 257
HEAD = D // HEADS
SCALE = HEAD ** -0.5
QCOLS = 1536
HALF = 768
OWN = 44
CHIP = 2 * OWN
LANES = 128
DEVICES = 32
F32 = jnp.float32
BF16 = jnp.bfloat16
VMEM_LIMIT = 66 * 1000 * 1000
G1, C1, BO, S1, G2, C2, B2, S2 = range(8)
Q, K, V, O = range(4)
SEQS = (2, SEQ, D)
LAST_SEQ = SEQS[0] - 1
SEQ_PAIR = range(SEQS[0])
TAIL = 16
BODY = SEQ - 1
TOK = BODY + TAIL
TT = 2 * TOK
ROWS = 4 * TOK
STEP = 256


def sds(dtype, *shape):
    return jax.ShapeDtypeStruct(shape, dtype)


MESH_ID = pl.DeviceIdType.MESH
SIDE = 4
SUB = 8
PAIR = 2
C = 3
COLOURS = range(C)
COLOUR_DIMS = ("xyz", "yzx", "zxy")
FIRST, SECOND, THIRD, LAST = range(4)
WAYS = range(PAIR)
NEAR, FAR, ADDED = 0, 2, 4
WIDE, DOWN = "wide", "down"
ANY = pl.BlockSpec(memory_space=pl.ANY)
ALL = slice(None)


def duo(m):
    return pl.ds(PAIR * m, PAIR)


def toward(m):
    return 1 - PAIR * (m % PAIR)


class Torus:
    def __init__(self):
        f = lax.axis_index("fsdp")
        self.at = {"x": lax.axis_index("rep"), "z": lax.div(f, SIDE * PAIR), "y": lax.rem(lax.div(f, PAIR), SIDE),
                   "c": lax.rem(f, PAIR)}

    def shift(self, dim, by):
        return lax.rem(self.at[dim] + (SIDE + by), SIDE)

    def device(self, **moved):
        p = {**self.at, **moved}
        return (p["x"], (p["z"] * SIDE + p["y"]) * PAIR + p["c"])

    def neighbour(self, dim, by):
        return self.device(**{dim: self.shift(dim, by)})

    def partner(self):
        return self.device(c=1 - self.at["c"])


def enter():
    me = Torus()
    barrier = pltpu.get_barrier_semaphore()
    others = [me.neighbour(d, toward(m)) for d in COLOUR_DIMS[0] for m in WAYS] + [me.partner()]
    for other in others:
        pl.semaphore_signal(barrier, device_id=other, device_id_type=MESH_ID)
    pl.semaphore_wait(barrier, len(others))


def remote(src, dst, sems, slot, device):
    return pltpu.make_async_remote_copy(src_ref=src, dst_ref=dst, send_sem=sems[0].at[slot], recv_sem=sems[1].at[slot],
                                        device_id=device, device_id_type=MESH_ID)


class Gather:
    def __init__(self, kind, src, dst, hop_send, hop_recv, push_send, push_recv, local):
        self.kind, self.src, self.dst, self.local = kind, src, dst, local
        self.hops, self.pushes = (hop_send, hop_recv), (push_send, push_recv)
        self.cols, self.cut = (256, 128) if kind == WIDE else (D, HALF)

    @staticmethod
    def semaphores():
        dma = pltpu.SemaphoreType.DMA
        return [dma((C, C, ADDED))] * PAIR + [dma((C, ADDED + 1))] * PAIR + [dma((C,))]

    @staticmethod
    def shape(kind):
        return (SIDE,) * 3 + (CHIP, QCOLS) if kind == WIDE else (SIDE, SIDE, PAIR, SIDE, C, 16, D)

    def source(self, k):
        return self.src.at[:, pl.ds(self.cols * k, self.cols)] if self.kind == WIDE else self.src.at[k]

    def piece(self, me, k, s, v, half=None):
        dims = COLOUR_DIMS[k]
        at = {**me.at, **{d: ALL for d in dims[:s]}, dims[s]: v}
        off, width = 0, self.cols
        if half is not None and s == FIRST:
            off, width = self.cut * half, (self.cut, self.cols - self.cut)[half]
        elif half is not None:
            at[dims[0]] = duo(half)
        if self.kind == WIDE:
            cols = pl.ds(pl.multiple_of(at["c"] * HALF + self.cols * k + off, 128), width)
            return self.dst.at[at["x"], at["z"], at["y"], :, cols]
        return self.dst.at[at["z"], at["y"], at["c"], at["x"], k, :, pl.ds(off, width)]

    def hop(self, k, s, m):
        me = Torus()
        dim = COLOUR_DIMS[k][s]
        by = toward(m)
        if m < FAR:
            ref = self.piece(me, k, s, me.at[dim])
        else:
            ref = self.piece(me, k, s, me.shift(dim, -by), m - FAR)
        src = self.source(k) if s == FIRST and m < FAR else ref
        return remote(src, ref, self.hops, (k, s, m), me.neighbour(dim, by))

    def push(self, k, n):
        me = Torus()
        dim = COLOUR_DIMS[k][THIRD]
        if n < FAR:
            ref = self.piece(me, k, THIRD, me.shift(dim, -toward(n)))
        elif n < ADDED:
            ref = self.piece(me, k, THIRD, me.shift(dim, FAR), n - FAR)
        else:
            ref = self.piece(me, k, THIRD, me.at[dim])
        return remote(ref, ref, self.pushes, (k, n), me.partner())

    def own(self, k):
        me = Torus()
        return pltpu.make_async_copy(self.source(k), self.piece(me, k, FIRST, me.at[COLOUR_DIMS[k][FIRST]]), self.local.at[k])

    def launch(self, s):
        for k in COLOURS:
            for m in WAYS:
                self.hop(k, s, m).start()
            if s == THIRD:
                self.push(k, ADDED).start()

    def relay(self, s):
        for k in COLOURS:
            for m in WAYS:
                self.hop(k, s, m).wait_recv()
                self.hop(k, s, FAR + m).start()
                if s == THIRD:
                    self.push(k, m).start()

    def settle(self, s):
        for k in COLOURS:
            for m in WAYS:
                self.hop(k, s, FAR + m).wait_recv()
                if s == THIRD:
                    self.push(k, FAR + m).start()
            if s == FIRST:
                self.own(k).wait()

    def begin(self):
        for k in COLOURS:
            self.own(k).start()
        self.launch(FIRST)

    def sent(self, *rings):
        for k in COLOURS:
            for s in rings:
                for m in range(ADDED):
                    self.hop(k, s, m).wait_send()
            if THIRD in rings:
                for n in range(ADDED + 1):
                    self.push(k, n).wait()

    def last_ring(self):
        return [functools.partial(f, THIRD) for f in (self.launch, self.relay, self.settle, self.sent)]


def add_into(total, *others):
    lead = total.shape[:-2]

    def body(i, carry):
        idx = []
        for n in reversed(lead):
            idx.insert(0, lax.rem(i, n))
            i = lax.div(i, n)
        value = total[tuple(idx)]
        for other in others:
            value = value + other[tuple(idx)]
        total[tuple(idx)] = value
        return carry

    lax.fori_loop(0, math.prod(lead), body, 0)


class Ring:
    def __init__(self, s, bands, terms, passed, relay, landing, send, recv):
        self.s, self.bands, self.terms, self.passed, self.relay, self.landing = s, bands, terms, passed, relay, landing
        self.sems = (send, recv)

    def zone(self, k, way, half):
        if self.s == THIRD:
            return self.landing.at[k, way, self.bands.cuts(k)[half]]
        return self.bands.rows(self.landing.at[k, way, duo(half)], k)

    def carried(self, ref, k, way):
        if self.s == THIRD:
            return ref.at[k, way, pl.ds(0, self.bands.cuts(k)[way].size)]
        return self.bands.rows(ref.at[k, way], k)

    def hop(self, k, m):
        me = Torus()
        dim = COLOUR_DIMS[k][self.s]
        way, by = m % PAIR, toward(m)
        if m < FAR:
            src, dst = self.terms(k, me.shift(dim, FAR), way), self.carried(self.relay, k, way)
        elif m < ADDED:
            src, dst = self.terms(k, me.shift(dim, by), 1 - way), self.zone(k, way, 1 - way)
        else:
            src, dst = self.carried(self.passed, k, way), self.zone(k, way, way)
        return remote(src, dst, self.sems, (k, m), me.neighbour(dim, by))

    def start(self, k, base):
        for m in WAYS:
            self.hop(k, base + m).start()

    def arrived(self, k, base):
        for m in WAYS:
            self.hop(k, base + m).wait_recv()

    def finish(self):
        for k in COLOURS:
            for m in range(ADDED + PAIR):
                self.hop(k, m).wait_send()

    @staticmethod
    def semaphores():
        return [pltpu.SemaphoreType.DMA((C, ADDED + PAIR))] * PAIR


UNIT = 32
BANDS = {WIDE: ((0, 24), (24, UNIT), (56, UNIT)), DOWN: ((0, UNIT), (UNIT, UNIT), (2 * UNIT, UNIT))}
ORDERS = {WIDE: "xzy", DOWN: "zyx"}


class Bands:
    def __init__(self, kind, half=None):
        self.order, self.bands = ORDERS[kind], BANDS[kind]
        self.width = HALF if half is None else HALF // PAIR
        self.cols = pl.ds(self.width * (half or 0), self.width)

    def band(self, k):
        return pl.ds(*self.bands[k])

    def rows(self, ref, k):
        return ref.at[(ALL,) * (len(ref.shape) - PAIR) + (pl.ds(0, self.bands[k][1]),)]

    def cuts(self, k):
        rows = self.bands[k][1]
        cut = (rows // SUB + 1) // PAIR * SUB
        return pl.ds(0, cut), pl.ds(cut, rows - cut)

    def rest(self, k):
        return [d for d in self.order if d != COLOUR_DIMS[k][FIRST]]

    def units(self, *lead):
        return lead + (UNIT, self.width)

    def vmem(self, *lead):
        return pltpu.VMEM(self.units(*lead), F32)

    def sums(self):
        return sds(F32, *self.units(C, SIDE, SIDE))

    def result(self):
        return sds(F32, *self.units(C))

    def total(self):
        return sds(F32, *self.units(SIDE, C))

    def first(self):
        relays = [self.vmem(C, PAIR, PAIR, SIDE)] * PAIR
        dma = pltpu.SemaphoreType.DMA
        return [self.vmem(C, SIDE, SIDE), *relays, self.vmem(C, PAIR, SIDE, SIDE), *Ring.semaphores(), dma((C, C)), dma((C,))]

    def later(self):
        dma = pltpu.SemaphoreType.DMA
        return [self.vmem(C, SIDE, SIDE), self.vmem(C, PAIR, PAIR), self.vmem(C, PAIR, SIDE),
                pltpu.VMEM((C, PAIR, UNIT // PAIR, self.width), F32), self.vmem(C, PAIR),
                *Ring.semaphores(), *Ring.semaphores(), dma((C,)), dma((C,))]


class First:
    def __init__(self, bands, part, acc, own, passed, relay, landing, send, recv, load, store):
        self.bands, self.part, self.acc, self.own_all, self.passed = bands, part, acc, own, passed
        self.relay_in, self.landing, self.load_sem, self.store_sem = relay, landing, load, store
        self.ring = Ring(FIRST, bands, self.terms, passed, relay, landing, send, recv)

    def own(self, k):
        return self.bands.rows(self.own_all.at[k], k)

    def terms(self, k, v, half=None):
        b = self.bands
        at = {d: ALL for d in b.order}
        at[COLOUR_DIMS[k][FIRST]] = v
        if half is not None:
            at[b.rest(k)[0]] = duo(half)
        return self.part.at[tuple(at[d] for d in b.order) + (b.band(k), b.cols)]

    def load(self, k, m):
        me = Torus()
        dim = COLOUR_DIMS[k][FIRST]
        if m in WAYS:
            src, dst = self.terms(k, me.shift(dim, toward(m)), m), self.ring.carried(self.passed, k, m)
        else:
            src, dst = self.terms(k, me.at[dim]), self.own(k)
        return pltpu.make_async_copy(src, dst, self.load_sem.at[k, m])

    def store(self, k):
        return pltpu.make_async_copy(self.own(k), self.bands.rows(self.acc.at[k], k), self.store_sem.at[k])

    def near(self):
        for k in COLOURS:
            self.ring.start(k, NEAR)

    def far(self):
        for k in COLOURS:
            self.ring.start(k, FAR)
        for m in COLOURS:
            for k in COLOURS:
                self.load(k, m).start()

    def relay(self):
        for k in COLOURS:
            self.ring.arrived(k, NEAR)
            for m in WAYS:
                self.load(k, m).wait()
                add_into(self.ring.carried(self.passed, k, m), self.ring.carried(self.relay_in, k, m))
            self.ring.start(k, ADDED)

    def settle(self, then=None):
        for k in COLOURS:
            self.load(k, FAR).wait()
            for base in (FAR, ADDED):
                self.ring.arrived(k, base)
            add_into(self.own(k), *(self.bands.rows(self.landing.at[k, m], k) for m in WAYS))
            if then is None:
                self.store(k).start()
            else:
                then(k)

    def finish(self):
        self.ring.finish()
        if self.acc is not None:
            for k in COLOURS:
                self.store(k).wait()


class Rest:
    def __init__(self, bands, acc, result, own, relay2, in2, relay3, in3, *sems):
        self.bands, self.acc, self.own, self.result = bands, acc, own, result
        self.in2, self.in3, self.relay2, self.relay3, self.load_sem, self.store_sem = in2, in3, relay2, relay3, *sems[-2:]
        self.second = Ring(SECOND, bands, functools.partial(self.terms, acc), relay2, relay2, in2, *sems[:PAIR])
        self.third = Ring(THIRD, bands, self.final, relay3, relay3, in3, *sems[PAIR:2 * PAIR])

    def terms(self, ref, k, v, half=None):
        other = ALL if half is None else duo(half)
        first = self.bands.rest(k)[0] == COLOUR_DIMS[k][SECOND]
        return self.bands.rows(ref.at[(k, v, other) if first else (k, other, v)], k)

    def final(self, k, v, half=None):
        if half is None:
            return self.bands.rows(self.in2.at[k, 0, v], k)
        return self.in2.at[k, 0, v, self.bands.cuts(k)[half]]

    def load(self, k):
        return pltpu.make_async_copy(self.bands.rows(self.acc.at[k], k), self.bands.rows(self.own.at[k], k), self.load_sem.at[k])

    def store(self, k):
        rows = self.bands.rows
        return pltpu.make_async_copy(rows(self.in3.at[k, 0], k), rows(self.result.at[k], k), self.store_sem.at[k])

    def send(self, k):
        for base in (NEAR, FAR):
            self.second.start(k, base)

    def begin(self):
        for k in COLOURS:
            self.send(k)
        for k in COLOURS:
            self.load(k).start()

    def loaded(self):
        for k in COLOURS:
            self.load(k).wait()

    def relay(self):
        me = Torus()
        for k in COLOURS:
            self.second.arrived(k, NEAR)
            for m in WAYS:
                terms = self.terms(self.own, k, me.shift(COLOUR_DIMS[k][SECOND], toward(m)), m)
                add_into(self.second.carried(self.relay2, k, m), terms)
            self.second.start(k, ADDED)

    def settle(self):
        me = Torus()
        for k in COLOURS:
            for base in (FAR, ADDED):
                self.second.arrived(k, base)
            plus, minus = (self.bands.rows(self.in2.at[k, m], k) for m in WAYS)
            add_into(plus, minus, self.terms(self.own, k, me.at[COLOUR_DIMS[k][SECOND]]))
            for base in (NEAR, FAR):
                self.third.start(k, base)

    def relay_third(self):
        me = Torus()
        for k in COLOURS:
            self.third.arrived(k, NEAR)
            for m in WAYS:
                mine = self.third.carried(self.relay3, k, m)
                mine[...] += self.final(k, me.shift(COLOUR_DIMS[k][THIRD], toward(m)), m)[...]
            self.third.start(k, ADDED)

    def settle_third(self):
        me = Torus()
        for k in COLOURS:
            for base in (FAR, ADDED):
                self.third.arrived(k, base)
            plus, minus = (self.bands.rows(self.in3.at[k, m], k) for m in WAYS)
            plus[...] += minus[...] + self.final(k, me.at[COLOUR_DIMS[k][THIRD]])[...]
            if self.result is not None:
                self.store(k).start()

    def finish(self):
        self.second.finish()
        self.third.finish()
        if self.result is not None:
            for k in COLOURS:
                self.store(k).wait()

    def sums(self):
        return self.in3.at[:, 0]


class Spread:
    def __init__(self, bands, result, total, send, recv, local):
        self.bands, self.result, self.total, self.sems, self.local = bands, result, total, (send, recv), local

    @staticmethod
    def scratch():
        return [pltpu.SemaphoreType.DMA((C, ADDED))] * PAIR + [pltpu.SemaphoreType.DMA((C,))]

    def mine(self, k):
        return self.bands.rows(self.result.at[k], k)

    def place(self, k):
        return self.bands.rows(self.total.at[Torus().at["x"], k], k)

    def hop(self, k, m):
        me = Torus()
        by = toward(m)
        if m < FAR:
            src, dst = self.mine(k), self.place(k)
        else:
            dst = src = self.total.at[me.shift("x", -by), k, self.bands.cuts(k)[m - FAR]]
        return remote(src, dst, self.sems, (k, m), me.neighbour("x", by))

    def own(self, k):
        return pltpu.make_async_copy(self.mine(k), self.place(k), self.local.at[k])

    def begin(self):
        for k in COLOURS:
            if self.local is None:
                self.place(k)[...] = self.mine(k)[...]
            else:
                self.own(k).start()
            for m in WAYS:
                self.hop(k, m).start()

    def forward(self):
        for k in COLOURS:
            for m in WAYS:
                self.hop(k, m).wait_recv()
                self.hop(k, FAR + m).start()

    def finish(self):
        for k in COLOURS:
            for m in WAYS:
                self.hop(k, FAR + m).wait_recv()
            if self.local is not None:
                self.own(k).wait()
            for m in range(ADDED):
                self.hop(k, m).wait_send()


def comm_params(collective_id):
    return pltpu.CompilerParams(collective_id=collective_id, has_side_effects=True, vmem_limit_bytes=VMEM_LIMIT)


def gather_kernel(*refs):
    n = len(Gather.semaphores())
    a, u, d = (Gather(kind, *refs[i::C][:PAIR], *refs[PAIR * C + n * i:][:n]) for i, kind in enumerate((WIDE, WIDE, DOWN)))
    enter()
    for gather in (a, u, d):
        gather.begin()
    for step, *ring in ((a.relay, FIRST), (u.relay, FIRST), (d.relay, FIRST), (a.settle, FIRST), (a.launch, SECOND),
                        (u.settle, FIRST), (u.launch, SECOND), (a.relay, SECOND), (d.settle, FIRST), (d.launch, SECOND),
                        (u.relay, SECOND), (a.settle, SECOND), (a.launch, THIRD), (d.relay, SECOND), (u.settle, SECOND),
                        (a.relay, THIRD), (d.settle, SECOND), (a.settle, THIRD), (u.sent, FIRST, SECOND),
                        (d.sent, FIRST, SECOND), (a.sent, FIRST, SECOND, THIRD)):
        step(*ring)


def gather_call(attn, up, down, collective_id):
    return pl.pallas_call(
        gather_kernel, out_shape=[sds(BF16, *Gather.shape(kind)) for kind in (WIDE, WIDE, DOWN)], in_specs=[ANY] * C,
        out_specs=[ANY] * C, scratch_shapes=Gather.semaphores() * C, compiler_params=comm_params(collective_id),
        name="gather")(attn, up, down)


class Background:
    def __init__(self, steps, plan):
        self.steps, self.plan = steps, plan

    def visit(self, place):
        for j, first, end in self.plan.get(place, ()):
            @at_step(j)
            def _():
                for step in self.steps[first:end]:
                    step()


class Feed:
    def __init__(self, block, steps, buffers, sems):
        self.block, self.steps, self.buffers, self.sems = block, steps, buffers, sems

    @staticmethod
    def scratch(dtype, *shape):
        return [pltpu.VMEM((PAIR,) + shape, dtype), pltpu.SemaphoreType.DMA((PAIR,))]

    def copy(self, j):
        slot = lax.rem(j, PAIR)
        return pltpu.make_async_copy(self.block(j), self.buffers.at[slot], self.sems.at[slot])

    def get(self, j):
        pl.when(j + 1 < self.steps)(lambda: self.copy(j + 1).start())
        self.copy(j).wait()
        return self.buffers.at[lax.rem(j, PAIR)]


def first_feeds(*feeds):
    @at_step(0)
    def _():
        for feed in feeds:
            feed.copy(0).start()


class Share:
    def __init__(self, mine, theirs, place, sems, slot):
        self.local = pltpu.make_async_copy(mine, place, sems[PAIR].at[slot])
        self.far = remote(theirs, place, sems, slot, Torus().partner())

    def start(self):
        self.far.start()
        self.local.start()

    def sent(self):
        self.local.wait()
        self.far.wait_send()

    def wait(self):
        self.sent()
        self.far.wait_recv()


class Push:
    def __init__(self, src, tail, rows, sems, slot=0):
        body = BODY * len(SEQ_PAIR)
        tails = TAIL * len(SEQ_PAIR)
        self.copies = [
            remote(src.at[pl.ds(start, size)], rows.at[pl.ds(to, size)], sems, (slot, i), Torus().partner())
            for i, (start, to, size) in enumerate(((0, body, body), (tail, PAIR * body + tails, tails)))]

    @staticmethod
    def semaphores(n):
        return [pltpu.SemaphoreType.DMA((n, PAIR))] * PAIR

    def start(self):
        for copy in self.copies:
            copy.start()

    def wait(self):
        for copy in self.copies:
            copy.wait_recv()

    def finish(self):
        for copy in self.copies:
            copy.wait_send()


class Exchange:
    def __init__(self, mine, theirs, rows, sems, slot):
        self.moves = []
        for s in SEQ_PAIR:
            for i, (start, size) in enumerate(((0, BODY), (BODY, TAIL))):
                place = lambda n: rows.at[pl.ds(start * len(SEQ_PAIR) * PAIR + size * n, size)]
                part = pl.ds(TOK * s + start, size)
                at = slot + (PAIR * s + i,)
                local = pltpu.make_async_copy(mine.at[part], place(s), sems[2].at[at])
                far = remote(theirs.at[part], place(len(SEQ_PAIR) + s), sems, at, Torus().partner())
                self.moves.append((local, far))

    @staticmethod
    def semaphores(*lead):
        return [pltpu.SemaphoreType.DMA(lead + (2 * PAIR,))] * 3

    def start(self):
        for local, far in self.moves:
            far.start()
            local.start()

    def wait(self):
        for local, far in self.moves:
            local.wait()
            far.wait_recv()

    def finish(self):
        for _, far in self.moves:
            far.wait_send()


NT = (((1,), (1,)), ((), ()))
TN = (((0,), (0,)), ((), ()))


def dot(a, b):
    return jnp.dot(a, b, preferred_element_type=F32)


def dot_nt(a, b):
    return lax.dot_general(a, b, NT, preferred_element_type=F32)


def dot_tn(a, b):
    return lax.dot_general(a, b, TN, preferred_element_type=F32)


def zeros_but(n, axis, value):
    return tuple(value if i == axis else 0 for i in range(n))


def whole(*shape):
    return pl.BlockSpec(shape, lambda *_: (0,) * len(shape))


def along(axis, *block, index=lambda j: j):
    return pl.BlockSpec(block, lambda j: zeros_but(len(block), axis, index(j)))


def row(vec, i):
    return vec[i:i + 1]


def row_mean(t):
    return jnp.mean(t, axis=-1, keepdims=True)


def norm_stats(t):
    centered = t - row_mean(t)
    rstd = lax.rsqrt(row_mean(centered * centered) + LN_EPS)
    return centered * rstd, rstd


def norm_back(xhat, rstd, g):
    return rstd * (g - row_mean(g) - xhat * row_mean(g * xhat))


def col_sum(t):
    return jnp.sum(t, axis=0, keepdims=True)


def at_step(j):
    return pl.when(pl.program_id(0) == j)


def accumulate(ref, value):
    @at_step(0)
    def _():
        ref[...] = value

    @pl.when(pl.program_id(0) > 0)
    def _():
        ref[...] += value


def pad(t):
    return jnp.concatenate([t.astype(F32), jnp.zeros((TOK - SEQ, t.shape[1]), F32)], axis=0).astype(BF16)


WINDOW = 2 * LANES


def window(h):
    first = h * HEAD
    start = jnp.minimum(lax.div(first, LANES) * LANES, D - WINDOW)
    lane = lax.broadcasted_iota(jnp.int32, (1, WINDOW), 1) + (start - first)
    return pl.ds(pl.multiple_of(start, LANES), WINDOW), (lane >= 0) & (lane < HEAD)


def each_head(body, unroll):
    def trip(i, carry):
        for n in range(unroll):
            body(i * unroll + n)
        return carry

    lax.fori_loop(0, HEADS // unroll, trip, 0)


def each_seq(body):
    def trip(s, carry):
        start = pl.multiple_of(s * TOK, TAIL)
        body(s, pl.ds(start, TOK), pl.ds(start, SEQ))
        return carry

    lax.fori_loop(0, len(SEQ_PAIR), trip, 0)


def only(mask, t):
    return jnp.where(mask, t, jnp.zeros_like(t))


def softmax(scores):
    e = jnp.exp(scores - jnp.max(scores, axis=-1, keepdims=True))
    return e * (1.0 / jnp.sum(e, axis=-1, keepdims=True))


def attention(s, rows, o, acc, visit):
    acc[...] = jnp.zeros_like(acc)
    start = pl.multiple_of(s * TOK, TAIL)
    tokens = pl.ds(start, SEQ)

    def head(h):
        lanes, mask = window(h)
        k = only(mask, rows[K, tokens, lanes])
        v = only(mask, rows[V, tokens, lanes])
        probs = softmax(dot_nt(rows[Q, tokens, lanes], k) * SCALE).astype(BF16)
        acc[:, lanes] += dot(probs, v)

    each_head(head, PAIR)
    visit("half")
    o[pl.ds(start, TOK)] = pad(acc[...])


FRONT_PLAN = {"start": ((0, 0, 1),), "half": ((O + 1, 1, 2),), "end": ((O + 1, 2, None),)}


def front_kernel(x_in, w_in, b, vec, _, qkv, h1, o, att, h2, up, rows, lhs, acc, x, x_sem, w_rows, w_sems, *sems):
    hosted = Background(Gather(WIDE, None, up, *sems).last_ring(), FRONT_PLAN)
    j = pl.program_id(0)
    weights = Feed(lambda n: w_in.at[n, :, pl.ds(0, D)], SIDE, w_rows, w_sems)
    fetch = pltpu.make_async_copy(x_in, x, x_sem)
    at_step(0)(fetch.start)
    first_feeds(weights)
    at_step(0)(enter)
    hosted.visit("start")

    @at_step(0)
    def _():
        fetch.wait()

        def norm(s, tile, tokens):
            xhat, _ = norm_stats(x[s].astype(F32))
            h1[tile] = pad(xhat * row(vec, G1) + row(vec, C1))

        each_seq(norm)
        lhs[...] = h1[...]

    @pl.when(j >= O)
    def _():
        attention(j - O, rows, o, acc, hosted.visit)
        lhs[...] = o[...]

    @pl.when((j < O) | (j == O + LAST_SEQ))
    def _():
        bias = jnp.where(j < O, b[0], row(vec, BO))
        att[...] = dot(lhs[...], weights.get(jnp.minimum(j, O))[...]) + bias

    @pl.when(j < O)
    def _():
        t = att[...].astype(BF16)
        qkv[0] = t
        rows[j] = t

    @at_step(O + LAST_SEQ)
    def _():
        def norm(s, tile, tokens):
            xhat, _ = norm_stats(x[s].astype(F32) + row(vec, S1) * att[tokens])
            h2[tile] = pad(xhat * row(vec, G2) + row(vec, C2))

        each_seq(norm)

    hosted.visit("end")


def upto(n):
    return lambda j: jnp.minimum(j, n)


def front_call(x, w_attn, b_qkv, vec, up, collective_id):
    return pl.pallas_call(
        front_kernel, grid=(O + PAIR,),
        out_shape=(sds(BF16, O, TT, D), sds(BF16, TT, D), sds(BF16, TT, D), sds(F32, TT, D), sds(BF16, TT, D),
                   sds(BF16, *Gather.shape(WIDE))),
        in_specs=[ANY, ANY, along(0, 1, 1, D, index=upto(V)), whole(8, D), ANY],
        out_specs=(along(0, 1, TT, D, index=upto(V)),) + (whole(TT, D),) * SIDE + (ANY,),
        scratch_shapes=[pltpu.VMEM((O, TT, D), BF16), pltpu.VMEM((TT, D), BF16), pltpu.VMEM((SEQ, D), F32),
                        pltpu.VMEM(SEQS, BF16), pltpu.SemaphoreType.DMA] + Feed.scratch(BF16, D, D) + Gather.semaphores(),
        input_output_aliases={SIDE: SIDE + 1},
        compiler_params=comm_params(collective_id), name="front",
    )(x, w_attn, b_qkv, vec, up)


TILES = FF // HALF
OWN_BODY = BODY * len(SEQ_PAIR)
TAILS = ROWS - TAIL * PAIR * len(SEQ_PAIR)


def put_rows(ref, tail, s, t):
    ref[pl.ds(pl.multiple_of(BODY * s, BODY), BODY)] = t[:BODY]
    ref[pl.ds(pl.multiple_of(tail + TAIL * s, TAIL), TAIL)] = t[BODY:]


DOWN_PLAN = {"start": ((0, 0, 1),), "end": ((TILES + 2, 1, 2), (2 * TILES - 1, 2, None))}


def mlp_in_kernel(h2_in, gz_in, up_in, b_up, vec, _, act, slope, d_down, down, a_rows, b_rows, b_away, *sems):
    (h2, gz, h2_sem, gz_sem, *tiles), sems = sems[:SIDE + PAIR], sems[SIDE + PAIR:]
    feed = Feed(lambda n: up_in.at[lax.div(n, PAIR), :, tile_cols(lax.rem(n, PAIR))], TILES, *tiles)
    fetches = [pltpu.make_async_copy(*move) for move in ((gz_in, gz, gz_sem), (h2_in, h2, h2_sem))]
    for move in fetches:
        at_step(0)(move.start)
    first_feeds(feed)
    a_sems, b_sems, sems = sems[:PAIR], sems[PAIR:2 * PAIR], sems[2 * PAIR:]
    hosted = Background(Gather(DOWN, None, down, *sems).last_ring(), DOWN_PLAN)
    j = pl.program_id(0)
    away = Push(b_away, OWN_BODY, b_rows, b_sems, 0)
    tile = lambda n: Push(a_rows.at[n], TAILS, a_rows.at[n], a_sems, n)
    at_step(0)(enter)
    hosted.visit("start")

    @at_step(0)
    def _():
        for move in fetches:
            move.wait()
        first = Torus().at["c"] == 0
        def scale(s, tile, tokens):
            d = pad(gz[s].astype(F32) * row(vec, S2))
            left, right = d[:, :HALF], d[:, D - HALF:]
            put_rows(b_rows, TAILS, s, jnp.where(first, left, right))
            put_rows(b_away, OWN_BODY, s, jnp.where(first, right, left))

        each_seq(scale)

    at_step(1)(away.start)
    for n in range(TILES):
        at_step(n + 1)(tile(n).start)

    @pl.when(j < TILES)
    def _():
        u = dot(h2[...], feed.get(j)[...]) + b_up[0]
        phi = 0.5 * (1.0 + lax.erf(u * math.sqrt(0.5)))
        slope[...] = phi + u * (jnp.exp(-0.5 * u * u) * math.sqrt(0.5 / math.pi))
        place = lax.rem(lax.broadcasted_iota(jnp.int32, (TT, 1), 0), TOK)
        a = only(place < SEQ, u * phi).astype(BF16)
        act[...] = a
        for s in SEQ_PAIR:
            put_rows(a_rows.at[j], TAILS, s, a[TOK * s:TOK * s + TOK])

    at_step(TILES)(away.wait)
    for n in range(TILES):
        at_step(TILES + n)(tile(n).wait)

    @pl.when(j >= TILES)
    def _():
        d_down[...] = dot_tn(a_rows[j - TILES], b_rows[...])

    hosted.visit("end")

    @at_step(2 * TILES - 1)
    def _():
        away.finish()
        for n in range(TILES):
            tile(n).finish()


def mlp_in_call(h2, gz, w_up, b_up, vec, down, collective_id):
    low = lambda j: jnp.minimum(j, TILES - 1)
    high = lambda j: jnp.maximum(j - TILES, 0)
    return pl.pallas_call(
        mlp_in_kernel, grid=(2 * TILES,),
        out_shape=(sds(BF16, TT, FF), sds(F32, TT, FF), sds(F32, FF, HALF), sds(BF16, *Gather.shape(DOWN))),
        in_specs=[ANY] * O + [along(0, 1, 1, HALF, index=low), whole(8, D), ANY],
        out_specs=(along(1, TT, HALF, index=low), along(1, TT, HALF, index=low),
                   along(0, HALF, HALF, index=high), ANY),
        scratch_shapes=[pltpu.VMEM((TILES, ROWS, HALF), BF16), pltpu.VMEM((ROWS, HALF), BF16),
                        pltpu.VMEM((PAIR * TOK, HALF), BF16), pltpu.VMEM((TT, D), BF16), pltpu.VMEM(SEQS, BF16),
                        pltpu.SemaphoreType.DMA, pltpu.SemaphoreType.DMA] + Feed.scratch(BF16, D, HALF) + Push.semaphores(TILES) + Push.semaphores(1) +
        Gather.semaphores(),
        input_output_aliases={SIDE + 1: O},
        compiler_params=comm_params(collective_id), name="mlp_in",
    )(h2, gz, w_up, b_up.reshape(TILES, 1, HALF), vec, down)


def tile_cols(n):
    return pl.ds(pl.multiple_of(n * HALF, HALF), HALF)


MLP_PLAN = {"start": ((0, 0, 1),), "end": ((1, 1, 2), (3, 2, 3), (TILES - 1, 3, None))}


def mlp_out_kernel(act_in, slope_in, gz, up_in, down_in, vec, part, d_pre, db_up, mlp_out, d_out, sums, dm, mlp, d_h2, mlp_sem,
                   d_sem, *scratch):
    scratch, tiles = scratch[:-8], scratch[-8:]
    stores = [pltpu.make_async_copy(*move) for move in ((mlp, mlp_out, mlp_sem), (d_h2, d_out, d_sem))]
    first = First(Bands(DOWN), part, sums, *scratch)
    hosted = Background([first.near, first.far, first.relay, first.settle, first.finish], MLP_PLAN)
    j = pl.program_id(0)
    blocks = (lambda n: act_in.at[:, tile_cols(n)], lambda n: slope_in.at[:, tile_cols(n)],
              lambda n: up_in.at[lax.div(n, PAIR), :, tile_cols(lax.rem(n, PAIR))], lambda n: down_in.at[tile_cols(n)])
    feeds = [Feed(block, TILES, *tiles[PAIR * i:][:PAIR]) for i, block in enumerate(blocks)]
    first_feeds(*feeds)
    at_step(0)(enter)
    hosted.visit("start")

    @at_step(0)
    def _():
        def scale(s, tile, tokens):
            dm[tile] = pad(gz[s].astype(F32) * row(vec, S2))

        each_seq(scale)

    act, slope, w_up, w_down = (feed.get(j) for feed in feeds)
    db_up[0] = jnp.zeros((1, HALF), F32)

    def back(s, tile, tokens):
        accumulate(mlp.at[tile], dot(act[tile], w_down[...]))
        d = dot_nt(dm[tile], w_down[...]) * slope[tile]
        db_up[0] += col_sum(d)
        d = d.astype(BF16)
        d_pre[0, 0, tile] = d
        accumulate(d_h2.at[tile], dot_nt(d, w_up[...]))

    each_seq(back)
    for move in stores:
        at_step(TILES - 1)(move.start)
    hosted.visit("end")
    for move in stores:
        at_step(TILES - 1)(move.wait)


def mlp_out_call(act, slope, gz, w_up, w_down, vec, part, collective_id):
    return pl.pallas_call(
        mlp_out_kernel, grid=(TILES,),
        out_shape=(sds(BF16, PAIR, SIDE, TT, HALF), sds(F32, TILES, 1, HALF), sds(F32, TT, D), sds(F32, TT, D),
                   Bands(DOWN).sums()),
        in_specs=[ANY, ANY, whole(*SEQS), ANY, ANY, whole(8, D), ANY],
        out_specs=(pl.BlockSpec((1, 1, TT, HALF), lambda j: (j % PAIR, j // PAIR, 0, 0)), along(0, 1, 1, HALF),
                   ANY, ANY, ANY),
        scratch_shapes=[pltpu.VMEM((TT, D), BF16), pltpu.VMEM((TT, D), F32), pltpu.VMEM((TT, D), F32),
                        pltpu.SemaphoreType.DMA, pltpu.SemaphoreType.DMA] + Bands(DOWN).first() + Feed.scratch(BF16, TT, HALF) +
        Feed.scratch(F32, TT, HALF) + Feed.scratch(BF16, D, HALF) + Feed.scratch(BF16, HALF, D),
        compiler_params=comm_params(collective_id), name="mlp_out",
    )(act, slope, gz, w_up, w_down, vec, part)


def halves_of(t):
    t = pad(t)
    return t[:, :HALF], jnp.concatenate([t[:, HALF:], jnp.zeros((TOK, QCOLS - D), BF16)], axis=1)


def mid(mlp, d_h2, att, x, gz, w_out, vec, z, g_res, d_att, d_o, sums):
    a = att[:SEQ]
    y = x[...].astype(F32) + row(vec, S1) * a
    m = mlp[:SEQ] + row(vec, B2)
    g = gz[...].astype(F32)
    z[0] = (y + row(vec, S2) * m).astype(BF16)
    xhat, rstd = norm_stats(y)
    dh = d_h2[:SEQ]
    gr = g + norm_back(xhat, rstd, dh * row(vec, G2))
    g_res[:SEQ] = gr
    da = gr * row(vec, S1)
    terms = (da, gr * a, dh * xhat, dh, g * row(vec, S2), g * m)
    accumulate(sums, jnp.concatenate([jnp.zeros((BO, D), F32)] + [col_sum(t) for t in terms], axis=0))
    for i, t in enumerate(halves_of(da)):
        d_att[i] = t
    d_o[...] = dot_nt(pad(da), w_out[...]).astype(BF16)


def attention_back(s, qkv, d_o, d_qkv, db, acc, b_rows, away, first, visit):
    acc[...] = jnp.zeros_like(acc)

    def head(h):
        lanes, mask = window(h)
        q, k, v = (only(mask, qkv[i, :SEQ, lanes]) for i in (Q, K, V))
        do = only(mask, d_o[:SEQ, lanes])
        scores = dot_nt(k, q) * SCALE
        e = jnp.exp(scores - jnp.max(scores, axis=0, keepdims=True))
        probs = e * (1.0 / col_sum(e))
        acc[V, :, lanes] += dot(probs.astype(BF16), do)
        dp = dot_nt(v, do)
        ds = probs * (dp - col_sum(dp * probs))
        ds = (ds * SCALE).astype(BF16)
        acc[K, :, lanes] += dot(ds, q)
        acc[Q, :, lanes] += dot_tn(ds, k)

    each_head(head, PAIR)
    visit("half")
    accumulate(db, jnp.concatenate([col_sum(acc[i]) for i in (Q, K, V)], axis=0))
    for n in (Q, K, V):
        left, right = halves_of(acc[n])
        d_qkv[0, n] = left
        d_qkv[1, n] = right
        put_rows(b_rows.at[n], TAILS, s, jnp.where(first, left, right))
        put_rows(away.at[n], OWN_BODY, s, jnp.where(first, right, left))


PER = HALF // STEP


class WideGrads:
    def __init__(self, inputs, a_of, cotangents, out, base, lead, a_rows, a_cols, b_rows):
        self.inputs, self.a_of, self.cotangents, self.out, self.base, self.lead = inputs, a_of, cotangents, out, base, lead
        self.a_rows, self.a_cols, self.b_rows = a_rows, a_cols, b_rows

    @staticmethod
    def scratch(inputs):
        return [pltpu.VMEM((inputs, ROWS, D), BF16), pltpu.VMEM((inputs, D, ROWS), BF16), pltpu.VMEM((SIDE, ROWS, HALF), BF16)]

    def turn(self, i):
        def trip(n, carry):
            lanes = pl.ds(pl.multiple_of(n * LANES, LANES), LANES)
            self.a_cols[i, lanes] = self.a_rows[i, :, lanes].T
            return carry

        lax.fori_loop(0, D // LANES, trip, 0)

    def step(self):
        j = pl.program_id(0)
        done = []
        for t in range(SIDE):
            n = (t + self.lead) % SIDE

            @at_step(self.base + PER * t)
            def _():
                i = self.a_of[n]
                if i not in done:
                    self.inputs[i].wait()
                    self.turn(i)
                    done.append(i)
                self.cotangents[n].wait()

        @pl.when(j >= self.base)
        def _():
            n = lax.rem(lax.div(j - self.base, PER) + self.lead, SIDE)
            cols = pl.ds(pl.multiple_of(lax.rem(j - self.base, PER) * STEP, STEP), STEP)
            i = 0 if len(self.inputs) == 1 else lax.div(n, O)
            self.out[0] = dot(self.a_cols[i], self.b_rows[n, :, cols])

    def finish(self):
        for move in (*self.inputs, *self.cotangents):
            move.finish()


def grads_block(base, lead):
    def index(j):
        n = jnp.maximum(j - base, 0)
        return (n // PER + lead) % SIDE, 0, n % PER

    return pl.BlockSpec((1, D, STEP), index)


GRAD_STEPS = PER * SIDE


def tok_block():
    return along(0, TOK, D, index=upto(LAST_SEQ))


def seq_block():
    return along(0, 1, SEQ, D, index=upto(LAST_SEQ))


MID_PLAN = {"start": ((0, 0, 1),), "end": ((1, 1, 3), (8, 3, 4), (11, 4, 5), (LAST_SEQ + GRAD_STEPS, 5, None))}


def mid_kernel(*refs):
    refs = list(refs)
    take = lambda n: [refs.pop(0) for _ in range(n)]
    ins, (w_attn, vec), (h2, d_pre, acc), outs, (d_up, result) = take(5), take(2), take(3), take(5), take(2)
    tiles, (w_out, w_sem) = [take(PAIR) for _ in ins], take(PAIR)
    tokens = lambda n: pl.ds(pl.multiple_of(n * TOK, TAIL), TOK)
    feeds = [Feed(lambda n, ref=ref: ref.at[tokens(n) if len(ref.shape) == PAIR else n], SEQS[0], *tile)
             for ref, tile in zip(ins, tiles)]
    fetch = pltpu.make_async_copy(w_attn.at[O, :, pl.ds(0, D)], w_out, w_sem)
    first_feeds(*feeds)
    at_step(0)(fetch.start)
    rows, a_sems, b_sems = take(3), take(C), take(C)
    rest = Rest(Bands(DOWN), acc, result, *refs)
    hosted = Background([rest.begin, rest.loaded, rest.relay, rest.settle, rest.relay_third, rest.settle_third, rest.finish],
                        MID_PLAN)
    c = Torus().at["c"]
    grads = WideGrads(
        [Exchange(h2, h2, rows[0].at[0], a_sems, ())], (0,) * SIDE,
        [Exchange(d_pre.at[c, n], d_pre.at[1 - c, n], rows[2].at[n], b_sems, (n,)) for n in range(SIDE)], d_up, SEQS[0], 0, *rows)
    at_step(0)(enter)
    hosted.visit("start")

    @at_step(0)
    def _():
        for move in (*grads.inputs, *grads.cotangents):
            move.start()

    j = pl.program_id(0)

    @pl.when(j < SEQS[0])
    def _():
        blocks = [feed.get(j) for feed in feeds]
        at_step(0)(fetch.wait)
        mid(*blocks, w_out, vec, *outs)

    grads.step()
    hosted.visit("end")
    at_step(LAST_SEQ + GRAD_STEPS)(grads.finish)


def mid_call(mlp, d_h2, att, x, gz, vec, w_attn, h2, d_pre, acc, collective_id):
    return pl.pallas_call(
        mid_kernel, grid=(SEQS[0] + GRAD_STEPS,),
        out_shape=(sds(BF16, *SEQS), sds(F32, TT, D), sds(BF16, PAIR, TT, HALF), sds(BF16, TT, D), sds(F32, 8, D),
                   sds(F32, SIDE, D, HALF), Bands(DOWN).result()),
        in_specs=[ANY] * (O + O) + [whole(8, D)] + [ANY] * O,
        out_specs=(seq_block(), tok_block(), along(1, PAIR, TOK, HALF, index=upto(LAST_SEQ)), tok_block(), whole(8, D),
                   grads_block(SEQS[0], 0), ANY),
        scratch_shapes=Feed.scratch(F32, TOK, D) * O + Feed.scratch(BF16, SEQ, D) * PAIR +
        [pltpu.VMEM((D, D), BF16), pltpu.SemaphoreType.DMA] + WideGrads.scratch(1) + Exchange.semaphores() + Exchange.semaphores(SIDE) +
        Bands(DOWN).later(),
        compiler_params=comm_params(collective_id), name="mid",
    )(mlp, d_h2, att, x, gz, w_attn, vec, h2, d_pre, acc)


ATTN_PLAN = {"start": ((0, 0, 2),), "half": ((0, 2, 4),), "end": ((SIDE, 4, 5), (LAST_SEQ + GRAD_STEPS, 5, None))}


def attn_back_kernel(*refs):
    refs = list(refs)
    take = lambda n: [refs.pop(0) for _ in range(n)]
    (qkv_in, do_in), (h1, o, d_att, part, result), (d_qkv, db, d_attn, sums, total) = take(2), take(5), take(5)
    acc, away, rows, tiles = refs.pop(0), refs.pop(0), take(3), take(SIDE)
    tokens = lambda n: pl.ds(pl.multiple_of(n * TOK, TAIL), TOK)
    feeds = [Feed(lambda n: qkv_in.at[:, tokens(n)], SEQS[0], *tiles[:PAIR]),
             Feed(lambda n: do_in.at[tokens(n)], SEQS[0], *tiles[PAIR:])]
    first_feeds(*feeds)
    a_sems, b_sems, away_sems = take(C), take(C), take(PAIR)
    first = First(Bands(WIDE), part, sums, *take(len(Bands(WIDE).first())))
    spread = Spread(Bands(DOWN), result, total, *refs)
    hosted = Background([spread.begin, first.near, first.far, spread.forward, first.relay, first.settle, first.finish,
                         spread.finish], ATTN_PLAN)
    c = Torus().at["c"]
    pushes = [Push(away.at[n], OWN_BODY, rows[2].at[n], away_sems, n) for n in range(O)]
    grads = WideGrads(
        [Exchange(a, a, rows[0].at[i], a_sems, (i,)) for i, a in enumerate((h1, o))], (0,) * O + (1,),
        pushes + [Exchange(d_att.at[c], d_att.at[1 - c], rows[2].at[O], b_sems, ())], d_attn, SEQS[0], O, *rows)
    at_step(0)(enter)
    hosted.visit("start")

    @at_step(0)
    def _():
        for move in (*grads.inputs, grads.cotangents[O]):
            move.start()

    @at_step(SEQS[0])
    def _():
        for push in pushes:
            push.start()

    j = pl.program_id(0)

    @pl.when(j < SEQS[0])
    def _():
        qkv, d_o = (feed.get(j) for feed in feeds)
        attention_back(j, qkv, d_o, d_qkv, db, acc, rows[2], away, c == 0, hosted.visit)


    grads.step()
    hosted.visit("end")
    at_step(LAST_SEQ + GRAD_STEPS)(grads.finish)


def attn_back_call(qkv, d_o, h1, o, d_att, part, result, collective_id):
    return pl.pallas_call(
        attn_back_kernel, grid=(SEQS[0] + GRAD_STEPS,),
        out_shape=(sds(BF16, PAIR, O, TT, HALF), sds(F32, O, D), sds(F32, SIDE, D, HALF), Bands(WIDE).sums(),
                   Bands(DOWN).total()),
        in_specs=[ANY] * 7,
        out_specs=(along(2, PAIR, O, TOK, HALF, index=upto(LAST_SEQ)), whole(O, D), grads_block(SEQS[0], O), ANY, ANY),
        scratch_shapes=[pltpu.VMEM((O, SEQ, D), F32), pltpu.VMEM((O, PAIR * TOK, HALF), BF16)] + WideGrads.scratch(2) +
        Feed.scratch(BF16, O, TOK, D) + Feed.scratch(BF16, TOK, D) + Exchange.semaphores(PAIR) + Exchange.semaphores() + Push.semaphores(O) + Bands(WIDE).first() + Spread.scratch(),
        compiler_params=comm_params(collective_id), name="attn_back",
    )(qkv, d_o, h1, o, d_att, part, result)


IN_STEPS = PAIR * O
SLOT = 40
LAST_PLAN = {"start": ((0, 0, 2),), "end": ((O, 2, None),)}


CORE_COLS = D - HALF
KEPT = 48
GRADS = ((KEPT, O * D), (KEPT, D), (KEPT, FF), (PAIR, C, UNIT, D), (SIDE, KEPT, LANES))
SHARES = PAIR * SIDE + SIDE + PAIR


def split_rows(totals, first, keep, give):
    def trip(x, carry):
        for total, bands in totals:
            rows = jnp.concatenate([total[x, k, :n] for k, (_, n) in enumerate(BANDS[WIDE])], axis=0)
            low, high = rows[:KEPT], jnp.concatenate([rows[OWN:], rows[:KEPT - OWN]], axis=0)
            keep[x, :, bands.cols] = jnp.where(first, low, high)
            give[x, :, bands.cols] = jnp.where(first, high, low)
        return carry

    lax.fori_loop(0, SIDE, trip, 0)


class Finals:
    def __init__(self, down, up, attn, outs, sems):
        self.c = Torus().at["c"]
        self.down, self.up, self.attn, self.sems = down, up, attn, sems
        self.qkv, self.out, self.up_out, self.down_out, self.pad = outs
        self.edge = pl.ds(CORE_COLS, LANES)

    def cols(self, base, width):
        return pl.ds(pl.multiple_of(base + self.c * HALF, LANES), width)

    def up_share(self, x):
        place = self.up_out.at[:, self.cols(QCOLS * x, HALF)]
        return Share(*(ref.at[x] for ref in self.up), place, self.sems, x)

    def block(self, x):
        return (self.out, 0) if x == O else (self.qkv, D * x)

    def attn_share(self, x):
        out, base = self.block(x)
        sides = (ref.at[x, :, pl.ds(0, CORE_COLS)] for ref in self.attn)
        return Share(*sides, out.at[:, self.cols(base, CORE_COLS)], self.sems, SIDE + x)

    def edge_share(self, x, padding):
        out, base = self.block(x)
        place = self.pad.at[x] if padding else out.at[:, pl.ds(base + CORE_COLS, LANES)]
        return Share(*(ref.at[x, :, self.edge] for ref in self.attn), place, self.sems, PAIR * SIDE + x)

    def down_share(self, edge):
        src = self.edge if edge else pl.ds(pl.multiple_of(self.c * LANES, LANES), CORE_COLS)
        sides = (self.down.at[pl.ds(PAIR * c, PAIR), :, :, src] for c in (self.c, 1 - self.c))
        place = self.down_out.at[:, :, :, self.edge if edge else self.cols(0, CORE_COLS)]
        return Share(*sides, place, self.sems, SHARES - PAIR + edge)

    def start_down(self):
        self.down_share(0).start()
        pl.when(self.c == 0)(lambda: self.down_share(1).start())

    def start(self):
        for x in range(SIDE):
            self.attn_share(x).start()
            pl.when(self.c == 0)(lambda: self.edge_share(x, False).start())
            pl.when(self.c == 1)(lambda: self.edge_share(x, True).start())

    def finish(self):
        for x in range(SIDE):
            for share in (self.up_share(x), self.attn_share(x), self.edge_share(x, True)):
                share.wait()
        self.down_share(0).wait()
        pl.when(self.c == 0)(lambda: self.down_share(1).sent())
        pl.when(self.c == 1)(lambda: self.down_share(1).far.wait_recv())


def last_kernel(*refs):
    refs = list(refs)
    take = lambda n: [refs.pop(0) for _ in range(n)]
    (d_qkv, w_attn, x_in, g_in, vec), (small, acc_up, down, _), (dx_out, part) = take(5), take(SIDE), take(PAIR)
    outs, (x, g_res, dx, x_sem, g_sem, dx_sem), tiles = take(len(GRADS)), take(SIDE + PAIR), take(SIDE)
    j = pl.program_id(0)
    fetches = [pltpu.make_async_copy(*move) for move in ((x_in, x, x_sem), (g_in, g_res, g_sem))]
    store = pltpu.make_async_copy(dx, dx_out, dx_sem)
    feeds = [Feed(lambda n: d_qkv.at[lax.rem(n, PAIR), lax.div(n, PAIR)], IN_STEPS, *tiles[:PAIR]),
             Feed(lambda n: w_attn.at[lax.div(n, PAIR), :, pl.ds(pl.multiple_of(lax.rem(n, PAIR) * HALF, HALF), HALF)],
                  IN_STEPS, *tiles[PAIR:])]
    first_feeds(*feeds)
    (acc, sums, pair_sums, block), (totals, sides), block_sem, swap_sems = take(4), (take(C), take(SIDE)), refs.pop(0), take(PAIR)
    finals = Finals(down, sides[:PAIR], sides[PAIR:], outs, take(C))
    halves = [Bands(WIDE, h) for h in WAYS]
    a, b = (First(bands, part, None, *take(len(bands.first()))) for bands in halves)
    rest_a, rest_b = (Rest(f.bands, f.own_all, None, f.own_all, *take(len(f.bands.later()) - 1)) for f in (a, b))
    rest_up = Rest(Bands(WIDE), acc_up, None, *take(len(Bands(WIDE).later())))
    spread_up, spread_a, spread_b = (
        Spread(r.bands, r.sums(), total, *take(PAIR), None) for r, total in zip((rest_up, rest_a, rest_b), totals))
    hosted = Background([rest_up.begin, a.near, rest_up.loaded, rest_up.relay], LAST_PLAN)
    first = finals.c == 0
    swap = remote(sums, pair_sums, swap_sems, (), Torus().partner())
    fetch = pltpu.make_async_copy(small, block, block_sem)
    at_step(0)(enter)
    hosted.visit("start")

    @at_step(0)
    def _():
        for move in (fetch, *fetches):
            move.start()
        finals.start_down()

    @pl.when(j < IN_STEPS)
    def _():
        d_half, w = (feed.get(j) for feed in feeds)
        each_seq(lambda s, tile, tokens: accumulate(acc.at[tile], dot_nt(d_half[tile], w[...])))

    @at_step(IN_STEPS - 1)
    def _():
        for move in fetches:
            move.wait()
        sums[...] = jnp.zeros_like(sums)

        def back(s, tile, tokens):
            xhat, rstd = norm_stats(x[s].astype(F32))
            dh = acc[tokens]
            sums[:BO] += jnp.concatenate([col_sum(dh * xhat), col_sum(dh)], axis=0)
            dx[s] = (g_res[tokens] + norm_back(xhat, rstd, dh * row(vec, G1))).astype(BF16)

        each_seq(back)
        store.start()

    hosted.visit("end")

    @at_step(IN_STEPS)
    def _():
        swap.start()
        fetch.wait()
        swap.wait()
        both = sums[...] + pair_sums[...]
        for d in range(DEVICES):
            at = CHIP * (d // PAIR) + SLOT + OWN * (d % PAIR)
            block[at:at + BO, :OWN] = both[:BO, OWN * d:OWN * d + OWN]

        @pl.when(finals.c == 1)
        def _():
            for z in range(SIDE):
                for y in range(SIDE):
                    rows = block.at[pl.ds(CHIP * (SIDE * z + y), CHIP)]
                    put = pltpu.make_async_copy(rows, part.at[0, z, y, :, pl.ds(CORE_COLS, LANES)], block_sem)
                    put.start()
            pltpu.make_async_copy(block, small, block_sem).wait()

        def share_up():
            spread_up.finish()
            split_rows([(totals[0], Bands(WIDE))], first, *sides[:PAIR])
            for x in range(SIDE):
                finals.up_share(x).start()

        for step in (b.near, rest_up.settle, a.far, rest_up.relay_third, b.far, a.relay, rest_up.settle_third, spread_up.begin,
                     b.relay, spread_up.forward, functools.partial(a.settle, rest_a.send),
                     functools.partial(b.settle, rest_b.send), rest_a.relay, rest_b.relay, rest_a.settle, rest_b.settle,
                     share_up, rest_a.relay_third, rest_b.relay_third, rest_a.settle_third, spread_a.begin,
                     rest_b.settle_third, spread_b.begin, spread_a.forward, spread_b.forward, spread_a.finish, spread_b.finish):
            step()
        split_rows(list(zip(totals[1:], halves)), first, *sides[PAIR:])
        finals.start()
        for user in (rest_up, rest_a, rest_b, a, b, finals):
            user.finish()
        store.wait()


def last_call(d_qkv, w_attn, x, g_res, vec, small, acc_up, down, part, collective_id):
    halves = [Bands(WIDE, h) for h in WAYS]
    dma = pltpu.SemaphoreType.DMA
    rings = [Bands(WIDE), *halves]
    return pl.pallas_call(
        last_kernel, grid=(IN_STEPS + 1,),
        out_shape=(sds(BF16, *SEQS), sds(F32, *part.shape), *(sds(F32, *shape) for shape in GRADS)),
        in_specs=[ANY] * SIDE + [whole(8, D)] + [ANY] * SIDE,
        out_specs=(ANY,) * (len(GRADS) + PAIR),
        scratch_shapes=[pltpu.VMEM(SEQS, BF16), pltpu.VMEM((TT, D), F32), pltpu.VMEM(SEQS, BF16), dma, dma, dma] + Feed.scratch(BF16, TT, HALF) +
        Feed.scratch(BF16, D, HALF) + [pltpu.VMEM((TT, D), F32), pltpu.VMEM((SUB, D), F32), pltpu.VMEM((SUB, D), F32),
                        pltpu.VMEM((D, LANES), F32)] + [r.vmem(SIDE, C) for r in rings] +
        [pltpu.VMEM((SIDE, KEPT, HALF), F32)] * SIDE + [dma, dma, dma] + [dma((SHARES,))] * C + halves[0].first() * PAIR +
        halves[0].later()[1:] * PAIR + Bands(WIDE).later() + Spread.scratch()[:PAIR] * C,
        input_output_aliases={8: 1},
        compiler_params=comm_params(collective_id), name="last",
    )(d_qkv, w_attn, x, g_res, vec, small, acc_up, down, part)


BQ, BU, VEC = 3 * D // 32, 3 * D // 32 + FF // 32, 3 * D // 32 + FF // 32 + 8 * OWN


def pair_swap(a):
    return lax.ppermute(a, "fsdp", [(i, i ^ 1) for i in range(DEVICES)])


def by_core(first, a, b):
    return jnp.where(first, a, b), jnp.where(first, b, a)


def my_pieces(shards, first):
    w_qkv, b_qkv, w_out, w_up, b_up, w_down, vec_params = shards
    x = lax.axis_index("rep")
    small = jnp.concatenate([b_qkv, b_up, vec_params.reshape(-1)])
    small = jnp.pad(small, (0, OWN * LANES - VEC)).reshape(OWN, LANES)
    attn = lax.dynamic_slice_in_dim(jnp.concatenate([w_qkv, w_out], axis=1), x * D, D, 1)
    attn = jnp.concatenate([attn, small], axis=1)
    up = lax.dynamic_slice_in_dim(w_up, x * QCOLS, QCOLS, 1)
    wide = jnp.stack([attn, up]).astype(BF16)
    mine, theirs = by_core(first, wide[..., :HALF], wide[..., HALF:])
    theirs = pair_swap(theirs)
    piece = jnp.concatenate(by_core(first, mine, theirs), axis=1)
    down = lax.dynamic_slice_in_dim(w_down, x * 48, 48, 0).astype(BF16).reshape(3, 16, D)
    return piece[0], piece[1], down


def small_params(w_attn):
    small = w_attn[0, :, D:].astype(F32).reshape(DEVICES, OWN * LANES)
    vec = small[:, BU:VEC].reshape(DEVICES, 8, OWN).transpose(1, 0, 2).reshape(8, D)
    return small[:, :BQ].reshape(O, 1, D), small[:, BQ:BU].reshape(FF), vec


ROOM = 5 * LANES


def small_grads(db_qkv, db_up, sums):
    vec = sums[BO:].reshape(8 - BO, DEVICES, OWN).transpose(1, 0, 2).reshape(DEVICES, VEC - BU - BO * OWN)
    small = jnp.concatenate([db_qkv.reshape(DEVICES, BQ), db_up.reshape(DEVICES, BU - BQ), vec], axis=1)
    small = small + pair_swap(small)
    small = jnp.pad(small, ((0, 0), (0, ROOM - small.shape[1]))).reshape(DEVICES, ROOM // LANES, LANES)
    return jnp.pad(small, ((0, 0), (0, OWN - ROOM // LANES), (0, 0))).reshape(D, LANES)


def device_step(x, gz, *shards):
    first = lax.rem(lax.axis_index("fsdp"), PAIR) == 0
    attn, up, down = my_pieces(shards, first)
    w_attn, up, down = gather_call(attn, up, down, 0)
    w_attn = w_attn.reshape(SIDE, D, QCOLS)
    b_qkv, b_up, vec = small_params(w_attn)
    qkv, h1, o, att, h2, w_up = front_call(x, w_attn, b_qkv, vec, up, 1)
    w_up = w_up.reshape(SIDE, D, QCOLS)
    act, slope, part, w_down = mlp_in_call(h2, gz, w_up, b_up, vec, down, 2)
    part = part.reshape((SIDE,) * 3 + (C * UNIT, HALF))
    d_pre, db_up, mlp, d_h2, acc = mlp_out_call(act, slope, gz, w_up, w_down.reshape(FF, D), vec, part, 3)
    z, g_res, d_att, d_o, sums, part, result = mid_call(mlp, d_h2, att, x, gz, vec, w_attn, h2, d_pre, acc, 4)
    part = part.reshape((SIDE,) * 3 + (CHIP, HALF))
    d_qkv, db_qkv, part, acc, down = attn_back_call(qkv, d_o, h1, o, d_att, part, result, 5)
    small = small_grads(db_qkv, db_up, sums)
    part = part.reshape((SIDE,) * 3 + (CHIP, HALF))
    dx, _, g_qkv, g_out, g_up, g_down, edge = last_call(d_qkv, w_attn, x, g_res, vec, small, acc, down, part, 6)
    small = edge[0, :ROOM // LANES].reshape(ROOM)
    vec = jnp.concatenate([edge[0, SLOT:SLOT + BO, :OWN], small[BU:VEC - BO * OWN].reshape(8 - BO, OWN)], axis=0)
    g_qkv, g_out, g_up = (g[:OWN] for g in (g_qkv, g_out, g_up))
    return z, dx, g_qkv, small[:BQ], g_out, g_up, small[BQ:BU], g_down.reshape(FF // DEVICES, D), vec


def solution(mesh):
    batch = P(("rep", "fsdp"), None, None)
    rows, flat, cols = P("fsdp", None), P("fsdp"), P(None, "fsdp")
    shards = (rows, flat, rows, rows, flat, rows, cols)
    return jax.shard_map(device_step, mesh=mesh, in_specs=(batch, batch) + shards,
                         out_specs=(batch, batch) + shards, check_vma=False)
```

```python
import functools
import math

import jax
import jax.numpy as jnp
from jax import lax
from jax.experimental import pallas as pl
from jax.experimental.pallas import tpu as pltpu
from jax.sharding import PartitionSpec as P

HEADS = 16
LN_EPS = 1e-5
D = 1408
FF = 6144
SEQ = 257
HEAD = D // HEADS
SCALE = HEAD ** -0.5
QCOLS = 1536
HALF = 768
OWN = 44
CHIP = 2 * OWN
LANES = 128
DEVICES = 32
F32 = jnp.float32
BF16 = jnp.bfloat16
VMEM_LIMIT = 66 * 1000 * 1000
G1, C1, BO, S1, G2, C2, B2, S2 = range(8)
Q, K, V, O = range(4)
SEQS = (2, SEQ, D)
LAST_SEQ = SEQS[0] - 1
SEQ_PAIR = range(SEQS[0])
TAIL = 16
BODY = SEQ - 1
TOK = BODY + TAIL
TT = 2 * TOK
ROWS = 4 * TOK
STEP = 256


def sds(dtype, *shape):
    return jax.ShapeDtypeStruct(shape, dtype)


MESH_ID = pl.DeviceIdType.MESH
SIDE = 4
SUB = 8
PAIR = 2
C = 3
COLOURS = range(C)
COLOUR_DIMS = ("xyz", "yzx", "zxy")
FIRST, SECOND, THIRD, LAST = range(4)
WAYS = range(PAIR)
NEAR, FAR, ADDED = 0, 2, 4
WIDE, DOWN = "wide", "down"
ANY = pl.BlockSpec(memory_space=pl.ANY)
ALL = slice(None)


def duo(m):
    return pl.ds(PAIR * m, PAIR)


def toward(m):
    return 1 - PAIR * (m % PAIR)


class Torus:
    def __init__(self):
        f = lax.axis_index("fsdp")
        self.at = {"x": lax.axis_index("rep"), "z": lax.div(f, SIDE * PAIR), "y": lax.rem(lax.div(f, PAIR), SIDE),
                   "c": lax.rem(f, PAIR)}

    def shift(self, dim, by):
        return lax.rem(self.at[dim] + (SIDE + by), SIDE)

    def device(self, **moved):
        p = {**self.at, **moved}
        return (p["x"], (p["z"] * SIDE + p["y"]) * PAIR + p["c"])

    def neighbour(self, dim, by):
        return self.device(**{dim: self.shift(dim, by)})

    def partner(self):
        return self.device(c=1 - self.at["c"])


def enter():
    me = Torus()
    barrier = pltpu.get_barrier_semaphore()
    others = [me.neighbour(d, toward(m)) for d in COLOUR_DIMS[0] for m in WAYS] + [me.partner()]
    for other in others:
        pl.semaphore_signal(barrier, device_id=other, device_id_type=MESH_ID)
    pl.semaphore_wait(barrier, len(others))


def remote(src, dst, sems, slot, device):
    return pltpu.make_async_remote_copy(src_ref=src, dst_ref=dst, send_sem=sems[0].at[slot], recv_sem=sems[1].at[slot],
                                        device_id=device, device_id_type=MESH_ID)


class Gather:
    def __init__(self, kind, src, dst, hop_send, hop_recv, push_send, push_recv, local):
        self.kind, self.src, self.dst, self.local = kind, src, dst, local
        self.hops, self.pushes = (hop_send, hop_recv), (push_send, push_recv)
        self.cols, self.cut = (256, 128) if kind == WIDE else (D, HALF)

    @staticmethod
    def semaphores():
        dma = pltpu.SemaphoreType.DMA
        return [dma((C, C, ADDED))] * PAIR + [dma((C, ADDED + 1))] * PAIR + [dma((C,))]

    @staticmethod
    def shape(kind):
        return (SIDE,) * 3 + (CHIP, QCOLS) if kind == WIDE else (SIDE, SIDE, PAIR, SIDE, C, 16, D)

    def source(self, k):
        return self.src.at[:, pl.ds(self.cols * k, self.cols)] if self.kind == WIDE else self.src.at[k]

    def piece(self, me, k, s, v, half=None):
        dims = COLOUR_DIMS[k]
        at = {**me.at, **{d: ALL for d in dims[:s]}, dims[s]: v}
        off, width = 0, self.cols
        if half is not None and s == FIRST:
            off, width = self.cut * half, (self.cut, self.cols - self.cut)[half]
        elif half is not None:
            at[dims[0]] = duo(half)
        if self.kind == WIDE:
            cols = pl.ds(pl.multiple_of(at["c"] * HALF + self.cols * k + off, 128), width)
            return self.dst.at[at["x"], at["z"], at["y"], :, cols]
        return self.dst.at[at["z"], at["y"], at["c"], at["x"], k, :, pl.ds(off, width)]

    def hop(self, k, s, m):
        me = Torus()
        dim = COLOUR_DIMS[k][s]
        by = toward(m)
        if m < FAR:
            ref = self.piece(me, k, s, me.at[dim])
        else:
            ref = self.piece(me, k, s, me.shift(dim, -by), m - FAR)
        src = self.source(k) if s == FIRST and m < FAR else ref
        return remote(src, ref, self.hops, (k, s, m), me.neighbour(dim, by))

    def push(self, k, n):
        me = Torus()
        dim = COLOUR_DIMS[k][THIRD]
        if n < FAR:
            ref = self.piece(me, k, THIRD, me.shift(dim, -toward(n)))
        elif n < ADDED:
            ref = self.piece(me, k, THIRD, me.shift(dim, FAR), n - FAR)
        else:
            ref = self.piece(me, k, THIRD, me.at[dim])
        return remote(ref, ref, self.pushes, (k, n), me.partner())

    def own(self, k):
        me = Torus()
        return pltpu.make_async_copy(self.source(k), self.piece(me, k, FIRST, me.at[COLOUR_DIMS[k][FIRST]]), self.local.at[k])

    def launch(self, s):
        for k in COLOURS:
            for m in WAYS:
                self.hop(k, s, m).start()
            if s == THIRD:
                self.push(k, ADDED).start()

    def relay(self, s):
        for k in COLOURS:
            for m in WAYS:
                self.hop(k, s, m).wait_recv()
                self.hop(k, s, FAR + m).start()
                if s == THIRD:
                    self.push(k, m).start()

    def settle(self, s):
        for k in COLOURS:
            for m in WAYS:
                self.hop(k, s, FAR + m).wait_recv()
                if s == THIRD:
                    self.push(k, FAR + m).start()
            if s == FIRST:
                self.own(k).wait()

    def begin(self):
        for k in COLOURS:
            self.own(k).start()
        self.launch(FIRST)

    def sent(self, *rings):
        for k in COLOURS:
            for s in rings:
                for m in range(ADDED):
                    self.hop(k, s, m).wait_send()
            if THIRD in rings:
                for n in range(ADDED + 1):
                    self.push(k, n).wait()

    def first_rings(self):
        ring = functools.partial
        return [self.begin, ring(self.relay, FIRST), lambda: (self.settle(FIRST), self.launch(SECOND)),
                ring(self.relay, SECOND), ring(self.settle, SECOND), ring(self.sent, FIRST, SECOND)]

    def last_ring(self):
        return [functools.partial(f, THIRD) for f in (self.launch, self.relay, self.settle, self.sent)]


def add_into(total, *others):
    lead = total.shape[:-2]

    def body(i, carry):
        idx = []
        for n in reversed(lead):
            idx.insert(0, lax.rem(i, n))
            i = lax.div(i, n)
        value = total[tuple(idx)]
        for other in others:
            value = value + other[tuple(idx)]
        total[tuple(idx)] = value
        return carry

    lax.fori_loop(0, math.prod(lead), body, 0)


class Ring:
    def __init__(self, s, bands, terms, passed, relay, landing, send, recv):
        self.s, self.bands, self.terms, self.passed, self.relay, self.landing = s, bands, terms, passed, relay, landing
        self.sems = (send, recv)

    def zone(self, k, way, half):
        if self.s == THIRD:
            return self.landing.at[k, way, self.bands.cuts(k)[half]]
        return self.bands.rows(self.landing.at[k, way, duo(half)], k)

    def carried(self, ref, k, way):
        if self.s == THIRD:
            return ref.at[k, way, pl.ds(0, self.bands.cuts(k)[way].size)]
        return self.bands.rows(ref.at[k, way], k)

    def hop(self, k, m):
        me = Torus()
        dim = COLOUR_DIMS[k][self.s]
        way, by = m % PAIR, toward(m)
        if m < FAR:
            src, dst = self.terms(k, me.shift(dim, FAR), way), self.carried(self.relay, k, way)
        elif m < ADDED:
            src, dst = self.terms(k, me.shift(dim, by), 1 - way), self.zone(k, way, 1 - way)
        else:
            src, dst = self.carried(self.passed, k, way), self.zone(k, way, way)
        return remote(src, dst, self.sems, (k, m), me.neighbour(dim, by))

    def start(self, k, base):
        for m in WAYS:
            self.hop(k, base + m).start()

    def arrived(self, k, base):
        for m in WAYS:
            self.hop(k, base + m).wait_recv()

    def finish(self):
        for k in COLOURS:
            for m in range(ADDED + PAIR):
                self.hop(k, m).wait_send()

    @staticmethod
    def semaphores():
        return [pltpu.SemaphoreType.DMA((C, ADDED + PAIR))] * PAIR


UNIT = 32
BANDS = {WIDE: ((0, 24), (24, UNIT), (56, UNIT)), DOWN: ((0, UNIT), (UNIT, UNIT), (2 * UNIT, UNIT))}
ORDERS = {WIDE: "xzy", DOWN: "zyx"}


class Bands:
    def __init__(self, kind, half=None):
        self.order, self.bands = ORDERS[kind], BANDS[kind]
        self.width = HALF if half is None else HALF // PAIR
        self.cols = pl.ds(self.width * (half or 0), self.width)

    def band(self, k):
        return pl.ds(*self.bands[k])

    def rows(self, ref, k):
        return ref.at[(ALL,) * (len(ref.shape) - PAIR) + (pl.ds(0, self.bands[k][1]),)]

    def cuts(self, k):
        rows = self.bands[k][1]
        cut = (rows // SUB + 1) // PAIR * SUB
        return pl.ds(0, cut), pl.ds(cut, rows - cut)

    def rest(self, k):
        return [d for d in self.order if d != COLOUR_DIMS[k][FIRST]]

    def units(self, *lead):
        return lead + (UNIT, self.width)

    def vmem(self, *lead):
        return pltpu.VMEM(self.units(*lead), F32)

    def sums(self):
        return sds(F32, *self.units(C, SIDE, SIDE))

    def result(self):
        return sds(F32, *self.units(C))

    def total(self):
        return sds(F32, *self.units(SIDE, C))

    def first(self):
        relays = [self.vmem(C, PAIR, PAIR, SIDE)] * PAIR
        dma = pltpu.SemaphoreType.DMA
        return [self.vmem(C, SIDE, SIDE), *relays, self.vmem(C, PAIR, SIDE, SIDE), *Ring.semaphores(), dma((C, C)), dma((C,))]

    def later(self):
        dma = pltpu.SemaphoreType.DMA
        return [self.vmem(C, SIDE, SIDE), self.vmem(C, PAIR, PAIR), self.vmem(C, PAIR, SIDE),
                pltpu.VMEM((C, PAIR, UNIT // PAIR, self.width), F32), self.vmem(C, PAIR),
                *Ring.semaphores(), *Ring.semaphores(), dma((C,)), dma((C,))]


class First:
    def __init__(self, bands, part, acc, own, passed, relay, landing, send, recv, load, store):
        self.bands, self.part, self.acc, self.own_all, self.passed = bands, part, acc, own, passed
        self.relay_in, self.landing, self.load_sem, self.store_sem = relay, landing, load, store
        self.ring = Ring(FIRST, bands, self.terms, passed, relay, landing, send, recv)

    def own(self, k):
        return self.bands.rows(self.own_all.at[k], k)

    def terms(self, k, v, half=None):
        b = self.bands
        at = {d: ALL for d in b.order}
        at[COLOUR_DIMS[k][FIRST]] = v
        if half is not None:
            at[b.rest(k)[0]] = duo(half)
        return self.part.at[tuple(at[d] for d in b.order) + (b.band(k), b.cols)]

    def load(self, k, m):
        me = Torus()
        dim = COLOUR_DIMS[k][FIRST]
        if m in WAYS:
            src, dst = self.terms(k, me.shift(dim, toward(m)), m), self.ring.carried(self.passed, k, m)
        else:
            src, dst = self.terms(k, me.at[dim]), self.own(k)
        return pltpu.make_async_copy(src, dst, self.load_sem.at[k, m])

    def store(self, k):
        return pltpu.make_async_copy(self.own(k), self.bands.rows(self.acc.at[k], k), self.store_sem.at[k])

    def near(self):
        for k in COLOURS:
            self.ring.start(k, NEAR)

    def far(self):
        for k in COLOURS:
            self.ring.start(k, FAR)
        for m in COLOURS:
            for k in COLOURS:
                self.load(k, m).start()

    def relay(self):
        for k in COLOURS:
            self.ring.arrived(k, NEAR)
            for m in WAYS:
                self.load(k, m).wait()
                add_into(self.ring.carried(self.passed, k, m), self.ring.carried(self.relay_in, k, m))
            self.ring.start(k, ADDED)

    def settle(self, then=None):
        for k in COLOURS:
            self.load(k, FAR).wait()
            for base in (FAR, ADDED):
                self.ring.arrived(k, base)
            add_into(self.own(k), *(self.bands.rows(self.landing.at[k, m], k) for m in WAYS))
            if then is None:
                self.store(k).start()
            else:
                then(k)

    def finish(self):
        self.ring.finish()
        if self.acc is not None:
            for k in COLOURS:
                self.store(k).wait()


class Rest:
    def __init__(self, bands, acc, result, own, relay2, in2, relay3, in3, *sems):
        self.bands, self.acc, self.own, self.result = bands, acc, own, result
        self.in2, self.in3, self.relay2, self.relay3, self.load_sem, self.store_sem = in2, in3, relay2, relay3, *sems[-2:]
        self.second = Ring(SECOND, bands, functools.partial(self.terms, acc), relay2, relay2, in2, *sems[:PAIR])
        self.third = Ring(THIRD, bands, self.final, relay3, relay3, in3, *sems[PAIR:2 * PAIR])

    def terms(self, ref, k, v, half=None):
        other = ALL if half is None else duo(half)
        first = self.bands.rest(k)[0] == COLOUR_DIMS[k][SECOND]
        return self.bands.rows(ref.at[(k, v, other) if first else (k, other, v)], k)

    def final(self, k, v, half=None):
        if half is None:
            return self.bands.rows(self.in2.at[k, 0, v], k)
        return self.in2.at[k, 0, v, self.bands.cuts(k)[half]]

    def load(self, k):
        return pltpu.make_async_copy(self.bands.rows(self.acc.at[k], k), self.bands.rows(self.own.at[k], k), self.load_sem.at[k])

    def store(self, k):
        rows = self.bands.rows
        return pltpu.make_async_copy(rows(self.in3.at[k, 0], k), rows(self.result.at[k], k), self.store_sem.at[k])

    def send(self, k):
        for base in (NEAR, FAR):
            self.second.start(k, base)

    def begin(self):
        for k in COLOURS:
            self.send(k)
        for k in COLOURS:
            self.load(k).start()

    def loaded(self):
        for k in COLOURS:
            self.load(k).wait()

    def relay(self):
        me = Torus()
        for k in COLOURS:
            self.second.arrived(k, NEAR)
            for m in WAYS:
                terms = self.terms(self.own, k, me.shift(COLOUR_DIMS[k][SECOND], toward(m)), m)
                add_into(self.second.carried(self.relay2, k, m), terms)
            self.second.start(k, ADDED)

    def settle(self):
        me = Torus()
        for k in COLOURS:
            for base in (FAR, ADDED):
                self.second.arrived(k, base)
            plus, minus = (self.bands.rows(self.in2.at[k, m], k) for m in WAYS)
            add_into(plus, minus, self.terms(self.own, k, me.at[COLOUR_DIMS[k][SECOND]]))
            for base in (NEAR, FAR):
                self.third.start(k, base)

    def relay_third(self):
        me = Torus()
        for k in COLOURS:
            self.third.arrived(k, NEAR)
            for m in WAYS:
                mine = self.third.carried(self.relay3, k, m)
                mine[...] += self.final(k, me.shift(COLOUR_DIMS[k][THIRD], toward(m)), m)[...]
            self.third.start(k, ADDED)

    def settle_third(self):
        me = Torus()
        for k in COLOURS:
            for base in (FAR, ADDED):
                self.third.arrived(k, base)
            plus, minus = (self.bands.rows(self.in3.at[k, m], k) for m in WAYS)
            plus[...] += minus[...] + self.final(k, me.at[COLOUR_DIMS[k][THIRD]])[...]
            if self.result is not None:
                self.store(k).start()

    def finish(self):
        self.second.finish()
        self.third.finish()
        if self.result is not None:
            for k in COLOURS:
                self.store(k).wait()

    def sums(self):
        return self.in3.at[:, 0]


class Spread:
    def __init__(self, bands, result, total, send, recv, local):
        self.bands, self.result, self.total, self.sems, self.local = bands, result, total, (send, recv), local

    @staticmethod
    def scratch():
        return [pltpu.SemaphoreType.DMA((C, ADDED))] * PAIR + [pltpu.SemaphoreType.DMA((C,))]

    def mine(self, k):
        return self.bands.rows(self.result.at[k], k)

    def place(self, k):
        return self.bands.rows(self.total.at[Torus().at["x"], k], k)

    def hop(self, k, m):
        me = Torus()
        by = toward(m)
        if m < FAR:
            src, dst = self.mine(k), self.place(k)
        else:
            dst = src = self.total.at[me.shift("x", -by), k, self.bands.cuts(k)[m - FAR]]
        return remote(src, dst, self.sems, (k, m), me.neighbour("x", by))

    def own(self, k):
        return pltpu.make_async_copy(self.mine(k), self.place(k), self.local.at[k])

    def begin(self):
        for k in COLOURS:
            if self.local is None:
                self.place(k)[...] = self.mine(k)[...]
            else:
                self.own(k).start()
            for m in WAYS:
                self.hop(k, m).start()

    def forward(self):
        for k in COLOURS:
            for m in WAYS:
                self.hop(k, m).wait_recv()
                self.hop(k, FAR + m).start()

    def finish(self):
        for k in COLOURS:
            for m in WAYS:
                self.hop(k, FAR + m).wait_recv()
            if self.local is not None:
                self.own(k).wait()
            for m in range(ADDED):
                self.hop(k, m).wait_send()


def comm_params(collective_id):
    return pltpu.CompilerParams(collective_id=collective_id, has_side_effects=True, vmem_limit_bytes=VMEM_LIMIT)


def gather_kernel(*refs):
    n = len(Gather.semaphores())
    a, u = (Gather(WIDE, *refs[i::PAIR][:PAIR], *refs[SIDE + n * i:][:n]) for i in WAYS)
    enter()
    for gather in (a, u):
        gather.begin()
    for step, *ring in ((a.relay, FIRST), (u.relay, FIRST), (a.settle, FIRST), (a.launch, SECOND), (u.settle, FIRST),
                        (a.relay, SECOND), (u.launch, SECOND), (a.settle, SECOND), (a.launch, THIRD), (u.relay, SECOND),
                        (u.settle, SECOND), (a.relay, THIRD), (a.settle, THIRD), (u.sent, FIRST, SECOND),
                        (a.sent, FIRST, SECOND, THIRD)):
        step(*ring)


def gather_call(attn, up, collective_id):
    return pl.pallas_call(
        gather_kernel, out_shape=[sds(BF16, *Gather.shape(WIDE))] * PAIR, in_specs=[ANY] * PAIR,
        out_specs=[ANY] * PAIR, scratch_shapes=Gather.semaphores() * PAIR, compiler_params=comm_params(collective_id),
        name="gather")(attn, up)


class Background:
    def __init__(self, steps, plan):
        self.steps, self.plan = steps, plan

    def visit(self, place):
        for j, first, end in self.plan.get(place, ()):
            @at_step(j)
            def _():
                for step in self.steps[first:end]:
                    step()


class Feed:
    def __init__(self, block, steps, buffers, sems):
        self.block, self.steps, self.buffers, self.sems = block, steps, buffers, sems

    @staticmethod
    def scratch(dtype, *shape):
        return [pltpu.VMEM((PAIR,) + shape, dtype), pltpu.SemaphoreType.DMA((PAIR,))]

    def copy(self, j):
        slot = lax.rem(j, PAIR)
        return pltpu.make_async_copy(self.block(j), self.buffers.at[slot], self.sems.at[slot])

    def get(self, j):
        pl.when(j + 1 < self.steps)(lambda: self.copy(j + 1).start())
        self.copy(j).wait()
        return self.buffers.at[lax.rem(j, PAIR)]


def first_feeds(*feeds):
    @at_step(0)
    def _():
        for feed in feeds:
            feed.copy(0).start()


class Share:
    def __init__(self, mine, theirs, place, sems, slot):
        self.local = pltpu.make_async_copy(mine, place, sems[PAIR].at[slot])
        self.far = remote(theirs, place, sems, slot, Torus().partner())

    def start(self):
        self.far.start()
        self.local.start()

    def sent(self):
        self.local.wait()
        self.far.wait_send()

    def wait(self):
        self.sent()
        self.far.wait_recv()


class Push:
    def __init__(self, src, tail, rows, sems, slot=0):
        body = BODY * len(SEQ_PAIR)
        tails = TAIL * len(SEQ_PAIR)
        self.copies = [
            remote(src.at[pl.ds(start, size)], rows.at[pl.ds(to, size)], sems, (slot, i), Torus().partner())
            for i, (start, to, size) in enumerate(((0, body, body), (tail, PAIR * body + tails, tails)))]

    @staticmethod
    def semaphores(n):
        return [pltpu.SemaphoreType.DMA((n, PAIR))] * PAIR

    def start(self):
        for copy in self.copies:
            copy.start()

    def wait(self):
        for copy in self.copies:
            copy.wait_recv()

    def finish(self):
        for copy in self.copies:
            copy.wait_send()


class Exchange:
    def __init__(self, mine, theirs, rows, sems, slot):
        self.moves = []
        for s in SEQ_PAIR:
            for i, (start, size) in enumerate(((0, BODY), (BODY, TAIL))):
                place = lambda n: rows.at[pl.ds(start * len(SEQ_PAIR) * PAIR + size * n, size)]
                part = pl.ds(TOK * s + start, size)
                at = slot + (PAIR * s + i,)
                local = pltpu.make_async_copy(mine.at[part], place(s), sems[2].at[at])
                far = remote(theirs.at[part], place(len(SEQ_PAIR) + s), sems, at, Torus().partner())
                self.moves.append((local, far))

    @staticmethod
    def semaphores(*lead):
        return [pltpu.SemaphoreType.DMA(lead + (2 * PAIR,))] * 3

    def start(self):
        for local, far in self.moves:
            far.start()
            local.start()

    def wait(self):
        for local, far in self.moves:
            local.wait()
            far.wait_recv()

    def finish(self):
        for _, far in self.moves:
            far.wait_send()


NT = (((1,), (1,)), ((), ()))
TN = (((0,), (0,)), ((), ()))


def dot(a, b):
    return jnp.dot(a, b, preferred_element_type=F32)


def dot_nt(a, b):
    return lax.dot_general(a, b, NT, preferred_element_type=F32)


def dot_tn(a, b):
    return lax.dot_general(a, b, TN, preferred_element_type=F32)


def zeros_but(n, axis, value):
    return tuple(value if i == axis else 0 for i in range(n))


def whole(*shape):
    return pl.BlockSpec(shape, lambda *_: (0,) * len(shape))


def along(axis, *block, index=lambda j: j):
    return pl.BlockSpec(block, lambda j: zeros_but(len(block), axis, index(j)))


def row(vec, i):
    return vec[i:i + 1]


def row_mean(t):
    return jnp.mean(t, axis=-1, keepdims=True)


def norm_stats(t):
    centered = t - row_mean(t)
    rstd = lax.rsqrt(row_mean(centered * centered) + LN_EPS)
    return centered * rstd, rstd


def norm_back(xhat, rstd, g):
    return rstd * (g - row_mean(g) - xhat * row_mean(g * xhat))


def col_sum(t):
    return jnp.sum(t, axis=0, keepdims=True)


def at_step(j):
    return pl.when(pl.program_id(0) == j)


def accumulate(ref, value):
    @at_step(0)
    def _():
        ref[...] = value

    @pl.when(pl.program_id(0) > 0)
    def _():
        ref[...] += value


def pad(t):
    return jnp.concatenate([t.astype(F32), jnp.zeros((TOK - SEQ, t.shape[1]), F32)], axis=0).astype(BF16)


WINDOW = 2 * LANES


def window(h):
    first = h * HEAD
    start = jnp.minimum(lax.div(first, LANES) * LANES, D - WINDOW)
    lane = lax.broadcasted_iota(jnp.int32, (1, WINDOW), 1) + (start - first)
    return pl.ds(pl.multiple_of(start, LANES), WINDOW), (lane >= 0) & (lane < HEAD)


def each_head(body, unroll):
    def trip(i, carry):
        for n in range(unroll):
            body(i * unroll + n)
        return carry

    lax.fori_loop(0, HEADS // unroll, trip, 0)


def each_seq(body):
    def trip(s, carry):
        start = pl.multiple_of(s * TOK, TAIL)
        body(s, pl.ds(start, TOK), pl.ds(start, SEQ))
        return carry

    lax.fori_loop(0, len(SEQ_PAIR), trip, 0)


def only(mask, t):
    return jnp.where(mask, t, jnp.zeros_like(t))


def softmax(scores):
    e = jnp.exp(scores - jnp.max(scores, axis=-1, keepdims=True))
    return e * (1.0 / jnp.sum(e, axis=-1, keepdims=True))


def attention(s, rows, o, acc, visit):
    acc[...] = jnp.zeros_like(acc)
    start = pl.multiple_of(s * TOK, TAIL)
    tokens = pl.ds(start, SEQ)

    def head(h):
        lanes, mask = window(h)
        k = only(mask, rows[K, tokens, lanes])
        v = only(mask, rows[V, tokens, lanes])
        probs = softmax(dot_nt(rows[Q, tokens, lanes], k) * SCALE).astype(BF16)
        acc[:, lanes] += dot(probs, v)

    each_head(head, PAIR)
    visit("half")
    o[pl.ds(start, TOK)] = pad(acc[...])


FRONT_PLAN = {"start": ((0, 0, 2),), "end": ((0, 2, 3), (1, 3, 4), (O, 4, 5), (O + 1, 6, None)), "half": ((O + 1, 5, 6),)}


def front_kernel(x_in, w_in, b, vec, _, down_in, qkv_out, h1_out, o_out, att_out, h2_out, up, down, rows, lhs, att, h2, acc, x,
                 x_sem, w_rows, w_sems, sems, *ring_sems):
    n = len(ring_sems) // PAIR
    early = Gather(DOWN, down_in, down, *ring_sems[n:]).first_rings()
    late = Gather(WIDE, None, up, *ring_sems[:n]).last_ring()
    hosted = Background([early[0], late[0], *early[1:SIDE], late[1], *early[SIDE:], *late[PAIR:]], FRONT_PLAN)
    j = pl.program_id(0)
    weights = Feed(lambda n: w_in.at[n, :, pl.ds(0, D)], SIDE, w_rows, w_sems)
    fetch = pltpu.make_async_copy(x_in, x, x_sem)
    h1, o = (lhs.at[i] for i in WAYS)
    stores = [pltpu.make_async_copy(*move, sems.at[i]) for i, move in enumerate(
        ((h1, h1_out), (rows, qkv_out), (o, o_out), (att, att_out), (h2, h2_out)))]
    at_step(0)(fetch.start)
    first_feeds(weights)
    at_step(0)(enter)
    hosted.visit("start")

    @at_step(0)
    def _():
        fetch.wait()

        def norm(s, tile, tokens):
            xhat, _ = norm_stats(x[s].astype(F32))
            h1[tile] = pad(xhat * row(vec, G1) + row(vec, C1))

        each_seq(norm)

    for i in WAYS:
        at_step(PAIR * i + 1)(stores[i].start)

    @pl.when(j >= O)
    def _():
        attention(j - O, rows, o, acc, hosted.visit)

    @pl.when((j < O) | (j == O + LAST_SEQ))
    def _():
        bias = jnp.where(j < O, b[0], row(vec, BO))
        att[...] = dot(lhs[lax.div(j, O)], weights.get(jnp.minimum(j, O))[...]) + bias

    @pl.when(j < O)
    def _():
        rows[j] = att[...].astype(BF16)

    @at_step(O + LAST_SEQ)
    def _():
        def norm(s, tile, tokens):
            xhat, _ = norm_stats(x[s].astype(F32) + row(vec, S1) * att[tokens])
            h2[tile] = pad(xhat * row(vec, G2) + row(vec, C2))

        each_seq(norm)
        for store in stores[PAIR:]:
            store.start()

    hosted.visit("end")

    @at_step(O + LAST_SEQ)
    def _():
        for store in stores:
            store.wait()


def upto(n):
    return lambda j: jnp.minimum(j, n)


def front_call(x, w_attn, b_qkv, vec, up, down, collective_id):
    outs = ((BF16, O, TT, D), (BF16, TT, D), (BF16, TT, D), (F32, TT, D), (BF16, TT, D), (BF16, *Gather.shape(WIDE)),
            (BF16, *Gather.shape(DOWN)))
    dma = pltpu.SemaphoreType.DMA
    return pl.pallas_call(
        front_kernel, grid=(O + PAIR,), out_shape=[sds(*out) for out in outs],
        in_specs=[ANY, ANY, along(0, 1, 1, D, index=upto(V)), whole(8, D), ANY, ANY], out_specs=[ANY] * len(outs),
        scratch_shapes=[pltpu.VMEM((O, TT, D), BF16), pltpu.VMEM((PAIR, TT, D), BF16), pltpu.VMEM((TT, D), F32),
                        pltpu.VMEM((TT, D), BF16), pltpu.VMEM((SEQ, D), F32), pltpu.VMEM(SEQS, BF16), dma] +
        Feed.scratch(BF16, D, D) + [dma((SIDE + 1,))] + Gather.semaphores() * PAIR,
        input_output_aliases={SIDE: SIDE + 1},
        compiler_params=comm_params(collective_id), name="front",
    )(x, w_attn, b_qkv, vec, up, down)


TILES = FF // HALF
OWN_BODY = BODY * len(SEQ_PAIR)
TAILS = ROWS - TAIL * PAIR * len(SEQ_PAIR)


def put_rows(ref, tail, s, t):
    ref[pl.ds(pl.multiple_of(BODY * s, BODY), BODY)] = t[:BODY]
    ref[pl.ds(pl.multiple_of(tail + TAIL * s, TAIL), TAIL)] = t[BODY:]


DOWN_PLAN = {"start": ((0, 0, 1),), "end": ((TILES + 2, 1, 2), (2 * TILES - 1, 2, None))}


def mlp_in_kernel(h2_in, gz_in, up_in, b_up, vec, _, act, slope, d_down, down, a_rows, b_rows, b_away, *sems):
    (h2, gz, h2_sem, gz_sem, *tiles), sems = sems[:SIDE + PAIR], sems[SIDE + PAIR:]
    feed = Feed(lambda n: up_in.at[lax.div(n, PAIR), :, tile_cols(lax.rem(n, PAIR))], TILES, *tiles)
    fetches = [pltpu.make_async_copy(*move) for move in ((gz_in, gz, gz_sem), (h2_in, h2, h2_sem))]
    for move in fetches:
        at_step(0)(move.start)
    first_feeds(feed)
    a_sems, b_sems, sems = sems[:PAIR], sems[PAIR:2 * PAIR], sems[2 * PAIR:]
    hosted = Background(Gather(DOWN, None, down, *sems).last_ring(), DOWN_PLAN)
    j = pl.program_id(0)
    away = Push(b_away, OWN_BODY, b_rows, b_sems, 0)
    tile = lambda n: Push(a_rows.at[n], TAILS, a_rows.at[n], a_sems, n)
    at_step(0)(enter)
    hosted.visit("start")

    @at_step(0)
    def _():
        for move in fetches:
            move.wait()
        first = Torus().at["c"] == 0
        def scale(s, tile, tokens):
            d = pad(gz[s].astype(F32) * row(vec, S2))
            left, right = d[:, :HALF], d[:, D - HALF:]
            put_rows(b_rows, TAILS, s, jnp.where(first, left, right))
            put_rows(b_away, OWN_BODY, s, jnp.where(first, right, left))

        each_seq(scale)

    at_step(1)(away.start)
    for n in range(TILES):
        at_step(n + 1)(tile(n).start)

    @pl.when(j < TILES)
    def _():
        u = dot(h2[...], feed.get(j)[...]) + b_up[0]
        phi = 0.5 * (1.0 + lax.erf(u * math.sqrt(0.5)))
        slope[...] = phi + u * (jnp.exp(-0.5 * u * u) * math.sqrt(0.5 / math.pi))
        place = lax.rem(lax.broadcasted_iota(jnp.int32, (TT, 1), 0), TOK)
        a = only(place < SEQ, u * phi).astype(BF16)
        act[...] = a
        for s in SEQ_PAIR:
            put_rows(a_rows.at[j], TAILS, s, a[TOK * s:TOK * s + TOK])

    at_step(TILES)(away.wait)
    for n in range(TILES):
        at_step(TILES + n)(tile(n).wait)

    @pl.when(j >= TILES)
    def _():
        d_down[...] = dot_tn(a_rows[j - TILES], b_rows[...])

    hosted.visit("end")

    @at_step(2 * TILES - 1)
    def _():
        away.finish()
        for n in range(TILES):
            tile(n).finish()


def mlp_in_call(h2, gz, w_up, b_up, vec, down, collective_id):
    low = lambda j: jnp.minimum(j, TILES - 1)
    high = lambda j: jnp.maximum(j - TILES, 0)
    return pl.pallas_call(
        mlp_in_kernel, grid=(2 * TILES,),
        out_shape=(sds(BF16, TT, FF), sds(F32, TT, FF), sds(F32, FF, HALF), sds(BF16, *Gather.shape(DOWN))),
        in_specs=[ANY] * O + [along(0, 1, 1, HALF, index=low), whole(8, D), ANY],
        out_specs=(along(1, TT, HALF, index=low), along(1, TT, HALF, index=low),
                   along(0, HALF, HALF, index=high), ANY),
        scratch_shapes=[pltpu.VMEM((TILES, ROWS, HALF), BF16), pltpu.VMEM((ROWS, HALF), BF16),
                        pltpu.VMEM((PAIR * TOK, HALF), BF16), pltpu.VMEM((TT, D), BF16), pltpu.VMEM(SEQS, BF16),
                        pltpu.SemaphoreType.DMA, pltpu.SemaphoreType.DMA] + Feed.scratch(BF16, D, HALF) + Push.semaphores(TILES) + Push.semaphores(1) +
        Gather.semaphores(),
        input_output_aliases={SIDE + 1: O},
        compiler_params=comm_params(collective_id), name="mlp_in",
    )(h2, gz, w_up, b_up.reshape(TILES, 1, HALF), vec, down)


def tile_cols(n):
    return pl.ds(pl.multiple_of(n * HALF, HALF), HALF)


MLP_PLAN = {"start": ((0, 0, 1),), "end": ((1, 1, 2), (3, 2, 3), (TILES - 1, 3, None))}


def mlp_out_kernel(act_in, slope_in, gz, up_in, down_in, vec, part, d_pre, db_up, mlp_out, d_out, sums, dm, mlp, d_h2, mlp_sem,
                   d_sem, *scratch):
    scratch, tiles = scratch[:-8], scratch[-8:]
    stores = [pltpu.make_async_copy(*move) for move in ((mlp, mlp_out, mlp_sem), (d_h2, d_out, d_sem))]
    first = First(Bands(DOWN), part, sums, *scratch)
    hosted = Background([first.near, first.far, first.relay, first.settle, first.finish], MLP_PLAN)
    j = pl.program_id(0)
    blocks = (lambda n: act_in.at[:, tile_cols(n)], lambda n: slope_in.at[:, tile_cols(n)],
              lambda n: up_in.at[lax.div(n, PAIR), :, tile_cols(lax.rem(n, PAIR))], lambda n: down_in.at[tile_cols(n)])
    feeds = [Feed(block, TILES, *tiles[PAIR * i:][:PAIR]) for i, block in enumerate(blocks)]
    first_feeds(*feeds)
    at_step(0)(enter)
    hosted.visit("start")

    @at_step(0)
    def _():
        def scale(s, tile, tokens):
            dm[tile] = pad(gz[s].astype(F32) * row(vec, S2))

        each_seq(scale)

    act, slope, w_up, w_down = (feed.get(j) for feed in feeds)
    db_up[0] = jnp.zeros((1, HALF), F32)

    def back(s, tile, tokens):
        accumulate(mlp.at[tile], dot(act[tile], w_down[...]))
        d = dot_nt(dm[tile], w_down[...]) * slope[tile]
        db_up[0] += col_sum(d)
        d = d.astype(BF16)
        d_pre[0, 0, tile] = d
        accumulate(d_h2.at[tile], dot_nt(d, w_up[...]))

    each_seq(back)
    for move in stores:
        at_step(TILES - 1)(move.start)
    hosted.visit("end")
    for move in stores:
        at_step(TILES - 1)(move.wait)


def mlp_out_call(act, slope, gz, w_up, w_down, vec, part, collective_id):
    return pl.pallas_call(
        mlp_out_kernel, grid=(TILES,),
        out_shape=(sds(BF16, PAIR, SIDE, TT, HALF), sds(F32, TILES, 1, HALF), sds(F32, TT, D), sds(F32, TT, D),
                   Bands(DOWN).sums()),
        in_specs=[ANY, ANY, whole(*SEQS), ANY, ANY, whole(8, D), ANY],
        out_specs=(pl.BlockSpec((1, 1, TT, HALF), lambda j: (j % PAIR, j // PAIR, 0, 0)), along(0, 1, 1, HALF),
                   ANY, ANY, ANY),
        scratch_shapes=[pltpu.VMEM((TT, D), BF16), pltpu.VMEM((TT, D), F32), pltpu.VMEM((TT, D), F32),
                        pltpu.SemaphoreType.DMA, pltpu.SemaphoreType.DMA] + Bands(DOWN).first() + Feed.scratch(BF16, TT, HALF) +
        Feed.scratch(F32, TT, HALF) + Feed.scratch(BF16, D, HALF) + Feed.scratch(BF16, HALF, D),
        compiler_params=comm_params(collective_id), name="mlp_out",
    )(act, slope, gz, w_up, w_down, vec, part)


def halves_of(t):
    t = pad(t)
    return t[:, :HALF], jnp.concatenate([t[:, HALF:], jnp.zeros((TOK, QCOLS - D), BF16)], axis=1)


def mid(mlp, d_h2, att, x, gz, w_out, vec, z, g_res, d_att, d_o, sums):
    a = att[:SEQ]
    y = x[...].astype(F32) + row(vec, S1) * a
    m = mlp[:SEQ] + row(vec, B2)
    g = gz[...].astype(F32)
    z[0] = (y + row(vec, S2) * m).astype(BF16)
    xhat, rstd = norm_stats(y)
    dh = d_h2[:SEQ]
    gr = g + norm_back(xhat, rstd, dh * row(vec, G2))
    g_res[:SEQ] = gr
    da = gr * row(vec, S1)
    terms = (da, gr * a, dh * xhat, dh, g * row(vec, S2), g * m)
    accumulate(sums, jnp.concatenate([jnp.zeros((BO, D), F32)] + [col_sum(t) for t in terms], axis=0))
    for i, t in enumerate(halves_of(da)):
        d_att[i] = t
    d_o[...] = dot_nt(pad(da), w_out[...]).astype(BF16)


def attention_back(s, qkv, d_o, d_qkv, db, acc, b_rows, away, first, visit):
    acc[...] = jnp.zeros_like(acc)

    def head(h):
        lanes, mask = window(h)
        q, k, v = (only(mask, qkv[i, :SEQ, lanes]) for i in (Q, K, V))
        do = only(mask, d_o[:SEQ, lanes])
        scores = dot_nt(k, q) * SCALE
        e = jnp.exp(scores - jnp.max(scores, axis=0, keepdims=True))
        probs = e * (1.0 / col_sum(e))
        acc[V, :, lanes] += dot(probs.astype(BF16), do)
        dp = dot_nt(v, do)
        ds = probs * (dp - col_sum(dp * probs))
        ds = (ds * SCALE).astype(BF16)
        acc[K, :, lanes] += dot(ds, q)
        acc[Q, :, lanes] += dot_tn(ds, k)

    each_head(head, PAIR)
    visit("half")
    accumulate(db, jnp.concatenate([col_sum(acc[i]) for i in (Q, K, V)], axis=0))
    for n in (Q, K, V):
        left, right = halves_of(acc[n])
        d_qkv[0, n] = left
        d_qkv[1, n] = right
        put_rows(b_rows.at[n], TAILS, s, jnp.where(first, left, right))
        put_rows(away.at[n], OWN_BODY, s, jnp.where(first, right, left))


PER = HALF // STEP


class WideGrads:
    def __init__(self, inputs, a_of, cotangents, out, base, lead, a_rows, a_cols, b_rows):
        self.inputs, self.a_of, self.cotangents, self.out, self.base, self.lead = inputs, a_of, cotangents, out, base, lead
        self.a_rows, self.a_cols, self.b_rows = a_rows, a_cols, b_rows

    @staticmethod
    def scratch(inputs):
        return [pltpu.VMEM((inputs, ROWS, D), BF16), pltpu.VMEM((inputs, D, ROWS), BF16), pltpu.VMEM((SIDE, ROWS, HALF), BF16)]

    def turn(self, i):
        def trip(n, carry):
            lanes = pl.ds(pl.multiple_of(n * LANES, LANES), LANES)
            self.a_cols[i, lanes] = self.a_rows[i, :, lanes].T
            return carry

        lax.fori_loop(0, D // LANES, trip, 0)

    def step(self):
        j = pl.program_id(0)
        done = []
        for t in range(SIDE):
            n = (t + self.lead) % SIDE

            @at_step(self.base + PER * t)
            def _():
                i = self.a_of[n]
                if i not in done:
                    self.inputs[i].wait()
                    self.turn(i)
                    done.append(i)
                self.cotangents[n].wait()

        @pl.when(j >= self.base)
        def _():
            n = lax.rem(lax.div(j - self.base, PER) + self.lead, SIDE)
            cols = pl.ds(pl.multiple_of(lax.rem(j - self.base, PER) * STEP, STEP), STEP)
            i = 0 if len(self.inputs) == 1 else lax.div(n, O)
            self.out[0] = dot(self.a_cols[i], self.b_rows[n, :, cols])

    def finish(self):
        for move in (*self.inputs, *self.cotangents):
            move.finish()


def grads_block(base, lead):
    def index(j):
        n = jnp.maximum(j - base, 0)
        return (n // PER + lead) % SIDE, 0, n % PER

    return pl.BlockSpec((1, D, STEP), index)


GRAD_STEPS = PER * SIDE


def tok_block():
    return along(0, TOK, D, index=upto(LAST_SEQ))


def seq_block():
    return along(0, 1, SEQ, D, index=upto(LAST_SEQ))


MID_PLAN = {"start": ((0, 0, 1),), "end": ((1, 1, 3), (8, 3, 4), (11, 4, 5), (LAST_SEQ + GRAD_STEPS, 5, None))}


def mid_kernel(*refs):
    refs = list(refs)
    take = lambda n: [refs.pop(0) for _ in range(n)]
    ins, (w_attn, vec), (h2, d_pre, acc), outs, (d_up, result) = take(5), take(2), take(3), take(5), take(2)
    tiles, (w_out, w_sem) = [take(PAIR) for _ in ins], take(PAIR)
    tokens = lambda n: pl.ds(pl.multiple_of(n * TOK, TAIL), TOK)
    feeds = [Feed(lambda n, ref=ref: ref.at[tokens(n) if len(ref.shape) == PAIR else n], SEQS[0], *tile)
             for ref, tile in zip(ins, tiles)]
    fetch = pltpu.make_async_copy(w_attn.at[O, :, pl.ds(0, D)], w_out, w_sem)
    first_feeds(*feeds)
    at_step(0)(fetch.start)
    rows, a_sems, b_sems = take(3), take(C), take(C)
    rest = Rest(Bands(DOWN), acc, result, *refs)
    hosted = Background([rest.begin, rest.loaded, rest.relay, rest.settle, rest.relay_third, rest.settle_third, rest.finish],
                        MID_PLAN)
    c = Torus().at["c"]
    grads = WideGrads(
        [Exchange(h2, h2, rows[0].at[0], a_sems, ())], (0,) * SIDE,
        [Exchange(d_pre.at[c, n], d_pre.at[1 - c, n], rows[2].at[n], b_sems, (n,)) for n in range(SIDE)], d_up, SEQS[0], 0, *rows)
    at_step(0)(enter)
    hosted.visit("start")

    @at_step(0)
    def _():
        for move in (*grads.inputs, *grads.cotangents):
            move.start()

    j = pl.program_id(0)

    @pl.when(j < SEQS[0])
    def _():
        blocks = [feed.get(j) for feed in feeds]
        at_step(0)(fetch.wait)
        mid(*blocks, w_out, vec, *outs)

    grads.step()
    hosted.visit("end")
    at_step(LAST_SEQ + GRAD_STEPS)(grads.finish)


def mid_call(mlp, d_h2, att, x, gz, vec, w_attn, h2, d_pre, acc, collective_id):
    return pl.pallas_call(
        mid_kernel, grid=(SEQS[0] + GRAD_STEPS,),
        out_shape=(sds(BF16, *SEQS), sds(F32, TT, D), sds(BF16, PAIR, TT, HALF), sds(BF16, TT, D), sds(F32, 8, D),
                   sds(F32, SIDE, D, HALF), Bands(DOWN).result()),
        in_specs=[ANY] * (O + O) + [whole(8, D)] + [ANY] * O,
        out_specs=(seq_block(), tok_block(), along(1, PAIR, TOK, HALF, index=upto(LAST_SEQ)), tok_block(), whole(8, D),
                   grads_block(SEQS[0], 0), ANY),
        scratch_shapes=Feed.scratch(F32, TOK, D) * O + Feed.scratch(BF16, SEQ, D) * PAIR +
        [pltpu.VMEM((D, D), BF16), pltpu.SemaphoreType.DMA] + WideGrads.scratch(1) + Exchange.semaphores() + Exchange.semaphores(SIDE) +
        Bands(DOWN).later(),
        compiler_params=comm_params(collective_id), name="mid",
    )(mlp, d_h2, att, x, gz, w_attn, vec, h2, d_pre, acc)


ATTN_PLAN = {"start": ((0, 0, 2),), "half": ((0, 2, 4),), "end": ((SIDE, 4, 5), (LAST_SEQ + GRAD_STEPS, 5, None))}


def attn_back_kernel(*refs):
    refs = list(refs)
    take = lambda n: [refs.pop(0) for _ in range(n)]
    (qkv_in, do_in), (h1, o, d_att, part, result), (d_qkv, db, d_attn, sums, total) = take(2), take(5), take(5)
    acc, away, rows, tiles = refs.pop(0), refs.pop(0), take(3), take(SIDE)
    tokens = lambda n: pl.ds(pl.multiple_of(n * TOK, TAIL), TOK)
    feeds = [Feed(lambda n: qkv_in.at[:, tokens(n)], SEQS[0], *tiles[:PAIR]),
             Feed(lambda n: do_in.at[tokens(n)], SEQS[0], *tiles[PAIR:])]
    first_feeds(*feeds)
    a_sems, b_sems, away_sems = take(C), take(C), take(PAIR)
    first = First(Bands(WIDE), part, sums, *take(len(Bands(WIDE).first())))
    spread = Spread(Bands(DOWN), result, total, *refs)
    hosted = Background([spread.begin, first.near, first.far, spread.forward, first.relay, first.settle, first.finish,
                         spread.finish], ATTN_PLAN)
    c = Torus().at["c"]
    pushes = [Push(away.at[n], OWN_BODY, rows[2].at[n], away_sems, n) for n in range(O)]
    grads = WideGrads(
        [Exchange(a, a, rows[0].at[i], a_sems, (i,)) for i, a in enumerate((h1, o))], (0,) * O + (1,),
        pushes + [Exchange(d_att.at[c], d_att.at[1 - c], rows[2].at[O], b_sems, ())], d_attn, SEQS[0], O, *rows)
    at_step(0)(enter)
    hosted.visit("start")

    @at_step(0)
    def _():
        for move in (*grads.inputs, grads.cotangents[O]):
            move.start()

    @at_step(SEQS[0])
    def _():
        for push in pushes:
            push.start()

    j = pl.program_id(0)

    @pl.when(j < SEQS[0])
    def _():
        qkv, d_o = (feed.get(j) for feed in feeds)
        attention_back(j, qkv, d_o, d_qkv, db, acc, rows[2], away, c == 0, hosted.visit)


    grads.step()
    hosted.visit("end")
    at_step(LAST_SEQ + GRAD_STEPS)(grads.finish)


def attn_back_call(qkv, d_o, h1, o, d_att, part, result, collective_id):
    return pl.pallas_call(
        attn_back_kernel, grid=(SEQS[0] + GRAD_STEPS,),
        out_shape=(sds(BF16, PAIR, O, TT, HALF), sds(F32, O, D), sds(F32, SIDE, D, HALF), Bands(WIDE).sums(),
                   Bands(DOWN).total()),
        in_specs=[ANY] * 7,
        out_specs=(along(2, PAIR, O, TOK, HALF, index=upto(LAST_SEQ)), whole(O, D), grads_block(SEQS[0], O), ANY, ANY),
        scratch_shapes=[pltpu.VMEM((O, SEQ, D), F32), pltpu.VMEM((O, PAIR * TOK, HALF), BF16)] + WideGrads.scratch(2) +
        Feed.scratch(BF16, O, TOK, D) + Feed.scratch(BF16, TOK, D) + Exchange.semaphores(PAIR) + Exchange.semaphores() + Push.semaphores(O) + Bands(WIDE).first() + Spread.scratch(),
        compiler_params=comm_params(collective_id), name="attn_back",
    )(qkv, d_o, h1, o, d_att, part, result)


IN_STEPS = PAIR * O
SLOT = 40
LAST_PLAN = {"start": ((0, 0, 2),), "end": ((O, 2, None),)}


CORE_COLS = D - HALF
KEPT = 48
GRADS = ((KEPT, O * D), (KEPT, D), (KEPT, FF), (PAIR, C, UNIT, D), (SIDE, KEPT, LANES))
SHARES = PAIR * SIDE + SIDE + PAIR


def split_rows(totals, first, keep, give):
    def trip(x, carry):
        for total, bands in totals:
            rows = jnp.concatenate([total[x, k, :n] for k, (_, n) in enumerate(BANDS[WIDE])], axis=0)
            low, high = rows[:KEPT], jnp.concatenate([rows[OWN:], rows[:KEPT - OWN]], axis=0)
            keep[x, :, bands.cols] = jnp.where(first, low, high)
            give[x, :, bands.cols] = jnp.where(first, high, low)
        return carry

    lax.fori_loop(0, SIDE, trip, 0)


class Finals:
    def __init__(self, down, up, attn, outs, sems):
        self.c = Torus().at["c"]
        self.down, self.up, self.attn, self.sems = down, up, attn, sems
        self.qkv, self.out, self.up_out, self.down_out, self.pad = outs
        self.edge = pl.ds(CORE_COLS, LANES)

    def cols(self, base, width):
        return pl.ds(pl.multiple_of(base + self.c * HALF, LANES), width)

    def up_share(self, x):
        place = self.up_out.at[:, self.cols(QCOLS * x, HALF)]
        return Share(*(ref.at[x] for ref in self.up), place, self.sems, x)

    def block(self, x):
        return (self.out, 0) if x == O else (self.qkv, D * x)

    def attn_share(self, x):
        out, base = self.block(x)
        sides = (ref.at[x, :, pl.ds(0, CORE_COLS)] for ref in self.attn)
        return Share(*sides, out.at[:, self.cols(base, CORE_COLS)], self.sems, SIDE + x)

    def edge_share(self, x, padding):
        out, base = self.block(x)
        place = self.pad.at[x] if padding else out.at[:, pl.ds(base + CORE_COLS, LANES)]
        return Share(*(ref.at[x, :, self.edge] for ref in self.attn), place, self.sems, PAIR * SIDE + x)

    def down_share(self, edge):
        src = self.edge if edge else pl.ds(pl.multiple_of(self.c * LANES, LANES), CORE_COLS)
        sides = (self.down.at[pl.ds(PAIR * c, PAIR), :, :, src] for c in (self.c, 1 - self.c))
        place = self.down_out.at[:, :, :, self.edge if edge else self.cols(0, CORE_COLS)]
        return Share(*sides, place, self.sems, SHARES - PAIR + edge)

    def start_down(self):
        self.down_share(0).start()
        pl.when(self.c == 0)(lambda: self.down_share(1).start())

    def start(self):
        for x in range(SIDE):
            self.attn_share(x).start()
            pl.when(self.c == 0)(lambda: self.edge_share(x, False).start())
            pl.when(self.c == 1)(lambda: self.edge_share(x, True).start())

    def finish(self):
        for x in range(SIDE):
            for share in (self.up_share(x), self.attn_share(x), self.edge_share(x, True)):
                share.wait()
        self.down_share(0).wait()
        pl.when(self.c == 0)(lambda: self.down_share(1).sent())
        pl.when(self.c == 1)(lambda: self.down_share(1).far.wait_recv())


def last_kernel(*refs):
    refs = list(refs)
    take = lambda n: [refs.pop(0) for _ in range(n)]
    (d_qkv, w_attn, x_in, g_in, vec), (small, acc_up, down, _), (dx_out, part) = take(5), take(SIDE), take(PAIR)
    outs, (x, g_res, dx, x_sem, g_sem, dx_sem), tiles = take(len(GRADS)), take(SIDE + PAIR), take(SIDE)
    j = pl.program_id(0)
    fetches = [pltpu.make_async_copy(*move) for move in ((x_in, x, x_sem), (g_in, g_res, g_sem))]
    store = pltpu.make_async_copy(dx, dx_out, dx_sem)
    feeds = [Feed(lambda n: d_qkv.at[lax.rem(n, PAIR), lax.div(n, PAIR)], IN_STEPS, *tiles[:PAIR]),
             Feed(lambda n: w_attn.at[lax.div(n, PAIR), :, pl.ds(pl.multiple_of(lax.rem(n, PAIR) * HALF, HALF), HALF)],
                  IN_STEPS, *tiles[PAIR:])]
    first_feeds(*feeds)
    (acc, sums, pair_sums, block), (totals, sides), block_sem, swap_sems = take(4), (take(C), take(SIDE)), refs.pop(0), take(PAIR)
    finals = Finals(down, sides[:PAIR], sides[PAIR:], outs, take(C))
    halves = [Bands(WIDE, h) for h in WAYS]
    a, b = (First(bands, part, None, *take(len(bands.first()))) for bands in halves)
    rest_a, rest_b = (Rest(f.bands, f.own_all, None, f.own_all, *take(len(f.bands.later()) - 1)) for f in (a, b))
    rest_up = Rest(Bands(WIDE), acc_up, None, *take(len(Bands(WIDE).later())))
    spread_up, spread_a, spread_b = (
        Spread(r.bands, r.sums(), total, *take(PAIR), None) for r, total in zip((rest_up, rest_a, rest_b), totals))
    hosted = Background([rest_up.begin, a.near, rest_up.loaded, rest_up.relay], LAST_PLAN)
    first = finals.c == 0
    swap = remote(sums, pair_sums, swap_sems, (), Torus().partner())
    fetch = pltpu.make_async_copy(small, block, block_sem)
    at_step(0)(enter)
    hosted.visit("start")

    @at_step(0)
    def _():
        for move in (fetch, *fetches):
            move.start()
        finals.start_down()

    @pl.when(j < IN_STEPS)
    def _():
        d_half, w = (feed.get(j) for feed in feeds)
        each_seq(lambda s, tile, tokens: accumulate(acc.at[tile], dot_nt(d_half[tile], w[...])))

    @at_step(IN_STEPS - 1)
    def _():
        for move in fetches:
            move.wait()
        sums[...] = jnp.zeros_like(sums)

        def back(s, tile, tokens):
            xhat, rstd = norm_stats(x[s].astype(F32))
            dh = acc[tokens]
            sums[:BO] += jnp.concatenate([col_sum(dh * xhat), col_sum(dh)], axis=0)
            dx[s] = (g_res[tokens] + norm_back(xhat, rstd, dh * row(vec, G1))).astype(BF16)

        each_seq(back)
        store.start()

    hosted.visit("end")

    @at_step(IN_STEPS)
    def _():
        swap.start()
        fetch.wait()
        swap.wait()
        both = sums[...] + pair_sums[...]
        for d in range(DEVICES):
            at = CHIP * (d // PAIR) + SLOT + OWN * (d % PAIR)
            block[at:at + BO, :OWN] = both[:BO, OWN * d:OWN * d + OWN]

        @pl.when(finals.c == 1)
        def _():
            for z in range(SIDE):
                for y in range(SIDE):
                    rows = block.at[pl.ds(CHIP * (SIDE * z + y), CHIP)]
                    put = pltpu.make_async_copy(rows, part.at[0, z, y, :, pl.ds(CORE_COLS, LANES)], block_sem)
                    put.start()
            pltpu.make_async_copy(block, small, block_sem).wait()

        def share_up():
            spread_up.finish()
            split_rows([(totals[0], Bands(WIDE))], first, *sides[:PAIR])
            for x in range(SIDE):
                finals.up_share(x).start()

        for step in (b.near, rest_up.settle, a.far, rest_up.relay_third, b.far, a.relay, rest_up.settle_third, spread_up.begin,
                     b.relay, spread_up.forward, functools.partial(a.settle, rest_a.send),
                     functools.partial(b.settle, rest_b.send), rest_a.relay, rest_b.relay, rest_a.settle, rest_b.settle,
                     share_up, rest_a.relay_third, rest_b.relay_third, rest_a.settle_third, spread_a.begin,
                     rest_b.settle_third, spread_b.begin, spread_a.forward, spread_b.forward, spread_a.finish, spread_b.finish):
            step()
        split_rows(list(zip(totals[1:], halves)), first, *sides[PAIR:])
        finals.start()
        for user in (rest_up, rest_a, rest_b, a, b, finals):
            user.finish()
        store.wait()


def last_call(d_qkv, w_attn, x, g_res, vec, small, acc_up, down, part, collective_id):
    halves = [Bands(WIDE, h) for h in WAYS]
    dma = pltpu.SemaphoreType.DMA
    rings = [Bands(WIDE), *halves]
    return pl.pallas_call(
        last_kernel, grid=(IN_STEPS + 1,),
        out_shape=(sds(BF16, *SEQS), sds(F32, *part.shape), *(sds(F32, *shape) for shape in GRADS)),
        in_specs=[ANY] * SIDE + [whole(8, D)] + [ANY] * SIDE,
        out_specs=(ANY,) * (len(GRADS) + PAIR),
        scratch_shapes=[pltpu.VMEM(SEQS, BF16), pltpu.VMEM((TT, D), F32), pltpu.VMEM(SEQS, BF16), dma, dma, dma] + Feed.scratch(BF16, TT, HALF) +
        Feed.scratch(BF16, D, HALF) + [pltpu.VMEM((TT, D), F32), pltpu.VMEM((SUB, D), F32), pltpu.VMEM((SUB, D), F32),
                        pltpu.VMEM((D, LANES), F32)] + [r.vmem(SIDE, C) for r in rings] +
        [pltpu.VMEM((SIDE, KEPT, HALF), F32)] * SIDE + [dma, dma, dma] + [dma((SHARES,))] * C + halves[0].first() * PAIR +
        halves[0].later()[1:] * PAIR + Bands(WIDE).later() + Spread.scratch()[:PAIR] * C,
        input_output_aliases={8: 1},
        compiler_params=comm_params(collective_id), name="last",
    )(d_qkv, w_attn, x, g_res, vec, small, acc_up, down, part)


BQ, BU, VEC = 3 * D // 32, 3 * D // 32 + FF // 32, 3 * D // 32 + FF // 32 + 8 * OWN


def pair_swap(a):
    return lax.ppermute(a, "fsdp", [(i, i ^ 1) for i in range(DEVICES)])


def by_core(first, a, b):
    return jnp.where(first, a, b), jnp.where(first, b, a)


def my_pieces(shards, first):
    w_qkv, b_qkv, w_out, w_up, b_up, w_down, vec_params = shards
    x = lax.axis_index("rep")
    small = jnp.concatenate([b_qkv, b_up, vec_params.reshape(-1)])
    small = jnp.pad(small, (0, OWN * LANES - VEC)).reshape(OWN, LANES)
    attn = lax.dynamic_slice_in_dim(jnp.concatenate([w_qkv, w_out], axis=1), x * D, D, 1)
    attn = jnp.concatenate([attn, small], axis=1)
    up = lax.dynamic_slice_in_dim(w_up, x * QCOLS, QCOLS, 1)
    wide = jnp.stack([attn, up]).astype(BF16)
    mine, theirs = by_core(first, wide[..., :HALF], wide[..., HALF:])
    theirs = pair_swap(theirs)
    piece = jnp.concatenate(by_core(first, mine, theirs), axis=1)
    down = lax.dynamic_slice_in_dim(w_down, x * 48, 48, 0).astype(BF16).reshape(3, 16, D)
    return piece[0], piece[1], down


def small_params(w_attn):
    small = w_attn[0, :, D:].astype(F32).reshape(DEVICES, OWN * LANES)
    vec = small[:, BU:VEC].reshape(DEVICES, 8, OWN).transpose(1, 0, 2).reshape(8, D)
    return small[:, :BQ].reshape(O, 1, D), small[:, BQ:BU].reshape(FF), vec


ROOM = 5 * LANES


def small_grads(db_qkv, db_up, sums):
    vec = sums[BO:].reshape(8 - BO, DEVICES, OWN).transpose(1, 0, 2).reshape(DEVICES, VEC - BU - BO * OWN)
    small = jnp.concatenate([db_qkv.reshape(DEVICES, BQ), db_up.reshape(DEVICES, BU - BQ), vec], axis=1)
    small = small + pair_swap(small)
    small = jnp.pad(small, ((0, 0), (0, ROOM - small.shape[1]))).reshape(DEVICES, ROOM // LANES, LANES)
    return jnp.pad(small, ((0, 0), (0, OWN - ROOM // LANES), (0, 0))).reshape(D, LANES)


def device_step(x, gz, *shards):
    first = lax.rem(lax.axis_index("fsdp"), PAIR) == 0
    attn, up, down = my_pieces(shards, first)
    w_attn, up = gather_call(attn, up, 0)
    w_attn = w_attn.reshape(SIDE, D, QCOLS)
    b_qkv, b_up, vec = small_params(w_attn)
    qkv, h1, o, att, h2, w_up, down = front_call(x, w_attn, b_qkv, vec, up, down, 1)
    w_up = w_up.reshape(SIDE, D, QCOLS)
    act, slope, part, w_down = mlp_in_call(h2, gz, w_up, b_up, vec, down, 2)
    part = part.reshape((SIDE,) * 3 + (C * UNIT, HALF))
    d_pre, db_up, mlp, d_h2, acc = mlp_out_call(act, slope, gz, w_up, w_down.reshape(FF, D), vec, part, 3)
    z, g_res, d_att, d_o, sums, part, result = mid_call(mlp, d_h2, att, x, gz, vec, w_attn, h2, d_pre, acc, 4)
    part = part.reshape((SIDE,) * 3 + (CHIP, HALF))
    d_qkv, db_qkv, part, acc, down = attn_back_call(qkv, d_o, h1, o, d_att, part, result, 5)
    small = small_grads(db_qkv, db_up, sums)
    part = part.reshape((SIDE,) * 3 + (CHIP, HALF))
    dx, _, g_qkv, g_out, g_up, g_down, edge = last_call(d_qkv, w_attn, x, g_res, vec, small, acc, down, part, 6)
    small = edge[0, :ROOM // LANES].reshape(ROOM)
    vec = jnp.concatenate([edge[0, SLOT:SLOT + BO, :OWN], small[BU:VEC - BO * OWN].reshape(8 - BO, OWN)], axis=0)
    g_qkv, g_out, g_up = (g[:OWN] for g in (g_qkv, g_out, g_up))
    return z, dx, g_qkv, small[:BQ], g_out, g_up, small[BQ:BU], g_down.reshape(FF // DEVICES, D), vec


def solution(mesh):
    batch = P(("rep", "fsdp"), None, None)
    rows, flat, cols = P("fsdp", None), P("fsdp"), P(None, "fsdp")
    shards = (rows, flat, rows, rows, flat, rows, cols)
    return jax.shard_map(device_step, mesh=mesh, in_specs=(batch, batch) + shards,
                         out_specs=(batch, batch) + shards, check_vma=False)
```

```python
import functools
import math

import jax
import jax.numpy as jnp
from jax import lax
from jax.experimental import pallas as pl
from jax.experimental.pallas import tpu as pltpu
from jax.sharding import PartitionSpec as P

HEADS = 16
LN_EPS = 1e-5
D = 1408
FF = 6144
SEQ = 257
HEAD = D // HEADS
SCALE = HEAD ** -0.5
QCOLS = 1536
HALF = 768
OWN = 44
CHIP = 2 * OWN
LANES = 128
DEVICES = 32
F32 = jnp.float32
BF16 = jnp.bfloat16
VMEM_LIMIT = 66 * 1000 * 1000
G1, C1, BO, S1, G2, C2, B2, S2 = range(8)
Q, K, V, O = range(4)
SEQS = (2, SEQ, D)
LAST_SEQ = SEQS[0] - 1
SEQ_PAIR = range(SEQS[0])
TAIL = 16
BODY = SEQ - 1
TOK = BODY + TAIL
TT = 2 * TOK
ROWS = 4 * TOK
STEP = 256


def sds(dtype, *shape):
    return jax.ShapeDtypeStruct(shape, dtype)


MESH_ID = pl.DeviceIdType.MESH
SIDE = 4
SUB = 8
PAIR = 2
C = 3
COLOURS = range(C)
COLOUR_DIMS = ("xyz", "yzx", "zxy")
FIRST, SECOND, THIRD, LAST = range(4)
WAYS = range(PAIR)
NEAR, FAR, ADDED = 0, 2, 4
WIDE, DOWN = "wide", "down"
ANY = pl.BlockSpec(memory_space=pl.ANY)
ALL = slice(None)


def duo(m):
    return pl.ds(PAIR * m, PAIR)


def toward(m):
    return 1 - PAIR * (m % PAIR)


class Torus:
    def __init__(self):
        f = lax.axis_index("fsdp")
        self.at = {"x": lax.axis_index("rep"), "z": lax.div(f, SIDE * PAIR), "y": lax.rem(lax.div(f, PAIR), SIDE),
                   "c": lax.rem(f, PAIR)}

    def shift(self, dim, by):
        return lax.rem(self.at[dim] + (SIDE + by), SIDE)

    def device(self, **moved):
        p = {**self.at, **moved}
        return (p["x"], (p["z"] * SIDE + p["y"]) * PAIR + p["c"])

    def neighbour(self, dim, by):
        return self.device(**{dim: self.shift(dim, by)})

    def partner(self):
        return self.device(c=1 - self.at["c"])


def enter():
    me = Torus()
    barrier = pltpu.get_barrier_semaphore()
    others = [me.neighbour(d, toward(m)) for d in COLOUR_DIMS[0] for m in WAYS] + [me.partner()]
    for other in others:
        pl.semaphore_signal(barrier, device_id=other, device_id_type=MESH_ID)
    pl.semaphore_wait(barrier, len(others))


def remote(src, dst, sems, slot, device):
    return pltpu.make_async_remote_copy(src_ref=src, dst_ref=dst, send_sem=sems[0].at[slot], recv_sem=sems[1].at[slot],
                                        device_id=device, device_id_type=MESH_ID)


class Gather:
    def __init__(self, kind, src, dst, hop_send, hop_recv, push_send, push_recv, local):
        self.kind, self.src, self.dst, self.local = kind, src, dst, local
        self.hops, self.pushes = (hop_send, hop_recv), (push_send, push_recv)
        self.cols, self.cut = (256, 128) if kind == WIDE else (D, HALF)

    @staticmethod
    def semaphores():
        dma = pltpu.SemaphoreType.DMA
        return [dma((C, C, ADDED))] * PAIR + [dma((C, ADDED + 1))] * PAIR + [dma((C,))]

    @staticmethod
    def shape(kind):
        return (SIDE,) * 3 + (CHIP, QCOLS) if kind == WIDE else (SIDE, SIDE, PAIR, SIDE, C, 16, D)

    def source(self, k):
        return self.src.at[:, pl.ds(self.cols * k, self.cols)] if self.kind == WIDE else self.src.at[k]

    def piece(self, me, k, s, v, half=None):
        dims = COLOUR_DIMS[k]
        at = {**me.at, **{d: ALL for d in dims[:s]}, dims[s]: v}
        off, width = 0, self.cols
        if half is not None and s == FIRST:
            off, width = self.cut * half, (self.cut, self.cols - self.cut)[half]
        elif half is not None:
            at[dims[0]] = duo(half)
        if self.kind == WIDE:
            cols = pl.ds(pl.multiple_of(at["c"] * HALF + self.cols * k + off, 128), width)
            return self.dst.at[at["x"], at["z"], at["y"], :, cols]
        return self.dst.at[at["z"], at["y"], at["c"], at["x"], k, :, pl.ds(off, width)]

    def hop(self, k, s, m):
        me = Torus()
        dim = COLOUR_DIMS[k][s]
        by = toward(m)
        if m < FAR:
            ref = self.piece(me, k, s, me.at[dim])
        else:
            ref = self.piece(me, k, s, me.shift(dim, -by), m - FAR)
        src = self.source(k) if s == FIRST and m < FAR else ref
        return remote(src, ref, self.hops, (k, s, m), me.neighbour(dim, by))

    def push(self, k, n):
        me = Torus()
        dim = COLOUR_DIMS[k][THIRD]
        if n < FAR:
            ref = self.piece(me, k, THIRD, me.shift(dim, -toward(n)))
        elif n < ADDED:
            ref = self.piece(me, k, THIRD, me.shift(dim, FAR), n - FAR)
        else:
            ref = self.piece(me, k, THIRD, me.at[dim])
        return remote(ref, ref, self.pushes, (k, n), me.partner())

    def own(self, k):
        me = Torus()
        return pltpu.make_async_copy(self.source(k), self.piece(me, k, FIRST, me.at[COLOUR_DIMS[k][FIRST]]), self.local.at[k])

    def launch(self, s):
        for k in COLOURS:
            for m in WAYS:
                self.hop(k, s, m).start()
            if s == THIRD:
                self.push(k, ADDED).start()

    def relay(self, s):
        for k in COLOURS:
            for m in WAYS:
                self.hop(k, s, m).wait_recv()
                self.hop(k, s, FAR + m).start()
                if s == THIRD:
                    self.push(k, m).start()

    def settle(self, s):
        for k in COLOURS:
            for m in WAYS:
                self.hop(k, s, FAR + m).wait_recv()
                if s == THIRD:
                    self.push(k, FAR + m).start()
            if s == FIRST:
                self.own(k).wait()

    def begin(self):
        for k in COLOURS:
            self.own(k).start()
        self.launch(FIRST)

    def sent(self, *rings):
        for k in COLOURS:
            for s in rings:
                for m in range(ADDED):
                    self.hop(k, s, m).wait_send()
            if THIRD in rings:
                for n in range(ADDED + 1):
                    self.push(k, n).wait()

    def last_ring(self):
        return [functools.partial(f, THIRD) for f in (self.launch, self.relay, self.settle, self.sent)]


def add_into(total, *others):
    lead = total.shape[:-2]

    def body(i, carry):
        idx = []
        for n in reversed(lead):
            idx.insert(0, lax.rem(i, n))
            i = lax.div(i, n)
        value = total[tuple(idx)]
        for other in others:
            value = value + other[tuple(idx)]
        total[tuple(idx)] = value
        return carry

    lax.fori_loop(0, math.prod(lead), body, 0)


class Ring:
    def __init__(self, s, bands, terms, passed, relay, landing, send, recv):
        self.s, self.bands, self.terms, self.passed, self.relay, self.landing = s, bands, terms, passed, relay, landing
        self.sems = (send, recv)

    def zone(self, k, way, half):
        if self.s == THIRD:
            return self.landing.at[k, way, self.bands.cuts(k)[half]]
        return self.bands.rows(self.landing.at[k, way, duo(half)], k)

    def carried(self, ref, k, way):
        if self.s == THIRD:
            return ref.at[k, way, pl.ds(0, self.bands.cuts(k)[way].size)]
        return self.bands.rows(ref.at[k, way], k)

    def hop(self, k, m):
        me = Torus()
        dim = COLOUR_DIMS[k][self.s]
        way, by = m % PAIR, toward(m)
        if m < FAR:
            src, dst = self.terms(k, me.shift(dim, FAR), way), self.carried(self.relay, k, way)
        elif m < ADDED:
            src, dst = self.terms(k, me.shift(dim, by), 1 - way), self.zone(k, way, 1 - way)
        else:
            src, dst = self.carried(self.passed, k, way), self.zone(k, way, way)
        return remote(src, dst, self.sems, (k, m), me.neighbour(dim, by))

    def start(self, k, base):
        for m in WAYS:
            self.hop(k, base + m).start()

    def arrived(self, k, base):
        for m in WAYS:
            self.hop(k, base + m).wait_recv()

    def finish(self):
        for k in COLOURS:
            for m in range(ADDED + PAIR):
                self.hop(k, m).wait_send()

    @staticmethod
    def semaphores():
        return [pltpu.SemaphoreType.DMA((C, ADDED + PAIR))] * PAIR


UNIT = 32
BANDS = {WIDE: ((0, 24), (24, UNIT), (56, UNIT)), DOWN: ((0, UNIT), (UNIT, UNIT), (2 * UNIT, UNIT))}
ORDERS = {WIDE: "xzy", DOWN: "zyx"}


class Bands:
    def __init__(self, kind, half=None):
        self.order, self.bands = ORDERS[kind], BANDS[kind]
        self.width = HALF if half is None else HALF // PAIR
        self.cols = pl.ds(self.width * (half or 0), self.width)

    def band(self, k):
        return pl.ds(*self.bands[k])

    def rows(self, ref, k):
        return ref.at[(ALL,) * (len(ref.shape) - PAIR) + (pl.ds(0, self.bands[k][1]),)]

    def cuts(self, k):
        rows = self.bands[k][1]
        cut = (rows // SUB + 1) // PAIR * SUB
        return pl.ds(0, cut), pl.ds(cut, rows - cut)

    def rest(self, k):
        return [d for d in self.order if d != COLOUR_DIMS[k][FIRST]]

    def units(self, *lead):
        return lead + (UNIT, self.width)

    def vmem(self, *lead):
        return pltpu.VMEM(self.units(*lead), F32)

    def sums(self):
        return sds(F32, *self.units(C, SIDE, SIDE))

    def result(self):
        return sds(F32, *self.units(C))

    def total(self):
        return sds(F32, *self.units(SIDE, C))

    def first(self):
        relays = [self.vmem(C, PAIR, PAIR, SIDE)] * PAIR
        dma = pltpu.SemaphoreType.DMA
        return [self.vmem(C, SIDE, SIDE), *relays, self.vmem(C, PAIR, SIDE, SIDE), *Ring.semaphores(), dma((C, C)), dma((C,))]

    def later(self):
        dma = pltpu.SemaphoreType.DMA
        return [self.vmem(C, SIDE, SIDE), self.vmem(C, PAIR, PAIR), self.vmem(C, PAIR, SIDE),
                pltpu.VMEM((C, PAIR, UNIT // PAIR, self.width), F32), self.vmem(C, PAIR),
                *Ring.semaphores(), *Ring.semaphores(), dma((C,)), dma((C,))]


class First:
    def __init__(self, bands, part, acc, own, passed, relay, landing, send, recv, load, store):
        self.bands, self.part, self.acc, self.own_all, self.passed = bands, part, acc, own, passed
        self.relay_in, self.landing, self.load_sem, self.store_sem = relay, landing, load, store
        self.ring = Ring(FIRST, bands, self.terms, passed, relay, landing, send, recv)

    def own(self, k):
        return self.bands.rows(self.own_all.at[k], k)

    def terms(self, k, v, half=None):
        b = self.bands
        at = {d: ALL for d in b.order}
        at[COLOUR_DIMS[k][FIRST]] = v
        if half is not None:
            at[b.rest(k)[0]] = duo(half)
        return self.part.at[tuple(at[d] for d in b.order) + (b.band(k), b.cols)]

    def load(self, k, m):
        me = Torus()
        dim = COLOUR_DIMS[k][FIRST]
        if m in WAYS:
            src, dst = self.terms(k, me.shift(dim, toward(m)), m), self.ring.carried(self.passed, k, m)
        else:
            src, dst = self.terms(k, me.at[dim]), self.own(k)
        return pltpu.make_async_copy(src, dst, self.load_sem.at[k, m])

    def store(self, k):
        return pltpu.make_async_copy(self.own(k), self.bands.rows(self.acc.at[k], k), self.store_sem.at[k])

    def near(self):
        for k in COLOURS:
            self.ring.start(k, NEAR)

    def far(self):
        for k in COLOURS:
            self.ring.start(k, FAR)
        for m in COLOURS:
            for k in COLOURS:
                self.load(k, m).start()

    def relay(self):
        for k in COLOURS:
            self.ring.arrived(k, NEAR)
            for m in WAYS:
                self.load(k, m).wait()
                add_into(self.ring.carried(self.passed, k, m), self.ring.carried(self.relay_in, k, m))
            self.ring.start(k, ADDED)

    def settle(self, then=None):
        for k in COLOURS:
            self.load(k, FAR).wait()
            for base in (FAR, ADDED):
                self.ring.arrived(k, base)
            add_into(self.own(k), *(self.bands.rows(self.landing.at[k, m], k) for m in WAYS))
            if then is None:
                self.store(k).start()
            else:
                then(k)

    def finish(self):
        self.ring.finish()
        if self.acc is not None:
            for k in COLOURS:
                self.store(k).wait()


class Rest:
    def __init__(self, bands, acc, result, own, relay2, in2, relay3, in3, *sems):
        self.bands, self.acc, self.own, self.result = bands, acc, own, result
        self.in2, self.in3, self.relay2, self.relay3, self.load_sem, self.store_sem = in2, in3, relay2, relay3, *sems[-2:]
        self.second = Ring(SECOND, bands, functools.partial(self.terms, acc), relay2, relay2, in2, *sems[:PAIR])
        self.third = Ring(THIRD, bands, self.final, relay3, relay3, in3, *sems[PAIR:2 * PAIR])

    def terms(self, ref, k, v, half=None):
        other = ALL if half is None else duo(half)
        first = self.bands.rest(k)[0] == COLOUR_DIMS[k][SECOND]
        return self.bands.rows(ref.at[(k, v, other) if first else (k, other, v)], k)

    def final(self, k, v, half=None):
        if half is None:
            return self.bands.rows(self.in2.at[k, 0, v], k)
        return self.in2.at[k, 0, v, self.bands.cuts(k)[half]]

    def load(self, k):
        return pltpu.make_async_copy(self.bands.rows(self.acc.at[k], k), self.bands.rows(self.own.at[k], k), self.load_sem.at[k])

    def store(self, k):
        rows = self.bands.rows
        return pltpu.make_async_copy(rows(self.in3.at[k, 0], k), rows(self.result.at[k], k), self.store_sem.at[k])

    def send(self, k):
        for base in (NEAR, FAR):
            self.second.start(k, base)

    def begin(self):
        for k in COLOURS:
            self.send(k)
        for k in COLOURS:
            self.load(k).start()

    def loaded(self):
        for k in COLOURS:
            self.load(k).wait()

    def relay(self):
        me = Torus()
        for k in COLOURS:
            self.second.arrived(k, NEAR)
            for m in WAYS:
                terms = self.terms(self.own, k, me.shift(COLOUR_DIMS[k][SECOND], toward(m)), m)
                add_into(self.second.carried(self.relay2, k, m), terms)
            self.second.start(k, ADDED)

    def settle(self):
        me = Torus()
        for k in COLOURS:
            for base in (FAR, ADDED):
                self.second.arrived(k, base)
            plus, minus = (self.bands.rows(self.in2.at[k, m], k) for m in WAYS)
            add_into(plus, minus, self.terms(self.own, k, me.at[COLOUR_DIMS[k][SECOND]]))
            for base in (NEAR, FAR):
                self.third.start(k, base)

    def relay_third(self):
        me = Torus()
        for k in COLOURS:
            self.third.arrived(k, NEAR)
            for m in WAYS:
                mine = self.third.carried(self.relay3, k, m)
                mine[...] += self.final(k, me.shift(COLOUR_DIMS[k][THIRD], toward(m)), m)[...]
            self.third.start(k, ADDED)

    def settle_third(self):
        me = Torus()
        for k in COLOURS:
            for base in (FAR, ADDED):
                self.third.arrived(k, base)
            plus, minus = (self.bands.rows(self.in3.at[k, m], k) for m in WAYS)
            plus[...] += minus[...] + self.final(k, me.at[COLOUR_DIMS[k][THIRD]])[...]
            if self.result is not None:
                self.store(k).start()

    def finish(self):
        self.second.finish()
        self.third.finish()
        if self.result is not None:
            for k in COLOURS:
                self.store(k).wait()

    def sums(self):
        return self.in3.at[:, 0]


class Spread:
    def __init__(self, bands, result, total, send, recv, local):
        self.bands, self.result, self.total, self.sems, self.local = bands, result, total, (send, recv), local

    @staticmethod
    def scratch():
        return [pltpu.SemaphoreType.DMA((C, ADDED))] * PAIR + [pltpu.SemaphoreType.DMA((C,))]

    def mine(self, k):
        return self.bands.rows(self.result.at[k], k)

    def place(self, k):
        return self.bands.rows(self.total.at[Torus().at["x"], k], k)

    def hop(self, k, m):
        me = Torus()
        by = toward(m)
        if m < FAR:
            src, dst = self.mine(k), self.place(k)
        else:
            dst = src = self.total.at[me.shift("x", -by), k, self.bands.cuts(k)[m - FAR]]
        return remote(src, dst, self.sems, (k, m), me.neighbour("x", by))

    def own(self, k):
        return pltpu.make_async_copy(self.mine(k), self.place(k), self.local.at[k])

    def begin(self):
        for k in COLOURS:
            if self.local is None:
                self.place(k)[...] = self.mine(k)[...]
            else:
                self.own(k).start()
            for m in WAYS:
                self.hop(k, m).start()

    def forward(self):
        for k in COLOURS:
            for m in WAYS:
                self.hop(k, m).wait_recv()
                self.hop(k, FAR + m).start()

    def finish(self):
        for k in COLOURS:
            for m in WAYS:
                self.hop(k, FAR + m).wait_recv()
            if self.local is not None:
                self.own(k).wait()
            for m in range(ADDED):
                self.hop(k, m).wait_send()


def comm_params(collective_id):
    return pltpu.CompilerParams(collective_id=collective_id, has_side_effects=True, vmem_limit_bytes=VMEM_LIMIT)


def gather_kernel(*refs):
    n = len(Gather.semaphores())
    a, u, d = (Gather(kind, *refs[i::C][:PAIR], *refs[PAIR * C + n * i:][:n]) for i, kind in enumerate((WIDE, WIDE, DOWN)))
    enter()
    for gather in (a, u, d):
        gather.begin()
    for step, *ring in ((a.relay, FIRST), (u.relay, FIRST), (d.relay, FIRST), (a.settle, FIRST), (a.launch, SECOND),
                        (u.settle, FIRST), (u.launch, SECOND), (a.relay, SECOND), (d.settle, FIRST), (d.launch, SECOND),
                        (u.relay, SECOND), (a.settle, SECOND), (a.launch, THIRD), (d.relay, SECOND), (u.settle, SECOND),
                        (a.relay, THIRD), (d.settle, SECOND), (a.settle, THIRD), (u.sent, FIRST, SECOND),
                        (d.sent, FIRST, SECOND), (a.sent, FIRST, SECOND, THIRD)):
        step(*ring)


def gather_call(attn, up, down, collective_id):
    return pl.pallas_call(
        gather_kernel, out_shape=[sds(BF16, *Gather.shape(kind)) for kind in (WIDE, WIDE, DOWN)], in_specs=[ANY] * C,
        out_specs=[ANY] * C, scratch_shapes=Gather.semaphores() * C, compiler_params=comm_params(collective_id),
        name="gather")(attn, up, down)


class Background:
    def __init__(self, steps, plan):
        self.steps, self.plan = steps, plan

    def visit(self, place):
        for j, first, end in self.plan.get(place, ()):
            @at_step(j)
            def _():
                for step in self.steps[first:end]:
                    step()


class Feed:
    def __init__(self, block, steps, buffers, sems):
        self.block, self.steps, self.buffers, self.sems = block, steps, buffers, sems

    @staticmethod
    def scratch(dtype, *shape):
        return [pltpu.VMEM((PAIR,) + shape, dtype), pltpu.SemaphoreType.DMA((PAIR,))]

    def copy(self, j):
        slot = lax.rem(j, PAIR)
        return pltpu.make_async_copy(self.block(j), self.buffers.at[slot], self.sems.at[slot])

    def get(self, j):
        pl.when(j + 1 < self.steps)(lambda: self.copy(j + 1).start())
        self.copy(j).wait()
        return self.buffers.at[lax.rem(j, PAIR)]


def first_feeds(*feeds):
    @at_step(0)
    def _():
        for feed in feeds:
            feed.copy(0).start()


class Share:
    def __init__(self, mine, theirs, place, sems, slot):
        self.local = pltpu.make_async_copy(mine, place, sems[PAIR].at[slot])
        self.far = remote(theirs, place, sems, slot, Torus().partner())

    def start(self):
        self.far.start()
        self.local.start()

    def sent(self):
        self.local.wait()
        self.far.wait_send()

    def wait(self):
        self.sent()
        self.far.wait_recv()


class Push:
    def __init__(self, src, tail, rows, sems, slot=0):
        body = BODY * len(SEQ_PAIR)
        tails = TAIL * len(SEQ_PAIR)
        self.copies = [
            remote(src.at[pl.ds(start, size)], rows.at[pl.ds(to, size)], sems, (slot, i), Torus().partner())
            for i, (start, to, size) in enumerate(((0, body, body), (tail, PAIR * body + tails, tails)))]

    @staticmethod
    def semaphores(n):
        return [pltpu.SemaphoreType.DMA((n, PAIR))] * PAIR

    def start(self):
        for copy in self.copies:
            copy.start()

    def wait(self):
        for copy in self.copies:
            copy.wait_recv()

    def finish(self):
        for copy in self.copies:
            copy.wait_send()


class Exchange:
    def __init__(self, mine, theirs, rows, sems, slot):
        self.moves = []
        for s in SEQ_PAIR:
            for i, (start, size) in enumerate(((0, BODY), (BODY, TAIL))):
                place = lambda n: rows.at[pl.ds(start * len(SEQ_PAIR) * PAIR + size * n, size)]
                part = pl.ds(TOK * s + start, size)
                at = slot + (PAIR * s + i,)
                local = pltpu.make_async_copy(mine.at[part], place(s), sems[2].at[at])
                far = remote(theirs.at[part], place(len(SEQ_PAIR) + s), sems, at, Torus().partner())
                self.moves.append((local, far))

    @staticmethod
    def semaphores(*lead):
        return [pltpu.SemaphoreType.DMA(lead + (2 * PAIR,))] * 3

    def start(self):
        for local, far in self.moves:
            far.start()
            local.start()

    def wait(self):
        for local, far in self.moves:
            local.wait()
            far.wait_recv()

    def finish(self):
        for _, far in self.moves:
            far.wait_send()


NT = (((1,), (1,)), ((), ()))
TN = (((0,), (0,)), ((), ()))


def dot(a, b):
    return jnp.dot(a, b, preferred_element_type=F32)


def dot_nt(a, b):
    return lax.dot_general(a, b, NT, preferred_element_type=F32)


def dot_tn(a, b):
    return lax.dot_general(a, b, TN, preferred_element_type=F32)


def zeros_but(n, axis, value):
    return tuple(value if i == axis else 0 for i in range(n))


def whole(*shape):
    return pl.BlockSpec(shape, lambda *_: (0,) * len(shape))


def along(axis, *block, index=lambda j: j):
    return pl.BlockSpec(block, lambda j: zeros_but(len(block), axis, index(j)))


def row(vec, i):
    return vec[i:i + 1]


def row_mean(t):
    return jnp.mean(t, axis=-1, keepdims=True)


def norm_stats(t):
    centered = t - row_mean(t)
    rstd = lax.rsqrt(row_mean(centered * centered) + LN_EPS)
    return centered * rstd, rstd


def norm_back(xhat, rstd, g):
    return rstd * (g - row_mean(g) - xhat * row_mean(g * xhat))


def col_sum(t):
    return jnp.sum(t, axis=0, keepdims=True)


def at_step(j):
    return pl.when(pl.program_id(0) == j)


def accumulate(ref, value):
    @at_step(0)
    def _():
        ref[...] = value

    @pl.when(pl.program_id(0) > 0)
    def _():
        ref[...] += value


def pad(t):
    return jnp.concatenate([t.astype(F32), jnp.zeros((TOK - SEQ, t.shape[1]), F32)], axis=0).astype(BF16)


WINDOW = 2 * LANES


def window(h):
    first = h * HEAD
    start = jnp.minimum(lax.div(first, LANES) * LANES, D - WINDOW)
    lane = lax.broadcasted_iota(jnp.int32, (1, WINDOW), 1) + (start - first)
    return pl.ds(pl.multiple_of(start, LANES), WINDOW), (lane >= 0) & (lane < HEAD)


def each_head(body, unroll):
    def trip(i, carry):
        for n in range(unroll):
            body(i * unroll + n)
        return carry

    lax.fori_loop(0, HEADS // unroll, trip, 0)


def each_seq(body):
    def trip(s, carry):
        start = pl.multiple_of(s * TOK, TAIL)
        body(s, pl.ds(start, TOK), pl.ds(start, SEQ))
        return carry

    lax.fori_loop(0, len(SEQ_PAIR), trip, 0)


def only(mask, t):
    return jnp.where(mask, t, jnp.zeros_like(t))


def softmax(scores):
    e = jnp.exp(scores - jnp.max(scores, axis=-1, keepdims=True))
    return e * (1.0 / jnp.sum(e, axis=-1, keepdims=True))


def attention(s, rows, o, acc, visit):
    acc[...] = jnp.zeros_like(acc)
    start = pl.multiple_of(s * TOK, TAIL)
    tokens = pl.ds(start, SEQ)

    def head(h):
        lanes, mask = window(h)
        k = only(mask, rows[K, tokens, lanes])
        v = only(mask, rows[V, tokens, lanes])
        probs = softmax(dot_nt(rows[Q, tokens, lanes], k) * SCALE).astype(BF16)
        acc[:, lanes] += dot(probs, v)

    each_head(head, PAIR)
    visit("half")
    o[pl.ds(start, TOK)] = pad(acc[...])


FRONT_PLAN = {"start": ((0, 0, 1),), "half": ((O + 1, 1, 2),), "end": ((O + 1, 2, None),)}


def front_kernel(x_in, w_in, b, vec, _, qkv_out, h1_out, o_out, att_out, h2_out, up, rows, lhs, att, h2, acc, x,
                 x_sem, w_rows, w_sems, sems, *ring_sems):
    hosted = Background(Gather(WIDE, None, up, *ring_sems).last_ring(), FRONT_PLAN)
    j = pl.program_id(0)
    weights = Feed(lambda n: w_in.at[n, :, pl.ds(0, D)], SIDE, w_rows, w_sems)
    fetch = pltpu.make_async_copy(x_in, x, x_sem)
    h1, o = (lhs.at[i] for i in WAYS)
    stores = [pltpu.make_async_copy(*move, sems.at[i]) for i, move in enumerate(
        ((h1, h1_out), (rows, qkv_out), (o, o_out), (att, att_out), (h2, h2_out)))]
    at_step(0)(fetch.start)
    first_feeds(weights)
    at_step(0)(enter)
    hosted.visit("start")

    @at_step(0)
    def _():
        fetch.wait()

        def norm(s, tile, tokens):
            xhat, _ = norm_stats(x[s].astype(F32))
            h1[tile] = pad(xhat * row(vec, G1) + row(vec, C1))

        each_seq(norm)

    for i in WAYS:
        at_step(PAIR * i + 1)(stores[i].start)

    @pl.when(j >= O)
    def _():
        attention(j - O, rows, o, acc, hosted.visit)

    @pl.when((j < O) | (j == O + LAST_SEQ))
    def _():
        bias = jnp.where(j < O, b[0], row(vec, BO))
        att[...] = dot(lhs[lax.div(j, O)], weights.get(jnp.minimum(j, O))[...]) + bias

    @pl.when(j < O)
    def _():
        rows[j] = att[...].astype(BF16)

    @at_step(O + LAST_SEQ)
    def _():
        def norm(s, tile, tokens):
            xhat, _ = norm_stats(x[s].astype(F32) + row(vec, S1) * att[tokens])
            h2[tile] = pad(xhat * row(vec, G2) + row(vec, C2))

        each_seq(norm)
        for store in stores[PAIR:]:
            store.start()

    hosted.visit("end")

    @at_step(O + LAST_SEQ)
    def _():
        for store in stores:
            store.wait()


def upto(n):
    return lambda j: jnp.minimum(j, n)


def front_call(x, w_attn, b_qkv, vec, up, collective_id):
    outs = ((BF16, O, TT, D), (BF16, TT, D), (BF16, TT, D), (F32, TT, D), (BF16, TT, D), (BF16, *Gather.shape(WIDE)))
    dma = pltpu.SemaphoreType.DMA
    return pl.pallas_call(
        front_kernel, grid=(O + PAIR,), out_shape=[sds(*out) for out in outs],
        in_specs=[ANY, ANY, along(0, 1, 1, D, index=upto(V)), whole(8, D), ANY], out_specs=[ANY] * len(outs),
        scratch_shapes=[pltpu.VMEM((O, TT, D), BF16), pltpu.VMEM((PAIR, TT, D), BF16), pltpu.VMEM((TT, D), F32),
                        pltpu.VMEM((TT, D), BF16), pltpu.VMEM((SEQ, D), F32), pltpu.VMEM(SEQS, BF16), dma] +
        Feed.scratch(BF16, D, D) + [dma((SIDE + 1,))] + Gather.semaphores(),
        input_output_aliases={SIDE: SIDE + 1},
        compiler_params=comm_params(collective_id), name="front",
    )(x, w_attn, b_qkv, vec, up)


TILES = FF // HALF
OWN_BODY = BODY * len(SEQ_PAIR)
TAILS = ROWS - TAIL * PAIR * len(SEQ_PAIR)


def put_rows(ref, tail, s, t):
    ref[pl.ds(pl.multiple_of(BODY * s, BODY), BODY)] = t[:BODY]
    ref[pl.ds(pl.multiple_of(tail + TAIL * s, TAIL), TAIL)] = t[BODY:]


DOWN_PLAN = {"start": ((0, 0, 1),), "end": ((TILES + 2, 1, 2), (2 * TILES - 1, 2, None))}


def mlp_in_kernel(h2_in, gz_in, up_in, b_up, vec, _, act, slope, d_down, down, a_rows, b_rows, b_away, *sems):
    (h2, gz, h2_sem, gz_sem, *tiles), sems = sems[:SIDE + PAIR], sems[SIDE + PAIR:]
    feed = Feed(lambda n: up_in.at[lax.div(n, PAIR), :, tile_cols(lax.rem(n, PAIR))], TILES, *tiles)
    fetches = [pltpu.make_async_copy(*move) for move in ((gz_in, gz, gz_sem), (h2_in, h2, h2_sem))]
    for move in fetches:
        at_step(0)(move.start)
    first_feeds(feed)
    a_sems, b_sems, sems = sems[:PAIR], sems[PAIR:2 * PAIR], sems[2 * PAIR:]
    hosted = Background(Gather(DOWN, None, down, *sems).last_ring(), DOWN_PLAN)
    j = pl.program_id(0)
    away = Push(b_away, OWN_BODY, b_rows, b_sems, 0)
    tile = lambda n: Push(a_rows.at[n], TAILS, a_rows.at[n], a_sems, n)
    at_step(0)(enter)
    hosted.visit("start")

    @at_step(0)
    def _():
        for move in fetches:
            move.wait()
        first = Torus().at["c"] == 0
        def scale(s, tile, tokens):
            d = pad(gz[s].astype(F32) * row(vec, S2))
            left, right = d[:, :HALF], d[:, D - HALF:]
            put_rows(b_rows, TAILS, s, jnp.where(first, left, right))
            put_rows(b_away, OWN_BODY, s, jnp.where(first, right, left))

        each_seq(scale)

    at_step(1)(away.start)
    for n in range(TILES):
        at_step(n + 1)(tile(n).start)

    @pl.when(j < TILES)
    def _():
        u = dot(h2[...], feed.get(j)[...]) + b_up[0]
        phi = 0.5 * (1.0 + lax.erf(u * math.sqrt(0.5)))
        slope[...] = phi + u * (jnp.exp(-0.5 * u * u) * math.sqrt(0.5 / math.pi))
        place = lax.rem(lax.broadcasted_iota(jnp.int32, (TT, 1), 0), TOK)
        a = only(place < SEQ, u * phi).astype(BF16)
        act[...] = a
        for s in SEQ_PAIR:
            put_rows(a_rows.at[j], TAILS, s, a[TOK * s:TOK * s + TOK])

    at_step(TILES)(away.wait)
    for n in range(TILES):
        at_step(TILES + n)(tile(n).wait)

    @pl.when(j >= TILES)
    def _():
        d_down[...] = dot_tn(a_rows[j - TILES], b_rows[...])

    hosted.visit("end")

    @at_step(2 * TILES - 1)
    def _():
        away.finish()
        for n in range(TILES):
            tile(n).finish()


def mlp_in_call(h2, gz, w_up, b_up, vec, down, collective_id):
    low = lambda j: jnp.minimum(j, TILES - 1)
    high = lambda j: jnp.maximum(j - TILES, 0)
    return pl.pallas_call(
        mlp_in_kernel, grid=(2 * TILES,),
        out_shape=(sds(BF16, TT, FF), sds(F32, TT, FF), sds(F32, FF, HALF), sds(BF16, *Gather.shape(DOWN))),
        in_specs=[ANY] * O + [along(0, 1, 1, HALF, index=low), whole(8, D), ANY],
        out_specs=(along(1, TT, HALF, index=low), along(1, TT, HALF, index=low),
                   along(0, HALF, HALF, index=high), ANY),
        scratch_shapes=[pltpu.VMEM((TILES, ROWS, HALF), BF16), pltpu.VMEM((ROWS, HALF), BF16),
                        pltpu.VMEM((PAIR * TOK, HALF), BF16), pltpu.VMEM((TT, D), BF16), pltpu.VMEM(SEQS, BF16),
                        pltpu.SemaphoreType.DMA, pltpu.SemaphoreType.DMA] + Feed.scratch(BF16, D, HALF) + Push.semaphores(TILES) + Push.semaphores(1) +
        Gather.semaphores(),
        input_output_aliases={SIDE + 1: O},
        compiler_params=comm_params(collective_id), name="mlp_in",
    )(h2, gz, w_up, b_up.reshape(TILES, 1, HALF), vec, down)


def tile_cols(n):
    return pl.ds(pl.multiple_of(n * HALF, HALF), HALF)


MLP_PLAN = {"start": ((0, 0, 1),), "end": ((1, 1, 2), (3, 2, 3), (TILES - 1, 3, None))}


def mlp_out_kernel(act_in, slope_in, gz, up_in, down_in, vec, part, d_pre, db_up, mlp_out, d_out, sums, dm, mlp, d_h2, mlp_sem,
                   d_sem, *scratch):
    scratch, tiles = scratch[:-8], scratch[-8:]
    stores = [pltpu.make_async_copy(*move) for move in ((mlp, mlp_out, mlp_sem), (d_h2, d_out, d_sem))]
    first = First(Bands(DOWN), part, sums, *scratch)
    hosted = Background([first.near, first.far, first.relay, first.settle, first.finish], MLP_PLAN)
    j = pl.program_id(0)
    blocks = (lambda n: act_in.at[:, tile_cols(n)], lambda n: slope_in.at[:, tile_cols(n)],
              lambda n: up_in.at[lax.div(n, PAIR), :, tile_cols(lax.rem(n, PAIR))], lambda n: down_in.at[tile_cols(n)])
    feeds = [Feed(block, TILES, *tiles[PAIR * i:][:PAIR]) for i, block in enumerate(blocks)]
    first_feeds(*feeds)
    at_step(0)(enter)
    hosted.visit("start")

    @at_step(0)
    def _():
        def scale(s, tile, tokens):
            dm[tile] = pad(gz[s].astype(F32) * row(vec, S2))

        each_seq(scale)

    act, slope, w_up, w_down = (feed.get(j) for feed in feeds)
    db_up[0] = jnp.zeros((1, HALF), F32)

    def back(s, tile, tokens):
        accumulate(mlp.at[tile], dot(act[tile], w_down[...]))
        d = dot_nt(dm[tile], w_down[...]) * slope[tile]
        db_up[0] += col_sum(d)
        d = d.astype(BF16)
        d_pre[0, 0, tile] = d
        accumulate(d_h2.at[tile], dot_nt(d, w_up[...]))

    each_seq(back)
    for move in stores:
        at_step(TILES - 1)(move.start)
    hosted.visit("end")
    for move in stores:
        at_step(TILES - 1)(move.wait)


def mlp_out_call(act, slope, gz, w_up, w_down, vec, part, collective_id):
    return pl.pallas_call(
        mlp_out_kernel, grid=(TILES,),
        out_shape=(sds(BF16, PAIR, SIDE, TT, HALF), sds(F32, TILES, 1, HALF), sds(F32, TT, D), sds(F32, TT, D),
                   Bands(DOWN).sums()),
        in_specs=[ANY, ANY, whole(*SEQS), ANY, ANY, whole(8, D), ANY],
        out_specs=(pl.BlockSpec((1, 1, TT, HALF), lambda j: (j % PAIR, j // PAIR, 0, 0)), along(0, 1, 1, HALF),
                   ANY, ANY, ANY),
        scratch_shapes=[pltpu.VMEM((TT, D), BF16), pltpu.VMEM((TT, D), F32), pltpu.VMEM((TT, D), F32),
                        pltpu.SemaphoreType.DMA, pltpu.SemaphoreType.DMA] + Bands(DOWN).first() + Feed.scratch(BF16, TT, HALF) +
        Feed.scratch(F32, TT, HALF) + Feed.scratch(BF16, D, HALF) + Feed.scratch(BF16, HALF, D),
        compiler_params=comm_params(collective_id), name="mlp_out",
    )(act, slope, gz, w_up, w_down, vec, part)


def halves_of(t):
    t = pad(t)
    return t[:, :HALF], jnp.concatenate([t[:, HALF:], jnp.zeros((TOK, QCOLS - D), BF16)], axis=1)


def mid(mlp, d_h2, att, x, gz, w_out, vec, z, g_res, d_att, d_o, sums):
    a = att[:SEQ]
    y = x[...].astype(F32) + row(vec, S1) * a
    m = mlp[:SEQ] + row(vec, B2)
    g = gz[...].astype(F32)
    z[0] = (y + row(vec, S2) * m).astype(BF16)
    xhat, rstd = norm_stats(y)
    dh = d_h2[:SEQ]
    gr = g + norm_back(xhat, rstd, dh * row(vec, G2))
    g_res[:SEQ] = gr
    da = gr * row(vec, S1)
    terms = (da, gr * a, dh * xhat, dh, g * row(vec, S2), g * m)
    accumulate(sums, jnp.concatenate([jnp.zeros((BO, D), F32)] + [col_sum(t) for t in terms], axis=0))
    for i, t in enumerate(halves_of(da)):
        d_att[i] = t
    d_o[...] = dot_nt(pad(da), w_out[...]).astype(BF16)


def attention_back(s, qkv, d_o, d_qkv, db, acc, b_rows, away, first, visit):
    acc[...] = jnp.zeros_like(acc)

    def head(h):
        lanes, mask = window(h)
        q, k, v = (only(mask, qkv[i, :SEQ, lanes]) for i in (Q, K, V))
        do = only(mask, d_o[:SEQ, lanes])
        scores = dot_nt(k, q) * SCALE
        e = jnp.exp(scores - jnp.max(scores, axis=0, keepdims=True))
        probs = e * (1.0 / col_sum(e))
        acc[V, :, lanes] += dot(probs.astype(BF16), do)
        dp = dot_nt(v, do)
        ds = probs * (dp - col_sum(dp * probs))
        ds = (ds * SCALE).astype(BF16)
        acc[K, :, lanes] += dot(ds, q)
        acc[Q, :, lanes] += dot_tn(ds, k)

    each_head(head, PAIR)
    visit("half")
    accumulate(db, jnp.concatenate([col_sum(acc[i]) for i in (Q, K, V)], axis=0))
    for n in (Q, K, V):
        left, right = halves_of(acc[n])
        d_qkv[0, n] = left
        d_qkv[1, n] = right
        put_rows(b_rows.at[n], TAILS, s, jnp.where(first, left, right))
        put_rows(away.at[n], OWN_BODY, s, jnp.where(first, right, left))


PER = HALF // STEP


class WideGrads:
    def __init__(self, inputs, a_of, cotangents, out, base, lead, a_rows, a_cols, b_rows):
        self.inputs, self.a_of, self.cotangents, self.out, self.base, self.lead = inputs, a_of, cotangents, out, base, lead
        self.a_rows, self.a_cols, self.b_rows = a_rows, a_cols, b_rows

    @staticmethod
    def scratch(inputs):
        return [pltpu.VMEM((inputs, ROWS, D), BF16), pltpu.VMEM((inputs, D, ROWS), BF16), pltpu.VMEM((SIDE, ROWS, HALF), BF16)]

    def turn(self, i):
        def trip(n, carry):
            lanes = pl.ds(pl.multiple_of(n * LANES, LANES), LANES)
            self.a_cols[i, lanes] = self.a_rows[i, :, lanes].T
            return carry

        lax.fori_loop(0, D // LANES, trip, 0)

    def step(self):
        j = pl.program_id(0)
        done = []
        for t in range(SIDE):
            n = (t + self.lead) % SIDE

            @at_step(self.base + PER * t)
            def _():
                i = self.a_of[n]
                if i not in done:
                    self.inputs[i].wait()
                    self.turn(i)
                    done.append(i)
                self.cotangents[n].wait()

        @pl.when(j >= self.base)
        def _():
            n = lax.rem(lax.div(j - self.base, PER) + self.lead, SIDE)
            cols = pl.ds(pl.multiple_of(lax.rem(j - self.base, PER) * STEP, STEP), STEP)
            i = 0 if len(self.inputs) == 1 else lax.div(n, O)
            self.out[0] = dot(self.a_cols[i], self.b_rows[n, :, cols])

    def finish(self):
        for move in (*self.inputs, *self.cotangents):
            move.finish()


def grads_block(base, lead):
    def index(j):
        n = jnp.maximum(j - base, 0)
        return (n // PER + lead) % SIDE, 0, n % PER

    return pl.BlockSpec((1, D, STEP), index)


GRAD_STEPS = PER * SIDE


def tok_block():
    return along(0, TOK, D, index=upto(LAST_SEQ))


def seq_block():
    return along(0, 1, SEQ, D, index=upto(LAST_SEQ))


MID_PLAN = {"start": ((0, 0, 1),), "end": ((1, 1, 3), (8, 3, 4), (11, 4, 5), (LAST_SEQ + GRAD_STEPS, 5, None))}


def mid_kernel(*refs):
    refs = list(refs)
    take = lambda n: [refs.pop(0) for _ in range(n)]
    ins, (w_attn, vec), (h2, d_pre, acc), outs, (d_up, result) = take(5), take(2), take(3), take(5), take(2)
    tiles, (w_out, w_sem) = [take(PAIR) for _ in ins], take(PAIR)
    tokens = lambda n: pl.ds(pl.multiple_of(n * TOK, TAIL), TOK)
    feeds = [Feed(lambda n, ref=ref: ref.at[tokens(n) if len(ref.shape) == PAIR else n], SEQS[0], *tile)
             for ref, tile in zip(ins, tiles)]
    fetch = pltpu.make_async_copy(w_attn.at[O, :, pl.ds(0, D)], w_out, w_sem)
    first_feeds(*feeds)
    at_step(0)(fetch.start)
    rows, a_sems, b_sems = take(3), take(C), take(C)
    rest = Rest(Bands(DOWN), acc, result, *refs)
    hosted = Background([rest.begin, rest.loaded, rest.relay, rest.settle, rest.relay_third, rest.settle_third, rest.finish],
                        MID_PLAN)
    c = Torus().at["c"]
    grads = WideGrads(
        [Exchange(h2, h2, rows[0].at[0], a_sems, ())], (0,) * SIDE,
        [Exchange(d_pre.at[c, n], d_pre.at[1 - c, n], rows[2].at[n], b_sems, (n,)) for n in range(SIDE)], d_up, SEQS[0], 0, *rows)
    at_step(0)(enter)
    hosted.visit("start")

    @at_step(0)
    def _():
        for move in (*grads.inputs, *grads.cotangents):
            move.start()

    j = pl.program_id(0)

    @pl.when(j < SEQS[0])
    def _():
        blocks = [feed.get(j) for feed in feeds]
        at_step(0)(fetch.wait)
        mid(*blocks, w_out, vec, *outs)

    grads.step()
    hosted.visit("end")
    at_step(LAST_SEQ + GRAD_STEPS)(grads.finish)


def mid_call(mlp, d_h2, att, x, gz, vec, w_attn, h2, d_pre, acc, collective_id):
    return pl.pallas_call(
        mid_kernel, grid=(SEQS[0] + GRAD_STEPS,),
        out_shape=(sds(BF16, *SEQS), sds(F32, TT, D), sds(BF16, PAIR, TT, HALF), sds(BF16, TT, D), sds(F32, 8, D),
                   sds(F32, SIDE, D, HALF), Bands(DOWN).result()),
        in_specs=[ANY] * (O + O) + [whole(8, D)] + [ANY] * O,
        out_specs=(seq_block(), tok_block(), along(1, PAIR, TOK, HALF, index=upto(LAST_SEQ)), tok_block(), whole(8, D),
                   grads_block(SEQS[0], 0), ANY),
        scratch_shapes=Feed.scratch(F32, TOK, D) * O + Feed.scratch(BF16, SEQ, D) * PAIR +
        [pltpu.VMEM((D, D), BF16), pltpu.SemaphoreType.DMA] + WideGrads.scratch(1) + Exchange.semaphores() + Exchange.semaphores(SIDE) +
        Bands(DOWN).later(),
        compiler_params=comm_params(collective_id), name="mid",
    )(mlp, d_h2, att, x, gz, w_attn, vec, h2, d_pre, acc)


ATTN_PLAN = {"start": ((0, 0, 2),), "half": ((0, 2, 4),), "end": ((SIDE, 4, 5), (LAST_SEQ + GRAD_STEPS, 5, None))}


def attn_back_kernel(*refs):
    refs = list(refs)
    take = lambda n: [refs.pop(0) for _ in range(n)]
    (qkv_in, do_in), (h1, o, d_att, part, result), (d_qkv, db, d_attn, sums, total) = take(2), take(5), take(5)
    acc, away, rows, tiles = refs.pop(0), refs.pop(0), take(3), take(SIDE)
    tokens = lambda n: pl.ds(pl.multiple_of(n * TOK, TAIL), TOK)
    feeds = [Feed(lambda n: qkv_in.at[:, tokens(n)], SEQS[0], *tiles[:PAIR]),
             Feed(lambda n: do_in.at[tokens(n)], SEQS[0], *tiles[PAIR:])]
    first_feeds(*feeds)
    a_sems, b_sems, away_sems = take(C), take(C), take(PAIR)
    first = First(Bands(WIDE), part, sums, *take(len(Bands(WIDE).first())))
    spread = Spread(Bands(DOWN), result, total, *refs)
    hosted = Background([spread.begin, first.near, first.far, spread.forward, first.relay, first.settle, first.finish,
                         spread.finish], ATTN_PLAN)
    c = Torus().at["c"]
    pushes = [Push(away.at[n], OWN_BODY, rows[2].at[n], away_sems, n) for n in range(O)]
    grads = WideGrads(
        [Exchange(a, a, rows[0].at[i], a_sems, (i,)) for i, a in enumerate((h1, o))], (0,) * O + (1,),
        pushes + [Exchange(d_att.at[c], d_att.at[1 - c], rows[2].at[O], b_sems, ())], d_attn, SEQS[0], O, *rows)
    at_step(0)(enter)
    hosted.visit("start")

    @at_step(0)
    def _():
        for move in (*grads.inputs, grads.cotangents[O]):
            move.start()

    @at_step(SEQS[0])
    def _():
        for push in pushes:
            push.start()

    j = pl.program_id(0)

    @pl.when(j < SEQS[0])
    def _():
        qkv, d_o = (feed.get(j) for feed in feeds)
        attention_back(j, qkv, d_o, d_qkv, db, acc, rows[2], away, c == 0, hosted.visit)


    grads.step()
    hosted.visit("end")
    at_step(LAST_SEQ + GRAD_STEPS)(grads.finish)


def attn_back_call(qkv, d_o, h1, o, d_att, part, result, collective_id):
    return pl.pallas_call(
        attn_back_kernel, grid=(SEQS[0] + GRAD_STEPS,),
        out_shape=(sds(BF16, PAIR, O, TT, HALF), sds(F32, O, D), sds(F32, SIDE, D, HALF), Bands(WIDE).sums(),
                   Bands(DOWN).total()),
        in_specs=[ANY] * 7,
        out_specs=(along(2, PAIR, O, TOK, HALF, index=upto(LAST_SEQ)), whole(O, D), grads_block(SEQS[0], O), ANY, ANY),
        scratch_shapes=[pltpu.VMEM((O, SEQ, D), F32), pltpu.VMEM((O, PAIR * TOK, HALF), BF16)] + WideGrads.scratch(2) +
        Feed.scratch(BF16, O, TOK, D) + Feed.scratch(BF16, TOK, D) + Exchange.semaphores(PAIR) + Exchange.semaphores() + Push.semaphores(O) + Bands(WIDE).first() + Spread.scratch(),
        compiler_params=comm_params(collective_id), name="attn_back",
    )(qkv, d_o, h1, o, d_att, part, result)


IN_STEPS = PAIR * O
SLOT = 40
LAST_PLAN = {"start": ((0, 0, 2),), "end": ((O, 2, None),)}


CORE_COLS = D - HALF
KEPT = 48
GRADS = ((KEPT, O * D), (KEPT, D), (KEPT, FF), (PAIR, C, UNIT, D), (SIDE, KEPT, LANES))
SHARES = PAIR * SIDE + SIDE + PAIR


def split_rows(totals, first, keep, give):
    def trip(x, carry):
        for total, bands in totals:
            rows = jnp.concatenate([total[x, k, :n] for k, (_, n) in enumerate(BANDS[WIDE])], axis=0)
            low, high = rows[:KEPT], jnp.concatenate([rows[OWN:], rows[:KEPT - OWN]], axis=0)
            keep[x, :, bands.cols] = jnp.where(first, low, high)
            give[x, :, bands.cols] = jnp.where(first, high, low)
        return carry

    lax.fori_loop(0, SIDE, trip, 0)


class Finals:
    def __init__(self, down, up, attn, outs, sems):
        self.c = Torus().at["c"]
        self.down, self.up, self.attn, self.sems = down, up, attn, sems
        self.qkv, self.out, self.up_out, self.down_out, self.pad = outs
        self.edge = pl.ds(CORE_COLS, LANES)

    def cols(self, base, width):
        return pl.ds(pl.multiple_of(base + self.c * HALF, LANES), width)

    def up_share(self, x):
        place = self.up_out.at[:, self.cols(QCOLS * x, HALF)]
        return Share(*(ref.at[x] for ref in self.up), place, self.sems, x)

    def block(self, x):
        return (self.out, 0) if x == O else (self.qkv, D * x)

    def attn_share(self, x):
        out, base = self.block(x)
        sides = (ref.at[x, :, pl.ds(0, CORE_COLS)] for ref in self.attn)
        return Share(*sides, out.at[:, self.cols(base, CORE_COLS)], self.sems, SIDE + x)

    def edge_share(self, x, padding):
        out, base = self.block(x)
        place = self.pad.at[x] if padding else out.at[:, pl.ds(base + CORE_COLS, LANES)]
        return Share(*(ref.at[x, :, self.edge] for ref in self.attn), place, self.sems, PAIR * SIDE + x)

    def down_share(self, edge):
        src = self.edge if edge else pl.ds(pl.multiple_of(self.c * LANES, LANES), CORE_COLS)
        sides = (self.down.at[pl.ds(PAIR * c, PAIR), :, :, src] for c in (self.c, 1 - self.c))
        place = self.down_out.at[:, :, :, self.edge if edge else self.cols(0, CORE_COLS)]
        return Share(*sides, place, self.sems, SHARES - PAIR + edge)

    def start_down(self):
        self.down_share(0).start()
        pl.when(self.c == 0)(lambda: self.down_share(1).start())

    def start(self):
        for x in range(SIDE):
            self.attn_share(x).start()
            pl.when(self.c == 0)(lambda: self.edge_share(x, False).start())
            pl.when(self.c == 1)(lambda: self.edge_share(x, True).start())

    def finish(self):
        for x in range(SIDE):
            for share in (self.up_share(x), self.attn_share(x), self.edge_share(x, True)):
                share.wait()
        self.down_share(0).wait()
        pl.when(self.c == 0)(lambda: self.down_share(1).sent())
        pl.when(self.c == 1)(lambda: self.down_share(1).far.wait_recv())


def last_kernel(*refs):
    refs = list(refs)
    take = lambda n: [refs.pop(0) for _ in range(n)]
    (d_qkv, w_attn, x_in, g_in, vec), (small, acc_up, down, _), (dx_out, part) = take(5), take(SIDE), take(PAIR)
    outs, (x, g_res, dx, x_sem, g_sem, dx_sem), tiles = take(len(GRADS)), take(SIDE + PAIR), take(SIDE)
    j = pl.program_id(0)
    fetches = [pltpu.make_async_copy(*move) for move in ((x_in, x, x_sem), (g_in, g_res, g_sem))]
    store = pltpu.make_async_copy(dx, dx_out, dx_sem)
    feeds = [Feed(lambda n: d_qkv.at[lax.rem(n, PAIR), lax.div(n, PAIR)], IN_STEPS, *tiles[:PAIR]),
             Feed(lambda n: w_attn.at[lax.div(n, PAIR), :, pl.ds(pl.multiple_of(lax.rem(n, PAIR) * HALF, HALF), HALF)],
                  IN_STEPS, *tiles[PAIR:])]
    first_feeds(*feeds)
    (acc, sums, pair_sums, block), (totals, sides), block_sem, swap_sems = take(4), (take(C), take(SIDE)), refs.pop(0), take(PAIR)
    finals = Finals(down, sides[:PAIR], sides[PAIR:], outs, take(C))
    halves = [Bands(WIDE, h) for h in WAYS]
    a, b = (First(bands, part, None, *take(len(bands.first()))) for bands in halves)
    rest_a, rest_b = (Rest(f.bands, f.own_all, None, f.own_all, *take(len(f.bands.later()) - 1)) for f in (a, b))
    rest_up = Rest(Bands(WIDE), acc_up, None, *take(len(Bands(WIDE).later())))
    spread_up, spread_a, spread_b = (
        Spread(r.bands, r.sums(), total, *take(PAIR), None) for r, total in zip((rest_up, rest_a, rest_b), totals))
    hosted = Background([rest_up.begin, a.near, rest_up.loaded, rest_up.relay], LAST_PLAN)
    first = finals.c == 0
    swap = remote(sums, pair_sums, swap_sems, (), Torus().partner())
    fetch = pltpu.make_async_copy(small, block, block_sem)
    at_step(0)(enter)
    hosted.visit("start")

    @at_step(0)
    def _():
        for move in (fetch, *fetches):
            move.start()
        finals.start_down()

    @pl.when(j < IN_STEPS)
    def _():
        d_half, w = (feed.get(j) for feed in feeds)
        each_seq(lambda s, tile, tokens: accumulate(acc.at[tile], dot_nt(d_half[tile], w[...])))

    @at_step(IN_STEPS - 1)
    def _():
        for move in fetches:
            move.wait()
        sums[...] = jnp.zeros_like(sums)

        def back(s, tile, tokens):
            xhat, rstd = norm_stats(x[s].astype(F32))
            dh = acc[tokens]
            sums[:BO] += jnp.concatenate([col_sum(dh * xhat), col_sum(dh)], axis=0)
            dx[s] = (g_res[tokens] + norm_back(xhat, rstd, dh * row(vec, G1))).astype(BF16)

        each_seq(back)
        store.start()

    hosted.visit("end")

    @at_step(IN_STEPS)
    def _():
        swap.start()
        fetch.wait()
        swap.wait()
        both = sums[...] + pair_sums[...]
        for d in range(DEVICES):
            at = CHIP * (d // PAIR) + SLOT + OWN * (d % PAIR)
            block[at:at + BO, :OWN] = both[:BO, OWN * d:OWN * d + OWN]

        @pl.when(finals.c == 1)
        def _():
            for z in range(SIDE):
                for y in range(SIDE):
                    rows = block.at[pl.ds(CHIP * (SIDE * z + y), CHIP)]
                    put = pltpu.make_async_copy(rows, part.at[0, z, y, :, pl.ds(CORE_COLS, LANES)], block_sem)
                    put.start()
            pltpu.make_async_copy(block, small, block_sem).wait()

        def share_up():
            spread_up.finish()
            split_rows([(totals[0], Bands(WIDE))], first, *sides[:PAIR])
            for x in range(SIDE):
                finals.up_share(x).start()

        for step in (b.near, rest_up.settle, a.far, rest_up.relay_third, b.far, a.relay, rest_up.settle_third, spread_up.begin,
                     b.relay, spread_up.forward, functools.partial(a.settle, rest_a.send),
                     functools.partial(b.settle, rest_b.send), rest_a.relay, rest_b.relay, rest_a.settle, rest_b.settle,
                     share_up, rest_a.relay_third, rest_b.relay_third, rest_a.settle_third, spread_a.begin,
                     rest_b.settle_third, spread_b.begin, spread_a.forward, spread_b.forward, spread_a.finish, spread_b.finish):
            step()
        split_rows(list(zip(totals[1:], halves)), first, *sides[PAIR:])
        finals.start()
        for user in (rest_up, rest_a, rest_b, a, b, finals):
            user.finish()
        store.wait()


def last_call(d_qkv, w_attn, x, g_res, vec, small, acc_up, down, part, collective_id):
    halves = [Bands(WIDE, h) for h in WAYS]
    dma = pltpu.SemaphoreType.DMA
    rings = [Bands(WIDE), *halves]
    return pl.pallas_call(
        last_kernel, grid=(IN_STEPS + 1,),
        out_shape=(sds(BF16, *SEQS), sds(F32, *part.shape), *(sds(F32, *shape) for shape in GRADS)),
        in_specs=[ANY] * SIDE + [whole(8, D)] + [ANY] * SIDE,
        out_specs=(ANY,) * (len(GRADS) + PAIR),
        scratch_shapes=[pltpu.VMEM(SEQS, BF16), pltpu.VMEM((TT, D), F32), pltpu.VMEM(SEQS, BF16), dma, dma, dma] + Feed.scratch(BF16, TT, HALF) +
        Feed.scratch(BF16, D, HALF) + [pltpu.VMEM((TT, D), F32), pltpu.VMEM((SUB, D), F32), pltpu.VMEM((SUB, D), F32),
                        pltpu.VMEM((D, LANES), F32)] + [r.vmem(SIDE, C) for r in rings] +
        [pltpu.VMEM((SIDE, KEPT, HALF), F32)] * SIDE + [dma, dma, dma] + [dma((SHARES,))] * C + halves[0].first() * PAIR +
        halves[0].later()[1:] * PAIR + Bands(WIDE).later() + Spread.scratch()[:PAIR] * C,
        input_output_aliases={8: 1},
        compiler_params=comm_params(collective_id), name="last",
    )(d_qkv, w_attn, x, g_res, vec, small, acc_up, down, part)


BQ, BU, VEC = 3 * D // 32, 3 * D // 32 + FF // 32, 3 * D // 32 + FF // 32 + 8 * OWN


def pair_swap(a):
    return lax.ppermute(a, "fsdp", [(i, i ^ 1) for i in range(DEVICES)])


def by_core(first, a, b):
    return jnp.where(first, a, b), jnp.where(first, b, a)


def my_pieces(shards, first):
    w_qkv, b_qkv, w_out, w_up, b_up, w_down, vec_params = shards
    x = lax.axis_index("rep")
    small = jnp.concatenate([b_qkv, b_up, vec_params.reshape(-1)])
    small = jnp.pad(small, (0, OWN * LANES - VEC)).reshape(OWN, LANES)
    attn = lax.dynamic_slice_in_dim(jnp.concatenate([w_qkv, w_out], axis=1), x * D, D, 1)
    attn = jnp.concatenate([attn, small], axis=1)
    up = lax.dynamic_slice_in_dim(w_up, x * QCOLS, QCOLS, 1)
    wide = jnp.stack([attn, up]).astype(BF16)
    mine, theirs = by_core(first, wide[..., :HALF], wide[..., HALF:])
    theirs = pair_swap(theirs)
    piece = jnp.concatenate(by_core(first, mine, theirs), axis=1)
    down = lax.dynamic_slice_in_dim(w_down, x * 48, 48, 0).astype(BF16).reshape(3, 16, D)
    return piece[0], piece[1], down


def small_params(w_attn):
    small = w_attn[0, :, D:].astype(F32).reshape(DEVICES, OWN * LANES)
    vec = small[:, BU:VEC].reshape(DEVICES, 8, OWN).transpose(1, 0, 2).reshape(8, D)
    return small[:, :BQ].reshape(O, 1, D), small[:, BQ:BU].reshape(FF), vec


ROOM = 5 * LANES


def small_grads(db_qkv, db_up, sums):
    vec = sums[BO:].reshape(8 - BO, DEVICES, OWN).transpose(1, 0, 2).reshape(DEVICES, VEC - BU - BO * OWN)
    small = jnp.concatenate([db_qkv.reshape(DEVICES, BQ), db_up.reshape(DEVICES, BU - BQ), vec], axis=1)
    small = small + pair_swap(small)
    small = jnp.pad(small, ((0, 0), (0, ROOM - small.shape[1]))).reshape(DEVICES, ROOM // LANES, LANES)
    return jnp.pad(small, ((0, 0), (0, OWN - ROOM // LANES), (0, 0))).reshape(D, LANES)


def device_step(x, gz, *shards):
    first = lax.rem(lax.axis_index("fsdp"), PAIR) == 0
    attn, up, down = my_pieces(shards, first)
    w_attn, up, down = gather_call(attn, up, down, 0)
    w_attn = w_attn.reshape(SIDE, D, QCOLS)
    b_qkv, b_up, vec = small_params(w_attn)
    qkv, h1, o, att, h2, w_up = front_call(x, w_attn, b_qkv, vec, up, 1)
    w_up = w_up.reshape(SIDE, D, QCOLS)
    act, slope, part, w_down = mlp_in_call(h2, gz, w_up, b_up, vec, down, 2)
    part = part.reshape((SIDE,) * 3 + (C * UNIT, HALF))
    d_pre, db_up, mlp, d_h2, acc = mlp_out_call(act, slope, gz, w_up, w_down.reshape(FF, D), vec, part, 3)
    z, g_res, d_att, d_o, sums, part, result = mid_call(mlp, d_h2, att, x, gz, vec, w_attn, h2, d_pre, acc, 4)
    part = part.reshape((SIDE,) * 3 + (CHIP, HALF))
    d_qkv, db_qkv, part, acc, down = attn_back_call(qkv, d_o, h1, o, d_att, part, result, 5)
    small = small_grads(db_qkv, db_up, sums)
    part = part.reshape((SIDE,) * 3 + (CHIP, HALF))
    dx, _, g_qkv, g_out, g_up, g_down, edge = last_call(d_qkv, w_attn, x, g_res, vec, small, acc, down, part, 6)
    small = edge[0, :ROOM // LANES].reshape(ROOM)
    vec = jnp.concatenate([edge[0, SLOT:SLOT + BO, :OWN], small[BU:VEC - BO * OWN].reshape(8 - BO, OWN)], axis=0)
    g_qkv, g_out, g_up = (g[:OWN] for g in (g_qkv, g_out, g_up))
    return z, dx, g_qkv, small[:BQ], g_out, g_up, small[BQ:BU], g_down.reshape(FF // DEVICES, D), vec


def solution(mesh):
    batch = P(("rep", "fsdp"), None, None)
    rows, flat, cols = P("fsdp", None), P("fsdp"), P(None, "fsdp")
    shards = (rows, flat, rows, rows, flat, rows, cols)
    return jax.shard_map(device_step, mesh=mesh, in_specs=(batch, batch) + shards,
                         out_specs=(batch, batch) + shards, check_vma=False)
```

```python
import functools
import math

import jax
import jax.numpy as jnp
from jax import lax
from jax.experimental import pallas as pl
from jax.experimental.pallas import tpu as pltpu
from jax.sharding import PartitionSpec as P

HEADS = 16
LN_EPS = 1e-5
D = 1408
FF = 6144
SEQ = 257
HEAD = D // HEADS
SCALE = HEAD ** -0.5
QCOLS = 1536
HALF = 768
OWN = 44
CHIP = 2 * OWN
LANES = 128
DEVICES = 32
F32 = jnp.float32
BF16 = jnp.bfloat16
VMEM_LIMIT = 66 * 1000 * 1000
G1, C1, BO, S1, G2, C2, B2, S2 = range(8)
Q, K, V, O = range(4)
SEQS = (2, SEQ, D)
LAST_SEQ = SEQS[0] - 1
SEQ_PAIR = range(SEQS[0])
TAIL = 16
BODY = SEQ - 1
TOK = BODY + TAIL
TT = 2 * TOK
ROWS = 4 * TOK
STEP = 256


def sds(dtype, *shape):
    return jax.ShapeDtypeStruct(shape, dtype)


MESH_ID = pl.DeviceIdType.MESH
SIDE = 4
SUB = 8
PAIR = 2
C = 3
COLOURS = range(C)
COLOUR_DIMS = ("xyz", "yzx", "zxy")
FIRST, SECOND, THIRD, LAST = range(4)
WAYS = range(PAIR)
NEAR, FAR, ADDED = 0, 2, 4
WIDE, DOWN = "wide", "down"
ANY = pl.BlockSpec(memory_space=pl.ANY)
ALL = slice(None)


def duo(m):
    return pl.ds(PAIR * m, PAIR)


def toward(m):
    return 1 - PAIR * (m % PAIR)


class Torus:
    def __init__(self):
        f = lax.axis_index("fsdp")
        self.at = {"x": lax.axis_index("rep"), "z": lax.div(f, SIDE * PAIR), "y": lax.rem(lax.div(f, PAIR), SIDE),
                   "c": lax.rem(f, PAIR)}

    def shift(self, dim, by):
        return lax.rem(self.at[dim] + (SIDE + by), SIDE)

    def device(self, **moved):
        p = {**self.at, **moved}
        return (p["x"], (p["z"] * SIDE + p["y"]) * PAIR + p["c"])

    def neighbour(self, dim, by):
        return self.device(**{dim: self.shift(dim, by)})

    def partner(self):
        return self.device(c=1 - self.at["c"])


def enter():
    me = Torus()
    barrier = pltpu.get_barrier_semaphore()
    others = [me.neighbour(d, toward(m)) for d in COLOUR_DIMS[0] for m in WAYS] + [me.partner()]
    for other in others:
        pl.semaphore_signal(barrier, device_id=other, device_id_type=MESH_ID)
    pl.semaphore_wait(barrier, len(others))


def remote(src, dst, sems, slot, device):
    return pltpu.make_async_remote_copy(src_ref=src, dst_ref=dst, send_sem=sems[0].at[slot], recv_sem=sems[1].at[slot],
                                        device_id=device, device_id_type=MESH_ID)


class Gather:
    def __init__(self, kind, src, dst, hop_send, hop_recv, push_send, push_recv, local):
        self.kind, self.src, self.dst, self.local = kind, src, dst, local
        self.hops, self.pushes = (hop_send, hop_recv), (push_send, push_recv)
        self.cols, self.cut = (256, 128) if kind == WIDE else (D, HALF)

    @staticmethod
    def semaphores():
        dma = pltpu.SemaphoreType.DMA
        return [dma((C, C, ADDED))] * PAIR + [dma((C, ADDED + 1))] * PAIR + [dma((C,))]

    @staticmethod
    def shape(kind):
        return (SIDE,) * 3 + (CHIP, QCOLS) if kind == WIDE else (SIDE, SIDE, PAIR, SIDE, C, 16, D)

    def source(self, k):
        return self.src.at[:, pl.ds(self.cols * k, self.cols)] if self.kind == WIDE else self.src.at[k]

    def piece(self, me, k, s, v, half=None):
        dims = COLOUR_DIMS[k]
        at = {**me.at, **{d: ALL for d in dims[:s]}, dims[s]: v}
        off, width = 0, self.cols
        if half is not None and s == FIRST:
            off, width = self.cut * half, (self.cut, self.cols - self.cut)[half]
        elif half is not None:
            at[dims[0]] = duo(half)
        if self.kind == WIDE:
            cols = pl.ds(pl.multiple_of(at["c"] * HALF + self.cols * k + off, 128), width)
            return self.dst.at[at["x"], at["z"], at["y"], :, cols]
        return self.dst.at[at["z"], at["y"], at["c"], at["x"], k, :, pl.ds(off, width)]

    def hop(self, k, s, m):
        me = Torus()
        dim = COLOUR_DIMS[k][s]
        by = toward(m)
        if m < FAR:
            ref = self.piece(me, k, s, me.at[dim])
        else:
            ref = self.piece(me, k, s, me.shift(dim, -by), m - FAR)
        src = self.source(k) if s == FIRST and m < FAR else ref
        return remote(src, ref, self.hops, (k, s, m), me.neighbour(dim, by))

    def push(self, k, n):
        me = Torus()
        dim = COLOUR_DIMS[k][THIRD]
        if n < FAR:
            ref = self.piece(me, k, THIRD, me.shift(dim, -toward(n)))
        elif n < ADDED:
            ref = self.piece(me, k, THIRD, me.shift(dim, FAR), n - FAR)
        else:
            ref = self.piece(me, k, THIRD, me.at[dim])
        return remote(ref, ref, self.pushes, (k, n), me.partner())

    def own(self, k):
        me = Torus()
        return pltpu.make_async_copy(self.source(k), self.piece(me, k, FIRST, me.at[COLOUR_DIMS[k][FIRST]]), self.local.at[k])

    def launch(self, s):
        for k in COLOURS:
            for m in WAYS:
                self.hop(k, s, m).start()
            if s == THIRD:
                self.push(k, ADDED).start()

    def relay(self, s):
        for k in COLOURS:
            for m in WAYS:
                self.hop(k, s, m).wait_recv()
                self.hop(k, s, FAR + m).start()
                if s == THIRD:
                    self.push(k, m).start()

    def settle(self, s):
        for k in COLOURS:
            for m in WAYS:
                self.hop(k, s, FAR + m).wait_recv()
                if s == THIRD:
                    self.push(k, FAR + m).start()
            if s == FIRST:
                self.own(k).wait()

    def begin(self):
        for k in COLOURS:
            self.own(k).start()
        self.launch(FIRST)

    def sent(self, *rings):
        for k in COLOURS:
            for s in rings:
                for m in range(ADDED):
                    self.hop(k, s, m).wait_send()
            if THIRD in rings:
                for n in range(ADDED + 1):
                    self.push(k, n).wait()

    def last_ring(self):
        return [functools.partial(f, THIRD) for f in (self.launch, self.relay, self.settle, self.sent)]


def add_into(total, *others):
    lead = total.shape[:-2]

    def body(i, carry):
        idx = []
        for n in reversed(lead):
            idx.insert(0, lax.rem(i, n))
            i = lax.div(i, n)
        value = total[tuple(idx)]
        for other in others:
            value = value + other[tuple(idx)]
        total[tuple(idx)] = value
        return carry

    lax.fori_loop(0, math.prod(lead), body, 0)


class Ring:
    def __init__(self, s, bands, terms, passed, relay, landing, send, recv):
        self.s, self.bands, self.terms, self.passed, self.relay, self.landing = s, bands, terms, passed, relay, landing
        self.sems = (send, recv)

    def zone(self, k, way, half):
        if self.s == THIRD:
            return self.landing.at[k, way, self.bands.cuts(k)[half]]
        return self.bands.rows(self.landing.at[k, way, duo(half)], k)

    def carried(self, ref, k, way):
        if self.s == THIRD:
            return ref.at[k, way, pl.ds(0, self.bands.cuts(k)[way].size)]
        return self.bands.rows(ref.at[k, way], k)

    def hop(self, k, m):
        me = Torus()
        dim = COLOUR_DIMS[k][self.s]
        way, by = m % PAIR, toward(m)
        if m < FAR:
            src, dst = self.terms(k, me.shift(dim, FAR), way), self.carried(self.relay, k, way)
        elif m < ADDED:
            src, dst = self.terms(k, me.shift(dim, by), 1 - way), self.zone(k, way, 1 - way)
        else:
            src, dst = self.carried(self.passed, k, way), self.zone(k, way, way)
        return remote(src, dst, self.sems, (k, m), me.neighbour(dim, by))

    def start(self, k, base):
        for m in WAYS:
            self.hop(k, base + m).start()

    def arrived(self, k, base):
        for m in WAYS:
            self.hop(k, base + m).wait_recv()

    def finish(self):
        for k in COLOURS:
            for m in range(ADDED + PAIR):
                self.hop(k, m).wait_send()

    @staticmethod
    def semaphores():
        return [pltpu.SemaphoreType.DMA((C, ADDED + PAIR))] * PAIR


UNIT = 32
BANDS = {WIDE: ((0, 24), (24, UNIT), (56, UNIT)), DOWN: ((0, UNIT), (UNIT, UNIT), (2 * UNIT, UNIT))}
ORDERS = {WIDE: "xzy", DOWN: "zyx"}


class Bands:
    def __init__(self, kind, half=None):
        self.order, self.bands = ORDERS[kind], BANDS[kind]
        self.width = HALF if half is None else HALF // PAIR
        self.cols = pl.ds(self.width * (half or 0), self.width)

    def band(self, k):
        return pl.ds(*self.bands[k])

    def rows(self, ref, k):
        return ref.at[(ALL,) * (len(ref.shape) - PAIR) + (pl.ds(0, self.bands[k][1]),)]

    def cuts(self, k):
        rows = self.bands[k][1]
        cut = (rows // SUB + 1) // PAIR * SUB
        return pl.ds(0, cut), pl.ds(cut, rows - cut)

    def rest(self, k):
        return [d for d in self.order if d != COLOUR_DIMS[k][FIRST]]

    def units(self, *lead):
        return lead + (UNIT, self.width)

    def vmem(self, *lead):
        return pltpu.VMEM(self.units(*lead), F32)

    def sums(self):
        return sds(F32, *self.units(C, SIDE, SIDE))

    def result(self):
        return sds(F32, *self.units(C))

    def total(self):
        return sds(F32, *self.units(SIDE, C))

    def first(self):
        relays = [self.vmem(C, PAIR, PAIR, SIDE)] * PAIR
        dma = pltpu.SemaphoreType.DMA
        return [self.vmem(C, SIDE, SIDE), *relays, self.vmem(C, PAIR, SIDE, SIDE), *Ring.semaphores(), dma((C, C)), dma((C,))]

    def later(self):
        dma = pltpu.SemaphoreType.DMA
        return [self.vmem(C, SIDE, SIDE), self.vmem(C, PAIR, PAIR), self.vmem(C, PAIR, SIDE),
                pltpu.VMEM((C, PAIR, UNIT // PAIR, self.width), F32), self.vmem(C, PAIR),
                *Ring.semaphores(), *Ring.semaphores(), dma((C,)), dma((C,))]


class First:
    def __init__(self, bands, part, acc, own, passed, relay, landing, send, recv, load, store):
        self.bands, self.part, self.acc, self.own_all, self.passed = bands, part, acc, own, passed
        self.relay_in, self.landing, self.load_sem, self.store_sem = relay, landing, load, store
        self.ring = Ring(FIRST, bands, self.terms, passed, relay, landing, send, recv)

    def own(self, k):
        return self.bands.rows(self.own_all.at[k], k)

    def terms(self, k, v, half=None):
        b = self.bands
        at = {d: ALL for d in b.order}
        at[COLOUR_DIMS[k][FIRST]] = v
        if half is not None:
            at[b.rest(k)[0]] = duo(half)
        return self.part.at[tuple(at[d] for d in b.order) + (b.band(k), b.cols)]

    def load(self, k, m):
        me = Torus()
        dim = COLOUR_DIMS[k][FIRST]
        if m in WAYS:
            src, dst = self.terms(k, me.shift(dim, toward(m)), m), self.ring.carried(self.passed, k, m)
        else:
            src, dst = self.terms(k, me.at[dim]), self.own(k)
        return pltpu.make_async_copy(src, dst, self.load_sem.at[k, m])

    def store(self, k):
        return pltpu.make_async_copy(self.own(k), self.bands.rows(self.acc.at[k], k), self.store_sem.at[k])

    def near(self):
        for k in COLOURS:
            self.ring.start(k, NEAR)

    def far(self):
        for k in COLOURS:
            self.ring.start(k, FAR)
        for m in COLOURS:
            for k in COLOURS:
                self.load(k, m).start()

    def relay(self):
        for k in COLOURS:
            self.ring.arrived(k, NEAR)
            for m in WAYS:
                self.load(k, m).wait()
                add_into(self.ring.carried(self.passed, k, m), self.ring.carried(self.relay_in, k, m))
            self.ring.start(k, ADDED)

    def settle(self, then=None):
        for k in COLOURS:
            self.load(k, FAR).wait()
            for base in (FAR, ADDED):
                self.ring.arrived(k, base)
            add_into(self.own(k), *(self.bands.rows(self.landing.at[k, m], k) for m in WAYS))
            if then is None:
                self.store(k).start()
            else:
                then(k)

    def finish(self):
        self.ring.finish()
        if self.acc is not None:
            for k in COLOURS:
                self.store(k).wait()


class Rest:
    def __init__(self, bands, acc, result, own, relay2, in2, relay3, in3, *sems):
        self.bands, self.acc, self.own, self.result = bands, acc, own, result
        self.in2, self.in3, self.relay2, self.relay3, self.load_sem, self.store_sem = in2, in3, relay2, relay3, *sems[-2:]
        self.second = Ring(SECOND, bands, functools.partial(self.terms, acc), relay2, relay2, in2, *sems[:PAIR])
        self.third = Ring(THIRD, bands, self.final, relay3, relay3, in3, *sems[PAIR:2 * PAIR])

    def terms(self, ref, k, v, half=None):
        other = ALL if half is None else duo(half)
        first = self.bands.rest(k)[0] == COLOUR_DIMS[k][SECOND]
        return self.bands.rows(ref.at[(k, v, other) if first else (k, other, v)], k)

    def final(self, k, v, half=None):
        if half is None:
            return self.bands.rows(self.in2.at[k, 0, v], k)
        return self.in2.at[k, 0, v, self.bands.cuts(k)[half]]

    def load(self, k):
        return pltpu.make_async_copy(self.bands.rows(self.acc.at[k], k), self.bands.rows(self.own.at[k], k), self.load_sem.at[k])

    def store(self, k):
        rows = self.bands.rows
        return pltpu.make_async_copy(rows(self.in3.at[k, 0], k), rows(self.result.at[k], k), self.store_sem.at[k])

    def send(self, k):
        for base in (NEAR, FAR):
            self.second.start(k, base)

    def begin(self):
        for k in COLOURS:
            self.send(k)
        for k in COLOURS:
            self.load(k).start()

    def loaded(self):
        for k in COLOURS:
            self.load(k).wait()

    def relay(self):
        me = Torus()
        for k in COLOURS:
            self.second.arrived(k, NEAR)
            for m in WAYS:
                terms = self.terms(self.own, k, me.shift(COLOUR_DIMS[k][SECOND], toward(m)), m)
                add_into(self.second.carried(self.relay2, k, m), terms)
            self.second.start(k, ADDED)

    def settle(self):
        me = Torus()
        for k in COLOURS:
            for base in (FAR, ADDED):
                self.second.arrived(k, base)
            plus, minus = (self.bands.rows(self.in2.at[k, m], k) for m in WAYS)
            add_into(plus, minus, self.terms(self.own, k, me.at[COLOUR_DIMS[k][SECOND]]))
            for base in (NEAR, FAR):
                self.third.start(k, base)

    def relay_third(self):
        me = Torus()
        for k in COLOURS:
            self.third.arrived(k, NEAR)
            for m in WAYS:
                mine = self.third.carried(self.relay3, k, m)
                mine[...] += self.final(k, me.shift(COLOUR_DIMS[k][THIRD], toward(m)), m)[...]
            self.third.start(k, ADDED)

    def settle_third(self):
        me = Torus()
        for k in COLOURS:
            for base in (FAR, ADDED):
                self.third.arrived(k, base)
            plus, minus = (self.bands.rows(self.in3.at[k, m], k) for m in WAYS)
            plus[...] += minus[...] + self.final(k, me.at[COLOUR_DIMS[k][THIRD]])[...]
            if self.result is not None:
                self.store(k).start()

    def finish(self):
        self.second.finish()
        self.third.finish()
        if self.result is not None:
            for k in COLOURS:
                self.store(k).wait()

    def sums(self):
        return self.in3.at[:, 0]


class Spread:
    def __init__(self, bands, result, total, send, recv, local):
        self.bands, self.result, self.total, self.sems, self.local = bands, result, total, (send, recv), local

    @staticmethod
    def scratch():
        return [pltpu.SemaphoreType.DMA((C, ADDED))] * PAIR + [pltpu.SemaphoreType.DMA((C,))]

    def mine(self, k):
        return self.bands.rows(self.result.at[k], k)

    def place(self, k):
        return self.bands.rows(self.total.at[Torus().at["x"], k], k)

    def hop(self, k, m):
        me = Torus()
        by = toward(m)
        if m < FAR:
            src, dst = self.mine(k), self.place(k)
        else:
            dst = src = self.total.at[me.shift("x", -by), k, self.bands.cuts(k)[m - FAR]]
        return remote(src, dst, self.sems, (k, m), me.neighbour("x", by))

    def own(self, k):
        return pltpu.make_async_copy(self.mine(k), self.place(k), self.local.at[k])

    def begin(self):
        for k in COLOURS:
            if self.local is None:
                self.place(k)[...] = self.mine(k)[...]
            else:
                self.own(k).start()
            for m in WAYS:
                self.hop(k, m).start()

    def forward(self):
        for k in COLOURS:
            for m in WAYS:
                self.hop(k, m).wait_recv()
                self.hop(k, FAR + m).start()

    def finish(self):
        for k in COLOURS:
            for m in WAYS:
                self.hop(k, FAR + m).wait_recv()
            if self.local is not None:
                self.own(k).wait()
            for m in range(ADDED):
                self.hop(k, m).wait_send()


def comm_params(collective_id):
    return pltpu.CompilerParams(collective_id=collective_id, has_side_effects=True, vmem_limit_bytes=VMEM_LIMIT)


def gather_kernel(*refs):
    n = len(Gather.semaphores())
    a, u, d = (Gather(kind, *refs[i::C][:PAIR], *refs[PAIR * C + n * i:][:n]) for i, kind in enumerate((WIDE, WIDE, DOWN)))
    enter()
    for gather in (a, u, d):
        gather.begin()
    for step, *ring in ((a.relay, FIRST), (u.relay, FIRST), (d.relay, FIRST), (a.settle, FIRST), (a.launch, SECOND),
                        (u.settle, FIRST), (u.launch, SECOND), (a.relay, SECOND), (d.settle, FIRST), (d.launch, SECOND),
                        (u.relay, SECOND), (a.settle, SECOND), (a.launch, THIRD), (d.relay, SECOND), (u.settle, SECOND),
                        (a.relay, THIRD), (d.settle, SECOND), (a.settle, THIRD), (u.sent, FIRST, SECOND),
                        (d.sent, FIRST, SECOND), (a.sent, FIRST, SECOND, THIRD)):
        step(*ring)


def gather_call(attn, up, down, collective_id):
    return pl.pallas_call(
        gather_kernel, out_shape=[sds(BF16, *Gather.shape(kind)) for kind in (WIDE, WIDE, DOWN)], in_specs=[ANY] * C,
        out_specs=[ANY] * C, scratch_shapes=Gather.semaphores() * C, compiler_params=comm_params(collective_id),
        name="gather")(attn, up, down)


class Background:
    def __init__(self, steps, plan):
        self.steps, self.plan = steps, plan

    def visit(self, place):
        for j, first, end in self.plan.get(place, ()):
            @at_step(j)
            def _():
                for step in self.steps[first:end]:
                    step()


class Feed:
    def __init__(self, block, steps, buffers, sems):
        self.block, self.steps, self.buffers, self.sems = block, steps, buffers, sems

    @staticmethod
    def scratch(dtype, *shape):
        return [pltpu.VMEM((PAIR,) + shape, dtype), pltpu.SemaphoreType.DMA((PAIR,))]

    def copy(self, j):
        slot = lax.rem(j, PAIR)
        return pltpu.make_async_copy(self.block(j), self.buffers.at[slot], self.sems.at[slot])

    def get(self, j):
        pl.when(j + 1 < self.steps)(lambda: self.copy(j + 1).start())
        self.copy(j).wait()
        return self.buffers.at[lax.rem(j, PAIR)]


def first_feeds(*feeds):
    @at_step(0)
    def _():
        for feed in feeds:
            feed.copy(0).start()


class Share:
    def __init__(self, mine, theirs, place, sems, slot):
        self.local = pltpu.make_async_copy(mine, place, sems[PAIR].at[slot])
        self.far = remote(theirs, place, sems, slot, Torus().partner())

    def start(self):
        self.far.start()
        self.local.start()

    def sent(self):
        self.local.wait()
        self.far.wait_send()

    def wait(self):
        self.sent()
        self.far.wait_recv()


class Push:
    def __init__(self, src, tail, rows, sems, slot=0):
        body = BODY * len(SEQ_PAIR)
        tails = TAIL * len(SEQ_PAIR)
        self.copies = [
            remote(src.at[pl.ds(start, size)], rows.at[pl.ds(to, size)], sems, (slot, i), Torus().partner())
            for i, (start, to, size) in enumerate(((0, body, body), (tail, PAIR * body + tails, tails)))]

    @staticmethod
    def semaphores(n):
        return [pltpu.SemaphoreType.DMA((n, PAIR))] * PAIR

    def start(self):
        for copy in self.copies:
            copy.start()

    def wait(self):
        for copy in self.copies:
            copy.wait_recv()

    def finish(self):
        for copy in self.copies:
            copy.wait_send()


class Exchange:
    def __init__(self, mine, theirs, rows, sems, slot):
        self.moves = []
        for s in SEQ_PAIR:
            for i, (start, size) in enumerate(((0, BODY), (BODY, TAIL))):
                place = lambda n: rows.at[pl.ds(start * len(SEQ_PAIR) * PAIR + size * n, size)]
                part = pl.ds(TOK * s + start, size)
                at = slot + (PAIR * s + i,)
                local = pltpu.make_async_copy(mine.at[part], place(s), sems[2].at[at])
                far = remote(theirs.at[part], place(len(SEQ_PAIR) + s), sems, at, Torus().partner())
                self.moves.append((local, far))

    @staticmethod
    def semaphores(*lead):
        return [pltpu.SemaphoreType.DMA(lead + (2 * PAIR,))] * 3

    def start(self):
        for local, far in self.moves:
            far.start()
            local.start()

    def wait(self):
        for local, far in self.moves:
            local.wait()
            far.wait_recv()

    def finish(self):
        for _, far in self.moves:
            far.wait_send()


NT = (((1,), (1,)), ((), ()))
TN = (((0,), (0,)), ((), ()))


def dot(a, b):
    return jnp.dot(a, b, preferred_element_type=F32)


def dot_nt(a, b):
    return lax.dot_general(a, b, NT, preferred_element_type=F32)


def dot_tn(a, b):
    return lax.dot_general(a, b, TN, preferred_element_type=F32)


def zeros_but(n, axis, value):
    return tuple(value if i == axis else 0 for i in range(n))


def whole(*shape):
    return pl.BlockSpec(shape, lambda *_: (0,) * len(shape))


def along(axis, *block, index=lambda j: j):
    return pl.BlockSpec(block, lambda j: zeros_but(len(block), axis, index(j)))


def row(vec, i):
    return vec[i:i + 1]


def row_mean(t):
    return jnp.mean(t, axis=-1, keepdims=True)


def norm_stats(t):
    centered = t - row_mean(t)
    rstd = lax.rsqrt(row_mean(centered * centered) + LN_EPS)
    return centered * rstd, rstd


def norm_back(xhat, rstd, g):
    return rstd * (g - row_mean(g) - xhat * row_mean(g * xhat))


def col_sum(t):
    return jnp.sum(t, axis=0, keepdims=True)


def at_step(j):
    return pl.when(pl.program_id(0) == j)


def accumulate(ref, value):
    @at_step(0)
    def _():
        ref[...] = value

    @pl.when(pl.program_id(0) > 0)
    def _():
        ref[...] += value


def pad(t):
    return jnp.concatenate([t.astype(F32), jnp.zeros((TOK - SEQ, t.shape[1]), F32)], axis=0).astype(BF16)


WINDOW = 2 * LANES


def window(h):
    first = h * HEAD
    start = jnp.minimum(lax.div(first, LANES) * LANES, D - WINDOW)
    lane = lax.broadcasted_iota(jnp.int32, (1, WINDOW), 1) + (start - first)
    return pl.ds(pl.multiple_of(start, LANES), WINDOW), (lane >= 0) & (lane < HEAD)


def each_head(body, unroll):
    def trip(i, carry):
        for n in range(unroll):
            body(i * unroll + n)
        return carry

    lax.fori_loop(0, HEADS // unroll, trip, 0)


def each_seq(body):
    def trip(s, carry):
        start = pl.multiple_of(s * TOK, TAIL)
        body(s, pl.ds(start, TOK), pl.ds(start, SEQ))
        return carry

    lax.fori_loop(0, len(SEQ_PAIR), trip, 0)


def only(mask, t):
    return jnp.where(mask, t, jnp.zeros_like(t))


def softmax(scores):
    e = jnp.exp(scores - jnp.max(scores, axis=-1, keepdims=True))
    return e * (1.0 / jnp.sum(e, axis=-1, keepdims=True))


def attention(s, rows, o, acc, visit):
    acc[...] = jnp.zeros_like(acc)
    start = pl.multiple_of(s * TOK, TAIL)
    tokens = pl.ds(start, SEQ)

    def head(h):
        lanes, mask = window(h)
        k = only(mask, rows[K, tokens, lanes])
        v = only(mask, rows[V, tokens, lanes])
        probs = softmax(dot_nt(rows[Q, tokens, lanes], k) * SCALE).astype(BF16)
        acc[:, lanes] += dot(probs, v)

    each_head(head, PAIR)
    visit("half")
    o[pl.ds(start, TOK)] = pad(acc[...])


FRONT_PLAN = {"start": ((0, 0, 1),), "end": ((O, 1, 2), (O + 1, 2, None))}


def front_kernel(x_in, w_in, b, vec, _, qkv_out, h1_out, o_out, att_out, h2_out, up, rows, lhs, att, h2, acc, x,
                 x_sem, w_rows, w_sems, sems, *ring_sems):
    hosted = Background(Gather(WIDE, None, up, *ring_sems).last_ring(), FRONT_PLAN)
    j = pl.program_id(0)
    weights = Feed(lambda n: w_in.at[n, :, pl.ds(0, D)], SIDE, w_rows, w_sems)
    fetch = pltpu.make_async_copy(x_in, x, x_sem)
    h1, o = (lhs.at[i] for i in WAYS)
    stores = [pltpu.make_async_copy(*move, sems.at[i]) for i, move in enumerate(
        ((h1, h1_out), (rows, qkv_out), (o, o_out), (att, att_out), (h2, h2_out)))]
    at_step(0)(fetch.start)
    first_feeds(weights)
    at_step(0)(enter)
    hosted.visit("start")

    @at_step(0)
    def _():
        fetch.wait()

        def norm(s, tile, tokens):
            xhat, _ = norm_stats(x[s].astype(F32))
            h1[tile] = pad(xhat * row(vec, G1) + row(vec, C1))

        each_seq(norm)

    for i in WAYS:
        at_step(PAIR * i + 1)(stores[i].start)

    @pl.when(j >= O)
    def _():
        attention(j - O, rows, o, acc, hosted.visit)

    @pl.when((j < O) | (j == O + LAST_SEQ))
    def _():
        bias = jnp.where(j < O, b[0], row(vec, BO))
        att[...] = dot(lhs[lax.div(j, O)], weights.get(jnp.minimum(j, O))[...]) + bias

    @pl.when(j < O)
    def _():
        rows[j] = att[...].astype(BF16)

    @at_step(O + LAST_SEQ)
    def _():
        def norm(s, tile, tokens):
            xhat, _ = norm_stats(x[s].astype(F32) + row(vec, S1) * att[tokens])
            h2[tile] = pad(xhat * row(vec, G2) + row(vec, C2))

        each_seq(norm)
        for store in stores[PAIR:]:
            store.start()

    hosted.visit("end")

    @at_step(O + LAST_SEQ)
    def _():
        for store in stores:
            store.wait()


def upto(n):
    return lambda j: jnp.minimum(j, n)


def front_call(x, w_attn, b_qkv, vec, up, collective_id):
    outs = ((BF16, O, TT, D), (BF16, TT, D), (BF16, TT, D), (F32, TT, D), (BF16, TT, D), (BF16, *Gather.shape(WIDE)))
    dma = pltpu.SemaphoreType.DMA
    return pl.pallas_call(
        front_kernel, grid=(O + PAIR,), out_shape=[sds(*out) for out in outs],
        in_specs=[ANY, ANY, along(0, 1, 1, D, index=upto(V)), whole(8, D), ANY], out_specs=[ANY] * len(outs),
        scratch_shapes=[pltpu.VMEM((O, TT, D), BF16), pltpu.VMEM((PAIR, TT, D), BF16), pltpu.VMEM((TT, D), F32),
                        pltpu.VMEM((TT, D), BF16), pltpu.VMEM((SEQ, D), F32), pltpu.VMEM(SEQS, BF16), dma] +
        Feed.scratch(BF16, D, D) + [dma((SIDE + 1,))] + Gather.semaphores(),
        input_output_aliases={SIDE: SIDE + 1},
        compiler_params=comm_params(collective_id), name="front",
    )(x, w_attn, b_qkv, vec, up)


TILES = FF // HALF
OWN_BODY = BODY * len(SEQ_PAIR)
TAILS = ROWS - TAIL * PAIR * len(SEQ_PAIR)


def put_rows(ref, tail, s, t):
    ref[pl.ds(pl.multiple_of(BODY * s, BODY), BODY)] = t[:BODY]
    ref[pl.ds(pl.multiple_of(tail + TAIL * s, TAIL), TAIL)] = t[BODY:]


DOWN_PLAN = {"start": ((0, 0, 1),), "end": ((TILES - 1, 1, 2), (TILES + SIDE, 2, 3), (2 * TILES - 1, 3, None))}


def mlp_in_kernel(h2_in, gz_in, up_in, b_up, vec, _, act, slope, d_down, down, a_rows, b_rows, b_away, *sems):
    (h2, gz, h2_sem, gz_sem, *tiles), sems = sems[:SIDE + PAIR], sems[SIDE + PAIR:]
    feed = Feed(lambda n: up_in.at[lax.div(n, PAIR), :, tile_cols(lax.rem(n, PAIR))], TILES, *tiles)
    fetches = [pltpu.make_async_copy(*move) for move in ((gz_in, gz, gz_sem), (h2_in, h2, h2_sem))]
    for move in fetches:
        at_step(0)(move.start)
    first_feeds(feed)
    a_sems, b_sems, sems = sems[:PAIR], sems[PAIR:2 * PAIR], sems[2 * PAIR:]
    hosted = Background(Gather(DOWN, None, down, *sems).last_ring(), DOWN_PLAN)
    j = pl.program_id(0)
    away = Push(b_away, OWN_BODY, b_rows, b_sems, 0)
    tile = lambda n: Push(a_rows.at[n], TAILS, a_rows.at[n], a_sems, n)
    at_step(0)(enter)
    hosted.visit("start")

    @at_step(0)
    def _():
        for move in fetches:
            move.wait()
        first = Torus().at["c"] == 0
        def scale(s, tile, tokens):
            d = pad(gz[s].astype(F32) * row(vec, S2))
            left, right = d[:, :HALF], d[:, D - HALF:]
            put_rows(b_rows, TAILS, s, jnp.where(first, left, right))
            put_rows(b_away, OWN_BODY, s, jnp.where(first, right, left))

        each_seq(scale)

    at_step(1)(away.start)
    for n in range(TILES):
        at_step(n + 1)(tile(n).start)

    @pl.when(j < TILES)
    def _():
        u = dot(h2[...], feed.get(j)[...]) + b_up[0]
        phi = 0.5 * (1.0 + lax.erf(u * math.sqrt(0.5)))
        slope[...] = phi + u * (jnp.exp(-0.5 * u * u) * math.sqrt(0.5 / math.pi))
        place = lax.rem(lax.broadcasted_iota(jnp.int32, (TT, 1), 0), TOK)
        a = only(place < SEQ, u * phi).astype(BF16)
        act[...] = a
        for s in SEQ_PAIR:
            put_rows(a_rows.at[j], TAILS, s, a[TOK * s:TOK * s + TOK])

    at_step(TILES)(away.wait)
    for n in range(TILES):
        at_step(TILES + n)(tile(n).wait)

    @pl.when(j >= TILES)
    def _():
        d_down[...] = dot_tn(a_rows[j - TILES], b_rows[...])

    hosted.visit("end")

    @at_step(2 * TILES - 1)
    def _():
        away.finish()
        for n in range(TILES):
            tile(n).finish()


def mlp_in_call(h2, gz, w_up, b_up, vec, down, collective_id):
    low = lambda j: jnp.minimum(j, TILES - 1)
    high = lambda j: jnp.maximum(j - TILES, 0)
    return pl.pallas_call(
        mlp_in_kernel, grid=(2 * TILES,),
        out_shape=(sds(BF16, TT, FF), sds(F32, TT, FF), sds(F32, FF, HALF), sds(BF16, *Gather.shape(DOWN))),
        in_specs=[ANY] * O + [along(0, 1, 1, HALF, index=low), whole(8, D), ANY],
        out_specs=(along(1, TT, HALF, index=low), along(1, TT, HALF, index=low),
                   along(0, HALF, HALF, index=high), ANY),
        scratch_shapes=[pltpu.VMEM((TILES, ROWS, HALF), BF16), pltpu.VMEM((ROWS, HALF), BF16),
                        pltpu.VMEM((PAIR * TOK, HALF), BF16), pltpu.VMEM((TT, D), BF16), pltpu.VMEM(SEQS, BF16),
                        pltpu.SemaphoreType.DMA, pltpu.SemaphoreType.DMA] + Feed.scratch(BF16, D, HALF) + Push.semaphores(TILES) + Push.semaphores(1) +
        Gather.semaphores(),
        input_output_aliases={SIDE + 1: O},
        compiler_params=comm_params(collective_id), name="mlp_in",
    )(h2, gz, w_up, b_up.reshape(TILES, 1, HALF), vec, down)


def tile_cols(n):
    return pl.ds(pl.multiple_of(n * HALF, HALF), HALF)


MLP_PLAN = {"start": ((0, 0, 1),), "end": ((1, 1, 2), (3, 2, 3), (TILES - 1, 3, None))}


def mlp_out_kernel(act_in, slope_in, gz, up_in, down_in, vec, part, d_pre, db_up, mlp_out, d_out, sums, dm, mlp, d_h2, mlp_sem,
                   d_sem, *scratch):
    scratch, tiles = scratch[:-8], scratch[-8:]
    stores = [pltpu.make_async_copy(*move) for move in ((mlp, mlp_out, mlp_sem), (d_h2, d_out, d_sem))]
    first = First(Bands(DOWN), part, sums, *scratch)
    hosted = Background([first.near, first.far, first.relay, first.settle, first.finish], MLP_PLAN)
    j = pl.program_id(0)
    blocks = (lambda n: act_in.at[:, tile_cols(n)], lambda n: slope_in.at[:, tile_cols(n)],
              lambda n: up_in.at[lax.div(n, PAIR), :, tile_cols(lax.rem(n, PAIR))], lambda n: down_in.at[tile_cols(n)])
    feeds = [Feed(block, TILES, *tiles[PAIR * i:][:PAIR]) for i, block in enumerate(blocks)]
    first_feeds(*feeds)
    at_step(0)(enter)
    hosted.visit("start")

    @at_step(0)
    def _():
        def scale(s, tile, tokens):
            dm[tile] = pad(gz[s].astype(F32) * row(vec, S2))

        each_seq(scale)

    act, slope, w_up, w_down = (feed.get(j) for feed in feeds)
    db_up[0] = jnp.zeros((1, HALF), F32)

    def back(s, tile, tokens):
        accumulate(mlp.at[tile], dot(act[tile], w_down[...]))
        d = dot_nt(dm[tile], w_down[...]) * slope[tile]
        db_up[0] += col_sum(d)
        d = d.astype(BF16)
        d_pre[0, 0, tile] = d
        accumulate(d_h2.at[tile], dot_nt(d, w_up[...]))

    each_seq(back)
    for move in stores:
        at_step(TILES - 1)(move.start)
    hosted.visit("end")
    for move in stores:
        at_step(TILES - 1)(move.wait)


def mlp_out_call(act, slope, gz, w_up, w_down, vec, part, collective_id):
    return pl.pallas_call(
        mlp_out_kernel, grid=(TILES,),
        out_shape=(sds(BF16, PAIR, SIDE, TT, HALF), sds(F32, TILES, 1, HALF), sds(F32, TT, D), sds(F32, TT, D),
                   Bands(DOWN).sums()),
        in_specs=[ANY, ANY, whole(*SEQS), ANY, ANY, whole(8, D), ANY],
        out_specs=(pl.BlockSpec((1, 1, TT, HALF), lambda j: (j % PAIR, j // PAIR, 0, 0)), along(0, 1, 1, HALF),
                   ANY, ANY, ANY),
        scratch_shapes=[pltpu.VMEM((TT, D), BF16), pltpu.VMEM((TT, D), F32), pltpu.VMEM((TT, D), F32),
                        pltpu.SemaphoreType.DMA, pltpu.SemaphoreType.DMA] + Bands(DOWN).first() + Feed.scratch(BF16, TT, HALF) +
        Feed.scratch(F32, TT, HALF) + Feed.scratch(BF16, D, HALF) + Feed.scratch(BF16, HALF, D),
        compiler_params=comm_params(collective_id), name="mlp_out",
    )(act, slope, gz, w_up, w_down, vec, part)


def halves_of(t):
    t = pad(t)
    return t[:, :HALF], jnp.concatenate([t[:, HALF:], jnp.zeros((TOK, QCOLS - D), BF16)], axis=1)


def mid(mlp, d_h2, att, x, gz, w_out, vec, z, g_res, d_att, d_o, sums):
    a = att[:SEQ]
    y = x[...].astype(F32) + row(vec, S1) * a
    m = mlp[:SEQ] + row(vec, B2)
    g = gz[...].astype(F32)
    z[0] = (y + row(vec, S2) * m).astype(BF16)
    xhat, rstd = norm_stats(y)
    dh = d_h2[:SEQ]
    gr = g + norm_back(xhat, rstd, dh * row(vec, G2))
    g_res[:SEQ] = gr
    da = gr * row(vec, S1)
    terms = (da, gr * a, dh * xhat, dh, g * row(vec, S2), g * m)
    accumulate(sums, jnp.concatenate([jnp.zeros((BO, D), F32)] + [col_sum(t) for t in terms], axis=0))
    for i, t in enumerate(halves_of(da)):
        d_att[i] = t
    d_o[...] = dot_nt(pad(da), w_out[...]).astype(BF16)


def attention_back(s, qkv, d_o, d_qkv, db, acc, b_rows, away, first, visit):
    acc[...] = jnp.zeros_like(acc)

    def head(h):
        lanes, mask = window(h)
        q, k, v = (only(mask, qkv[i, :SEQ, lanes]) for i in (Q, K, V))
        do = only(mask, d_o[:SEQ, lanes])
        scores = dot_nt(k, q) * SCALE
        e = jnp.exp(scores - jnp.max(scores, axis=0, keepdims=True))
        probs = e * (1.0 / col_sum(e))
        acc[V, :, lanes] += dot(probs.astype(BF16), do)
        dp = dot_nt(v, do)
        ds = probs * (dp - col_sum(dp * probs))
        ds = (ds * SCALE).astype(BF16)
        acc[K, :, lanes] += dot(ds, q)
        acc[Q, :, lanes] += dot_tn(ds, k)

    each_head(head, PAIR)
    visit("half")
    accumulate(db, jnp.concatenate([col_sum(acc[i]) for i in (Q, K, V)], axis=0))
    for n in (Q, K, V):
        left, right = halves_of(acc[n])
        d_qkv[0, n] = left
        d_qkv[1, n] = right
        put_rows(b_rows.at[n], TAILS, s, jnp.where(first, left, right))
        put_rows(away.at[n], OWN_BODY, s, jnp.where(first, right, left))


PER = HALF // STEP


class WideGrads:
    def __init__(self, inputs, a_of, cotangents, out, base, lead, a_rows, a_cols, b_rows):
        self.inputs, self.a_of, self.cotangents, self.out, self.base, self.lead = inputs, a_of, cotangents, out, base, lead
        self.a_rows, self.a_cols, self.b_rows = a_rows, a_cols, b_rows

    @staticmethod
    def scratch(inputs):
        return [pltpu.VMEM((inputs, ROWS, D), BF16), pltpu.VMEM((inputs, D, ROWS), BF16), pltpu.VMEM((SIDE, ROWS, HALF), BF16)]

    def turn(self, i):
        def trip(n, carry):
            lanes = pl.ds(pl.multiple_of(n * LANES, LANES), LANES)
            self.a_cols[i, lanes] = self.a_rows[i, :, lanes].T
            return carry

        lax.fori_loop(0, D // LANES, trip, 0)

    def step(self):
        j = pl.program_id(0)
        done = []
        for t in range(SIDE):
            n = (t + self.lead) % SIDE

            @at_step(self.base + PER * t)
            def _():
                i = self.a_of[n]
                if i not in done:
                    self.inputs[i].wait()
                    self.turn(i)
                    done.append(i)
                self.cotangents[n].wait()

        @pl.when(j >= self.base)
        def _():
            n = lax.rem(lax.div(j - self.base, PER) + self.lead, SIDE)
            cols = pl.ds(pl.multiple_of(lax.rem(j - self.base, PER) * STEP, STEP), STEP)
            i = 0 if len(self.inputs) == 1 else lax.div(n, O)
            self.out[0] = dot(self.a_cols[i], self.b_rows[n, :, cols])

    def finish(self):
        for move in (*self.inputs, *self.cotangents):
            move.finish()


def grads_block(base, lead):
    def index(j):
        n = jnp.maximum(j - base, 0)
        return (n // PER + lead) % SIDE, 0, n % PER

    return pl.BlockSpec((1, D, STEP), index)


GRAD_STEPS = PER * SIDE


def tok_block():
    return along(0, TOK, D, index=upto(LAST_SEQ))


def seq_block():
    return along(0, 1, SEQ, D, index=upto(LAST_SEQ))


MID_PLAN = {"start": ((0, 0, 1),), "end": ((1, 1, 3), (8, 3, 4), (11, 4, 5), (LAST_SEQ + GRAD_STEPS, 5, None))}


def mid_kernel(*refs):
    refs = list(refs)
    take = lambda n: [refs.pop(0) for _ in range(n)]
    ins, (w_attn, vec), (h2, d_pre, acc), outs, (d_up, result) = take(5), take(2), take(3), take(5), take(2)
    tiles, (w_out, w_sem) = [take(PAIR) for _ in ins], take(PAIR)
    tokens = lambda n: pl.ds(pl.multiple_of(n * TOK, TAIL), TOK)
    feeds = [Feed(lambda n, ref=ref: ref.at[tokens(n) if len(ref.shape) == PAIR else n], SEQS[0], *tile)
             for ref, tile in zip(ins, tiles)]
    fetch = pltpu.make_async_copy(w_attn.at[O, :, pl.ds(0, D)], w_out, w_sem)
    first_feeds(*feeds)
    at_step(0)(fetch.start)
    rows, a_sems, b_sems = take(3), take(C), take(C)
    rest = Rest(Bands(DOWN), acc, result, *refs)
    hosted = Background([rest.begin, rest.loaded, rest.relay, rest.settle, rest.relay_third, rest.settle_third, rest.finish],
                        MID_PLAN)
    c = Torus().at["c"]
    grads = WideGrads(
        [Exchange(h2, h2, rows[0].at[0], a_sems, ())], (0,) * SIDE,
        [Exchange(d_pre.at[c, n], d_pre.at[1 - c, n], rows[2].at[n], b_sems, (n,)) for n in range(SIDE)], d_up, SEQS[0], 0, *rows)
    at_step(0)(enter)
    hosted.visit("start")

    @at_step(0)
    def _():
        for move in (*grads.inputs, *grads.cotangents):
            move.start()

    j = pl.program_id(0)

    @pl.when(j < SEQS[0])
    def _():
        blocks = [feed.get(j) for feed in feeds]
        at_step(0)(fetch.wait)
        mid(*blocks, w_out, vec, *outs)

    grads.step()
    hosted.visit("end")
    at_step(LAST_SEQ + GRAD_STEPS)(grads.finish)


def mid_call(mlp, d_h2, att, x, gz, vec, w_attn, h2, d_pre, acc, collective_id):
    return pl.pallas_call(
        mid_kernel, grid=(SEQS[0] + GRAD_STEPS,),
        out_shape=(sds(BF16, *SEQS), sds(F32, TT, D), sds(BF16, PAIR, TT, HALF), sds(BF16, TT, D), sds(F32, 8, D),
                   sds(F32, SIDE, D, HALF), Bands(DOWN).result()),
        in_specs=[ANY] * (O + O) + [whole(8, D)] + [ANY] * O,
        out_specs=(seq_block(), tok_block(), along(1, PAIR, TOK, HALF, index=upto(LAST_SEQ)), tok_block(), whole(8, D),
                   grads_block(SEQS[0], 0), ANY),
        scratch_shapes=Feed.scratch(F32, TOK, D) * O + Feed.scratch(BF16, SEQ, D) * PAIR +
        [pltpu.VMEM((D, D), BF16), pltpu.SemaphoreType.DMA] + WideGrads.scratch(1) + Exchange.semaphores() + Exchange.semaphores(SIDE) +
        Bands(DOWN).later(),
        compiler_params=comm_params(collective_id), name="mid",
    )(mlp, d_h2, att, x, gz, w_attn, vec, h2, d_pre, acc)


ATTN_PLAN = {"start": ((0, 0, 2),), "half": ((0, 2, 4),), "end": ((SIDE, 4, 5), (LAST_SEQ + GRAD_STEPS, 5, None))}


def attn_back_kernel(*refs):
    refs = list(refs)
    take = lambda n: [refs.pop(0) for _ in range(n)]
    (qkv_in, do_in), (h1, o, d_att, part, result), (d_qkv, db, d_attn, sums, total) = take(2), take(5), take(5)
    acc, away, rows, tiles = refs.pop(0), refs.pop(0), take(3), take(SIDE)
    tokens = lambda n: pl.ds(pl.multiple_of(n * TOK, TAIL), TOK)
    feeds = [Feed(lambda n: qkv_in.at[:, tokens(n)], SEQS[0], *tiles[:PAIR]),
             Feed(lambda n: do_in.at[tokens(n)], SEQS[0], *tiles[PAIR:])]
    first_feeds(*feeds)
    a_sems, b_sems, away_sems = take(C), take(C), take(PAIR)
    first = First(Bands(WIDE), part, sums, *take(len(Bands(WIDE).first())))
    spread = Spread(Bands(DOWN), result, total, *refs)
    hosted = Background([spread.begin, first.near, first.far, spread.forward, first.relay, first.settle, first.finish,
                         spread.finish], ATTN_PLAN)
    c = Torus().at["c"]
    pushes = [Push(away.at[n], OWN_BODY, rows[2].at[n], away_sems, n) for n in range(O)]
    grads = WideGrads(
        [Exchange(a, a, rows[0].at[i], a_sems, (i,)) for i, a in enumerate((h1, o))], (0,) * O + (1,),
        pushes + [Exchange(d_att.at[c], d_att.at[1 - c], rows[2].at[O], b_sems, ())], d_attn, SEQS[0], O, *rows)
    at_step(0)(enter)
    hosted.visit("start")

    @at_step(0)
    def _():
        for move in (*grads.inputs, grads.cotangents[O]):
            move.start()

    @at_step(SEQS[0])
    def _():
        for push in pushes:
            push.start()

    j = pl.program_id(0)

    @pl.when(j < SEQS[0])
    def _():
        qkv, d_o = (feed.get(j) for feed in feeds)
        attention_back(j, qkv, d_o, d_qkv, db, acc, rows[2], away, c == 0, hosted.visit)


    grads.step()
    hosted.visit("end")
    at_step(LAST_SEQ + GRAD_STEPS)(grads.finish)


def attn_back_call(qkv, d_o, h1, o, d_att, part, result, collective_id):
    return pl.pallas_call(
        attn_back_kernel, grid=(SEQS[0] + GRAD_STEPS,),
        out_shape=(sds(BF16, PAIR, O, TT, HALF), sds(F32, O, D), sds(F32, SIDE, D, HALF), Bands(WIDE).sums(),
                   Bands(DOWN).total()),
        in_specs=[ANY] * 7,
        out_specs=(along(2, PAIR, O, TOK, HALF, index=upto(LAST_SEQ)), whole(O, D), grads_block(SEQS[0], O), ANY, ANY),
        scratch_shapes=[pltpu.VMEM((O, SEQ, D), F32), pltpu.VMEM((O, PAIR * TOK, HALF), BF16)] + WideGrads.scratch(2) +
        Feed.scratch(BF16, O, TOK, D) + Feed.scratch(BF16, TOK, D) + Exchange.semaphores(PAIR) + Exchange.semaphores() + Push.semaphores(O) + Bands(WIDE).first() + Spread.scratch(),
        compiler_params=comm_params(collective_id), name="attn_back",
    )(qkv, d_o, h1, o, d_att, part, result)


IN_STEPS = PAIR * O
SLOT = 40
LAST_PLAN = {"start": ((0, 0, 2),), "end": ((O, 2, None),)}


CORE_COLS = D - HALF
KEPT = 48
GRADS = ((KEPT, O * D), (KEPT, D), (KEPT, FF), (PAIR, C, UNIT, D), (SIDE, KEPT, LANES))
SHARES = PAIR * SIDE + SIDE + PAIR


def split_rows(totals, first, keep, give):
    def trip(x, carry):
        for total, bands in totals:
            rows = jnp.concatenate([total[x, k, :n] for k, (_, n) in enumerate(BANDS[WIDE])], axis=0)
            low, high = rows[:KEPT], jnp.concatenate([rows[OWN:], rows[:KEPT - OWN]], axis=0)
            keep[x, :, bands.cols] = jnp.where(first, low, high)
            give[x, :, bands.cols] = jnp.where(first, high, low)
        return carry

    lax.fori_loop(0, SIDE, trip, 0)


class Finals:
    def __init__(self, down, up, attn, outs, sems):
        self.c = Torus().at["c"]
        self.down, self.up, self.attn, self.sems = down, up, attn, sems
        self.qkv, self.out, self.up_out, self.down_out, self.pad = outs
        self.edge = pl.ds(CORE_COLS, LANES)

    def cols(self, base, width):
        return pl.ds(pl.multiple_of(base + self.c * HALF, LANES), width)

    def up_share(self, x):
        place = self.up_out.at[:, self.cols(QCOLS * x, HALF)]
        return Share(*(ref.at[x] for ref in self.up), place, self.sems, x)

    def block(self, x):
        return (self.out, 0) if x == O else (self.qkv, D * x)

    def attn_share(self, x):
        out, base = self.block(x)
        sides = (ref.at[x, :, pl.ds(0, CORE_COLS)] for ref in self.attn)
        return Share(*sides, out.at[:, self.cols(base, CORE_COLS)], self.sems, SIDE + x)

    def edge_share(self, x, padding):
        out, base = self.block(x)
        place = self.pad.at[x] if padding else out.at[:, pl.ds(base + CORE_COLS, LANES)]
        return Share(*(ref.at[x, :, self.edge] for ref in self.attn), place, self.sems, PAIR * SIDE + x)

    def down_share(self, edge):
        src = self.edge if edge else pl.ds(pl.multiple_of(self.c * LANES, LANES), CORE_COLS)
        sides = (self.down.at[pl.ds(PAIR * c, PAIR), :, :, src] for c in (self.c, 1 - self.c))
        place = self.down_out.at[:, :, :, self.edge if edge else self.cols(0, CORE_COLS)]
        return Share(*sides, place, self.sems, SHARES - PAIR + edge)

    def start_down(self):
        self.down_share(0).start()
        pl.when(self.c == 0)(lambda: self.down_share(1).start())

    def start(self):
        for x in range(SIDE):
            self.attn_share(x).start()
            pl.when(self.c == 0)(lambda: self.edge_share(x, False).start())
            pl.when(self.c == 1)(lambda: self.edge_share(x, True).start())

    def finish(self):
        for x in range(SIDE):
            for share in (self.up_share(x), self.attn_share(x), self.edge_share(x, True)):
                share.wait()
        self.down_share(0).wait()
        pl.when(self.c == 0)(lambda: self.down_share(1).sent())
        pl.when(self.c == 1)(lambda: self.down_share(1).far.wait_recv())


def last_kernel(*refs):
    refs = list(refs)
    take = lambda n: [refs.pop(0) for _ in range(n)]
    (d_qkv, w_attn, x_in, g_in, vec), (small, acc_up, down, _), (dx_out, part) = take(5), take(SIDE), take(PAIR)
    outs, (x, g_res, dx, x_sem, g_sem, dx_sem), tiles = take(len(GRADS)), take(SIDE + PAIR), take(SIDE)
    j = pl.program_id(0)
    fetches = [pltpu.make_async_copy(*move) for move in ((x_in, x, x_sem), (g_in, g_res, g_sem))]
    store = pltpu.make_async_copy(dx, dx_out, dx_sem)
    feeds = [Feed(lambda n: d_qkv.at[lax.rem(n, PAIR), lax.div(n, PAIR)], IN_STEPS, *tiles[:PAIR]),
             Feed(lambda n: w_attn.at[lax.div(n, PAIR), :, pl.ds(pl.multiple_of(lax.rem(n, PAIR) * HALF, HALF), HALF)],
                  IN_STEPS, *tiles[PAIR:])]
    first_feeds(*feeds)
    (acc, sums, pair_sums, block), (totals, sides), block_sem, swap_sems = take(4), (take(C), take(SIDE)), refs.pop(0), take(PAIR)
    finals = Finals(down, sides[:PAIR], sides[PAIR:], outs, take(C))
    halves = [Bands(WIDE, h) for h in WAYS]
    a, b = (First(bands, part, None, *take(len(bands.first()))) for bands in halves)
    rest_a, rest_b = (Rest(f.bands, f.own_all, None, f.own_all, *take(len(f.bands.later()) - 1)) for f in (a, b))
    rest_up = Rest(Bands(WIDE), acc_up, None, *take(len(Bands(WIDE).later())))
    spread_up, spread_a, spread_b = (
        Spread(r.bands, r.sums(), total, *take(PAIR), None) for r, total in zip((rest_up, rest_a, rest_b), totals))
    hosted = Background([rest_up.begin, a.near, rest_up.loaded, rest_up.relay], LAST_PLAN)
    first = finals.c == 0
    swap = remote(sums, pair_sums, swap_sems, (), Torus().partner())
    fetch = pltpu.make_async_copy(small, block, block_sem)
    at_step(0)(enter)
    hosted.visit("start")

    @at_step(0)
    def _():
        for move in (fetch, *fetches):
            move.start()
        finals.start_down()

    @pl.when(j < IN_STEPS)
    def _():
        d_half, w = (feed.get(j) for feed in feeds)
        each_seq(lambda s, tile, tokens: accumulate(acc.at[tile], dot_nt(d_half[tile], w[...])))

    @at_step(IN_STEPS - 1)
    def _():
        for move in fetches:
            move.wait()
        sums[...] = jnp.zeros_like(sums)

        def back(s, tile, tokens):
            xhat, rstd = norm_stats(x[s].astype(F32))
            dh = acc[tokens]
            sums[:BO] += jnp.concatenate([col_sum(dh * xhat), col_sum(dh)], axis=0)
            dx[s] = (g_res[tokens] + norm_back(xhat, rstd, dh * row(vec, G1))).astype(BF16)

        each_seq(back)
        store.start()

    hosted.visit("end")

    @at_step(IN_STEPS)
    def _():
        swap.start()
        fetch.wait()
        swap.wait()
        both = sums[...] + pair_sums[...]
        for d in range(DEVICES):
            at = CHIP * (d // PAIR) + SLOT + OWN * (d % PAIR)
            block[at:at + BO, :OWN] = both[:BO, OWN * d:OWN * d + OWN]

        @pl.when(finals.c == 1)
        def _():
            for z in range(SIDE):
                for y in range(SIDE):
                    rows = block.at[pl.ds(CHIP * (SIDE * z + y), CHIP)]
                    put = pltpu.make_async_copy(rows, part.at[0, z, y, :, pl.ds(CORE_COLS, LANES)], block_sem)
                    put.start()
            pltpu.make_async_copy(block, small, block_sem).wait()

        def share_up():
            spread_up.finish()
            split_rows([(totals[0], Bands(WIDE))], first, *sides[:PAIR])
            for x in range(SIDE):
                finals.up_share(x).start()

        for step in (b.near, rest_up.settle, a.far, rest_up.relay_third, b.far, a.relay, rest_up.settle_third, spread_up.begin,
                     b.relay, spread_up.forward, functools.partial(a.settle, rest_a.send),
                     functools.partial(b.settle, rest_b.send), rest_a.relay, rest_b.relay, rest_a.settle, rest_b.settle,
                     share_up, rest_a.relay_third, rest_b.relay_third, rest_a.settle_third, spread_a.begin,
                     rest_b.settle_third, spread_b.begin, spread_a.forward, spread_b.forward, spread_a.finish, spread_b.finish):
            step()
        split_rows(list(zip(totals[1:], halves)), first, *sides[PAIR:])
        finals.start()
        for user in (rest_up, rest_a, rest_b, a, b, finals):
            user.finish()
        store.wait()


def last_call(d_qkv, w_attn, x, g_res, vec, small, acc_up, down, part, collective_id):
    halves = [Bands(WIDE, h) for h in WAYS]
    dma = pltpu.SemaphoreType.DMA
    rings = [Bands(WIDE), *halves]
    return pl.pallas_call(
        last_kernel, grid=(IN_STEPS + 1,),
        out_shape=(sds(BF16, *SEQS), sds(F32, *part.shape), *(sds(F32, *shape) for shape in GRADS)),
        in_specs=[ANY] * SIDE + [whole(8, D)] + [ANY] * SIDE,
        out_specs=(ANY,) * (len(GRADS) + PAIR),
        scratch_shapes=[pltpu.VMEM(SEQS, BF16), pltpu.VMEM((TT, D), F32), pltpu.VMEM(SEQS, BF16), dma, dma, dma] + Feed.scratch(BF16, TT, HALF) +
        Feed.scratch(BF16, D, HALF) + [pltpu.VMEM((TT, D), F32), pltpu.VMEM((SUB, D), F32), pltpu.VMEM((SUB, D), F32),
                        pltpu.VMEM((D, LANES), F32)] + [r.vmem(SIDE, C) for r in rings] +
        [pltpu.VMEM((SIDE, KEPT, HALF), F32)] * SIDE + [dma, dma, dma] + [dma((SHARES,))] * C + halves[0].first() * PAIR +
        halves[0].later()[1:] * PAIR + Bands(WIDE).later() + Spread.scratch()[:PAIR] * C,
        input_output_aliases={8: 1},
        compiler_params=comm_params(collective_id), name="last",
    )(d_qkv, w_attn, x, g_res, vec, small, acc_up, down, part)


BQ, BU, VEC = 3 * D // 32, 3 * D // 32 + FF // 32, 3 * D // 32 + FF // 32 + 8 * OWN


def pair_swap(a):
    return lax.ppermute(a, "fsdp", [(i, i ^ 1) for i in range(DEVICES)])


def by_core(first, a, b):
    return jnp.where(first, a, b), jnp.where(first, b, a)


def my_pieces(shards, first):
    w_qkv, b_qkv, w_out, w_up, b_up, w_down, vec_params = shards
    x = lax.axis_index("rep")
    small = jnp.concatenate([b_qkv, b_up, vec_params.reshape(-1)])
    small = jnp.pad(small, (0, OWN * LANES - VEC)).reshape(OWN, LANES)
    attn = lax.dynamic_slice_in_dim(jnp.concatenate([w_qkv, w_out], axis=1), x * D, D, 1)
    attn = jnp.concatenate([attn, small], axis=1)
    up = lax.dynamic_slice_in_dim(w_up, x * QCOLS, QCOLS, 1)
    wide = jnp.stack([attn, up]).astype(BF16)
    mine, theirs = by_core(first, wide[..., :HALF], wide[..., HALF:])
    theirs = pair_swap(theirs)
    piece = jnp.concatenate(by_core(first, mine, theirs), axis=1)
    down = lax.dynamic_slice_in_dim(w_down, x * 48, 48, 0).astype(BF16).reshape(3, 16, D)
    return piece[0], piece[1], down


def small_params(w_attn):
    small = w_attn[0, :, D:].astype(F32).reshape(DEVICES, OWN * LANES)
    vec = small[:, BU:VEC].reshape(DEVICES, 8, OWN).transpose(1, 0, 2).reshape(8, D)
    return small[:, :BQ].reshape(O, 1, D), small[:, BQ:BU].reshape(FF), vec


ROOM = 5 * LANES


def small_grads(db_qkv, db_up, sums):
    vec = sums[BO:].reshape(8 - BO, DEVICES, OWN).transpose(1, 0, 2).reshape(DEVICES, VEC - BU - BO * OWN)
    small = jnp.concatenate([db_qkv.reshape(DEVICES, BQ), db_up.reshape(DEVICES, BU - BQ), vec], axis=1)
    small = small + pair_swap(small)
    small = jnp.pad(small, ((0, 0), (0, ROOM - small.shape[1]))).reshape(DEVICES, ROOM // LANES, LANES)
    return jnp.pad(small, ((0, 0), (0, OWN - ROOM // LANES), (0, 0))).reshape(D, LANES)


def device_step(x, gz, *shards):
    first = lax.rem(lax.axis_index("fsdp"), PAIR) == 0
    attn, up, down = my_pieces(shards, first)
    w_attn, up, down = gather_call(attn, up, down, 0)
    w_attn = w_attn.reshape(SIDE, D, QCOLS)
    b_qkv, b_up, vec = small_params(w_attn)
    qkv, h1, o, att, h2, w_up = front_call(x, w_attn, b_qkv, vec, up, 1)
    w_up = w_up.reshape(SIDE, D, QCOLS)
    act, slope, part, w_down = mlp_in_call(h2, gz, w_up, b_up, vec, down, 2)
    part = part.reshape((SIDE,) * 3 + (C * UNIT, HALF))
    d_pre, db_up, mlp, d_h2, acc = mlp_out_call(act, slope, gz, w_up, w_down.reshape(FF, D), vec, part, 3)
    z, g_res, d_att, d_o, sums, part, result = mid_call(mlp, d_h2, att, x, gz, vec, w_attn, h2, d_pre, acc, 4)
    part = part.reshape((SIDE,) * 3 + (CHIP, HALF))
    d_qkv, db_qkv, part, acc, down = attn_back_call(qkv, d_o, h1, o, d_att, part, result, 5)
    small = small_grads(db_qkv, db_up, sums)
    part = part.reshape((SIDE,) * 3 + (CHIP, HALF))
    dx, _, g_qkv, g_out, g_up, g_down, edge = last_call(d_qkv, w_attn, x, g_res, vec, small, acc, down, part, 6)
    small = edge[0, :ROOM // LANES].reshape(ROOM)
    vec = jnp.concatenate([edge[0, SLOT:SLOT + BO, :OWN], small[BU:VEC - BO * OWN].reshape(8 - BO, OWN)], axis=0)
    g_qkv, g_out, g_up = (g[:OWN] for g in (g_qkv, g_out, g_up))
    return z, dx, g_qkv, small[:BQ], g_out, g_up, small[BQ:BU], g_down.reshape(FF // DEVICES, D), vec


def solution(mesh):
    batch = P(("rep", "fsdp"), None, None)
    rows, flat, cols = P("fsdp", None), P("fsdp"), P(None, "fsdp")
    shards = (rows, flat, rows, rows, flat, rows, cols)
    return jax.shard_map(device_step, mesh=mesh, in_specs=(batch, batch) + shards,
                         out_specs=(batch, batch) + shards, check_vma=False)
```
